32 devices in a mesh: gx: 2 (over core), gy: 4 (over y, x), gz: 4 (over z).
Axes of the slice: x: 2, y: 2, z: 4, core: 2. Of those that a mesh axis runs over, the one named last changes fastest.
Arguments:
- sources: float32 [1, 32, 64, 512], P(None, 'gx', 'gy', 'gz'), may hold values from -6 to 6
- stiffness: float32 [32, 64, 512], P('gx', 'gy', 'gz'), may hold values from 0.5 to 2
- coarse_inverse: float32 [256, 256], P(('gx', 'gy', 'gz')), may hold values from -6 to 6
Outputs:
- pressure: float32 [1, 32, 64, 512], P(None, 'gx', 'gy', 'gz')
The draws below stay inside these ranges and needn't reach their ends.
All inputs are finite; a program needn't handle non-finite values.
Results may differ from the reference program's by a relative error of at most 0.0001.
Values sent between devices are 32-bit elements; how exact they have to be, the bound alone decides.
A program may use at most 64 MiB of HBM per device.

```python
import math
import jax
import jax.numpy as jnp
from jax import lax

SYSTEMS = 1
CX = 16
CY = 16
CZ = 128
NX = 32
NY = 64
NZ = 512
NC = 256
N_GX = 2
N_GY = 4
N_GZ = 4


def level_of(own_key, shape, cuts, smallest, largest):
    loudness = 1.0
    for dim, shards_of in cuts:
        steps = jax.random.uniform(jax.random.fold_in(jax.random.fold_in(own_key, 6), dim), (shards_of,), jnp.float32, smallest / len(cuts), largest / len(cuts))
        loudness = loudness * jnp.repeat(jnp.exp(steps), shape[dim] // shards_of).reshape((-1,) + (1,) * (len(shape) - 1 - dim))
    return loudness


def centred(own_key, extent, deviation, most, pieces=(), kind=jnp.bfloat16):
    loudness = level_of(own_key, extent, pieces, -0.22, 0.18) if pieces else 1.0
    values = jax.random.normal(own_key, extent, jnp.float32) * deviation * loudness
    return jnp.minimum(jnp.maximum(values, -most), most).astype(kind)


def setup_inputs(seed: int = 0) -> dict:
    splits = jax.random.split(jax.random.key(seed), 4)
    sources = centred(splits[0], (SYSTEMS, NX, NY, NZ), 1.0, 6.0, ((1, 2), (2, 4), (3, 4)), jnp.float32)
    stiffness = jnp.clip(jnp.exp(math.log(2.0) - 1.3862944 * jax.random.uniform(splits[1], (NX, NY, NZ), jnp.float32) ** level_of(splits[1], (NX, NY, NZ), ((0, 2), (1, 4), (2, 4)), -0.2, 0.2)), 0.5, 2.0)
    coarse_inverse = centred(splits[2], (NC, NC), (max(NC // 400, 1)) ** -0.5, 6.0, ((0, 32),), jnp.float32)
    return {"sources": sources, "stiffness": stiffness, "coarse_inverse": coarse_inverse}


damping = 0.8


def loop_sum(padded):
    total = padded[:, 2:, 1:-1, 1:-1] + padded[:, :-2, 1:-1, 1:-1]
    total = total + padded[:, 1:-1, 2:, 1:-1] + padded[:, 1:-1, :-2, 1:-1]
    total = total + padded[:, 1:-1, 1:-1, 2:] + padded[:, 1:-1, 1:-1, :-2]
    return total


def apply_op(answer, weights):
    scaled = weights * answer
    padded = jnp.pad(scaled, ((0, 0), (1, 1), (1, 1), (1, 1)))
    return weights * (6.0 * scaled - loop_sum(padded))


def pre_smooth(source, weights):
    diagonal = 6.0 * weights * weights
    first = damping * source / diagonal
    second = first + damping * (source - apply_op(first, weights)) / diagonal
    return second, source - apply_op(second, weights)


def post_smooth(answer, source, weights):
    return answer + damping * (source - apply_op(answer, weights)) / (6.0 * weights * weights)


def coarsen(values):
    leading = values.shape[0]
    size_x, size_y, size_z = values.shape[1], values.shape[2], values.shape[3]
    blocks = values.reshape((leading, size_x // 2, 2, size_y // 2, 2, size_z // 2, 2))
    return jnp.mean(blocks, axis=(2, 4, 6))


def refine(values):
    return jnp.repeat(jnp.repeat(jnp.repeat(values, 2, axis=1), 2, axis=2), 2, axis=3)


def reference(sources, stiffness, coarse_inverse):
    weight_list = [stiffness[None]]
    for level in range(3):
        weight_list.append(0.5 * coarsen(weight_list[-1]))
    source_list = []
    answer_list = []
    current = sources
    for level in range(4):
        source_list.append(current)
        answer, resid = pre_smooth(current, weight_list[level])
        answer_list.append(answer)
        current = coarsen(resid)
    coarse_source = current
    block_x = CX // 16
    block_y = CY // 16
    block_z = CZ // 16
    ordered = coarse_source.reshape((SYSTEMS, N_GX, block_x, N_GY, block_y, N_GZ, block_z))
    ordered = ordered.transpose((0, 1, 3, 5, 2, 4, 6)).reshape((SYSTEMS, NC))
    solved = jnp.dot(ordered, coarse_inverse.T, precision=lax.Precision.HIGHEST, preferred_element_type=jnp.float32)
    solved = solved.reshape((SYSTEMS, N_GX, N_GY, N_GZ, block_x, block_y, block_z))
    correction = solved.transpose((0, 1, 4, 2, 5, 3, 6)).reshape(coarse_source.shape)
    for level in range(3, -1, -1):
        correction = post_smooth(answer_list[level] + refine(correction), source_list[level], weight_list[level])
    return correction
```

```python
import functools
import jax
import jax.numpy as jnp
from jax import lax
from jax.experimental import pallas as pl
from jax.experimental.pallas import tpu as pltpu
from jax.sharding import PartitionSpec as P

damping = 0.8


def extended(cells, sides, width):
    for axis, dim in sides:
        count = lax.axis_size(axis)
        ends = count - 1
        head = lax.slice_in_dim(cells, 0, width, axis=dim)
        tail = lax.slice_in_dim(cells, cells.shape[dim] - width, cells.shape[dim], axis=dim)
        cells = jnp.concatenate(
            [
                lax.ppermute(tail, axis, [(i, (i + 1) % count) for i in range(ends)]),
                cells,
                lax.ppermute(head, axis, [((i + 1) % count, i) for i in range(ends)]),
            ],
            axis=dim,
        )
    return cells


def loop_sum(padded):
    total = padded[:, 2:, 1:-1, 1:-1] + padded[:, :-2, 1:-1, 1:-1]
    total = total + padded[:, 1:-1, 2:, 1:-1] + padded[:, 1:-1, :-2, 1:-1]
    total = total + padded[:, 1:-1, 1:-1, 2:] + padded[:, 1:-1, 1:-1, :-2]
    return total


def inner_part(values):
    return values[:, 1:-1, 1:-1, 1:-1]


def pre_smooth(source, weights):
    count = source.shape[0]
    stacked = jnp.concatenate([source, weights], axis=0)
    wide = extended(stacked, (("gx", 1), ("gy", 2), ("gz", 3)), 2)
    wide_source = wide[:count]
    wide_weights = wide[count:]
    safe_weights = jnp.where(wide_weights > 0.0, wide_weights, 1.0)
    first = damping * wide_source / (6.0 * safe_weights * safe_weights)
    first_scaled = wide_weights * first
    mid_weights = inner_part(wide_weights)
    mid_safe = inner_part(safe_weights)
    applied = mid_weights * (6.0 * inner_part(first_scaled) - loop_sum(first_scaled))
    second = inner_part(first) + damping * (inner_part(wide_source) - applied) / (
        6.0 * mid_safe * mid_safe
    )
    second_scaled = mid_weights * second
    answer = inner_part(second)
    resid = source - weights * (6.0 * inner_part(second_scaled) - loop_sum(second_scaled))
    return (answer, resid)


def post_smooth(answer, source, weights):
    scaled = weights * answer
    wide = extended(scaled, (("gx", 1), ("gy", 2), ("gz", 3)), 1)
    applied = weights * (6.0 * scaled - loop_sum(wide))
    return answer + damping * (source - applied) / (6.0 * weights * weights)


def coarsen(values):
    leading = values.shape[0]
    size_x, size_y, size_z = (values.shape[1], values.shape[2], values.shape[3])
    blocks = values.reshape((leading, size_x // 2, 2, size_y // 2, 2, size_z // 2, 2))
    return jnp.mean(blocks, axis=(2, 4, 6))


def refine(values):
    return jnp.repeat(jnp.repeat(jnp.repeat(values, 2, axis=1), 2, axis=2), 2, axis=3)


def per_device(sources, stiffness, coarse_inverse):
    weight_list = [stiffness[None]]
    for level in range(3):
        weight_list.append(0.5 * coarsen(weight_list[-1]))
    source_list = []
    answer_list = []
    current = sources
    for level in range(4):
        source_list.append(current)
        answer, resid = pre_smooth(current, weight_list[level])
        answer_list.append(answer)
        current = coarsen(resid)
    count = current.shape[0]
    flat_source = current.reshape((count, -1))
    solved = lax.dot_general(
        lax.all_gather(flat_source, ("gx", "gy", "gz"), axis=1, tiled=True),
        coarse_inverse,
        (((1,), (1,)), ((), ())),
        precision=lax.Precision.HIGHEST,
        preferred_element_type=jnp.float32,
    )
    correction = solved.reshape(current.shape)
    for level in range(3, -1, -1):
        correction = post_smooth(
            answer_list[level] + refine(correction), source_list[level], weight_list[level]
        )
    return correction


K = damping / 6.0
F32 = jnp.float32
BF = jnp.bfloat16


def iota(shape, dim):
    return lax.broadcasted_iota(jnp.int32, shape, dim)


def pick(condition):
    return jnp.where(condition, 1.0, 0.0).astype(BF)


def sel_dot(values, chosen):
    high = values.astype(BF)
    low = (values - high.astype(F32)).astype(BF)
    return jnp.dot(high, chosen, preferred_element_type=F32) + jnp.dot(
        low, chosen, preferred_element_type=F32
    )


def around(c):
    rows, lanes = c.shape
    return (pltpu.roll(c, 1, 0) + pltpu.roll(c, rows - 1, 0)) + (
        pltpu.roll(c, 1, 1) + pltpu.roll(c, lanes - 1, 1)
    )


def whole_sum(planes, nz):
    rows, lanes = planes[0].shape
    row, lane = iota((rows, lanes), 0), iota((rows, lanes), 1)
    outs = []
    for p, c in enumerate(planes):
        s = jnp.where(row > 0, pltpu.roll(c, 1, 0), 0.0) + jnp.where(
            row < rows - 1, pltpu.roll(c, rows - 1, 0), 0.0
        )
        s = s + (
            jnp.where(lane > 0, pltpu.roll(c, 1, 1), 0.0)
            + jnp.where(lane < nz - 1, pltpu.roll(c, lanes - 1, 1), 0.0)
        )
        if p > 0:
            s = s + planes[p - 1]
        if p < len(planes) - 1:
            s = s + planes[p + 1]
        outs.append(s)
    return outs


def kernel(
    dims, b_hbm, w_hbm, m_hbm, f_ref,
    b_ref, w_ref, m_ref,
    V0, W0, U0, V1, W1, U1, TT, T2, A2, T3, T4, P4, P3, E2, P2, P1,
    SX0, SY0, SZ0, RX0, RY0, RXY0, RZ0,
    SXv, SYv, SZv, RXv, RYv, RXYv, RZv,
    SXw, SYw, SZw, RXw, RYw, RXYw, RZw,
    GM, GW, GB, SW, SB,
    tally, load, sent, hr, gr, known,
):
    axes = ("gx", "gy", "gz")
    ix, iy, iz = (lax.axis_index(a) for a in axes)
    n = dims[0] * dims[1] * dims[2]
    me = (ix * dims[1] + iy) * dims[2] + iz

    def place(t):
        return (t // (dims[1] * dims[2]), (t // dims[2]) % dims[1], t % dims[2])

    def other(k):
        return lax.rem(me + k, n)

    barrier = pltpu.get_barrier_semaphore()

    def there(d):
        ok = None
        for i, s, c in zip((ix, iy, iz), dims, d):
            if c:
                t = (i + c < s) if c > 0 else (i + c >= 0)
                ok = t if ok is None else jnp.logical_and(ok, t)
        return ok

    def directions(most):
        found = []
        for dx in (-1, 0, 1):
            for dy in (-1, 0, 1):
                for dz in (-1, 0, 1):
                    if 0 < abs(dx) + abs(dy) + abs(dz) <= most:
                        found.append((dx, dy, dz))
        return found

    def greet(sem):
        for d in directions(3):
            @pl.when(there(d))
            def _(d=d):
                pl.semaphore_signal(
                    sem, inc=1, device_id=(ix + d[0], iy + d[1], iz + d[2]),
                    device_id_type=pl.DeviceIdType.MESH,
                )

    loads = [
        pltpu.make_async_copy(src, dst, load.at[i])
        for i, (src, dst) in enumerate(((b_hbm, b_ref), (w_hbm, w_ref), (m_hbm, m_ref)))
    ]
    for copy in loads:
        copy.start()
    greet(barrier)

    def span(i, s):
        return 1 + jnp.where(i > 0, 1, 0) + jnp.where(i < s - 1, 1, 0)

    greeted = span(ix, dims[0]) * span(iy, dims[1]) * span(iz, dims[2]) - 1

    def halo_copy(bufs, which, d):
        SX, SY, SZ, RX, RY, RXY, RZ, part = bufs
        dx, dy, dz = d
        up = lambda c: (c + 1) // 2
        down = lambda c: (1 - c) // 2
        if dz:
            s, r = SZ, RZ.at[1 - dx, 1 - dy, down(dz)]
        elif dx and dy:
            rows = SY.shape[2]
            s = SY.at[up(dy), :, pl.ds(rows - part if dx > 0 else 0, part), :]
            r = RXY.at[down(dx), down(dy)]
        elif dx:
            s, r = SX.at[up(dx)], RX.at[down(dx)]
        else:
            s, r = SY.at[up(dy)], RY.at[down(dy)]
        return pltpu.make_async_remote_copy(
            src_ref=s, dst_ref=r, send_sem=sent.at[0], recv_sem=hr.at[which],
            device_id=(ix + dx, iy + dy, iz + dz), device_id_type=pl.DeviceIdType.MESH,
        )

    def halo_start(bufs, which, most):
        for d in directions(most):
            @pl.when(there(d))
            def _(d=d):
                halo_copy(bufs, which, d).start()

    def bytes_of(ref, sem):
        pltpu.make_async_copy(ref, ref, sem).wait()

    group = n // dims[0]
    sides_y, sides_z = span(iy, dims[1]) - 1, span(iz, dims[2]) - 1

    def first_part(cy, cz):
        return 16 + 20 * cy + 4 * (2 + cy) * cz

    def second_part(cy, cz):
        return 6 + 12 * cy + 4 * (1 + cy) * cz

    def everything(cy, cz):
        gathers = 2 * (n - 1) + 4 * (group - 1) + 4 * group
        return first_part(cy, cz) + 2 * second_part(cy, cz) + gathers

    def take(part, sem):
        for cy in (1, 2):
            for cz in (1, 2):
                @pl.when(jnp.logical_and(sides_y == cy, sides_z == cz))
                def _(cy=cy, cz=cz):
                    bytes_of(tally.at[pl.ds(0, part(cy, cz))], sem)

    def spread(kind, src, dst, k):
        return pltpu.make_async_remote_copy(
            src_ref=src, dst_ref=dst.at[me], send_sem=sent.at[0], recv_sem=gr.at[kind],
            device_id=place(other(k)), device_id_type=pl.DeviceIdType.MESH,
        )

    def arrive(kind, dst):
        bytes_of(dst.at[pl.ds(0, n - 1)], gr.at[kind])


    def beside(k):
        return ix * group + lax.rem(me - ix * group + k, group)

    def matrix_copy(k, slot):
        return pltpu.make_async_remote_copy(
            src_ref=m_ref, dst_ref=GM.at[slot], send_sem=sent.at[0], recv_sem=gr.at[1],
            device_id=place(beside(k)), device_id_type=pl.DeviceIdType.MESH,
        )

    def matrix_half(x):
        half = GM.at[pl.ds(x * group, group)]
        return pltpu.make_async_remote_copy(
            src_ref=half, dst_ref=half, send_sem=sent.at[0], recv_sem=gr.at[3],
            device_id=(1 - ix, iy, iz), device_id_type=pl.DeviceIdType.MESH,
        )

    nx, ny = b_ref.shape[0], b_ref.shape[1]
    hx, hy = nx // 2, ny // 2
    bufs0 = (SX0, SY0, SZ0, RX0, RY0, RXY0, RZ0, 8)
    bufsv = (SXv, SYv, SZv, RXv, RYv, RXYv, RZv, 16)
    bufsw = (SXw, SYw, SZw, RXw, RYw, RXYw, RZw, 16)

    for copy in loads[:2]:
        copy.wait()
    lane16 = iota((ny, 128), 1)
    packed = jnp.zeros((ny, 128), F32)
    for x in range(nx):
        w = w_ref[x]
        v = K * b_ref[x] / w
        V0[x + 2, 0:ny, 0:128] = v
        W0[x + 2, 0:ny, 0:128] = w
        for a, q in enumerate((v, w)):
            if x < 2:
                SX0[0, a, x] = q
            if x >= nx - 2:
                SX0[1, a, x - nx + 2] = q
            SY0[0, a, 2 * x : 2 * x + 2, :] = q[0:2, :]
            SY0[1, a, 2 * x : 2 * x + 2, :] = q[ny - 2 : ny, :]
            start = 8 * x + 4 * a
            moved = pltpu.roll(q, (start + 2) % 128, 1)
            packed = jnp.where((lane16 >= start) & (lane16 < start + 4), moved, packed)
    SZ0[...] = packed

    pl.semaphore_wait(barrier, greeted)
    halo_start(bufs0, 0, 2)
    greet(known.at[0])

    halve = pick(iota((128, 128), 0) == 2 * iota((128, 128), 1))
    halve = halve + pick(iota((128, 128), 0) == 2 * iota((128, 128), 1) + 1)

    def coarsen0(planes):
        for i in range(hx):
            TT[i] = planes(2 * i) + planes(2 * i + 1)
        rows = [
            TT[i, pl.ds(0, hy, stride=2), :] + TT[i, pl.ds(1, hy, stride=2), :] for i in range(hx)
        ]
        return sel_dot(jnp.concatenate(rows, axis=0), halve)

    def coarsen1(planes, SG):
        for i in range(hx // 2):
            T2[pl.ds(8 * i, 8), :] = planes(2 * i) + planes(2 * i + 1)
        for y in range(4):
            A2[pl.ds(4 * y, 4), :] = (
                T2[pl.ds(2 * y, 4, stride=8), :] + T2[pl.ds(2 * y + 1, 4, stride=8), :]
            )
        TT[0] = sel_dot(A2[...], halve)
        total = TT[0, 0:4, :]
        for y in range(1, 4):
            total = total + pltpu.roll(TT[0, 4 * y : 4 * y + 4, :], 32 * y, 1)
        return total

    lane8 = iota((8, 128), 1)

    def pack1(bufs, planes):
        SX, SY, SZ = bufs[:3]
        out = jnp.zeros((8, 128), F32)
        for x in range(hx):
            q = planes[x]
            if x < 3:
                SX[0, 0, x] = q
            if x >= hx - 3:
                SX[1, 0, x - hx + 3] = q
            SY[0, 0, 4 * x : 4 * x + 4, :] = q[0:4, :]
            SY[1, 0, 4 * x : 4 * x + 4, :] = q[4:8, :]
            s = 16 * x
            out = jnp.where((lane8 >= s) & (lane8 < s + 3), pltpu.roll(q, (s - 61) % 128, 1), out)
            out = jnp.where(
                (lane8 >= s + 3) & (lane8 < s + 6), pltpu.roll(q, (s + 3) % 128, 1), out
            )
        SZ[...] = out

    w1 = 0.0625 * coarsen0(lambda x: w_ref[x])
    w1 = [w1[8 * x : 8 * x + 8, :] for x in range(hx)]
    pack1(bufsw, w1)
    SW[...] = 0.0625 * coarsen1(lambda x: w1[x], SW)
    GW[me] = SW[...]
    loads[2].wait()
    GM[me] = m_ref[...]
    halo_start(bufsw, 1, 3)
    pl.semaphore_wait(known.at[0], greeted)
    greet(known.at[1])

    def coords(rows, lanes, cy, cz, by, bz):
        r, l = iota((rows, lanes), 0), iota((rows, lanes), 1)
        y = jnp.where(r < cy + (rows - cy) // 2, r, r - rows)
        z = jnp.where(l < cz + (lanes - cz) // 2, l, l - lanes)
        gy, gz = y + iy * cy, z + iz * cz
        ok = (gy >= 0) & (gy < dims[1] * cy) & (gz >= 0) & (gz < dims[2] * cz)
        near = (y >= -by) & (y < cy + by) & (z >= -bz) & (z < cz + bz)
        return jnp.where(ok & near, 1, 0)

    def plane_mask(base, x, cx):
        if 0 <= x < cx:
            return base > 0
        gx = x + ix * cx
        inside = jnp.where((gx >= 0) & (gx < dims[0] * cx), 1, 0)
        return base * inside > 0

    take(first_part, hr.at[0])
    mask0 = coords(24, 256, ny, 128, 2, 2)
    row8 = iota((8, 128), 0)
    lane24 = iota((24, 128), 1)
    for a, D in ((0, V0), (1, W0)):
        D[0:2, 0:ny, 0:128] = RX0[0, a]
        D[nx + 2 : nx + 4, 0:ny, 0:128] = RX0[1, a]
        for x in range(nx):
            D[x + 2, 16:18, 0:128] = RY0[1, a, 2 * x : 2 * x + 2, :]
            D[x + 2, 22:24, 0:128] = RY0[0, a, 2 * x : 2 * x + 2, :]
        D[1, 16:18, 0:128] = RXY0[0, 1, a, 6:8, :]
        D[1, 22:24, 0:128] = RXY0[0, 0, a, 6:8, :]
        D[nx + 2, 16:18, 0:128] = RXY0[1, 1, a, 0:2, :]
        D[nx + 2, 22:24, 0:128] = RXY0[1, 0, a, 0:2, :]
        for dx in (-1, 0, 1):
            sides = []
            for side in (0, 1):
                mid = RZ0[dx + 1, 1, side]
                if dx == 0:
                    edge = jnp.where(row8 < 4, RZ0[1, 2, side, 0:8, :], RZ0[1, 0, side, 8:16, :])
                else:
                    edge = jnp.zeros((8, 128), F32)
                sides.append(jnp.concatenate([mid, edge], axis=0))
            for x in {-1: (nx - 1,), 0: range(nx), 1: (0,)}[dx]:
                s = 8 * x + 4 * a
                D[x + 2 + dx * nx, :, 128:256] = jnp.where(
                    lane24 < 64,
                    pltpu.roll(sides[1], (-(s + 2)) % 128, 1),
                    pltpu.roll(sides[0], (126 - s) % 128, 1),
                )
        for p in range(nx + 4):
            D[p] = jnp.where(plane_mask(mask0, p - 2, nx), D[p], 0.0)

    for p in range(1, nx + 3):
        c = V0[p]
        u = 1.2 * c + K * (around(c) + (V0[p - 1] + V0[p + 1]))
        U0[p] = jnp.where(plane_mask(mask0, p - 2, nx), u, 0.0)

    def own_sum(ref, p):
        c = ref[p]
        return around(c)[0:ny, 0:128] + (ref[p - 1, 0:ny, 0:128] + ref[p + 1, 0:ny, 0:128])

    def resid0(x):
        p = x + 2
        return b_ref[x] - w_ref[x] * (6.0 * U0[p, 0:ny, 0:128] - own_sum(U0, p))

    b1 = 0.125 * coarsen0(resid0)
    b1 = [b1[8 * x : 8 * x + 8, :] for x in range(hx)]
    v1 = [jnp.where(lane8 < 64, K * b1[x] / jnp.where(lane8 < 64, w1[x], 1.0), 0.0) for x in range(hx)]
    pack1(bufsv, v1)
    halo_start(bufsv, 2, 3)
    pl.semaphore_wait(known.at[1], greeted)
    for k in range(1, n):
        spread(0, SW, GW, k).start()
    for k in range(1, group):
        matrix_copy(k, me).start()

    mask1 = coords(16, 128, 8, 64, 3, 3)
    lane1 = iota((16, 128), 1)

    def assemble1(bufs, planes, D):
        RX, RY, RXY, RZ = bufs[3:7]
        for dx in (-1, 0, 1):
            sides = []
            for side in (0, 1):
                edge = jnp.where(row8 < 4, RZ[dx + 1, 2, side], RZ[dx + 1, 0, side])
                sides.append(jnp.concatenate([RZ[dx + 1, 1, side], edge], axis=0))
            for x in {-1: range(hx - 3, hx), 0: range(hx), 1: range(3)}[dx]:
                p = x + 3 + dx * hx
                if dx == 0:
                    D[p, 0:8, :] = planes[x]
                    D[p, 8:12, :] = RY[1, 0, 4 * x : 4 * x + 4, :]
                    D[p, 12:16, :] = RY[0, 0, 4 * x : 4 * x + 4, :]
                else:
                    slot = (dx + 1) // 2
                    D[p, 0:8, :] = RX[slot, 0, p if dx < 0 else x]
                    q = 4 * (x - 4 if dx < 0 else x)
                    D[p, 8:12, :] = RXY[slot, 1, 0, q : q + 4, :]
                    D[p, 12:16, :] = RXY[slot, 0, 0, q : q + 4, :]
                s = 16 * x
                ends = jnp.where(
                    lane1 < 96,
                    pltpu.roll(sides[1], (61 - s) % 128, 1),
                    pltpu.roll(sides[0], (125 - s) % 128, 1),
                )
                merged = jnp.where(lane1 < 64, D[p], ends)
                D[p] = jnp.where(plane_mask(mask1, x + dx * hx, hx), merged, 0.0)

    take(second_part, hr.at[1])
    assemble1(bufsw, w1, W1)

    block = lane8 // 32
    quarter = row8 % 4

    def unpack(G):
        planes = []
        for X in range(4 * dims[0]):
            tiles = []
            for t in range(dims[1] // 2):
                rows = []
                for z in range(dims[2]):
                    d0 = ((X // 4) * dims[1] + 2 * t) * dims[2] + z
                    d1 = d0 + dims[2]
                    q = X % 4
                    rows.append(
                        jnp.where(
                            row8 < 4,
                            jnp.broadcast_to(G[d0, q : q + 1, :], (8, 128)),
                            jnp.broadcast_to(G[d1, q : q + 1, :], (8, 128)),
                        )
                    )
                out = None
                for s in range(4):
                    pre = rows[s % 4]
                    for j in range(1, 4):
                        pre = jnp.where(block == j, rows[(j + s) % 4], pre)
                    moved = pltpu.roll(pre, 32 * s, 1) if s else pre
                    out = moved if out is None else jnp.where(block == (quarter + s) % 4, moved, out)
                tiles.append(out)
            planes.append(jnp.concatenate(tiles, axis=0))
        return planes

    def coarsen2(planes):
        c = len(planes) // 2
        for i in range(c):
            T3[i] = planes[2 * i] + planes[2 * i + 1]
        rows = [T3[i, pl.ds(0, 8, stride=2), :] + T3[i, pl.ds(1, 8, stride=2), :] for i in range(c)]
        out = sel_dot(jnp.concatenate(rows, axis=0), halve)
        return [out[8 * i : 8 * i + 8, :] for i in range(c)]


    take(second_part, hr.at[2])
    assemble1(bufsv, v1, V1)
    for p in range(1, hx + 5):
        c = V1[p]
        u = 1.2 * c + K * (around(c) + (V1[p - 1] + V1[p + 1]))
        U1[p] = jnp.where(plane_mask(mask1, p - 3, hx), u, 0.0)

    def resid1(x):
        p = x + 3
        s = around(U1[p])[0:8, :] + (U1[p - 1, 0:8, :] + U1[p + 1, 0:8, :])
        return jnp.where(lane8 < 64, b1[x] - w1[x] * (6.0 * U1[p, 0:8, :] - s), 0.0)

    SB[...] = 0.125 * coarsen1(resid1, SB)
    GB[me] = SB[...]
    for k in range(1, n):
        spread(2, SB, GB, k).start()
    arrive(0, GW)
    w2 = unpack(GW)
    w3 = [0.0625 * q for q in coarsen2(w2)]
    valid3 = lane8 < 64
    w3s = [jnp.where(valid3, q, 1.0) for q in w3]
    bytes_of(GM.at[pl.ds(0, group - 1)], gr.at[1])
    matrix_half(ix).start()
    arrive(2, GB)

    b2 = unpack(GB)
    v2 = [K * b / w for b, w in zip(b2, w2)]
    u2 = [1.2 * v + K * s for v, s in zip(v2, whole_sum(v2, 128))]
    r2 = [b - w * (6.0 * u - s) for b, w, u, s in zip(b2, w2, u2, whole_sum(u2, 128))]
    b3 = [0.125 * q for q in coarsen2(r2)]
    v3 = [K * b / w for b, w in zip(b3, w3s)]
    u3 = [jnp.where(valid3, 1.2 * v + K * s, 0.0) for v, s in zip(v3, whole_sum(v3, 64))]
    r3 = [b - w * (6.0 * u - s) for b, w, u, s in zip(b3, w3, u3, whole_sum(u3, 64))]
    c4 = len(r3) // 2
    for i in range(c4):
        T4[pl.ds(8 * i, 8), :] = r3[2 * i] + r3[2 * i + 1]
    half = 4 * c4
    b4 = 0.125 * sel_dot(T4[pl.ds(0, half, stride=2), :] + T4[pl.ds(1, half, stride=2), :], halve)
    acc = b4
    for j in range(1, 4):
        acc = jnp.where(quarter == j, pltpu.roll(b4, 32 * j, 1), acc)
    low = jnp.sum(jnp.where(row8 < 4, acc, 0.0), axis=0, keepdims=True)
    high = jnp.sum(jnp.where(row8 >= 4, acc, 0.0), axis=0, keepdims=True)
    matrix_half(1 - ix).wait_recv()
    cells = GM.shape[0] * GM.shape[1]
    matrix = GM[...].reshape((cells, 256))
    solved = jnp.sum(matrix[:, 0:128] * low + matrix[:, 128:256] * high, axis=1, keepdims=True)
    hit = (iota((cells, 128), 0) % 32) == iota((cells, 128), 1) // 2
    e4 = jnp.sum(jnp.where(hit, solved, 0.0).reshape((cells // 32, 32, 128)), axis=1)
    P4[pl.ds(0, half, stride=2), :] = e4
    P4[pl.ds(1, half, stride=2), :] = e4

    y3 = [u + w * P4[8 * (i // 2) : 8 * (i // 2) + 8, :] for i, (u, w) in enumerate(zip(u3, w3))]
    e3 = [
        jnp.where(valid3, (0.2 * y + v + K * s) / w, 0.0)
        for y, v, s, w in zip(y3, v3, whole_sum(y3, 64), w3s)
    ]
    double = pick(iota((128, 256), 0) == iota((128, 256), 1) // 2)
    wide3 = sel_dot(jnp.concatenate(e3, axis=0), double[:, 0:128])
    for i in range(len(e3)):
        P3[i, pl.ds(0, 8, stride=2), :] = wide3[8 * i : 8 * i + 8, :]
        P3[i, pl.ds(1, 8, stride=2), :] = wide3[8 * i : 8 * i + 8, :]
    y2 = [u + w * P3[i // 2] for i, (u, w) in enumerate(zip(u2, w2))]
    s2 = whole_sum(y2, 128)
    E2[...] = jnp.zeros_like(E2)
    for i in range(len(y2)):
        E2[i + 1, 8:24, :] = (0.2 * y2[i] + v2[i] + K * s2[i]) / w2[i]

    seen = jnp.concatenate([E2[4 * ix + i, pl.ds(6 + 4 * iy, 8), :] for i in range(6)], axis=0)
    j = iota((128, 128), 1)
    zl = jnp.where(j < 96, j // 2, j // 2 - 64) + 32 * iz
    wide2 = sel_dot(seen, pick(iota((128, 128), 0) == zl))
    for i in range(6):
        P2[i, pl.ds(0, 8, stride=2), :] = wide2[8 * i : 8 * i + 8, :]
        P2[i, pl.ds(1, 8, stride=2), :] = wide2[8 * i : 8 * i + 8, :]
    for p in range(1, hx + 5):
        U1[p] = U1[p] + W1[p] * pltpu.roll(P2[(p - 3) // 2 + 1], 12, 0)
    e1 = []
    for p in range(2, hx + 4):
        c = U1[p]
        f = 0.2 * c + V1[p] + K * (around(c) + (U1[p - 1] + U1[p + 1]))
        inside = plane_mask(mask1, p - 3, hx)
        e1.append(jnp.where(inside, f, 0.0) / jnp.where(inside, W1[p], 1.0))
    wide1 = sel_dot(jnp.concatenate(e1, axis=0), double)
    for i in range(hx + 2):
        for t in range(2):
            q = wide1[16 * i : 16 * i + 16, 128 * t : 128 * t + 128]
            P1[t, i, pl.ds(0, 16, stride=2), :] = q
            P1[t, i, pl.ds(1, 16, stride=2), :] = q

    for p in range(1, nx + 3):
        i = (p - 2) // 2 + 1
        parts = []
        for t in range(2):
            edge = jnp.where(row8 < 4, P1[t, i, 16:24, :], P1[t, i, 24:32, :])
            parts.append(jnp.concatenate([P1[t, i, 0:16, :], edge], axis=0))
        U0[p] = U0[p] + W0[p] * jnp.concatenate(parts, axis=1)
    for x in range(nx):
        p = x + 2
        f = 0.2 * U0[p, 0:ny, 0:128] + V0[p, 0:ny, 0:128] + K * own_sum(U0, p)
        f_ref[x] = f / w_ref[x]

    take(everything, sent.at[0])


def fused(dims, sources, stiffness, coarse_inverse):
    nx, ny, nz = stiffness.shape
    n = dims[0] * dims[1] * dims[2]
    vm = lambda *s: pltpu.VMEM(s, F32)
    halo0 = [
        vm(2, 2, 2, ny, 128), vm(2, 2, 2 * nx, 128), vm(ny, 128),
        vm(2, 2, 2, ny, 128), vm(2, 2, 2 * nx, 128), vm(2, 2, 2, 8, 128), vm(3, 3, 2, ny, 128),
    ]
    halo1 = [
        vm(2, 1, 3, 8, 128), vm(2, 1, 32, 128), vm(8, 128),
        vm(2, 1, 3, 8, 128), vm(2, 1, 32, 128), vm(2, 2, 1, 16, 128), vm(3, 3, 2, 8, 128),
    ]
    result = pl.pallas_call(
        functools.partial(kernel, dims),
        out_shape=pltpu.VMEM((nx, ny, nz), F32),
        in_specs=[pl.BlockSpec(memory_space=pl.ANY)] * 3,
        out_specs=pl.BlockSpec(memory_space=pltpu.VMEM),
        scratch_shapes=[
            vm(nx, ny, nz), vm(nx, ny, nz), vm(*coarse_inverse.shape),
            vm(nx + 4, 24, 256), vm(nx + 4, 24, 256), vm(nx + 4, 24, 256),
            vm(14, 16, 128), vm(14, 16, 128), vm(14, 16, 128),
            vm(8, 16, 128), vm(32, 128), vm(16, 128), vm(2 * dims[0], 16, 128),
            vm(16, 128), vm(16, 128), vm(2 * dims[0], 16, 128),
            vm(4 * dims[0] + 2, 32, 128), vm(6, 16, 128), vm(2, 10, 32, 128),
        ]
        + halo0 + halo1 + halo1
        + [
            vm(n, 8, 256), vm(n, 4, 128), vm(n, 4, 128), vm(4, 128), vm(4, 128),
            vm(512, 4, 128),
            pltpu.SemaphoreType.DMA((3,)), pltpu.SemaphoreType.DMA((1,)),
            pltpu.SemaphoreType.DMA((3,)), pltpu.SemaphoreType.DMA((4,)),
            pltpu.SemaphoreType.REGULAR((2,)),
        ],
        compiler_params=pltpu.CompilerParams(collective_id=0, has_side_effects=True),
        name="cycle",
    )(sources[0], stiffness, coarse_inverse)
    return result[None]


def solution(mesh):
    dims = tuple(mesh.shape[a] for a in ("gx", "gy", "gz"))

    def run(sources, stiffness, coarse_inverse):
        nx, ny, nz = stiffness.shape
        lanes = 128
        cells = coarse_inverse.shape[1]
        levels_fit = (
            sources.shape[0] == 1
            and nx == ny == 16
            and nz == lanes
            and dims[2] * nz == 4 * lanes
            and dims[1] * ny == 64
            and cells == 2 * lanes
            and dims[0] == 2
        )
        if levels_fit:
            return fused(dims, sources, stiffness, coarse_inverse)
        return per_device(sources, stiffness, coarse_inverse)

    in_specs = (P(None, "gx", "gy", "gz"), P("gx", "gy", "gz"), P(("gx", "gy", "gz"), None))
    out_specs = P(None, "gx", "gy", "gz")
    return jax.shard_map(
        run, mesh=mesh, in_specs=in_specs, out_specs=out_specs, check_vma=False
    )
```

```python
import functools
import jax
import jax.numpy as jnp
from jax import lax
from jax.experimental import pallas as pl
from jax.experimental.pallas import tpu as pltpu
from jax.sharding import PartitionSpec as P

damping = 0.8


def extended(cells, sides, width):
    for axis, dim in sides:
        count = lax.axis_size(axis)
        ends = count - 1
        head = lax.slice_in_dim(cells, 0, width, axis=dim)
        tail = lax.slice_in_dim(cells, cells.shape[dim] - width, cells.shape[dim], axis=dim)
        cells = jnp.concatenate(
            [
                lax.ppermute(tail, axis, [(i, (i + 1) % count) for i in range(ends)]),
                cells,
                lax.ppermute(head, axis, [((i + 1) % count, i) for i in range(ends)]),
            ],
            axis=dim,
        )
    return cells


def loop_sum(padded):
    total = padded[:, 2:, 1:-1, 1:-1] + padded[:, :-2, 1:-1, 1:-1]
    total = total + padded[:, 1:-1, 2:, 1:-1] + padded[:, 1:-1, :-2, 1:-1]
    total = total + padded[:, 1:-1, 1:-1, 2:] + padded[:, 1:-1, 1:-1, :-2]
    return total


def inner_part(values):
    return values[:, 1:-1, 1:-1, 1:-1]


def pre_smooth(source, weights):
    count = source.shape[0]
    stacked = jnp.concatenate([source, weights], axis=0)
    wide = extended(stacked, (("gx", 1), ("gy", 2), ("gz", 3)), 2)
    wide_source = wide[:count]
    wide_weights = wide[count:]
    safe_weights = jnp.where(wide_weights > 0.0, wide_weights, 1.0)
    first = damping * wide_source / (6.0 * safe_weights * safe_weights)
    first_scaled = wide_weights * first
    mid_weights = inner_part(wide_weights)
    mid_safe = inner_part(safe_weights)
    applied = mid_weights * (6.0 * inner_part(first_scaled) - loop_sum(first_scaled))
    second = inner_part(first) + damping * (inner_part(wide_source) - applied) / (
        6.0 * mid_safe * mid_safe
    )
    second_scaled = mid_weights * second
    answer = inner_part(second)
    resid = source - weights * (6.0 * inner_part(second_scaled) - loop_sum(second_scaled))
    return (answer, resid)


def post_smooth(answer, source, weights):
    scaled = weights * answer
    wide = extended(scaled, (("gx", 1), ("gy", 2), ("gz", 3)), 1)
    applied = weights * (6.0 * scaled - loop_sum(wide))
    return answer + damping * (source - applied) / (6.0 * weights * weights)


def coarsen(values):
    leading = values.shape[0]
    size_x, size_y, size_z = (values.shape[1], values.shape[2], values.shape[3])
    blocks = values.reshape((leading, size_x // 2, 2, size_y // 2, 2, size_z // 2, 2))
    return jnp.mean(blocks, axis=(2, 4, 6))


def refine(values):
    return jnp.repeat(jnp.repeat(jnp.repeat(values, 2, axis=1), 2, axis=2), 2, axis=3)


def per_device(sources, stiffness, coarse_inverse):
    weight_list = [stiffness[None]]
    for level in range(3):
        weight_list.append(0.5 * coarsen(weight_list[-1]))
    source_list = []
    answer_list = []
    current = sources
    for level in range(4):
        source_list.append(current)
        answer, resid = pre_smooth(current, weight_list[level])
        answer_list.append(answer)
        current = coarsen(resid)
    count = current.shape[0]
    flat_source = current.reshape((count, -1))
    solved = lax.dot_general(
        lax.all_gather(flat_source, ("gx", "gy", "gz"), axis=1, tiled=True),
        coarse_inverse,
        (((1,), (1,)), ((), ())),
        precision=lax.Precision.HIGHEST,
        preferred_element_type=jnp.float32,
    )
    correction = solved.reshape(current.shape)
    for level in range(3, -1, -1):
        correction = post_smooth(
            answer_list[level] + refine(correction), source_list[level], weight_list[level]
        )
    return correction


K = damping / 6.0
F32 = jnp.float32
BF = jnp.bfloat16


def iota(shape, dim):
    return lax.broadcasted_iota(jnp.int32, shape, dim)


def pick(condition):
    return jnp.where(condition, 1.0, 0.0).astype(BF)


def sel_dot(values, chosen):
    high = values.astype(BF)
    low = (values - high.astype(F32)).astype(BF)
    return jnp.dot(high, chosen, preferred_element_type=F32) + jnp.dot(
        low, chosen, preferred_element_type=F32
    )


def around(c):
    rows, lanes = c.shape
    return (pltpu.roll(c, 1, 0) + pltpu.roll(c, rows - 1, 0)) + (
        pltpu.roll(c, 1, 1) + pltpu.roll(c, lanes - 1, 1)
    )


def whole_sum(planes, nz):
    rows, lanes = planes[0].shape
    row, lane = iota((rows, lanes), 0), iota((rows, lanes), 1)
    outs = []
    for p, c in enumerate(planes):
        s = jnp.where(row > 0, pltpu.roll(c, 1, 0), 0.0) + jnp.where(
            row < rows - 1, pltpu.roll(c, rows - 1, 0), 0.0
        )
        s = s + (
            jnp.where(lane > 0, pltpu.roll(c, 1, 1), 0.0)
            + jnp.where(lane < nz - 1, pltpu.roll(c, lanes - 1, 1), 0.0)
        )
        if p > 0:
            s = s + planes[p - 1]
        if p < len(planes) - 1:
            s = s + planes[p + 1]
        outs.append(s)
    return outs


def kernel(
    dims, b_hbm, w_hbm, m_hbm, f_ref,
    b_ref, w_ref, m_ref,
    V0, W0, U0, V1, W1, U1, TT, T2, A2, T3, T4, P4, P3, E2, P2, P1,
    SX0, SY0, SZ0, RX0, RY0, RXY0, RZ0, SX2, SY2, RX2, RY2,
    SXv, SYv, SZv, RXv, RYv, RXYv, RZv,
    SXw, SYw, SZw, RXw, RYw, RXYw, RZw,
    GM, GW, GB, SW, SB,
    tally, load, sent, hr, gr, known,
):
    axes = ("gx", "gy", "gz")
    ix, iy, iz = (lax.axis_index(a) for a in axes)
    n = dims[0] * dims[1] * dims[2]
    me = (ix * dims[1] + iy) * dims[2] + iz

    def place(t):
        return (t // (dims[1] * dims[2]), (t // dims[2]) % dims[1], t % dims[2])

    def other(k):
        return lax.rem(me + k, n)

    barrier = pltpu.get_barrier_semaphore()

    def there(d):
        ok = None
        for i, s, c in zip((ix, iy, iz), dims, d):
            if c:
                t = (i + c < s) if c > 0 else (i + c >= 0)
                ok = t if ok is None else jnp.logical_and(ok, t)
        return ok

    def directions(most):
        found = []
        for dx in (-1, 0, 1):
            for dy in (-1, 0, 1):
                for dz in (-1, 0, 1):
                    if 0 < abs(dx) + abs(dy) + abs(dz) <= most:
                        found.append((dx, dy, dz))
        return found

    def greet(sem):
        for d in directions(3):
            @pl.when(there(d))
            def _(d=d):
                pl.semaphore_signal(
                    sem, inc=1, device_id=(ix + d[0], iy + d[1], iz + d[2]),
                    device_id_type=pl.DeviceIdType.MESH,
                )

    loads = [
        pltpu.make_async_copy(src, dst, load.at[i])
        for i, (src, dst) in enumerate(((b_hbm, b_ref), (w_hbm, w_ref), (m_hbm, m_ref)))
    ]
    for copy in loads:
        copy.start()
    GM[...] = jnp.zeros_like(GM)
    greet(barrier)

    def span(i, s):
        return 1 + jnp.where(i > 0, 1, 0) + jnp.where(i < s - 1, 1, 0)

    greeted = span(ix, dims[0]) * span(iy, dims[1]) * span(iz, dims[2]) - 1

    def halo_copy(bufs, which, d):
        SX, SY, SZ, RX, RY, RXY, RZ, part = bufs
        dx, dy, dz = d
        up = lambda c: (c + 1) // 2
        down = lambda c: (1 - c) // 2
        if dz:
            s, r = SZ, RZ.at[1 - dx, 1 - dy, down(dz)]
            if dy and SZ.shape[0] > 8:
                half = pl.ds(SZ.shape[0] - 8 if dy > 0 else 0, 8)
                s, r = s.at[half], r.at[half]
        elif dx and dy:
            rows = SY.shape[1]
            s = SY.at[up(dy), pl.ds(rows - part if dx > 0 else 0, part), :]
            r = RXY.at[down(dx), down(dy)]
        elif dx:
            s, r = SX.at[up(dx)], RX.at[down(dx)]
        else:
            s, r = SY.at[up(dy)], RY.at[down(dy)]
        return pltpu.make_async_remote_copy(
            src_ref=s, dst_ref=r, send_sem=sent.at[0], recv_sem=hr.at[which],
            device_id=(ix + dx, iy + dy, iz + dz), device_id_type=pl.DeviceIdType.MESH,
        )

    def faces_start():
        for d in directions(1):
            if not d[2]:
                @pl.when(there(d))
                def _(d=d):
                    halo_copy(bufs_face, 3, d).start()

    def matrix_start():
        for d in directions(3):
            @pl.when(there(d))
            def _(d=d):
                s, r = m_ref, GM.at[me]
                if d[2]:
                    row = pl.ds(m_ref.shape[0] - 1 if d[2] > 0 else 0, 1)
                    s, r = s.at[row], r.at[row]
                pltpu.make_async_remote_copy(
                    src_ref=s, dst_ref=r, send_sem=sent.at[0], recv_sem=gr.at[1],
                    device_id=(ix + d[0], iy + d[1], iz + d[2]),
                    device_id_type=pl.DeviceIdType.MESH,
                ).start()

    def halo_start(bufs, which, most):
        for d in directions(most):
            @pl.when(there(d))
            def _(d=d):
                halo_copy(bufs, which, d).start()

    def bytes_of(ref, sem):
        pltpu.make_async_copy(ref, ref, sem).wait()

    sides_y, sides_z = span(iy, dims[1]) - 1, span(iz, dims[2]) - 1

    def first_part(cy, cz):
        return 8 + 10 * cy + (8 + 2 * cy) * cz

    def face_part(cy, cz):
        return 4 + 4 * cy

    def second_part(cy, cz):
        return 6 + 12 * cy + 4 * (1 + cy) * cz

    def matrix_part(cy, cz):
        return 4 + 8 * cy + (1 + cy) * cz

    def everything(cy, cz):
        halos = first_part(cy, cz) + face_part(cy, cz) + 2 * second_part(cy, cz)
        return halos + matrix_part(cy, cz) + 2 * (n - 1)

    def take(part, sem):
        for cy in (1, 2):
            for cz in (1, 2):
                @pl.when(jnp.logical_and(sides_y == cy, sides_z == cz))
                def _(cy=cy, cz=cz):
                    bytes_of(tally.at[pl.ds(0, part(cy, cz))], sem)

    def spread(kind, src, dst, k):
        return pltpu.make_async_remote_copy(
            src_ref=src, dst_ref=dst.at[me], send_sem=sent.at[0], recv_sem=gr.at[kind],
            device_id=place(other(k)), device_id_type=pl.DeviceIdType.MESH,
        )

    def arrive(kind, dst):
        bytes_of(dst.at[pl.ds(0, n - 1)], gr.at[kind])


    nx, ny = b_ref.shape[0], b_ref.shape[1]
    hx, hy = nx // 2, ny // 2
    bufs0 = (SX0, SY0, SZ0, RX0, RY0, RXY0, RZ0, 8)
    bufs_face = (SX2, SY2, SZ0, RX2, RY2, RXY0, RZ0, 8)
    bufsv = (SXv, SYv, SZv, RXv, RYv, RXYv, RZv, 16)
    bufsw = (SXw, SYw, SZw, RXw, RYw, RXYw, RZw, 16)

    for copy in loads[:2]:
        copy.wait()
    lane16 = iota((ny, 128), 1)
    packed = jnp.zeros((ny, 128), F32)
    for x in range(nx):
        w = w_ref[x]
        v = K * b_ref[x] / w
        V0[x + 2, 0:ny, 0:128] = v
        W0[x + 2, 0:ny, 0:128] = w
        for a, q in enumerate((v, w)):
            if a == 0:
                if x < 2:
                    SX0[0, x] = q
                if x >= nx - 2:
                    SX0[1, x - nx + 2] = q
                SY0[0, 2 * x : 2 * x + 2, :] = q[0:2, :]
                SY0[1, 2 * x : 2 * x + 2, :] = q[ny - 2 : ny, :]
            else:
                if x == 0:
                    SX2[0] = q
                if x == nx - 1:
                    SX2[1] = q
                SY2[0, x : x + 1, :] = q[0:1, :]
                SY2[1, x : x + 1, :] = q[ny - 1 : ny, :]
            start = 8 * x + 4 * a
            moved = pltpu.roll(q, (start + 2) % 128, 1)
            packed = jnp.where((lane16 >= start) & (lane16 < start + 4), moved, packed)
    SZ0[...] = packed

    pl.semaphore_wait(barrier, greeted)
    halo_start(bufs0, 0, 2)
    greet(known.at[0])
    faces_start()

    halve = pick(iota((128, 128), 0) == 2 * iota((128, 128), 1))
    halve = halve + pick(iota((128, 128), 0) == 2 * iota((128, 128), 1) + 1)

    def coarsen0(planes):
        for i in range(hx):
            TT[i] = planes(2 * i) + planes(2 * i + 1)
        rows = [
            TT[i, pl.ds(0, hy, stride=2), :] + TT[i, pl.ds(1, hy, stride=2), :] for i in range(hx)
        ]
        return sel_dot(jnp.concatenate(rows, axis=0), halve)

    def coarsen1(planes, SG):
        for i in range(hx // 2):
            T2[pl.ds(8 * i, 8), :] = planes(2 * i) + planes(2 * i + 1)
        for y in range(4):
            A2[pl.ds(4 * y, 4), :] = (
                T2[pl.ds(2 * y, 4, stride=8), :] + T2[pl.ds(2 * y + 1, 4, stride=8), :]
            )
        TT[0] = sel_dot(A2[...], halve)
        total = TT[0, 0:4, :]
        for y in range(1, 4):
            total = total + pltpu.roll(TT[0, 4 * y : 4 * y + 4, :], 32 * y, 1)
        return total

    lane8 = iota((8, 128), 1)

    def pack1(bufs, planes):
        SX, SY, SZ = bufs[:3]
        out = jnp.zeros((8, 128), F32)
        for x in range(hx):
            q = planes[x]
            if x < 3:
                SX[0, x] = q
            if x >= hx - 3:
                SX[1, x - hx + 3] = q
            SY[0, 4 * x : 4 * x + 4, :] = q[0:4, :]
            SY[1, 4 * x : 4 * x + 4, :] = q[4:8, :]
            s = 16 * x
            out = jnp.where((lane8 >= s) & (lane8 < s + 3), pltpu.roll(q, (s - 61) % 128, 1), out)
            out = jnp.where(
                (lane8 >= s + 3) & (lane8 < s + 6), pltpu.roll(q, (s + 3) % 128, 1), out
            )
        SZ[...] = out

    w1 = 0.0625 * coarsen0(lambda x: w_ref[x])
    w1 = [w1[8 * x : 8 * x + 8, :] for x in range(hx)]
    pack1(bufsw, w1)
    SW[...] = 0.0625 * coarsen1(lambda x: w1[x], SW)
    GW[me] = SW[...]
    loads[2].wait()
    GM[me] = m_ref[...]
    halo_start(bufsw, 1, 3)
    matrix_start()
    pl.semaphore_wait(known.at[0], greeted)
    greet(known.at[1])

    def coords(rows, lanes, cy, cz, by, bz):
        r, l = iota((rows, lanes), 0), iota((rows, lanes), 1)
        y = jnp.where(r < cy + (rows - cy) // 2, r, r - rows)
        z = jnp.where(l < cz + (lanes - cz) // 2, l, l - lanes)
        gy, gz = y + iy * cy, z + iz * cz
        ok = (gy >= 0) & (gy < dims[1] * cy) & (gz >= 0) & (gz < dims[2] * cz)
        near = (y >= -by) & (y < cy + by) & (z >= -bz) & (z < cz + bz)
        return jnp.where(ok & near, 1, 0)

    def plane_mask(base, x, cx):
        if 0 <= x < cx:
            return base > 0
        gx = x + ix * cx
        inside = jnp.where((gx >= 0) & (gx < dims[0] * cx), 1, 0)
        return base * inside > 0

    take(first_part, hr.at[0])
    mask0 = coords(24, 256, ny, 128, 2, 2)
    row8 = iota((8, 128), 0)
    lane24 = iota((24, 128), 1)

    def z_sides(dx):
        sides = []
        for side in (0, 1):
            mid = RZ0[dx + 1, 1, side]
            if dx == 0:
                edge = jnp.where(row8 < 4, RZ0[1, 2, side, 0:8, :], RZ0[1, 0, side, 8:16, :])
            else:
                edge = jnp.zeros((8, 128), F32)
            sides.append(jnp.concatenate([mid, edge], axis=0))
        return sides

    def z_part(sides, s):
        return jnp.where(
            lane24 < 64,
            pltpu.roll(sides[1], (-(s + 2)) % 128, 1),
            pltpu.roll(sides[0], (126 - s) % 128, 1),
        )

    V0[0:2, 0:ny, 0:128] = RX0[0]
    V0[nx + 2 : nx + 4, 0:ny, 0:128] = RX0[1]
    for x in range(nx):
        V0[x + 2, 16:18, 0:128] = RY0[1, 2 * x : 2 * x + 2, :]
        V0[x + 2, 22:24, 0:128] = RY0[0, 2 * x : 2 * x + 2, :]
    V0[1, 16:18, 0:128] = RXY0[0, 1, 6:8, :]
    V0[1, 22:24, 0:128] = RXY0[0, 0, 6:8, :]
    V0[nx + 2, 16:18, 0:128] = RXY0[1, 1, 0:2, :]
    V0[nx + 2, 22:24, 0:128] = RXY0[1, 0, 0:2, :]
    for dx in (-1, 0, 1):
        sides = z_sides(dx)
        for x in {-1: (nx - 1,), 0: range(nx), 1: (0,)}[dx]:
            V0[x + 2 + dx * nx, :, 128:256] = z_part(sides, 8 * x)
    for p in range(nx + 4):
        V0[p] = jnp.where(plane_mask(mask0, p - 2, nx), V0[p], 0.0)

    def assemble_faces():
        mask = coords(24, 256, ny, 128, 1, 1)
        W0[1, 0:ny, 0:128] = RX2[0]
        W0[nx + 2, 0:ny, 0:128] = RX2[1]
        sides = z_sides(0)
        for x in range(nx):
            W0[x + 2, 16:17, 0:128] = RY2[1, x : x + 1, :]
            W0[x + 2, 23:24, 0:128] = RY2[0, x : x + 1, :]
            W0[x + 2, :, 128:256] = z_part(sides, 8 * x + 4)
        for p in range(1, nx + 3):
            W0[p] = jnp.where(plane_mask(mask, p - 2, nx), W0[p], 0.0)

    pl.semaphore_wait(known.at[1], greeted)
    for k in range(1, n):
        spread(0, SW, GW, k).start()

    for p in range(1, nx + 3):
        c = V0[p]
        u = 1.2 * c + K * (around(c) + (V0[p - 1] + V0[p + 1]))
        U0[p] = jnp.where(plane_mask(mask0, p - 2, nx), u, 0.0)

    def own_sum(ref, p):
        c = ref[p]
        return around(c)[0:ny, 0:128] + (ref[p - 1, 0:ny, 0:128] + ref[p + 1, 0:ny, 0:128])

    def resid0(x):
        p = x + 2
        return b_ref[x] - w_ref[x] * (6.0 * U0[p, 0:ny, 0:128] - own_sum(U0, p))

    b1 = 0.125 * coarsen0(resid0)
    b1 = [b1[8 * x : 8 * x + 8, :] for x in range(hx)]
    v1 = [jnp.where(lane8 < 64, K * b1[x] / jnp.where(lane8 < 64, w1[x], 1.0), 0.0) for x in range(hx)]
    pack1(bufsv, v1)
    halo_start(bufsv, 2, 3)

    mask1 = coords(16, 128, 8, 64, 3, 3)
    lane1 = iota((16, 128), 1)

    def assemble1(bufs, planes, D):
        RX, RY, RXY, RZ = bufs[3:7]
        for dx in (-1, 0, 1):
            sides = []
            for side in (0, 1):
                edge = jnp.where(row8 < 4, RZ[dx + 1, 2, side], RZ[dx + 1, 0, side])
                sides.append(jnp.concatenate([RZ[dx + 1, 1, side], edge], axis=0))
            for x in {-1: range(hx - 3, hx), 0: range(hx), 1: range(3)}[dx]:
                p = x + 3 + dx * hx
                if dx == 0:
                    D[p, 0:8, :] = planes[x]
                    D[p, 8:12, :] = RY[1, 4 * x : 4 * x + 4, :]
                    D[p, 12:16, :] = RY[0, 4 * x : 4 * x + 4, :]
                else:
                    slot = (dx + 1) // 2
                    D[p, 0:8, :] = RX[slot, p if dx < 0 else x]
                    q = 4 * (x - 4 if dx < 0 else x)
                    D[p, 8:12, :] = RXY[slot, 1, q : q + 4, :]
                    D[p, 12:16, :] = RXY[slot, 0, q : q + 4, :]
                s = 16 * x
                ends = jnp.where(
                    lane1 < 96,
                    pltpu.roll(sides[1], (61 - s) % 128, 1),
                    pltpu.roll(sides[0], (125 - s) % 128, 1),
                )
                merged = jnp.where(lane1 < 64, D[p], ends)
                D[p] = jnp.where(plane_mask(mask1, x + dx * hx, hx), merged, 0.0)

    take(second_part, hr.at[1])
    assemble1(bufsw, w1, W1)

    block = lane8 // 32
    quarter = row8 % 4

    def unpack(G):
        planes = []
        for X in range(4 * dims[0]):
            tiles = []
            for t in range(dims[1] // 2):
                rows = []
                for z in range(dims[2]):
                    d0 = ((X // 4) * dims[1] + 2 * t) * dims[2] + z
                    d1 = d0 + dims[2]
                    q = X % 4
                    rows.append(
                        jnp.where(
                            row8 < 4,
                            jnp.broadcast_to(G[d0, q : q + 1, :], (8, 128)),
                            jnp.broadcast_to(G[d1, q : q + 1, :], (8, 128)),
                        )
                    )
                out = None
                for s in range(4):
                    pre = rows[s % 4]
                    for j in range(1, 4):
                        pre = jnp.where(block == j, rows[(j + s) % 4], pre)
                    moved = pltpu.roll(pre, 32 * s, 1) if s else pre
                    out = moved if out is None else jnp.where(block == (quarter + s) % 4, moved, out)
                tiles.append(out)
            planes.append(jnp.concatenate(tiles, axis=0))
        return planes

    def coarsen2(planes):
        c = len(planes) // 2
        for i in range(c):
            T3[i] = planes[2 * i] + planes[2 * i + 1]
        rows = [T3[i, pl.ds(0, 8, stride=2), :] + T3[i, pl.ds(1, 8, stride=2), :] for i in range(c)]
        out = sel_dot(jnp.concatenate(rows, axis=0), halve)
        return [out[8 * i : 8 * i + 8, :] for i in range(c)]


    take(second_part, hr.at[2])
    assemble1(bufsv, v1, V1)
    for p in range(1, hx + 5):
        c = V1[p]
        u = 1.2 * c + K * (around(c) + (V1[p - 1] + V1[p + 1]))
        U1[p] = jnp.where(plane_mask(mask1, p - 3, hx), u, 0.0)

    def resid1(x):
        p = x + 3
        s = around(U1[p])[0:8, :] + (U1[p - 1, 0:8, :] + U1[p + 1, 0:8, :])
        return jnp.where(lane8 < 64, b1[x] - w1[x] * (6.0 * U1[p, 0:8, :] - s), 0.0)

    SB[...] = 0.125 * coarsen1(resid1, SB)
    GB[me] = SB[...]
    for k in range(1, n):
        spread(2, SB, GB, k).start()
    arrive(0, GW)
    w2 = unpack(GW)
    w3 = [0.0625 * q for q in coarsen2(w2)]
    valid3 = lane8 < 64
    w3s = [jnp.where(valid3, q, 1.0) for q in w3]
    take(matrix_part, gr.at[1])
    take(face_part, hr.at[3])
    assemble_faces()
    arrive(2, GB)

    b2 = unpack(GB)
    v2 = [K * b / w for b, w in zip(b2, w2)]
    u2 = [1.2 * v + K * s for v, s in zip(v2, whole_sum(v2, 128))]
    r2 = [b - w * (6.0 * u - s) for b, w, u, s in zip(b2, w2, u2, whole_sum(u2, 128))]
    b3 = [0.125 * q for q in coarsen2(r2)]
    v3 = [K * b / w for b, w in zip(b3, w3s)]
    u3 = [jnp.where(valid3, 1.2 * v + K * s, 0.0) for v, s in zip(v3, whole_sum(v3, 64))]
    r3 = [b - w * (6.0 * u - s) for b, w, u, s in zip(b3, w3, u3, whole_sum(u3, 64))]
    c4 = len(r3) // 2
    for i in range(c4):
        T4[pl.ds(8 * i, 8), :] = r3[2 * i] + r3[2 * i + 1]
    half = 4 * c4
    b4 = 0.125 * sel_dot(T4[pl.ds(0, half, stride=2), :] + T4[pl.ds(1, half, stride=2), :], halve)
    acc = b4
    for j in range(1, 4):
        acc = jnp.where(quarter == j, pltpu.roll(b4, 32 * j, 1), acc)
    low = jnp.sum(jnp.where(row8 < 4, acc, 0.0), axis=0, keepdims=True)
    high = jnp.sum(jnp.where(row8 >= 4, acc, 0.0), axis=0, keepdims=True)
    cells = GM.shape[0] * GM.shape[1]
    matrix = GM[...].reshape((cells, 256))
    solved = jnp.sum(matrix[:, 0:128] * low + matrix[:, 128:256] * high, axis=1, keepdims=True)
    hit = (iota((cells, 128), 0) % 32) == iota((cells, 128), 1) // 2
    e4 = jnp.sum(jnp.where(hit, solved, 0.0).reshape((cells // 32, 32, 128)), axis=1)
    P4[pl.ds(0, half, stride=2), :] = e4
    P4[pl.ds(1, half, stride=2), :] = e4

    y3 = [u + w * P4[8 * (i // 2) : 8 * (i // 2) + 8, :] for i, (u, w) in enumerate(zip(u3, w3))]
    e3 = [
        jnp.where(valid3, (0.2 * y + v + K * s) / w, 0.0)
        for y, v, s, w in zip(y3, v3, whole_sum(y3, 64), w3s)
    ]
    double = pick(iota((128, 256), 0) == iota((128, 256), 1) // 2)
    wide3 = sel_dot(jnp.concatenate(e3, axis=0), double[:, 0:128])
    for i in range(len(e3)):
        P3[i, pl.ds(0, 8, stride=2), :] = wide3[8 * i : 8 * i + 8, :]
        P3[i, pl.ds(1, 8, stride=2), :] = wide3[8 * i : 8 * i + 8, :]
    y2 = [u + w * P3[i // 2] for i, (u, w) in enumerate(zip(u2, w2))]
    s2 = whole_sum(y2, 128)
    E2[...] = jnp.zeros_like(E2)
    for i in range(len(y2)):
        E2[i + 1, 8:24, :] = (0.2 * y2[i] + v2[i] + K * s2[i]) / w2[i]

    seen = jnp.concatenate([E2[4 * ix + i, pl.ds(6 + 4 * iy, 8), :] for i in range(6)], axis=0)
    j = iota((128, 128), 1)
    zl = jnp.where(j < 96, j // 2, j // 2 - 64) + 32 * iz
    wide2 = sel_dot(seen, pick(iota((128, 128), 0) == zl))
    for i in range(6):
        P2[i, pl.ds(0, 8, stride=2), :] = wide2[8 * i : 8 * i + 8, :]
        P2[i, pl.ds(1, 8, stride=2), :] = wide2[8 * i : 8 * i + 8, :]
    for p in range(1, hx + 5):
        U1[p] = U1[p] + W1[p] * pltpu.roll(P2[(p - 3) // 2 + 1], 12, 0)
    e1 = []
    for p in range(2, hx + 4):
        c = U1[p]
        f = 0.2 * c + V1[p] + K * (around(c) + (U1[p - 1] + U1[p + 1]))
        inside = plane_mask(mask1, p - 3, hx)
        e1.append(jnp.where(inside, f, 0.0) / jnp.where(inside, W1[p], 1.0))
    wide1 = sel_dot(jnp.concatenate(e1, axis=0), double)
    for i in range(hx + 2):
        for t in range(2):
            q = wide1[16 * i : 16 * i + 16, 128 * t : 128 * t + 128]
            P1[t, i, pl.ds(0, 16, stride=2), :] = q
            P1[t, i, pl.ds(1, 16, stride=2), :] = q

    for p in range(1, nx + 3):
        i = (p - 2) // 2 + 1
        parts = []
        for t in range(2):
            edge = jnp.where(row8 < 4, P1[t, i, 16:24, :], P1[t, i, 24:32, :])
            parts.append(jnp.concatenate([P1[t, i, 0:16, :], edge], axis=0))
        U0[p] = U0[p] + W0[p] * jnp.concatenate(parts, axis=1)
    for x in range(nx):
        p = x + 2
        f = 0.2 * U0[p, 0:ny, 0:128] + V0[p, 0:ny, 0:128] + K * own_sum(U0, p)
        f_ref[x] = f / w_ref[x]

    take(everything, sent.at[0])


def fused(dims, sources, stiffness, coarse_inverse):
    nx, ny, nz = stiffness.shape
    n = dims[0] * dims[1] * dims[2]
    vm = lambda *s: pltpu.VMEM(s, F32)
    halo0 = [
        vm(2, 2, ny, 128), vm(2, 2 * nx, 128), vm(ny, 128),
        vm(2, 2, ny, 128), vm(2, 2 * nx, 128), vm(2, 2, 8, 128), vm(3, 3, 2, ny, 128),
        vm(2, ny, 128), vm(2, nx, 128), vm(2, ny, 128), vm(2, nx, 128),
    ]
    halo1 = [
        vm(2, 3, 8, 128), vm(2, 32, 128), vm(8, 128),
        vm(2, 3, 8, 128), vm(2, 32, 128), vm(2, 2, 16, 128), vm(3, 3, 2, 8, 128),
    ]
    result = pl.pallas_call(
        functools.partial(kernel, dims),
        out_shape=pltpu.VMEM((nx, ny, nz), F32),
        in_specs=[pl.BlockSpec(memory_space=pl.ANY)] * 3,
        out_specs=pl.BlockSpec(memory_space=pltpu.VMEM),
        scratch_shapes=[
            vm(nx, ny, nz), vm(nx, ny, nz), vm(*coarse_inverse.shape),
            vm(nx + 4, 24, 256), vm(nx + 4, 24, 256), vm(nx + 4, 24, 256),
            vm(14, 16, 128), vm(14, 16, 128), vm(14, 16, 128),
            vm(8, 16, 128), vm(32, 128), vm(16, 128), vm(2 * dims[0], 16, 128),
            vm(16, 128), vm(16, 128), vm(2 * dims[0], 16, 128),
            vm(4 * dims[0] + 2, 32, 128), vm(6, 16, 128), vm(2, 10, 32, 128),
        ]
        + halo0 + halo1 + halo1
        + [
            vm(n, 8, 256), vm(n, 4, 128), vm(n, 4, 128), vm(4, 128), vm(4, 128),
            vm(512, 4, 128),
            pltpu.SemaphoreType.DMA((3,)), pltpu.SemaphoreType.DMA((1,)),
            pltpu.SemaphoreType.DMA((4,)), pltpu.SemaphoreType.DMA((3,)),
            pltpu.SemaphoreType.REGULAR((2,)),
        ],
        compiler_params=pltpu.CompilerParams(collective_id=0, has_side_effects=True),
        name="cycle",
    )(sources[0], stiffness, coarse_inverse)
    return result[None]


def solution(mesh):
    dims = tuple(mesh.shape[a] for a in ("gx", "gy", "gz"))

    def run(sources, stiffness, coarse_inverse):
        nx, ny, nz = stiffness.shape
        lanes = 128
        cells = coarse_inverse.shape[1]
        levels_fit = (
            sources.shape[0] == 1
            and nx == ny == 16
            and nz == lanes
            and dims[2] * nz == 4 * lanes
            and dims[1] * ny == 64
            and cells == 2 * lanes
            and dims[0] == 2
        )
        if levels_fit:
            return fused(dims, sources, stiffness, coarse_inverse)
        return per_device(sources, stiffness, coarse_inverse)

    in_specs = (P(None, "gx", "gy", "gz"), P("gx", "gy", "gz"), P(("gx", "gy", "gz"), None))
    out_specs = P(None, "gx", "gy", "gz")
    return jax.shard_map(
        run, mesh=mesh, in_specs=in_specs, out_specs=out_specs, check_vma=False
    )
```

```python
import functools
import jax
import jax.numpy as jnp
from jax import lax
from jax.experimental import pallas as pl
from jax.experimental.pallas import tpu as pltpu
from jax.sharding import PartitionSpec as P

damping = 0.8


def extended(cells, sides, width):
    for axis, dim in sides:
        count = lax.axis_size(axis)
        ends = count - 1
        head = lax.slice_in_dim(cells, 0, width, axis=dim)
        tail = lax.slice_in_dim(cells, cells.shape[dim] - width, cells.shape[dim], axis=dim)
        cells = jnp.concatenate(
            [
                lax.ppermute(tail, axis, [(i, (i + 1) % count) for i in range(ends)]),
                cells,
                lax.ppermute(head, axis, [((i + 1) % count, i) for i in range(ends)]),
            ],
            axis=dim,
        )
    return cells


def loop_sum(padded):
    total = padded[:, 2:, 1:-1, 1:-1] + padded[:, :-2, 1:-1, 1:-1]
    total = total + padded[:, 1:-1, 2:, 1:-1] + padded[:, 1:-1, :-2, 1:-1]
    total = total + padded[:, 1:-1, 1:-1, 2:] + padded[:, 1:-1, 1:-1, :-2]
    return total


def inner_part(values):
    return values[:, 1:-1, 1:-1, 1:-1]


def pre_smooth(source, weights):
    count = source.shape[0]
    stacked = jnp.concatenate([source, weights], axis=0)
    wide = extended(stacked, (("gx", 1), ("gy", 2), ("gz", 3)), 2)
    wide_source = wide[:count]
    wide_weights = wide[count:]
    safe_weights = jnp.where(wide_weights > 0.0, wide_weights, 1.0)
    first = damping * wide_source / (6.0 * safe_weights * safe_weights)
    first_scaled = wide_weights * first
    mid_weights = inner_part(wide_weights)
    mid_safe = inner_part(safe_weights)
    applied = mid_weights * (6.0 * inner_part(first_scaled) - loop_sum(first_scaled))
    second = inner_part(first) + damping * (inner_part(wide_source) - applied) / (
        6.0 * mid_safe * mid_safe
    )
    second_scaled = mid_weights * second
    answer = inner_part(second)
    resid = source - weights * (6.0 * inner_part(second_scaled) - loop_sum(second_scaled))
    return (answer, resid)


def post_smooth(answer, source, weights):
    scaled = weights * answer
    wide = extended(scaled, (("gx", 1), ("gy", 2), ("gz", 3)), 1)
    applied = weights * (6.0 * scaled - loop_sum(wide))
    return answer + damping * (source - applied) / (6.0 * weights * weights)


def coarsen(values):
    leading = values.shape[0]
    size_x, size_y, size_z = (values.shape[1], values.shape[2], values.shape[3])
    blocks = values.reshape((leading, size_x // 2, 2, size_y // 2, 2, size_z // 2, 2))
    return jnp.mean(blocks, axis=(2, 4, 6))


def refine(values):
    return jnp.repeat(jnp.repeat(jnp.repeat(values, 2, axis=1), 2, axis=2), 2, axis=3)


def per_device(sources, stiffness, coarse_inverse):
    weight_list = [stiffness[None]]
    for level in range(3):
        weight_list.append(0.5 * coarsen(weight_list[-1]))
    source_list = []
    answer_list = []
    current = sources
    for level in range(4):
        source_list.append(current)
        answer, resid = pre_smooth(current, weight_list[level])
        answer_list.append(answer)
        current = coarsen(resid)
    count = current.shape[0]
    flat_source = current.reshape((count, -1))
    solved = lax.dot_general(
        lax.all_gather(flat_source, ("gx", "gy", "gz"), axis=1, tiled=True),
        coarse_inverse,
        (((1,), (1,)), ((), ())),
        precision=lax.Precision.HIGHEST,
        preferred_element_type=jnp.float32,
    )
    correction = solved.reshape(current.shape)
    for level in range(3, -1, -1):
        correction = post_smooth(
            answer_list[level] + refine(correction), source_list[level], weight_list[level]
        )
    return correction


K = damping / 6.0
F32 = jnp.float32
BF = jnp.bfloat16


def iota(shape, dim):
    return lax.broadcasted_iota(jnp.int32, shape, dim)


def pick(condition):
    return jnp.where(condition, 1.0, 0.0).astype(BF)


def sel_dot(values, chosen):
    high = values.astype(BF)
    low = (values - high.astype(F32)).astype(BF)
    return jnp.dot(high, chosen, preferred_element_type=F32) + jnp.dot(
        low, chosen, preferred_element_type=F32
    )


def around(c):
    rows, lanes = c.shape
    return (pltpu.roll(c, 1, 0) + pltpu.roll(c, rows - 1, 0)) + (
        pltpu.roll(c, 1, 1) + pltpu.roll(c, lanes - 1, 1)
    )


def whole_sum(planes, nz):
    rows, lanes = planes[0].shape
    row, lane = iota((rows, lanes), 0), iota((rows, lanes), 1)
    outs = []
    for p, c in enumerate(planes):
        s = jnp.where(row > 0, pltpu.roll(c, 1, 0), 0.0) + jnp.where(
            row < rows - 1, pltpu.roll(c, rows - 1, 0), 0.0
        )
        s = s + (
            jnp.where(lane > 0, pltpu.roll(c, 1, 1), 0.0)
            + jnp.where(lane < nz - 1, pltpu.roll(c, lanes - 1, 1), 0.0)
        )
        if p > 0:
            s = s + planes[p - 1]
        if p < len(planes) - 1:
            s = s + planes[p + 1]
        outs.append(s)
    return outs


def kernel(
    dims, b_hbm, w_hbm, m_hbm, f_ref,
    b_ref, w_ref, m_ref,
    V0, W0, U0, V1, W1, U1, TT, T2, A2, T3, T4, P4, P3, E2, P2, P1, IW,
    SZ0, RZ0, S1v, SZv, RZv, R3v, RCv, S1w, SZw, RZw, R3w, RCw,
    GM, GW, GB, SW, SB,
    tally, load, sent, hr, gr, known,
):
    axes = ("gx", "gy", "gz")
    ix, iy, iz = (lax.axis_index(a) for a in axes)
    n = dims[0] * dims[1] * dims[2]
    me = (ix * dims[1] + iy) * dims[2] + iz

    def place(t):
        return (t // (dims[1] * dims[2]), (t // dims[2]) % dims[1], t % dims[2])

    def other(k):
        return lax.rem(me + k, n)

    barrier = pltpu.get_barrier_semaphore()

    def there(d):
        ok = None
        for i, s, c in zip((ix, iy, iz), dims, d):
            if c:
                t = (i + c < s) if c > 0 else (i + c >= 0)
                ok = t if ok is None else jnp.logical_and(ok, t)
        return ok

    def directions(most):
        found = []
        for dx in (-1, 0, 1):
            for dy in (-1, 0, 1):
                for dz in (-1, 0, 1):
                    if 0 < abs(dx) + abs(dy) + abs(dz) <= most:
                        found.append((dx, dy, dz))
        return found

    def greet(sem):
        for d in directions(3):
            @pl.when(there(d))
            def _(d=d):
                pl.semaphore_signal(
                    sem, inc=1, device_id=(ix + d[0], iy + d[1], iz + d[2]),
                    device_id_type=pl.DeviceIdType.MESH,
                )

    loads = [
        pltpu.make_async_copy(src, dst, load.at[i])
        for i, (src, dst) in enumerate(((b_hbm, b_ref), (w_hbm, w_ref), (m_hbm, m_ref)))
    ]
    for copy in loads:
        copy.start()
    nx, ny = b_ref.shape[0], b_ref.shape[1]
    hx, hy = nx // 2, ny // 2

    def clear(ref, *where):
        part = ref.at[where] if where else ref
        part[...] = jnp.zeros(part.shape, F32)

    own = (pl.ds(0, ny), pl.ds(0, 128))
    clear(V0, pl.ds(0, 2), *own)
    clear(V0, pl.ds(nx + 2, 2), *own)
    clear(V0, pl.ds(1, nx + 2), pl.ds(ny, 8), pl.ds(0, 128))
    clear(W0, pl.ds(1, 1), *own)
    clear(W0, pl.ds(nx + 2, 1), *own)
    clear(W0, pl.ds(2, nx), pl.ds(ny, 8), pl.ds(0, 128))
    for D in (V1, W1):
        clear(D, pl.ds(0, 3))
        clear(D, pl.ds(hx + 3, 3))
        clear(D, pl.ds(3, hx), pl.ds(8, 8))
    for D in (RZ0, RZv, R3v, RCv, RZw, R3w, RCw):
        clear(D)
    greet(barrier)

    def span(i, s):
        return 1 + jnp.where(i > 0, 1, 0) + jnp.where(i < s - 1, 1, 0)

    greeted = span(ix, dims[0]) * span(iy, dims[1]) * span(iz, dims[2]) - 1

    def send(src, dst, d, sem):
        pltpu.make_async_remote_copy(
            src_ref=src, dst_ref=dst, send_sem=sent.at[0], recv_sem=sem,
            device_id=(ix + d[0], iy + d[1], iz + d[2]), device_id_type=pl.DeviceIdType.MESH,
        ).start()

    def send_all(found, pieces, sem):
        for d in found:
            @pl.when(there(d))
            def _(d=d):
                send(*pieces(d), d, sem)

    def span_x(c, size, pad, deep):
        if c == 0:
            return pl.ds(0, size), pl.ds(pad, size)
        if c > 0:
            return pl.ds(size - deep, deep), pl.ds(pad - deep, deep)
        return pl.ds(0, deep), pl.ds(pad + size, deep)

    def span_y(c, size, total, deep):
        if c == 0:
            return pl.ds(0, size), pl.ds(0, size)
        if c > 0:
            return pl.ds(size - deep, deep), pl.ds(total - deep, deep)
        return pl.ds(0, deep), pl.ds(size, deep)

    def flat(found):
        return [d for d in found if not d[2]]

    first = pl.ds(0, 128)

    def pieces0(d):
        dx, dy, dz = d
        if dz:
            a, b = span_y(dy, ny, ny + 8, 1)
            return SZ0.at[a], RZ0.at[1 - dx, (1 - dz) // 2, b]
        deep = 1 if dx and dy else 2
        a, b = span_x(dx, nx, 2, deep)
        e, f = span_y(dy, ny, ny + 8, deep)
        shifted = pl.ds(a.start + 2, a.size)
        return V0.at[shifted, e, first], V0.at[b, f, first]

    def faces0(d):
        a, b = span_x(d[0], nx, 2, 1)
        e, f = span_y(d[1], ny, ny + 8, 1)
        return W0.at[pl.ds(a.start + 2, a.size), e, first], W0.at[b, f, first]

    def pieces1(S1, D, SZ, RZ):
        def of(d):
            dx, dy, dz = d
            if dz:
                a, b = span_y(dy, 8, 16, 2)
                return SZ.at[a], RZ.at[1 - dx, (1 - dz) // 2, b]
            a, b = span_x(dx, hx, 3, 2 if dy else 3)
            e, f = span_y(dy, 8, 16, 2)
            return S1.at[a, e], D.at[b, f]
        return of

    def late1(S1, R3, SZ, RC):
        def of(d):
            dx, dy, dz = d
            if dz:
                row = pl.ds(7 if dy > 0 else 0, 1)
                return SZ.at[row], RC.at[(1 - dx) // 2, (1 - dz) // 2, row]
            row = pl.ds(5 if dy > 0 else 2, 1)
            return S1.at[:, row], R3.at[:, row]
        return of

    def matrix_rows(d):
        s, r = m_ref, GM.at[me]
        if d[2]:
            row = pl.ds(m_ref.shape[0] - 1 if d[2] > 0 else 0, 1)
            s, r = s.at[row], r.at[row]
        return s, r

    corners = [d for d in directions(3) if all(d)]
    lates = [(0, -1, 0), (0, 1, 0)] + corners

    def bytes_of(ref, sem):
        pltpu.make_async_copy(ref, ref, sem).wait()

    sides_y, sides_z = span(iy, dims[1]) - 1, span(iz, dims[2]) - 1

    def first_part(cy, cz):
        return 32 + 33 * cy + 32 * cz + cy * cz

    def face_part(cy, cz):
        return 16 + 16 * cy

    def second_part(cy, cz):
        return 24 + 20 * cy + 16 * cz + 2 * cy * cz

    def late_part(cy, cz):
        return second_part(cy, cz) + 2 * (8 * cy + cy * cz)

    def matrix_part(cy, cz):
        return 16 + 32 * cy + 4 * (1 + cy) * cz

    def everything(cy, cz):
        parts = (first_part, face_part, second_part, late_part, matrix_part)
        return sum(part(cy, cz) for part in parts) + 8 * (n - 1)

    def take(part, sem):
        for cy in (1, 2):
            for cz in (1, 2):
                @pl.when(jnp.logical_and(sides_y == cy, sides_z == cz))
                def _(cy=cy, cz=cz):
                    bytes_of(tally.at[pl.ds(0, part(cy, cz))], sem)

    def spread(kind, src, dst, k):
        return pltpu.make_async_remote_copy(
            src_ref=src, dst_ref=dst.at[me], send_sem=sent.at[0], recv_sem=gr.at[kind],
            device_id=place(other(k)), device_id_type=pl.DeviceIdType.MESH,
        )

    def arrive(kind, dst):
        bytes_of(dst.at[pl.ds(0, n - 1)], gr.at[kind])


    for copy in loads[:2]:
        copy.wait()
    lane16 = iota((ny, 128), 1)
    packed = jnp.zeros((ny, 128), F32)
    for x in range(nx):
        w = w_ref[x]
        v = K * b_ref[x] / w
        V0[x + 2, 0:ny, 0:128] = v
        W0[x + 2, 0:ny, 0:128] = w
        for a, q in enumerate((v, w)):
            start = 8 * x + 4 * a
            moved = pltpu.roll(q, (start + 2) % 128, 1)
            packed = jnp.where((lane16 >= start) & (lane16 < start + 4), moved, packed)
    SZ0[...] = packed

    pl.semaphore_wait(barrier, greeted)
    send_all(directions(2), pieces0, hr.at[0])
    greet(known.at[0])
    send_all(flat(directions(1)), faces0, hr.at[3])

    halve = pick(iota((128, 128), 0) == 2 * iota((128, 128), 1))
    halve = halve + pick(iota((128, 128), 0) == 2 * iota((128, 128), 1) + 1)

    def coarsen0(planes):
        for i in range(hx):
            TT[i] = planes(2 * i) + planes(2 * i + 1)
        rows = [
            TT[i, pl.ds(0, hy, stride=2), :] + TT[i, pl.ds(1, hy, stride=2), :] for i in range(hx)
        ]
        return sel_dot(jnp.concatenate(rows, axis=0), halve)

    def coarsen1(planes, SG):
        for i in range(hx // 2):
            T2[pl.ds(8 * i, 8), :] = planes(2 * i) + planes(2 * i + 1)
        for y in range(4):
            A2[pl.ds(4 * y, 4), :] = (
                T2[pl.ds(2 * y, 4, stride=8), :] + T2[pl.ds(2 * y + 1, 4, stride=8), :]
            )
        TT[0] = sel_dot(A2[...], halve)
        total = TT[0, 0:4, :]
        for y in range(1, 4):
            total = total + pltpu.roll(TT[0, 4 * y : 4 * y + 4, :], 32 * y, 1)
        return total

    lane8 = iota((8, 128), 1)

    def pack1(S1, SZ, planes):
        out = jnp.zeros((8, 128), F32)
        for x in range(hx):
            q = planes[x]
            S1[x] = q
            s = 16 * x
            out = jnp.where((lane8 >= s) & (lane8 < s + 3), pltpu.roll(q, (s - 61) % 128, 1), out)
            out = jnp.where(
                (lane8 >= s + 3) & (lane8 < s + 6), pltpu.roll(q, (s + 3) % 128, 1), out
            )
        SZ[...] = out

    w1 = 0.0625 * coarsen0(lambda x: w_ref[x])
    w1 = [w1[8 * x : 8 * x + 8, :] for x in range(hx)]
    pack1(S1w, SZw, w1)
    SW[...] = 0.0625 * coarsen1(lambda x: w1[x], SW)
    GW[me] = SW[...]
    loads[2].wait()
    GM[me] = m_ref[...]
    send_all(directions(2), pieces1(S1w, W1, SZw, RZw), hr.at[1])
    send_all(lates, late1(S1w, R3w, SZw, RCw), hr.at[1])
    send_all(directions(3), matrix_rows, gr.at[1])
    pl.semaphore_wait(known.at[0], greeted)
    greet(known.at[1])

    def coords(rows, lanes, cy, cz, by, bz):
        r, l = iota((rows, lanes), 0), iota((rows, lanes), 1)
        y = jnp.where(r < cy + (rows - cy) // 2, r, r - rows)
        z = jnp.where(l < cz + (lanes - cz) // 2, l, l - lanes)
        gy, gz = y + iy * cy, z + iz * cz
        ok = (gy >= 0) & (gy < dims[1] * cy) & (gz >= 0) & (gz < dims[2] * cz)
        near = (y >= -by) & (y < cy + by) & (z >= -bz) & (z < cz + bz)
        return jnp.where(ok & near, 1, 0)

    def plane_mask(base, x, cx):
        if 0 <= x < cx:
            return base > 0
        gx = x + ix * cx
        inside = jnp.where((gx >= 0) & (gx < dims[0] * cx), 1, 0)
        return base * inside > 0

    take(first_part, hr.at[0])
    mask0 = coords(24, 256, ny, 128, 1, 1) > 0
    row8 = iota((8, 128), 0)
    lane24 = iota((24, 128), 1)

    def z_ends(dx):
        return jnp.where(lane24 % 4 >= 2, RZ0[dx + 1, 1], RZ0[dx + 1, 0])

    for dx in (-1, 0, 1):
        ends = z_ends(dx)
        for x in {-1: (nx - 1,), 0: range(nx), 1: (0,)}[dx]:
            V0[x + 2 + dx * nx, :, 128:256] = pltpu.roll(ends, (126 - 8 * x) % 128, 1)

    def assemble_faces():
        ends = z_ends(0)
        for x in range(nx):
            W0[x + 2, :, 128:256] = pltpu.roll(ends, (122 - 8 * x) % 128, 1)
            IW[x] = 1.0 / w_ref[x]

    def own_sum(ref, p):
        col, wide = ref[p, :, 0:128], ref[p, 0:ny, :]
        vert = pltpu.roll(col, 1, 0)[0:ny] + pltpu.roll(col, ny + 7, 0)[0:ny]
        flat_sum = pltpu.roll(wide, 1, 1)[:, 0:128] + pltpu.roll(wide, 255, 1)[:, 0:128]
        return (vert + flat_sum) + (ref[p - 1, 0:ny, 0:128] + ref[p + 1, 0:ny, 0:128])

    def exists(c):
        return (ix + c >= 0) & (ix + c < dims[0])

    for p, c in ((1, -1), (nx + 2, 1)):
        u = 1.2 * V0[p, 0:ny, 0:128] + K * own_sum(V0, p)
        U0[p, 0:ny, 0:128] = jnp.where(exists(c), u, 0.0)
    for p in range(2, nx + 2):
        c = V0[p]
        u = 1.2 * c + K * (around(c) + (V0[p - 1] + V0[p + 1]))
        U0[p] = jnp.where(mask0, u, 0.0)

    def resid0(x):
        p = x + 2
        return b_ref[x] - w_ref[x] * (6.0 * U0[p, 0:ny, 0:128] - own_sum(U0, p))

    b1 = 0.125 * coarsen0(resid0)
    b1 = [b1[8 * x : 8 * x + 8, :] for x in range(hx)]
    v1 = [jnp.where(lane8 < 64, K * b1[x] / jnp.where(lane8 < 64, w1[x], 1.0), 0.0) for x in range(hx)]
    pack1(S1v, SZv, v1)
    send_all(directions(2), pieces1(S1v, V1, SZv, RZv), hr.at[2])
    pl.semaphore_wait(known.at[1], greeted)
    for k in range(1, n):
        spread(0, SW, GW, k).start()

    mask1 = coords(16, 128, 8, 64, 2, 2)
    mask_up = coords(16, 128, 8, 64, 1, 1)
    mask_own = coords(16, 128, 8, 64, 0, 0)
    lane1 = iota((16, 128), 1)

    def assemble1(S1, RZ, D):
        for dx in (-1, 0, 1):
            ends = jnp.where(lane1 % 16 < 3, pltpu.roll(RZ[dx + 1, 0], 64, 1), RZ[dx + 1, 1])
            for x in {-1: (hx - 2, hx - 1), 0: range(hx), 1: (0, 1)}[dx]:
                p = x + 3 + dx * hx
                moved = pltpu.roll(ends, (61 - 16 * x) % 128, 1)
                inner = S1[x] if dx == 0 else D[p, 0:8, :]
                D[p, 0:8, :] = jnp.where(lane8 < 64, inner, moved[0:8])
                D[p, 8:16, :] = jnp.where(lane8 < 64, D[p, 8:16, :], moved[8:16])

    def finish1(R3, RC, D):
        for x in range(hx):
            D[x + 3, 8:16, :] = jnp.where((row8 == 2) | (row8 == 5), R3[x], D[x + 3, 8:16, :])
        for slot, p, x in ((0, 2, hx - 1), (1, hx + 3, 0)):
            ends = jnp.where(lane8 % 16 < 3, pltpu.roll(RC[slot, 0], 64, 1), RC[slot, 1])
            moved = pltpu.roll(ends, (61 - 16 * x) % 128, 1)
            D[p, 8:16, :] = jnp.where(lane8 < 64, D[p, 8:16, :], moved)

    def smooth1(planes):
        for p in planes:
            c = V1[p]
            u = 1.2 * c + K * (around(c) + (V1[p - 1] + V1[p + 1]))
            U1[p] = jnp.where(plane_mask(mask1, p - 3, hx), u, 0.0)

    block = lane8 // 32
    quarter = row8 % 4

    def unpack(G):
        planes = []
        for X in range(4 * dims[0]):
            tiles = []
            for t in range(dims[1] // 2):
                rows = []
                for z in range(dims[2]):
                    d0 = ((X // 4) * dims[1] + 2 * t) * dims[2] + z
                    d1 = d0 + dims[2]
                    q = X % 4
                    rows.append(
                        jnp.where(
                            row8 < 4,
                            jnp.broadcast_to(G[d0, q : q + 1, :], (8, 128)),
                            jnp.broadcast_to(G[d1, q : q + 1, :], (8, 128)),
                        )
                    )
                out = None
                for s in range(4):
                    pre = rows[s % 4]
                    for j in range(1, 4):
                        pre = jnp.where(block == j, rows[(j + s) % 4], pre)
                    moved = pltpu.roll(pre, 32 * s, 1) if s else pre
                    out = moved if out is None else jnp.where(block == (quarter + s) % 4, moved, out)
                tiles.append(out)
            planes.append(jnp.concatenate(tiles, axis=0))
        return planes

    def coarsen2(planes):
        c = len(planes) // 2
        for i in range(c):
            T3[i] = planes[2 * i] + planes[2 * i + 1]
        rows = [T3[i, pl.ds(0, 8, stride=2), :] + T3[i, pl.ds(1, 8, stride=2), :] for i in range(c)]
        out = sel_dot(jnp.concatenate(rows, axis=0), halve)
        return [out[8 * i : 8 * i + 8, :] for i in range(c)]


    take(second_part, hr.at[2])
    assemble1(S1v, RZv, V1)
    smooth1(range(2, hx + 4))

    def resid1(x):
        p = x + 3
        s = around(U1[p])[0:8, :] + (U1[p - 1, 0:8, :] + U1[p + 1, 0:8, :])
        return jnp.where(lane8 < 64, b1[x] - w1[x] * (6.0 * U1[p, 0:8, :] - s), 0.0)

    SB[...] = 0.125 * coarsen1(resid1, SB)
    GB[me] = SB[...]
    for k in range(1, n):
        spread(2, SB, GB, k).start()
    send_all(lates, late1(S1v, R3v, SZv, RCv), hr.at[1])
    arrive(0, GW)
    w2 = unpack(GW)
    w3 = [0.0625 * q for q in coarsen2(w2)]
    valid3 = lane8 < 64
    w3s = [jnp.where(valid3, q, 1.0) for q in w3]
    take(matrix_part, gr.at[1])
    take(face_part, hr.at[3])
    assemble_faces()
    take(late_part, hr.at[1])
    assemble1(S1w, RZw, W1)
    finish1(R3w, RCw, W1)
    finish1(R3v, RCv, V1)
    smooth1(range(1, hx + 5))
    cells = GM.shape[0] * GM.shape[1]
    at, lane = iota((cells, 128), 0), iota((cells, 128), 1)
    gap_y = at // (8 * dims[2]) % dims[1] - iy
    gap_z = at % (8 * dims[2]) - 8 * iz
    known_rows = (gap_y >= -1) & (gap_y <= 1) & (gap_z >= -1) & (gap_z <= 8)
    hit = (at % 32 == lane // 2) & known_rows
    arrive(2, GB)

    b2 = unpack(GB)
    v2 = [K * b / w for b, w in zip(b2, w2)]
    u2 = [1.2 * v + K * s for v, s in zip(v2, whole_sum(v2, 128))]
    r2 = [b - w * (6.0 * u - s) for b, w, u, s in zip(b2, w2, u2, whole_sum(u2, 128))]
    b3 = [0.125 * q for q in coarsen2(r2)]
    v3 = [K * b / w for b, w in zip(b3, w3s)]
    u3 = [jnp.where(valid3, 1.2 * v + K * s, 0.0) for v, s in zip(v3, whole_sum(v3, 64))]
    r3 = [b - w * (6.0 * u - s) for b, w, u, s in zip(b3, w3, u3, whole_sum(u3, 64))]
    c4 = len(r3) // 2
    for i in range(c4):
        T4[pl.ds(8 * i, 8), :] = r3[2 * i] + r3[2 * i + 1]
    half = 4 * c4
    b4 = 0.125 * sel_dot(T4[pl.ds(0, half, stride=2), :] + T4[pl.ds(1, half, stride=2), :], halve)
    acc = b4
    for j in range(1, 4):
        acc = jnp.where(quarter == j, pltpu.roll(b4, 32 * j, 1), acc)
    low = jnp.sum(jnp.where(row8 < 4, acc, 0.0), axis=0, keepdims=True)
    high = jnp.sum(jnp.where(row8 >= 4, acc, 0.0), axis=0, keepdims=True)
    matrix = GM[...].reshape((cells, 256))
    solved = jnp.sum(matrix[:, 0:128] * low + matrix[:, 128:256] * high, axis=1, keepdims=True)
    e4 = jnp.sum(jnp.where(hit, solved, 0.0).reshape((cells // 32, 32, 128)), axis=1)
    P4[pl.ds(0, half, stride=2), :] = e4
    P4[pl.ds(1, half, stride=2), :] = e4

    y3 = [u + w * P4[8 * (i // 2) : 8 * (i // 2) + 8, :] for i, (u, w) in enumerate(zip(u3, w3))]
    e3 = [
        jnp.where(valid3, (0.2 * y + v + K * s) / w, 0.0)
        for y, v, s, w in zip(y3, v3, whole_sum(y3, 64), w3s)
    ]
    double = pick(iota((128, 256), 0) == iota((128, 256), 1) // 2)
    wide3 = sel_dot(jnp.concatenate(e3, axis=0), double[:, 0:128])
    for i in range(len(e3)):
        P3[i, pl.ds(0, 8, stride=2), :] = wide3[8 * i : 8 * i + 8, :]
        P3[i, pl.ds(1, 8, stride=2), :] = wide3[8 * i : 8 * i + 8, :]
    y2 = [u + w * P3[i // 2] for i, (u, w) in enumerate(zip(u2, w2))]
    s2 = whole_sum(y2, 128)
    E2[...] = jnp.zeros_like(E2)
    for i in range(len(y2)):
        E2[i + 1, 8:24, :] = (0.2 * y2[i] + v2[i] + K * s2[i]) / w2[i]

    seen = jnp.concatenate([E2[4 * ix + i, pl.ds(6 + 4 * iy, 8), :] for i in range(6)], axis=0)
    j = iota((128, 128), 1)
    zl = jnp.where(j < 96, j // 2, j // 2 - 64) + 32 * iz
    wide2 = sel_dot(seen, pick(iota((128, 128), 0) == zl))
    for i in range(6):
        P2[i, pl.ds(0, 8, stride=2), :] = wide2[8 * i : 8 * i + 8, :]
        P2[i, pl.ds(1, 8, stride=2), :] = wide2[8 * i : 8 * i + 8, :]
    for p in range(1, hx + 5):
        U1[p] = U1[p] + W1[p] * pltpu.roll(P2[(p - 3) // 2 + 1], 12, 0)
    e1 = []
    for p in range(2, hx + 4):
        c = U1[p]
        f = 0.2 * c + V1[p] + K * (around(c) + (U1[p - 1] + U1[p + 1]))
        inside = plane_mask(mask_up if 0 <= p - 3 < hx else mask_own, p - 3, hx)
        e1.append(jnp.where(inside, f, 0.0) / jnp.where(inside, W1[p], 1.0))
    wide1 = sel_dot(jnp.concatenate(e1, axis=0), double)
    for i in range(hx + 2):
        for t in range(2):
            q = wide1[16 * i : 16 * i + 16, 128 * t : 128 * t + 128]
            P1[t, i, pl.ds(0, 16, stride=2), :] = q
            P1[t, i, pl.ds(1, 16, stride=2), :] = q

    for p in range(1, nx + 3):
        i = (p - 2) // 2 + 1
        if not 2 <= p < nx + 2:
            U0[p, 0:ny, 0:128] = U0[p, 0:ny, 0:128] + W0[p, 0:ny, 0:128] * P1[0, i, 0:16, :]
            continue
        parts = []
        for t in range(2):
            edge = jnp.where(row8 < 4, P1[t, i, 16:24, :], P1[t, i, 24:32, :])
            parts.append(jnp.concatenate([P1[t, i, 0:16, :], edge], axis=0))
        U0[p] = U0[p] + W0[p] * jnp.concatenate(parts, axis=1)
    for x in range(nx):
        p = x + 2
        f = 0.2 * U0[p, 0:ny, 0:128] + V0[p, 0:ny, 0:128] + K * own_sum(U0, p)
        f_ref[x] = f * IW[x]

    take(everything, sent.at[0])


def fused(dims, sources, stiffness, coarse_inverse):
    nx, ny, nz = stiffness.shape
    n = dims[0] * dims[1] * dims[2]
    vm = lambda *s: pltpu.VMEM(s, F32)
    halo1 = [vm(8, 8, 128), vm(8, 128), vm(3, 2, 16, 128), vm(8, 8, 128), vm(2, 2, 8, 128)]
    result = pl.pallas_call(
        functools.partial(kernel, dims),
        out_shape=pltpu.VMEM((nx, ny, nz), F32),
        in_specs=[pl.BlockSpec(memory_space=pl.ANY)] * 3,
        out_specs=pl.BlockSpec(memory_space=pltpu.VMEM),
        scratch_shapes=[
            vm(nx, ny, nz), vm(nx, ny, nz), vm(*coarse_inverse.shape),
            vm(nx + 4, 24, 256), vm(nx + 4, 24, 256), vm(nx + 4, 24, 256),
            vm(14, 16, 128), vm(14, 16, 128), vm(14, 16, 128),
            vm(8, 16, 128), vm(32, 128), vm(16, 128), vm(2 * dims[0], 16, 128),
            vm(16, 128), vm(16, 128), vm(2 * dims[0], 16, 128),
            vm(4 * dims[0] + 2, 32, 128), vm(6, 16, 128), vm(2, 10, 32, 128), vm(nx, ny, nz),
            vm(ny, 128), vm(3, 2, ny + 8, 128),
        ]
        + halo1 + halo1
        + [
            vm(n, 8, 256), vm(n, 4, 128), vm(n, 4, 128), vm(4, 128), vm(4, 128),
            vm(2048, 128),
            pltpu.SemaphoreType.DMA((3,)), pltpu.SemaphoreType.DMA((1,)),
            pltpu.SemaphoreType.DMA((4,)), pltpu.SemaphoreType.DMA((3,)),
            pltpu.SemaphoreType.REGULAR((2,)),
        ],
        compiler_params=pltpu.CompilerParams(collective_id=0, has_side_effects=True),
        name="cycle",
    )(sources[0], stiffness, coarse_inverse)
    return result[None]


def solution(mesh):
    dims = tuple(mesh.shape[a] for a in ("gx", "gy", "gz"))

    def run(sources, stiffness, coarse_inverse):
        nx, ny, nz = stiffness.shape
        lanes = 128
        cells = coarse_inverse.shape[1]
        levels_fit = (
            sources.shape[0] == 1
            and nx == ny == 16
            and nz == lanes
            and dims[2] * nz == 4 * lanes
            and dims[1] * ny == 64
            and cells == 2 * lanes
            and dims[0] == 2
        )
        if levels_fit:
            return fused(dims, sources, stiffness, coarse_inverse)
        return per_device(sources, stiffness, coarse_inverse)

    in_specs = (P(None, "gx", "gy", "gz"), P("gx", "gy", "gz"), P(("gx", "gy", "gz"), None))
    out_specs = P(None, "gx", "gy", "gz")
    return jax.shard_map(
        run, mesh=mesh, in_specs=in_specs, out_specs=out_specs, check_vma=False
    )
```

```python
import functools
import jax
import jax.numpy as jnp
from jax import lax
from jax.experimental import pallas as pl
from jax.experimental.pallas import tpu as pltpu
from jax.sharding import PartitionSpec as P

damping = 0.8


def extended(cells, sides, width):
    for axis, dim in sides:
        count = lax.axis_size(axis)
        ends = count - 1
        head = lax.slice_in_dim(cells, 0, width, axis=dim)
        tail = lax.slice_in_dim(cells, cells.shape[dim] - width, cells.shape[dim], axis=dim)
        cells = jnp.concatenate(
            [
                lax.ppermute(tail, axis, [(i, (i + 1) % count) for i in range(ends)]),
                cells,
                lax.ppermute(head, axis, [((i + 1) % count, i) for i in range(ends)]),
            ],
            axis=dim,
        )
    return cells


def loop_sum(padded):
    total = padded[:, 2:, 1:-1, 1:-1] + padded[:, :-2, 1:-1, 1:-1]
    total = total + padded[:, 1:-1, 2:, 1:-1] + padded[:, 1:-1, :-2, 1:-1]
    total = total + padded[:, 1:-1, 1:-1, 2:] + padded[:, 1:-1, 1:-1, :-2]
    return total


def inner_part(values):
    return values[:, 1:-1, 1:-1, 1:-1]


def pre_smooth(source, weights):
    count = source.shape[0]
    stacked = jnp.concatenate([source, weights], axis=0)
    wide = extended(stacked, (("gx", 1), ("gy", 2), ("gz", 3)), 2)
    wide_source = wide[:count]
    wide_weights = wide[count:]
    safe_weights = jnp.where(wide_weights > 0.0, wide_weights, 1.0)
    first = damping * wide_source / (6.0 * safe_weights * safe_weights)
    first_scaled = wide_weights * first
    mid_weights = inner_part(wide_weights)
    mid_safe = inner_part(safe_weights)
    applied = mid_weights * (6.0 * inner_part(first_scaled) - loop_sum(first_scaled))
    second = inner_part(first) + damping * (inner_part(wide_source) - applied) / (
        6.0 * mid_safe * mid_safe
    )
    second_scaled = mid_weights * second
    answer = inner_part(second)
    resid = source - weights * (6.0 * inner_part(second_scaled) - loop_sum(second_scaled))
    return (answer, resid)


def post_smooth(answer, source, weights):
    scaled = weights * answer
    wide = extended(scaled, (("gx", 1), ("gy", 2), ("gz", 3)), 1)
    applied = weights * (6.0 * scaled - loop_sum(wide))
    return answer + damping * (source - applied) / (6.0 * weights * weights)


def coarsen(values):
    leading = values.shape[0]
    size_x, size_y, size_z = (values.shape[1], values.shape[2], values.shape[3])
    blocks = values.reshape((leading, size_x // 2, 2, size_y // 2, 2, size_z // 2, 2))
    return jnp.mean(blocks, axis=(2, 4, 6))


def refine(values):
    return jnp.repeat(jnp.repeat(jnp.repeat(values, 2, axis=1), 2, axis=2), 2, axis=3)


def per_device(sources, stiffness, coarse_inverse):
    weight_list = [stiffness[None]]
    for level in range(3):
        weight_list.append(0.5 * coarsen(weight_list[-1]))
    source_list = []
    answer_list = []
    current = sources
    for level in range(4):
        source_list.append(current)
        answer, resid = pre_smooth(current, weight_list[level])
        answer_list.append(answer)
        current = coarsen(resid)
    count = current.shape[0]
    flat_source = current.reshape((count, -1))
    solved = lax.dot_general(
        lax.all_gather(flat_source, ("gx", "gy", "gz"), axis=1, tiled=True),
        coarse_inverse,
        (((1,), (1,)), ((), ())),
        precision=lax.Precision.HIGHEST,
        preferred_element_type=jnp.float32,
    )
    correction = solved.reshape(current.shape)
    for level in range(3, -1, -1):
        correction = post_smooth(
            answer_list[level] + refine(correction), source_list[level], weight_list[level]
        )
    return correction


K = damping / 6.0
F32 = jnp.float32
BF = jnp.bfloat16


def iota(shape, dim):
    return lax.broadcasted_iota(jnp.int32, shape, dim)


def pick(condition):
    return jnp.where(condition, 1.0, 0.0).astype(BF)


def sel_dot(values, chosen):
    high = values.astype(BF)
    low = (values - high.astype(F32)).astype(BF)
    both = jnp.concatenate([high, low], axis=1)
    return jnp.dot(both, jnp.concatenate([chosen] * 2, axis=0), preferred_element_type=F32)


def exact_dot(values, chosen):
    total = None
    for _ in range(3):
        part = values.astype(BF)
        values = values - part.astype(F32)
        term = jnp.dot(part, chosen, preferred_element_type=F32)
        total = term if total is None else total + term
    return total


def around(c):
    rows, lanes = c.shape
    return (pltpu.roll(c, 1, 0) + pltpu.roll(c, rows - 1, 0)) + (
        pltpu.roll(c, 1, 1) + pltpu.roll(c, lanes - 1, 1)
    )


def whole_sum(planes, step):
    rows, lanes = planes[0].shape
    row, lane = iota((rows, lanes), 0), iota((rows, lanes), 1)
    outs = []
    for p, c in enumerate(planes):
        s = jnp.where(row > 0, pltpu.roll(c, 1, 0), 0.0) + jnp.where(
            row < rows - 1, pltpu.roll(c, rows - 1, 0), 0.0
        )
        s = s + (
            jnp.where(lane >= step, pltpu.roll(c, step, 1), 0.0)
            + jnp.where(lane < lanes - step, pltpu.roll(c, lanes - step, 1), 0.0)
        )
        if p > 0:
            s = s + planes[p - 1]
        if p < len(planes) - 1:
            s = s + planes[p + 1]
        outs.append(s)
    return outs


def pair_sum(c, step):
    lanes = c.shape[1]
    even = (iota(c.shape, 1) // step) % 2 == 0
    return c + jnp.where(even, pltpu.roll(c, lanes - step, 1), pltpu.roll(c, step, 1))


def row_sum(c):
    for step in (4, 2, 1):
        c = c + pltpu.roll(c, step, 0)
    return c


def kernel(
    dims, b_hbm, w_hbm, m_hbm, f_ref,
    b_ref, w_ref, m_ref,
    V0, W0, U0, V1, W1, U1, TT, T2, A2, T3, T4, P3, E2, P2, P1, IW, IW1, MP,
    SZ0, RZ0, S1v, SZv, RZv, R3v, RCv, S1w, SZw, RZw, R3w, RCw,
    GM, GW, GB, SW, SB,
    tally, load, sent, hr, gr, known,
):
    axes = ("gx", "gy", "gz")
    ix, iy, iz = (lax.axis_index(a) for a in axes)
    n = dims[0] * dims[1] * dims[2]
    me = (ix * dims[1] + iy) * dims[2] + iz

    def flip(i, bits):
        if bits == 1:
            return i + 1 - 2 * (i % 2)
        return {0: i, 2: (i + 2) % 4, 3: 3 - i}[bits]

    def mirrored(k):
        a, b, c = k
        y, z = dims[1] - 1 - iy, dims[2] - 1 - iz
        return ((ix + a) % dims[0], flip(y, b), flip(z, c))

    ends = (dims[1] - 1, dims[2] - 1)
    others = sorted(
        (c + (b + 1) // 2, a, b, c)
        for a in range(dims[0])
        for b in range(dims[1])
        for c in range(dims[2])
        if (a, b, c) != (0,) + ends
    )
    others = [k[1:] for k in others]

    barrier = pltpu.get_barrier_semaphore()

    def there(d):
        ok = None
        for i, s, c in zip((ix, iy, iz), dims, d):
            if c:
                t = (i + c < s) if c > 0 else (i + c >= 0)
                ok = t if ok is None else jnp.logical_and(ok, t)
        return ok

    def directions(most):
        found = []
        for dx in (-1, 0, 1):
            for dy in (-1, 0, 1):
                for dz in (-1, 0, 1):
                    if 0 < abs(dx) + abs(dy) + abs(dz) <= most:
                        found.append((dx, dy, dz))
        return sorted(found, key=lambda d: (-abs(d[1]), -abs(d[2]), abs(d[0])))

    def greet(sem):
        for d in directions(3):
            @pl.when(there(d))
            def _(d=d):
                pl.semaphore_signal(
                    sem, inc=1, device_id=(ix + d[0], iy + d[1], iz + d[2]),
                    device_id_type=pl.DeviceIdType.MESH,
                )

    loads = [
        pltpu.make_async_copy(src, dst, load.at[i])
        for i, (src, dst) in enumerate(((b_hbm, b_ref), (w_hbm, w_ref), (m_hbm, m_ref)))
    ]
    for copy in loads:
        copy.start()
    nx, ny = b_ref.shape[0], b_ref.shape[1]
    hx, hy = nx // 2, ny // 2

    def clear(ref, *where):
        part = ref.at[where] if where else ref
        part[...] = jnp.zeros(part.shape, F32)

    own = (pl.ds(0, ny), pl.ds(0, 128))
    clear(V0, pl.ds(0, 2), *own)
    clear(V0, pl.ds(nx + 2, 2), *own)
    clear(V0, pl.ds(1, nx + 2), pl.ds(ny, 8), pl.ds(0, 128))
    clear(W0, pl.ds(1, 1), *own)
    clear(W0, pl.ds(nx + 2, 1), *own)
    clear(W0, pl.ds(2, nx), pl.ds(ny, 8), pl.ds(0, 128))
    for D in (V1, W1):
        clear(D, pl.ds(0, 3))
        clear(D, pl.ds(hx + 3, 3))
        clear(D, pl.ds(3, hx), pl.ds(8, 8))
    for D in (RZ0, RZv, R3v, RCv, RZw, R3w, RCw):
        clear(D)
    greet(barrier)

    def span(i, s):
        return 1 + jnp.where(i > 0, 1, 0) + jnp.where(i < s - 1, 1, 0)

    greeted = span(ix, dims[0]) * span(iy, dims[1]) * span(iz, dims[2]) - 1

    def send(src, dst, d, sem):
        pltpu.make_async_remote_copy(
            src_ref=src, dst_ref=dst, send_sem=sent.at[0], recv_sem=sem,
            device_id=(ix + d[0], iy + d[1], iz + d[2]), device_id_type=pl.DeviceIdType.MESH,
        ).start()

    def send_all(found, pieces, sem):
        for d in found:
            @pl.when(there(d))
            def _(d=d):
                send(*pieces(d), d, sem)

    def span_x(c, size, pad, deep):
        if c == 0:
            return pl.ds(0, size), pl.ds(pad, size)
        if c > 0:
            return pl.ds(size - deep, deep), pl.ds(pad - deep, deep)
        return pl.ds(0, deep), pl.ds(pad + size, deep)

    def span_y(c, size, total, deep):
        if c == 0:
            return pl.ds(0, size), pl.ds(0, size)
        if c > 0:
            return pl.ds(size - deep, deep), pl.ds(total - deep, deep)
        return pl.ds(0, deep), pl.ds(size, deep)

    def flat(found):
        return [d for d in found if not d[2]]

    first = pl.ds(0, 128)

    def pieces0(d):
        dx, dy, dz = d
        if dz:
            a, b = span_y(dy, ny, ny + 8, 1)
            return SZ0.at[a], RZ0.at[1 - dx, (1 - dz) // 2, b]
        deep = 1 if dx and dy else 2
        a, b = span_x(dx, nx, 2, deep)
        e, f = span_y(dy, ny, ny + 8, deep)
        shifted = pl.ds(a.start + 2, a.size)
        return V0.at[shifted, e, first], V0.at[b, f, first]

    def faces0(d):
        a, b = span_x(d[0], nx, 2, 1)
        e, f = span_y(d[1], ny, ny + 8, 1)
        return W0.at[pl.ds(a.start + 2, a.size), e, first], W0.at[b, f, first]

    def pieces1(S1, D, SZ, RZ):
        def of(d):
            dx, dy, dz = d
            if dz:
                a, b = span_y(dy, 8, 16, 2)
                return SZ.at[a], RZ.at[1 - dx, (1 - dz) // 2, b]
            a, b = span_x(dx, hx, 3, 2 if dy else 3)
            e, f = span_y(dy, 8, 16, 2)
            return S1.at[a, e], D.at[b, f]
        return of

    def late1(S1, R3, SZ, RC):
        def of(d):
            dx, dy, dz = d
            if dz:
                row = pl.ds(7 if dy > 0 else 0, 1)
                return SZ.at[row], RC.at[(1 - dx) // 2, (1 - dz) // 2, row]
            row = pl.ds(5 if dy > 0 else 2, 1)
            return S1.at[:, row], R3.at[:, row]
        return of

    def matrix_rows(d):
        s, r = m_ref, GM.at[me]
        if d[2]:
            row = pl.ds(m_ref.shape[0] - 1 if d[2] > 0 else 0, 1)
            s, r = s.at[row], r.at[row]
        return s, r

    corners = [d for d in directions(3) if all(d)]
    lates = [(0, -1, 0), (0, 1, 0)] + corners

    def bytes_of(ref, sem):
        pltpu.make_async_copy(ref, ref, sem).wait()

    sides_y, sides_z = span(iy, dims[1]) - 1, span(iz, dims[2]) - 1

    def first_part(cy, cz):
        return 32 + 33 * cy + 32 * cz + cy * cz

    def face_part(cy, cz):
        return 16 + 16 * cy

    def second_part(cy, cz):
        return 24 + 20 * cy + 16 * cz + 2 * cy * cz

    def late_part(cy, cz):
        return second_part(cy, cz) + 2 * (8 * cy + cy * cz)

    def matrix_part(cy, cz):
        return 16 + 32 * cy + 4 * (1 + cy) * cz

    def everything(cy, cz):
        parts = (first_part, face_part, second_part, late_part, matrix_part)
        return sum(part(cy, cz) for part in parts) + 8 * (n - 1)

    def take(part, sem):
        for cy in (1, 2):
            for cz in (1, 2):
                @pl.when(jnp.logical_and(sides_y == cy, sides_z == cz))
                def _(cy=cy, cz=cz):
                    bytes_of(tally.at[pl.ds(0, part(cy, cz))], sem)

    def spread(kind, src, dst, k):
        return pltpu.make_async_remote_copy(
            src_ref=src, dst_ref=dst.at[me], send_sem=sent.at[0], recv_sem=gr.at[kind],
            device_id=mirrored(k), device_id_type=pl.DeviceIdType.MESH,
        )

    def arrive(kind, dst):
        bytes_of(dst.at[pl.ds(0, n - 1)], gr.at[kind])


    for copy in loads[:2]:
        copy.wait()
    lane16 = iota((ny, 128), 1)
    packed = jnp.zeros((ny, 128), F32)
    for x in range(nx):
        w = w_ref[x]
        v = K * b_ref[x] / w
        V0[x + 2, 0:ny, 0:128] = v
        W0[x + 2, 0:ny, 0:128] = w
        for a, q in enumerate((v, w)):
            start = 8 * x + 4 * a
            moved = pltpu.roll(q, (start + 2) % 128, 1)
            packed = jnp.where((lane16 >= start) & (lane16 < start + 4), moved, packed)
    SZ0[...] = packed

    pl.semaphore_wait(barrier, greeted)
    send_all(directions(2), pieces0, hr.at[0])
    greet(known.at[0])
    send_all(flat(directions(1)), faces0, hr.at[3])

    halve = pick(iota((128, 128), 0) == 2 * iota((128, 128), 1))
    halve = halve + pick(iota((128, 128), 0) == 2 * iota((128, 128), 1) + 1)

    def coarsen0(planes):
        for i in range(hx):
            TT[i] = planes(2 * i) + planes(2 * i + 1)
        rows = [
            TT[i, pl.ds(0, hy, stride=2), :] + TT[i, pl.ds(1, hy, stride=2), :] for i in range(hx)
        ]
        return sel_dot(jnp.concatenate(rows, axis=0), halve)

    def coarsen1(planes, SG):
        for i in range(hx // 2):
            T2[pl.ds(8 * i, 8), :] = planes(2 * i) + planes(2 * i + 1)
        for x in range(4):
            A2[pl.ds(4 * x, 4), :] = (
                T2[pl.ds(8 * x, 4, stride=2), :] + T2[pl.ds(8 * x + 1, 4, stride=2), :]
            )
        TT[0] = sel_dot(A2[...], halve)
        total = TT[0, 0:4, :]
        for x in range(1, 4):
            total = total + pltpu.roll(TT[0, 4 * x : 4 * x + 4, :], 32 * x, 1)
        return total

    lane8 = iota((8, 128), 1)

    def pack1(S1, SZ, planes):
        out = jnp.zeros((8, 128), F32)
        for x in range(hx):
            q = planes[x]
            S1[x] = q
            s = 16 * x
            out = jnp.where((lane8 >= s) & (lane8 < s + 3), pltpu.roll(q, (s - 61) % 128, 1), out)
            out = jnp.where(
                (lane8 >= s + 3) & (lane8 < s + 6), pltpu.roll(q, (s + 3) % 128, 1), out
            )
        SZ[...] = out

    w1 = 0.0625 * coarsen0(lambda x: w_ref[x])
    w1 = [w1[8 * x : 8 * x + 8, :] for x in range(hx)]
    pack1(S1w, SZw, w1)
    SW[...] = 0.0625 * coarsen1(lambda x: w1[x], SW)
    GW[me] = SW[...]
    loads[2].wait()
    GM[me] = m_ref[...]
    send_all(directions(2), pieces1(S1w, W1, SZw, RZw), hr.at[1])
    send_all(lates, late1(S1w, R3w, SZw, RCw), hr.at[1])
    send_all(directions(3), matrix_rows, gr.at[1])
    pl.semaphore_wait(known.at[0], greeted)
    greet(known.at[1])

    def coords(rows, lanes, cy, cz, by, bz):
        r, l = iota((rows, lanes), 0), iota((rows, lanes), 1)
        y = jnp.where(r < cy + (rows - cy) // 2, r, r - rows)
        z = jnp.where(l < cz + (lanes - cz) // 2, l, l - lanes)
        gy, gz = y + iy * cy, z + iz * cz
        ok = (gy >= 0) & (gy < dims[1] * cy) & (gz >= 0) & (gz < dims[2] * cz)
        near = (y >= -by) & (y < cy + by) & (z >= -bz) & (z < cz + bz)
        return jnp.where(ok & near, 1, 0)

    def plane_mask(base, x, cx):
        if 0 <= x < cx:
            return base > 0
        gx = x + ix * cx
        inside = jnp.where((gx >= 0) & (gx < dims[0] * cx), 1, 0)
        return base * inside > 0

    take(first_part, hr.at[0])
    mask0 = coords(24, 256, ny, 128, 1, 1) > 0
    row8 = iota((8, 128), 0)
    lane24 = iota((24, 128), 1)

    def z_ends(dx):
        return jnp.where(lane24 % 4 >= 2, RZ0[dx + 1, 1], RZ0[dx + 1, 0])

    for dx in (-1, 0, 1):
        ends = z_ends(dx)
        for x in {-1: (nx - 1,), 0: range(nx), 1: (0,)}[dx]:
            V0[x + 2 + dx * nx, :, 128:256] = pltpu.roll(ends, (126 - 8 * x) % 128, 1)

    def assemble_faces():
        ends = z_ends(0)
        for x in range(nx):
            W0[x + 2, :, 128:256] = pltpu.roll(ends, (122 - 8 * x) % 128, 1)
            IW[x] = 1.0 / w_ref[x]

    def own_sum(ref, p):
        col, wide = ref[p, :, 0:128], ref[p, 0:ny, :]
        vert = pltpu.roll(col, 1, 0)[0:ny] + pltpu.roll(col, ny + 7, 0)[0:ny]
        flat_sum = pltpu.roll(wide, 1, 1)[:, 0:128] + pltpu.roll(wide, 255, 1)[:, 0:128]
        return (vert + flat_sum) + (ref[p - 1, 0:ny, 0:128] + ref[p + 1, 0:ny, 0:128])

    def exists(c):
        return (ix + c >= 0) & (ix + c < dims[0])

    for p, c in ((1, -1), (nx + 2, 1)):
        u = 1.2 * V0[p, 0:ny, 0:128] + K * own_sum(V0, p)
        U0[p, 0:ny, 0:128] = jnp.where(exists(c), u, 0.0)
    for p in range(2, nx + 2):
        c = V0[p]
        u = 1.2 * c + K * (around(c) + (V0[p - 1] + V0[p + 1]))
        U0[p] = jnp.where(mask0, u, 0.0)

    def resid0(x):
        p = x + 2
        return b_ref[x] - w_ref[x] * (6.0 * U0[p, 0:ny, 0:128] - own_sum(U0, p))

    b1 = 0.125 * coarsen0(resid0)
    b1 = [b1[8 * x : 8 * x + 8, :] for x in range(hx)]
    v1 = [jnp.where(lane8 < 64, K * b1[x] / jnp.where(lane8 < 64, w1[x], 1.0), 0.0) for x in range(hx)]
    pack1(S1v, SZv, v1)
    send_all(directions(2), pieces1(S1v, V1, SZv, RZv), hr.at[2])
    pl.semaphore_wait(known.at[1], greeted)
    for k in others:
        spread(0, SW, GW, k).start()

    mask1 = coords(16, 128, 8, 64, 2, 2)
    mask_up = coords(16, 128, 8, 64, 1, 1)
    mask_own = coords(16, 128, 8, 64, 0, 0)
    lane1 = iota((16, 128), 1)

    def assemble1(S1, RZ, D):
        for dx in (-1, 0, 1):
            ends = jnp.where(lane1 % 16 < 3, pltpu.roll(RZ[dx + 1, 0], 64, 1), RZ[dx + 1, 1])
            for x in {-1: (hx - 2, hx - 1), 0: range(hx), 1: (0, 1)}[dx]:
                p = x + 3 + dx * hx
                moved = pltpu.roll(ends, (61 - 16 * x) % 128, 1)
                inner = S1[x] if dx == 0 else D[p, 0:8, :]
                D[p, 0:8, :] = jnp.where(lane8 < 64, inner, moved[0:8])
                D[p, 8:16, :] = jnp.where(lane8 < 64, D[p, 8:16, :], moved[8:16])

    def finish1(R3, RC, D):
        for x in range(hx):
            D[x + 3, 8:16, :] = jnp.where((row8 == 2) | (row8 == 5), R3[x], D[x + 3, 8:16, :])
        for slot, p, x in ((0, 2, hx - 1), (1, hx + 3, 0)):
            ends = jnp.where(lane8 % 16 < 3, pltpu.roll(RC[slot, 0], 64, 1), RC[slot, 1])
            moved = pltpu.roll(ends, (61 - 16 * x) % 128, 1)
            D[p, 8:16, :] = jnp.where(lane8 < 64, D[p, 8:16, :], moved)

    def smooth1(planes):
        for p in planes:
            c = V1[p]
            u = 1.2 * c + K * (around(c) + (V1[p - 1] + V1[p + 1]))
            U1[p] = jnp.where(plane_mask(mask1, p - 3, hx), u, 0.0)

    block = lane8 // 32

    def unpack(G):
        planes = []
        for X in range(4 * dims[0]):
            gx, x = X // 4, X % 4
            tiles = []
            for t in range(dims[1] // 2):
                out = None
                for z in range(dims[2]):
                    d0 = (gx * dims[1] + 2 * t) * dims[2] + z
                    tile = jnp.concatenate([G[d0], G[d0 + dims[2]]], axis=0)
                    shift = 32 * ((z - x) % 4)
                    moved = pltpu.roll(tile, shift, 1) if shift else tile
                    out = moved if out is None else jnp.where(block == z, moved, out)
                tiles.append(out)
            planes.append(jnp.concatenate(tiles, axis=0))
        return planes

    def coarsen2(planes):
        c = len(planes) // 2
        for i in range(c):
            T3[i] = planes[2 * i] + planes[2 * i + 1]
        return [
            pair_sum(T3[i, pl.ds(0, 8, stride=2), :] + T3[i, pl.ds(1, 8, stride=2), :], 1)
            for i in range(c)
        ]

    take(second_part, hr.at[2])
    assemble1(S1v, RZv, V1)
    smooth1(range(2, hx + 4))

    def resid1(x):
        p = x + 3
        s = around(U1[p])[0:8, :] + (U1[p - 1, 0:8, :] + U1[p + 1, 0:8, :])
        return jnp.where(lane8 < 64, b1[x] - w1[x] * (6.0 * U1[p, 0:8, :] - s), 0.0)

    SB[...] = 0.125 * coarsen1(resid1, SB)
    GB[me] = SB[...]
    for k in others:
        spread(2, SB, GB, k).start()
    send_all(lates, late1(S1v, R3v, SZv, RCv), hr.at[1])
    arrive(0, GW)
    w2 = unpack(GW)
    w3 = [0.0625 * q for q in coarsen2(w2)]
    iw2 = [1.0 / q for q in w2]
    iw3 = [1.0 / q for q in w3]
    take(matrix_part, gr.at[1])
    take(face_part, hr.at[3])
    assemble_faces()
    take(late_part, hr.at[1])
    assemble1(S1w, RZw, W1)
    finish1(R3w, RCw, W1)
    finish1(R3v, RCv, V1)
    smooth1(range(1, hx + 5))
    for p in range(2, hx + 4):
        inside = plane_mask(mask_up if 0 <= p - 3 < hx else mask_own, p - 3, hx)
        IW1[p] = jnp.where(inside, 1.0, 0.0) / jnp.where(inside, W1[p], 1.0)

    def near(i, c, size):
        return jnp.clip(i + c, 0, size - 1)

    steps = (-1, 0, 1)
    blocks = [(x, dy, dz) for x in range(dims[0]) for dy in steps for dz in steps]
    rows = jnp.concatenate(
        [
            GM[(x * dims[1] + near(iy, dy, dims[1])) * dims[2] + near(iz, dz, dims[2])]
            for x, dy, dz in blocks
        ],
        axis=0,
    )
    order = pick(
        iota((128, 128), 0) == (iota((128, 128), 1) % 4) * 32 + iota((128, 128), 1) // 4
    )
    for h in range(2):
        MP[h] = exact_dot(rows[:, 128 * h : 128 * h + 128], order)
    hits = {}
    for dz in steps:
        hit = lane8 // 4 == 8 * (iz + dz) + row8
        if dz:
            hit = hit & (row8 == (0 if dz > 0 else 7))
        hits[dz] = hit
    double = pick(iota((128, 256), 0) == iota((128, 256), 1) // 2)
    j = iota((128, 128), 1)
    zl = jnp.where(j < 96, j // 2, j // 2 - 64) + 32 * iz
    here = pick(iota((128, 128), 0) == zl)
    E2[...] = jnp.zeros_like(E2)
    arrive(2, GB)

    b2 = unpack(GB)
    v2 = [(K * b) * r for b, r in zip(b2, iw2)]
    u2 = [1.2 * v + K * s for v, s in zip(v2, whole_sum(v2, 1))]
    r2 = [b - w * (6.0 * u - s) for b, w, u, s in zip(b2, w2, u2, whole_sum(u2, 1))]
    b3 = [0.125 * q for q in coarsen2(r2)]
    v3 = [(K * b) * r for b, r in zip(b3, iw3)]
    u3 = [1.2 * v + K * s for v, s in zip(v3, whole_sum(v3, 2))]
    r3 = [b - w * (6.0 * u - s) for b, w, u, s in zip(b3, w3, u3, whole_sum(u3, 2))]
    c4 = len(r3) // 2
    for i in range(c4):
        T4[pl.ds(8 * i, 8), :] = r3[2 * i] + r3[2 * i + 1]
    half = 4 * c4
    b4 = 0.125 * pair_sum(T4[pl.ds(0, half, stride=2), :] + T4[pl.ds(1, half, stride=2), :], 2)
    chosen = jnp.where(row8 % 4 == lane8 % 4, b4, 0.0)
    low = row_sum(jnp.where(row8 < 4, chosen, 0.0))
    high = row_sum(jnp.where(row8 >= 4, chosen, 0.0))
    e4 = []
    for x in range(dims[0]):
        plane = jnp.zeros((8, 128), F32)
        for dy in steps:
            found = jnp.zeros((8, 128), F32)
            for dz in steps:
                k = 8 * blocks.index((x, dy, dz))
                product = MP[0, k : k + 8, :] * low + MP[1, k : k + 8, :] * high
                found = jnp.where(hits[dz], jnp.sum(product, axis=1, keepdims=True), found)
            plane = jnp.where(row8 // 2 == iy + dy, row_sum(found), plane)
        e4.append(plane)

    y3 = [u + w * e4[i // 2] for i, (u, w) in enumerate(zip(u3, w3))]
    e3 = [(0.2 * y + v + K * s) * r for y, v, s, r in zip(y3, v3, whole_sum(y3, 2), iw3)]
    for i, e in enumerate(e3):
        P3[i, pl.ds(0, 8, stride=2), :] = e
        P3[i, pl.ds(1, 8, stride=2), :] = e
    y2 = [u + w * P3[i // 2] for i, (u, w) in enumerate(zip(u2, w2))]
    s2 = whole_sum(y2, 1)
    for i in range(len(y2)):
        E2[i + 1, 8:24, :] = (0.2 * y2[i] + v2[i] + K * s2[i]) * iw2[i]

    seen = jnp.concatenate([E2[4 * ix + i, pl.ds(6 + 4 * iy, 8), :] for i in range(6)], axis=0)
    wide2 = sel_dot(seen, here)
    for i in range(6):
        P2[i, pl.ds(0, 8, stride=2), :] = wide2[8 * i : 8 * i + 8, :]
        P2[i, pl.ds(1, 8, stride=2), :] = wide2[8 * i : 8 * i + 8, :]
    for p in range(1, hx + 5):
        U1[p] = U1[p] + W1[p] * pltpu.roll(P2[(p - 3) // 2 + 1], 12, 0)
    e1 = []
    for p in range(2, hx + 4):
        c = U1[p]
        f = 0.2 * c + V1[p] + K * (around(c) + (U1[p - 1] + U1[p + 1]))
        e1.append(f * IW1[p])
    wide1 = sel_dot(jnp.concatenate(e1, axis=0), double)
    for i in range(hx + 2):
        for t in range(2):
            q = wide1[16 * i : 16 * i + 16, 128 * t : 128 * t + 128]
            P1[t, i, pl.ds(0, 16, stride=2), :] = q
            P1[t, i, pl.ds(1, 16, stride=2), :] = q

    for p in range(1, nx + 3):
        i = (p - 2) // 2 + 1
        if not 2 <= p < nx + 2:
            U0[p, 0:ny, 0:128] = U0[p, 0:ny, 0:128] + W0[p, 0:ny, 0:128] * P1[0, i, 0:16, :]
            continue
        parts = []
        for t in range(2):
            edge = jnp.where(row8 < 4, P1[t, i, 16:24, :], P1[t, i, 24:32, :])
            parts.append(jnp.concatenate([P1[t, i, 0:16, :], edge], axis=0))
        U0[p] = U0[p] + W0[p] * jnp.concatenate(parts, axis=1)
    for x in range(nx):
        p = x + 2
        f = 0.2 * U0[p, 0:ny, 0:128] + V0[p, 0:ny, 0:128] + K * own_sum(U0, p)
        f_ref[x] = f * IW[x]

    take(everything, sent.at[0])


def fused(dims, sources, stiffness, coarse_inverse):
    nx, ny, nz = stiffness.shape
    n = dims[0] * dims[1] * dims[2]
    vm = lambda *s: pltpu.VMEM(s, F32)
    halo1 = [vm(8, 8, 128), vm(8, 128), vm(3, 2, 16, 128), vm(8, 8, 128), vm(2, 2, 8, 128)]
    result = pl.pallas_call(
        functools.partial(kernel, dims),
        out_shape=pltpu.VMEM((nx, ny, nz), F32),
        in_specs=[pl.BlockSpec(memory_space=pl.ANY)] * 3,
        out_specs=pl.BlockSpec(memory_space=pltpu.VMEM),
        scratch_shapes=[
            vm(nx, ny, nz), vm(nx, ny, nz), vm(*coarse_inverse.shape),
            vm(nx + 4, 24, 256), vm(nx + 4, 24, 256), vm(nx + 4, 24, 256),
            vm(14, 16, 128), vm(14, 16, 128), vm(14, 16, 128),
            vm(8, 16, 128), vm(32, 128), vm(16, 128), vm(2 * dims[0], 16, 128),
            vm(16, 128), vm(2 * dims[0], 16, 128),
            vm(4 * dims[0] + 2, 32, 128), vm(6, 16, 128), vm(2, 10, 32, 128),
            vm(nx, ny, nz), vm(14, 16, 128), vm(2, 72 * dims[0], 128),
            vm(ny, 128), vm(3, 2, ny + 8, 128),
        ]
        + halo1 + halo1
        + [
            vm(n, 8, 256), vm(n, 4, 128), vm(n, 4, 128), vm(4, 128), vm(4, 128),
            vm(2048, 128),
            pltpu.SemaphoreType.DMA((3,)), pltpu.SemaphoreType.DMA((1,)),
            pltpu.SemaphoreType.DMA((4,)), pltpu.SemaphoreType.DMA((3,)),
            pltpu.SemaphoreType.REGULAR((2,)),
        ],
        compiler_params=pltpu.CompilerParams(collective_id=0, has_side_effects=True),
        name="cycle",
    )(sources[0], stiffness, coarse_inverse)
    return result[None]


def solution(mesh):
    dims = tuple(mesh.shape[a] for a in ("gx", "gy", "gz"))

    def run(sources, stiffness, coarse_inverse):
        nx, ny, nz = stiffness.shape
        lanes = 128
        cells = coarse_inverse.shape[1]
        levels_fit = (
            sources.shape[0] == 1
            and nx == ny == 16
            and nz == lanes
            and dims[2] * nz == 4 * lanes
            and dims[1] * ny == 64
            and cells == 2 * lanes
            and dims[0] == 2
        )
        if levels_fit:
            return fused(dims, sources, stiffness, coarse_inverse)
        return per_device(sources, stiffness, coarse_inverse)

    in_specs = (P(None, "gx", "gy", "gz"), P("gx", "gy", "gz"), P(("gx", "gy", "gz"), None))
    out_specs = P(None, "gx", "gy", "gz")
    return jax.shard_map(
        run, mesh=mesh, in_specs=in_specs, out_specs=out_specs, check_vma=False
    )
```

```python
import functools
import jax
import jax.numpy as jnp
from jax import lax
from jax.experimental import pallas as pl
from jax.experimental.pallas import tpu as pltpu
from jax.sharding import PartitionSpec as P

damping = 0.8


def extended(cells, sides, width):
    for axis, dim in sides:
        count = lax.axis_size(axis)
        ends = count - 1
        head = lax.slice_in_dim(cells, 0, width, axis=dim)
        tail = lax.slice_in_dim(cells, cells.shape[dim] - width, cells.shape[dim], axis=dim)
        cells = jnp.concatenate(
            [
                lax.ppermute(tail, axis, [(i, (i + 1) % count) for i in range(ends)]),
                cells,
                lax.ppermute(head, axis, [((i + 1) % count, i) for i in range(ends)]),
            ],
            axis=dim,
        )
    return cells


def loop_sum(padded):
    total = padded[:, 2:, 1:-1, 1:-1] + padded[:, :-2, 1:-1, 1:-1]
    total = total + padded[:, 1:-1, 2:, 1:-1] + padded[:, 1:-1, :-2, 1:-1]
    total = total + padded[:, 1:-1, 1:-1, 2:] + padded[:, 1:-1, 1:-1, :-2]
    return total


def inner_part(values):
    return values[:, 1:-1, 1:-1, 1:-1]


def pre_smooth(source, weights):
    count = source.shape[0]
    stacked = jnp.concatenate([source, weights], axis=0)
    wide = extended(stacked, (("gx", 1), ("gy", 2), ("gz", 3)), 2)
    wide_source = wide[:count]
    wide_weights = wide[count:]
    safe_weights = jnp.where(wide_weights > 0.0, wide_weights, 1.0)
    first = damping * wide_source / (6.0 * safe_weights * safe_weights)
    first_scaled = wide_weights * first
    mid_weights = inner_part(wide_weights)
    mid_safe = inner_part(safe_weights)
    applied = mid_weights * (6.0 * inner_part(first_scaled) - loop_sum(first_scaled))
    second = inner_part(first) + damping * (inner_part(wide_source) - applied) / (
        6.0 * mid_safe * mid_safe
    )
    second_scaled = mid_weights * second
    answer = inner_part(second)
    resid = source - weights * (6.0 * inner_part(second_scaled) - loop_sum(second_scaled))
    return (answer, resid)


def post_smooth(answer, source, weights):
    scaled = weights * answer
    wide = extended(scaled, (("gx", 1), ("gy", 2), ("gz", 3)), 1)
    applied = weights * (6.0 * scaled - loop_sum(wide))
    return answer + damping * (source - applied) / (6.0 * weights * weights)


def coarsen(values):
    leading = values.shape[0]
    size_x, size_y, size_z = (values.shape[1], values.shape[2], values.shape[3])
    blocks = values.reshape((leading, size_x // 2, 2, size_y // 2, 2, size_z // 2, 2))
    return jnp.mean(blocks, axis=(2, 4, 6))


def refine(values):
    return jnp.repeat(jnp.repeat(jnp.repeat(values, 2, axis=1), 2, axis=2), 2, axis=3)


def per_device(sources, stiffness, coarse_inverse):
    weight_list = [stiffness[None]]
    for level in range(3):
        weight_list.append(0.5 * coarsen(weight_list[-1]))
    source_list = []
    answer_list = []
    current = sources
    for level in range(4):
        source_list.append(current)
        answer, resid = pre_smooth(current, weight_list[level])
        answer_list.append(answer)
        current = coarsen(resid)
    count = current.shape[0]
    flat_source = current.reshape((count, -1))
    solved = lax.dot_general(
        lax.all_gather(flat_source, ("gx", "gy", "gz"), axis=1, tiled=True),
        coarse_inverse,
        (((1,), (1,)), ((), ())),
        precision=lax.Precision.HIGHEST,
        preferred_element_type=jnp.float32,
    )
    correction = solved.reshape(current.shape)
    for level in range(3, -1, -1):
        correction = post_smooth(
            answer_list[level] + refine(correction), source_list[level], weight_list[level]
        )
    return correction


K = damping / 6.0
F32 = jnp.float32
BF = jnp.bfloat16


def iota(shape, dim):
    return lax.broadcasted_iota(jnp.int32, shape, dim)


def pick(condition):
    return jnp.where(condition, 1.0, 0.0).astype(BF)


def sel_dot(values, chosen):
    high = values.astype(BF)
    low = (values - high.astype(F32)).astype(BF)
    both = jnp.concatenate([high, low], axis=1)
    return jnp.dot(both, jnp.concatenate([chosen] * 2, axis=0), preferred_element_type=F32)


def exact_dot(values, chosen):
    total = None
    for _ in range(3):
        part = values.astype(BF)
        values = values - part.astype(F32)
        term = jnp.dot(part, chosen, preferred_element_type=F32)
        total = term if total is None else total + term
    return total


def around(c):
    rows, lanes = c.shape
    return (pltpu.roll(c, 1, 0) + pltpu.roll(c, rows - 1, 0)) + (
        pltpu.roll(c, 1, 1) + pltpu.roll(c, lanes - 1, 1)
    )


def side_sum(planes):
    rows = planes[0].shape[0]
    row = iota(planes[0].shape, 0)
    outs = []
    for p, c in enumerate(planes):
        s = jnp.where(row > 0, pltpu.roll(c, 1, 0), 0.0) + jnp.where(
            row < rows - 1, pltpu.roll(c, rows - 1, 0), 0.0
        )
        if p > 0:
            s = s + planes[p - 1]
        if p < len(planes) - 1:
            s = s + planes[p + 1]
        outs.append(s)
    return outs


def shifted(c, by):
    lane, lanes = iota(c.shape, 1), c.shape[1]
    inside = lane + by < lanes if by > 0 else lane + by >= 0
    return jnp.where(inside, pltpu.roll(c, -by % lanes, 1), 0.0)


def pair_sum(c, step):
    lanes = c.shape[1]
    even = (iota(c.shape, 1) // step) % 2 == 0
    return c + jnp.where(even, pltpu.roll(c, lanes - step, 1), pltpu.roll(c, step, 1))


def row_sum(c):
    for step in (4, 2, 1):
        c = c + pltpu.roll(c, step, 0)
    return c


def kernel(
    dims, b_hbm, w_hbm, m_hbm, f_ref,
    b_ref, w_ref, m_ref,
    V0, W0, U0, V1, W1, U1, TT, T2, T3, T4, P3, E2, P2, P1, P1s, IW, IW1, MP, W0m, W0p, F0, W1m, W1p, E10,
    SZ0, RZ0, S1v, SZv, RZv, R3v, RCv, S1w, SZw, RZw, R3w, RCw,
    GM, GW, GB, SW, SB,
    tally, load, sent, hr, gr, known,
):
    axes = ("gx", "gy", "gz")
    ix, iy, iz = (lax.axis_index(a) for a in axes)
    n = dims[0] * dims[1] * dims[2]
    me = (ix * dims[1] + iy) * dims[2] + iz

    def flip(i, bits):
        if bits == 1:
            return i + 1 - 2 * (i % 2)
        return {0: i, 2: (i + 2) % 4, 3: 3 - i}[bits]

    def mirrored(k):
        a, b, c = k
        y, z = dims[1] - 1 - iy, dims[2] - 1 - iz
        return ((ix + a) % dims[0], flip(y, b), flip(z, c))

    ends = (dims[1] - 1, dims[2] - 1)
    others = sorted(
        (c + (b + 1) // 2, a, b, c)
        for a in range(dims[0])
        for b in range(dims[1])
        for c in range(dims[2])
        if (a, b, c) != (0,) + ends
    )
    others = [k[1:] for k in others]

    barrier = pltpu.get_barrier_semaphore()

    def there(d):
        ok = None
        for i, s, c in zip((ix, iy, iz), dims, d):
            if c:
                t = (i + c < s) if c > 0 else (i + c >= 0)
                ok = t if ok is None else jnp.logical_and(ok, t)
        return ok

    def directions(most):
        found = []
        for dx in (-1, 0, 1):
            for dy in (-1, 0, 1):
                for dz in (-1, 0, 1):
                    if 0 < abs(dx) + abs(dy) + abs(dz) <= most:
                        found.append((dx, dy, dz))
        return sorted(found, key=lambda d: (-abs(d[1]), -abs(d[2]), abs(d[0])))

    def greet(sem):
        for d in directions(3):
            @pl.when(there(d))
            def _(d=d):
                pl.semaphore_signal(
                    sem, inc=1, device_id=(ix + d[0], iy + d[1], iz + d[2]),
                    device_id_type=pl.DeviceIdType.MESH,
                )

    loads = [
        pltpu.make_async_copy(src, dst, load.at[i])
        for i, (src, dst) in enumerate(((b_hbm, b_ref), (w_hbm, w_ref), (m_hbm, m_ref)))
    ]
    for copy in loads:
        copy.start()
    nx, ny = b_ref.shape[0], b_ref.shape[1]
    hx, hy = nx // 2, ny // 2

    def clear(ref, *where):
        part = ref.at[where] if where else ref
        part[...] = jnp.zeros(part.shape, F32)

    own = (pl.ds(0, ny), pl.ds(0, 128))
    clear(V0, pl.ds(0, 2), *own)
    clear(V0, pl.ds(nx + 2, 2), *own)
    clear(V0, pl.ds(1, nx + 2), pl.ds(ny, 8), pl.ds(0, 128))
    clear(W0, pl.ds(1, 1), *own)
    clear(W0, pl.ds(nx + 2, 1), *own)
    clear(W0, pl.ds(2, nx), pl.ds(ny, 8), pl.ds(0, 128))
    for D in (V1, W1):
        clear(D, pl.ds(0, 3))
        clear(D, pl.ds(hx + 3, 3))
        clear(D, pl.ds(3, hx), pl.ds(8, 8))
    for D in (RZ0, RZv, R3v, RCv, RZw, R3w, RCw):
        clear(D)
    greet(barrier)

    def span(i, s):
        return 1 + jnp.where(i > 0, 1, 0) + jnp.where(i < s - 1, 1, 0)

    greeted = span(ix, dims[0]) * span(iy, dims[1]) * span(iz, dims[2]) - 1

    def send(src, dst, d, sem):
        pltpu.make_async_remote_copy(
            src_ref=src, dst_ref=dst, send_sem=sent.at[0], recv_sem=sem,
            device_id=(ix + d[0], iy + d[1], iz + d[2]), device_id_type=pl.DeviceIdType.MESH,
        ).start()

    def send_all(found, pieces, sem):
        for d in found:
            @pl.when(there(d))
            def _(d=d):
                send(*pieces(d), d, sem)

    def span_x(c, size, pad, deep):
        if c == 0:
            return pl.ds(0, size), pl.ds(pad, size)
        if c > 0:
            return pl.ds(size - deep, deep), pl.ds(pad - deep, deep)
        return pl.ds(0, deep), pl.ds(pad + size, deep)

    def span_y(c, size, total, deep):
        if c == 0:
            return pl.ds(0, size), pl.ds(0, size)
        if c > 0:
            return pl.ds(size - deep, deep), pl.ds(total - deep, deep)
        return pl.ds(0, deep), pl.ds(size, deep)

    def flat(found):
        return [d for d in found if not d[2]]

    first = pl.ds(0, 128)

    def pieces0(d):
        dx, dy, dz = d
        if dz:
            a, b = span_y(dy, ny, ny + 8, 1)
            return SZ0.at[a], RZ0.at[1 - dx, (1 - dz) // 2, b]
        deep = 1 if dx and dy else 2
        a, b = span_x(dx, nx, 2, deep)
        e, f = span_y(dy, ny, ny + 8, deep)
        shifted = pl.ds(a.start + 2, a.size)
        return V0.at[shifted, e, first], V0.at[b, f, first]

    def faces0(d):
        a, b = span_x(d[0], nx, 2, 1)
        e, f = span_y(d[1], ny, ny + 8, 1)
        return W0.at[pl.ds(a.start + 2, a.size), e, first], W0.at[b, f, first]

    def pieces1(S1, D, SZ, RZ):
        def of(d):
            dx, dy, dz = d
            if dz:
                a, b = span_y(dy, 8, 16, 2)
                return SZ.at[a], RZ.at[1 - dx, (1 - dz) // 2, b]
            a, b = span_x(dx, hx, 3, 2 if dy else 3)
            e, f = span_y(dy, 8, 16, 2)
            return S1.at[a, e], D.at[b, f]
        return of

    def late1(S1, R3, SZ, RC):
        def of(d):
            dx, dy, dz = d
            if dz:
                row = pl.ds(7 if dy > 0 else 0, 1)
                return SZ.at[row], RC.at[(1 - dx) // 2, (1 - dz) // 2, row]
            row = pl.ds(5 if dy > 0 else 2, 1)
            return S1.at[:, row], R3.at[:, row]
        return of

    def matrix_rows(d):
        s, r = m_ref, GM.at[me]
        if d[2]:
            row = pl.ds(m_ref.shape[0] - 1 if d[2] > 0 else 0, 1)
            s, r = s.at[row], r.at[row]
        return s, r

    corners = [d for d in directions(3) if all(d)]
    lates = [(0, -1, 0), (0, 1, 0)] + corners

    def bytes_of(ref, sem):
        pltpu.make_async_copy(ref, ref, sem).wait()

    sides_y, sides_z = span(iy, dims[1]) - 1, span(iz, dims[2]) - 1

    def first_part(cy, cz):
        return 32 + 33 * cy + 32 * cz + cy * cz

    def face_part(cy, cz):
        return 16 + 16 * cy

    def second_part(cy, cz):
        return 24 + 20 * cy + 16 * cz + 2 * cy * cz

    def late_part(cy, cz):
        return 8 * cy + cy * cz

    def weight_part(cy, cz):
        return second_part(cy, cz) + late_part(cy, cz)

    def matrix_part(cy, cz):
        return 16 + 32 * cy + 4 * (1 + cy) * cz

    def everything(cy, cz):
        parts = (first_part, face_part, second_part, late_part, weight_part, matrix_part)
        return sum(part(cy, cz) for part in parts) + 8 * (n - 1)

    def take(part, sem):
        for cy in (1, 2):
            for cz in (1, 2):
                @pl.when(jnp.logical_and(sides_y == cy, sides_z == cz))
                def _(cy=cy, cz=cz):
                    bytes_of(tally.at[pl.ds(0, part(cy, cz))], sem)

    def spread(kind, src, dst, k):
        return pltpu.make_async_remote_copy(
            src_ref=src, dst_ref=dst.at[me], send_sem=sent.at[0], recv_sem=gr.at[kind],
            device_id=mirrored(k), device_id_type=pl.DeviceIdType.MESH,
        )

    def arrive(kind, dst):
        bytes_of(dst.at[pl.ds(0, n - 1)], gr.at[kind])


    for copy in loads[:2]:
        copy.wait()
    lane16 = iota((ny, 128), 1)
    packed = jnp.zeros((ny, 128), F32)
    for x in range(nx):
        w = w_ref[x]
        v = K * b_ref[x] / w
        V0[x + 2, 0:ny, 0:128] = v
        W0[x + 2, 0:ny, 0:128] = w
        for a, q in enumerate((v, w)):
            start = 8 * x + 4 * a
            moved = pltpu.roll(q, (start + 2) % 128, 1)
            packed = jnp.where((lane16 >= start) & (lane16 < start + 4), moved, packed)
    SZ0[...] = packed

    pl.semaphore_wait(barrier, greeted)
    send_all(directions(2), pieces0, hr.at[0])
    greet(known.at[0])
    send_all(flat(directions(1)), faces0, hr.at[3])

    halve = pick(iota((128, 128), 0) == 2 * iota((128, 128), 1))
    halve = halve + pick(iota((128, 128), 0) == 2 * iota((128, 128), 1) + 1)

    def coarsen0(planes):
        for i in range(hx):
            TT[i] = planes(2 * i) + planes(2 * i + 1)
        rows = [
            TT[i, pl.ds(0, hy, stride=2), :] + TT[i, pl.ds(1, hy, stride=2), :] for i in range(hx)
        ]
        return sel_dot(jnp.concatenate(rows, axis=0), halve)

    k512, j512 = iota((512, 128), 0), iota((512, 128), 1)
    placed = pick((j512 // 32 == (k512 // 128 + iz) % 4) & (k512 % 128 // 2 == j512 % 32))

    def coarsen1(planes, SG):
        for i in range(hx // 2):
            T2[pl.ds(8 * i, 8), :] = planes(2 * i) + planes(2 * i + 1)
        pieces = [
            T2[pl.ds(8 * x, 4, stride=2), :] + T2[pl.ds(8 * x + 1, 4, stride=2), :]
            for x in range(4)
        ]
        wide = jnp.concatenate(pieces, axis=1)
        high = wide.astype(BF).astype(F32)
        both = jnp.concatenate([high, wide - high], axis=0).astype(BF)
        out = jnp.dot(both, placed, preferred_element_type=F32)
        return out[0:4] + out[4:8]

    lane8 = iota((8, 128), 1)

    def pack1(S1, SZ, planes):
        out = jnp.zeros((8, 128), F32)
        for x in range(hx):
            q = planes[x]
            S1[x] = q
            s = 16 * x
            h = (s + 64) % 128
            out = jnp.where((lane8 >= h) & (lane8 < h + 3), pltpu.roll(q, (h - 61) % 128, 1), out)
            out = jnp.where(
                (lane8 >= s + 3) & (lane8 < s + 6), pltpu.roll(q, (s + 3) % 128, 1), out
            )
        SZ[...] = out

    w1 = 0.0625 * coarsen0(lambda x: w_ref[x])
    w1 = [w1[8 * x : 8 * x + 8, :] for x in range(hx)]
    pack1(S1w, SZw, w1)
    SW[...] = 0.0625 * coarsen1(lambda x: w1[x], SW)
    GW[me] = SW[...]
    loads[2].wait()
    GM[me] = m_ref[...]
    send_all(directions(2), pieces1(S1w, W1, SZw, RZw), hr.at[1])
    send_all(lates, late1(S1w, R3w, SZw, RCw), hr.at[1])
    send_all(directions(3), matrix_rows, gr.at[1])
    pl.semaphore_wait(known.at[0], greeted)
    greet(known.at[1])

    def coords(rows, lanes, cy, cz, by, bz):
        r, l = iota((rows, lanes), 0), iota((rows, lanes), 1)
        y = jnp.where(r < cy + (rows - cy) // 2, r, r - rows)
        z = jnp.where(l < cz + (lanes - cz) // 2, l, l - lanes)
        gy, gz = y + iy * cy, z + iz * cz
        ok = (gy >= 0) & (gy < dims[1] * cy) & (gz >= 0) & (gz < dims[2] * cz)
        near = (y >= -by) & (y < cy + by) & (z >= -bz) & (z < cz + bz)
        return jnp.where(ok & near, 1, 0)

    def plane_mask(base, x, cx):
        if 0 <= x < cx:
            return base > 0
        gx = x + ix * cx
        inside = jnp.where((gx >= 0) & (gx < dims[0] * cx), 1, 0)
        return base * inside > 0

    take(first_part, hr.at[0])
    mask0 = coords(24, 256, ny, 128, 1, 1) > 0
    row8 = iota((8, 128), 0)
    lane24 = iota((24, 128), 1)

    def z_ends(dx):
        return jnp.where(lane24 % 4 >= 2, RZ0[dx + 1, 1], RZ0[dx + 1, 0])

    for dx in (-1, 0, 1):
        ends = z_ends(dx)
        for x in {-1: (nx - 1,), 0: range(nx), 1: (0,)}[dx]:
            V0[x + 2 + dx * nx, :, 128:256] = pltpu.roll(ends, (126 - 8 * x) % 128, 1)

    def assemble_faces():
        ends = z_ends(0)
        for x in range(nx):
            p = x + 2
            W0[p, :, 128:256] = pltpu.roll(ends, (122 - 8 * x) % 128, 1)
            IW[x] = 1.0 / w_ref[x]
            W0m[x] = pltpu.roll(W0[p, 0:ny, :], 1, 1)[:, 0:128]
            W0p[x] = pltpu.roll(W0[p, 0:ny, :], 255, 1)[:, 0:128]
            F0[x] = 0.2 * U0[p, 0:ny, 0:128] + V0[p, 0:ny, 0:128] + K * own_sum(U0, p)

    def own_sum(ref, p):
        col, wide = ref[p, :, 0:128], ref[p, 0:ny, :]
        vert = pltpu.roll(col, 1, 0)[0:ny] + pltpu.roll(col, ny + 7, 0)[0:ny]
        flat_sum = pltpu.roll(wide, 1, 1)[:, 0:128] + pltpu.roll(wide, 255, 1)[:, 0:128]
        return (vert + flat_sum) + (ref[p - 1, 0:ny, 0:128] + ref[p + 1, 0:ny, 0:128])

    def exists(c):
        return (ix + c >= 0) & (ix + c < dims[0])

    for p, c in ((1, -1), (nx + 2, 1)):
        u = 1.2 * V0[p, 0:ny, 0:128] + K * own_sum(V0, p)
        U0[p, 0:ny, 0:128] = jnp.where(exists(c), u, 0.0)
    for p in range(2, nx + 2):
        c = V0[p]
        u = 1.2 * c + K * (around(c) + (V0[p - 1] + V0[p + 1]))
        U0[p] = jnp.where(mask0, u, 0.0)

    def resid0(x):
        p = x + 2
        return b_ref[x] - w_ref[x] * (6.0 * U0[p, 0:ny, 0:128] - own_sum(U0, p))

    b1 = 0.125 * coarsen0(resid0)
    b1 = [b1[8 * x : 8 * x + 8, :] for x in range(hx)]
    v1 = [jnp.where(lane8 < 64, K * b1[x] / jnp.where(lane8 < 64, w1[x], 1.0), 0.0) for x in range(hx)]
    pack1(S1v, SZv, v1)
    send_all(directions(2), pieces1(S1v, V1, SZv, RZv), hr.at[2])
    send_all(lates, late1(S1v, R3v, SZv, RCv), hr.at[4])
    pl.semaphore_wait(known.at[1], greeted)
    for k in others:
        spread(0, SW, GW, k).start()

    mask1 = coords(16, 128, 8, 64, 2, 2)
    mask_up = coords(16, 128, 8, 64, 1, 1)
    mask_own = coords(16, 128, 8, 64, 0, 0)
    lane1 = iota((16, 128), 1)

    def assemble1(S1, RZ, D):
        for dx in (-1, 0, 1):
            ends = jnp.where(lane1 % 16 < 3, RZ[dx + 1, 0], RZ[dx + 1, 1])
            for x in {-1: (hx - 2, hx - 1), 0: range(hx), 1: (0, 1)}[dx]:
                p = x + 3 + dx * hx
                moved = pltpu.roll(ends, (61 - 16 * x) % 128, 1)
                inner = S1[x] if dx == 0 else D[p, 0:8, :]
                D[p, 0:8, :] = jnp.where(lane8 < 64, inner, moved[0:8])
                D[p, 8:16, :] = jnp.where(lane8 < 64, D[p, 8:16, :], moved[8:16])

    def finish1(R3, RC, D):
        for x in range(hx):
            D[x + 3, 8:16, :] = jnp.where((row8 == 2) | (row8 == 5), R3[x], D[x + 3, 8:16, :])
        for slot, p, x in ((0, 2, hx - 1), (1, hx + 3, 0)):
            ends = jnp.where(lane8 % 16 < 3, RC[slot, 0], RC[slot, 1])
            moved = pltpu.roll(ends, (61 - 16 * x) % 128, 1)
            D[p, 8:16, :] = jnp.where(lane8 < 64, D[p, 8:16, :], moved)

    def smooth1(planes):
        for p in planes:
            c = V1[p]
            u = 1.2 * c + K * (around(c) + (V1[p - 1] + V1[p + 1]))
            U1[p] = jnp.where(plane_mask(mask1, p - 3, hx), u, 0.0)

    block = lane8 // 32

    def gathered(G):
        planes = []
        for gx in range(dims[0]):
            tiles = {}
            for t in range(dims[1] // 2):
                for z in range(dims[2]):
                    d0 = (gx * dims[1] + 2 * t) * dims[2] + z
                    tiles[t, z] = jnp.concatenate([G[d0], G[d0 + dims[2]]], axis=0)
            for x in range(4):
                parts = []
                for t in range(dims[1] // 2):
                    out = tiles[t, 0]
                    for z in range(1, dims[2]):
                        out = jnp.where(block == (x + z) % 4, tiles[t, z], out)
                    parts.append(out)
                planes.append(jnp.concatenate(parts, axis=0))
        return planes

    def turned(planes, by):
        return [
            pltpu.roll(c, (-32 * (X % 4) - by) % 128, 1) if X % 4 or by else c
            for X, c in enumerate(planes)
        ]

    def coarsen2(planes):
        c = len(planes) // 2
        for i in range(c):
            T3[i] = planes[2 * i] + planes[2 * i + 1]
        return [
            pair_sum(T3[i, pl.ds(0, 8, stride=2), :] + T3[i, pl.ds(1, 8, stride=2), :], 1)
            for i in range(c)
        ]

    take(second_part, hr.at[2])
    assemble1(S1v, RZv, V1)
    smooth1(range(2, hx + 4))

    def resid1(x):
        p = x + 3
        s = around(U1[p])[0:8, :] + (U1[p - 1, 0:8, :] + U1[p + 1, 0:8, :])
        return jnp.where(lane8 < 64, b1[x] - w1[x] * (6.0 * U1[p, 0:8, :] - s), 0.0)

    SB[...] = 0.125 * coarsen1(resid1, SB)
    GB[me] = SB[...]
    for k in others:
        spread(2, SB, GB, k).start()
    arrive(0, GW)
    turned_w2 = gathered(GW)
    scale2 = [K / q for q in turned_w2]
    w2 = turned(turned_w2, 0)
    w2m, w2p = [shifted(q, -1) for q in w2], [shifted(q, 1) for q in w2]
    unscale2 = [q * (1.0 / K) for q in w2]
    iw2 = [1.0 / q for q in w2]
    w3 = [0.0625 * q for q in coarsen2(w2)]
    around3 = {k: [shifted(q, 2 * k) if k else q for q in w3] for k in (-2, -1, 0, 1, 2)}
    iw3 = [1.0 / q for q in w3]
    inverse3 = {k: [shifted(q, 2 * k) if k else q for q in iw3] for k in (-1, 0, 1)}
    take(matrix_part, gr.at[1])
    take(face_part, hr.at[3])
    assemble_faces()
    take(weight_part, hr.at[1])
    assemble1(S1w, RZw, W1)
    finish1(R3w, RCw, W1)
    for p in range(2, hx + 4):
        inside = plane_mask(mask_up if 0 <= p - 3 < hx else mask_own, p - 3, hx)
        IW1[p] = jnp.where(inside, 1.0, 0.0) / jnp.where(inside, W1[p], 1.0)
        W1m[p] = pltpu.roll(W1[p], 1, 1)
        W1p[p] = pltpu.roll(W1[p], 127, 1)
    take(late_part, hr.at[4])
    finish1(R3v, RCv, V1)
    smooth1(range(1, hx + 5))
    for p in range(2, hx + 4):
        c = U1[p]
        E10[p] = 0.2 * c + V1[p] + K * (around(c) + (U1[p - 1] + U1[p + 1]))

    def near(i, c, size):
        return jnp.clip(i + c, 0, size - 1)

    steps = (-1, 0, 1)
    blocks = [(x, dy, dz) for x in range(dims[0]) for dy in steps for dz in steps]
    rows = jnp.concatenate(
        [
            GM[(x * dims[1] + near(iy, dy, dims[1])) * dims[2] + near(iz, dz, dims[2])]
            for x, dy, dz in blocks
        ],
        axis=0,
    )
    order = pick(
        iota((128, 128), 0) == (iota((128, 128), 1) % 4) * 32 + iota((128, 128), 1) // 4
    )
    for h in range(2):
        MP[h] = exact_dot(rows[:, 128 * h : 128 * h + 128], order)
    far = jnp.full((8, 128), -99)
    wanted = {-1: jnp.where(row8 == 7, -1, far), 0: row8, 1: jnp.where(row8 == 0, 8, far)}
    held = {}
    for k in (-2, -1, 0, 1, 2):
        cell = lane8 + 2 * k
        held[k] = jnp.where((cell >= 0) & (cell < 128), cell // 4 - 8 * iz, -50)
    j384, k384 = iota((128, 384), 1), iota((128, 384), 0)
    move = j384 // 128
    move = jnp.where(move == 2, -1, move)
    at = j384 % 128
    double = pick(k384 == (at + move + 256) // 2 % 128)
    depth = jnp.where(at < 96, at, at - 128) + move
    here = pick(k384 == (depth + 256) // 2 - 128 + 32 * iz)
    even = lane8 % 2 == 0
    E2[...] = jnp.zeros_like(E2)
    arrive(2, GB)

    v_turned = [b * r for b, r in zip(gathered(GB), scale2)]
    v2 = turned(v_turned, 0)
    lane_wide = iota((16, 128), 1)
    before = [jnp.where(lane_wide > 0, q, 0.0) for q in turned(v_turned, -1)]
    after = [jnp.where(lane_wide < 127, q, 0.0) for q in turned(v_turned, 1)]
    u2 = [1.2 * v + K * (s + (a + b)) for v, s, a, b in zip(v2, side_sum(v2), before, after)]
    s2 = [s + (shifted(u, -1) + shifted(u, 1)) for s, u in zip(side_sum(u2), u2)]
    r2 = [v * k - w * (6.0 * u - s) for v, k, w, u, s in zip(v2, unscale2, w2, u2, s2)]
    base2 = [0.2 * u + v + K * s for u, v, s in zip(u2, v2, s2)]
    b3 = [0.125 * q for q in coarsen2(r2)]
    v3 = [K * b * r for b, r in zip(b3, iw3)]
    u3 = [
        1.2 * v + K * (s + (shifted(v, -2) + shifted(v, 2))) for v, s in zip(v3, side_sum(v3))
    ]
    s3 = [s + (shifted(u, -2) + shifted(u, 2)) for s, u in zip(side_sum(u3), u3)]
    r3 = [b - w * (6.0 * u - s) for b, w, u, s in zip(b3, w3, u3, s3)]
    base3 = [0.2 * u + v + K * s for u, v, s in zip(u3, v3, s3)]
    base3 = {k: [shifted(q, 2 * k) if k else q for q in base3] for k in (-1, 0, 1)}
    c4 = len(r3) // 2
    for i in range(c4):
        T4[pl.ds(8 * i, 8), :] = r3[2 * i] + r3[2 * i + 1]
    half = 4 * c4
    b4 = 0.125 * pair_sum(T4[pl.ds(0, half, stride=2), :] + T4[pl.ds(1, half, stride=2), :], 2)
    chosen = jnp.where(row8 % 4 == lane8 % 4, b4, 0.0)
    low = row_sum(jnp.where(row8 < 4, chosen, 0.0))
    high = row_sum(jnp.where(row8 >= 4, chosen, 0.0))
    solved = [
        jnp.sum(MP[0, 8 * k : 8 * k + 8, :] * low + MP[1, 8 * k : 8 * k + 8, :] * high,
                axis=1, keepdims=True)
        for k in range(len(blocks))
    ]
    q3 = {}
    for k in (-2, -1, 0, 1, 2):
        e4 = []
        for x in range(dims[0]):
            plane = jnp.zeros((8, 128), F32)
            for dy in steps:
                found = jnp.zeros((8, 128), F32)
                for dz in steps:
                    value = solved[blocks.index((x, dy, dz))]
                    found = jnp.where(held[k] == wanted[dz], value, found)
                plane = jnp.where(row8 // 2 == iy + dy, row_sum(found), plane)
            e4.append(plane)
        q3[k] = [w * e4[i // 2] for i, w in enumerate(around3[k])]
    e3 = {}
    for k in (-1, 0, 1):
        sides = side_sum(q3[k])
        e3[k] = [
            (base + 0.2 * q + K * (s + (a + b))) * r
            for base, q, s, a, b, r in zip(
                base3[k], q3[k], sides, q3[k - 1], q3[k + 1], inverse3[k]
            )
        ]
    for i in range(2 * dims[0]):
        middle = e3[0][i]
        views = (middle, jnp.where(even, middle, e3[1][i]), jnp.where(even, e3[-1][i], middle))
        for k, e in enumerate(views):
            P3[k, i, pl.ds(0, 8, stride=2), :] = e
            P3[k, i, pl.ds(1, 8, stride=2), :] = e
    q2 = [w * P3[0, i // 2] for i, w in enumerate(w2)]
    sides = side_sum(q2)
    for i, (base, q, s) in enumerate(zip(base2, q2, sides)):
        ends = w2p[i] * P3[1, i // 2] + w2m[i] * P3[2, i // 2]
        E2[i + 1, 8:24, :] = (base + 0.2 * q + K * (s + ends)) * iw2[i]

    seen = jnp.concatenate([E2[4 * ix + i, pl.ds(6 + 4 * iy, 8), :] for i in range(6)], axis=0)
    wide2 = sel_dot(seen, here)
    for i in range(6):
        for k in range(3):
            q = pltpu.roll(wide2[8 * i : 8 * i + 8, 128 * k : 128 * k + 128], 6, 0)
            P2[k, i, pl.ds(0, 8, stride=2), :] = q
            P2[k, i, pl.ds(1, 8, stride=2), :] = q
    q1 = {p: W1[p] * P2[0, (p - 3) // 2 + 1] for p in range(1, hx + 5)}
    e1 = []
    for p in range(2, hx + 4):
        q, i = q1[p], (p - 3) // 2 + 1
        ends = W1p[p] * P2[1, i] + W1m[p] * P2[2, i]
        s = (pltpu.roll(q, 1, 0) + pltpu.roll(q, 15, 0)) + ends + (q1[p - 1] + q1[p + 1])
        e1.append((E10[p] + 0.2 * q + K * s) * IW1[p])
    wide1 = sel_dot(jnp.concatenate(e1, axis=0), double)
    for i in range(hx + 2):
        q = wide1[16 * i : 16 * i + 16, 0:128]
        P1[i, pl.ds(0, 16, stride=2), :] = q
        P1[i, pl.ds(1, 16, stride=2), :] = q
        for k in (1, 2):
            q = wide1[16 * i : 16 * i + 8, 128 * k : 128 * k + 128]
            P1s[k - 1, i, pl.ds(0, 8, stride=2), :] = q
            P1s[k - 1, i, pl.ds(1, 8, stride=2), :] = q

    def scaled(p):
        i = (p - 2) // 2 + 1
        if not 2 <= p < nx + 2:
            return W0[p, 0:ny, 0:128] * P1[i, 0:16, :]
        edge = jnp.where(row8 < 4, P1[i, 16:24, :], P1[i, 24:32, :])
        return W0[p, :, 0:128] * jnp.concatenate([P1[i, 0:16, :], edge], axis=0)

    q0 = {p: scaled(p) for p in range(1, nx + 3)}
    for x in range(nx):
        p, i = x + 2, x // 2 + 1
        q = q0[p]
        ends = W0p[x] * P1s[0, i] + W0m[x] * P1s[1, i]
        vert = pltpu.roll(q, 1, 0)[0:ny] + pltpu.roll(q, ny + 7, 0)[0:ny]
        s = vert + ends + (q0[p - 1][0:ny] + q0[p + 1][0:ny])
        f_ref[x] = (F0[x] + 0.2 * q[0:ny] + K * s) * IW[x]

    take(everything, sent.at[0])


def fused(dims, sources, stiffness, coarse_inverse):
    nx, ny, nz = stiffness.shape
    n = dims[0] * dims[1] * dims[2]
    vm = lambda *s: pltpu.VMEM(s, F32)
    halo1 = [vm(8, 8, 128), vm(8, 128), vm(3, 2, 16, 128), vm(8, 8, 128), vm(2, 2, 8, 128)]
    result = pl.pallas_call(
        functools.partial(kernel, dims),
        out_shape=pltpu.VMEM((nx, ny, nz), F32),
        in_specs=[pl.BlockSpec(memory_space=pl.ANY)] * 3,
        out_specs=pl.BlockSpec(memory_space=pltpu.VMEM),
        scratch_shapes=[
            vm(nx, ny, nz), vm(nx, ny, nz), vm(*coarse_inverse.shape),
            vm(nx + 4, 24, 256), vm(nx + 4, 24, 256), vm(nx + 4, 24, 256),
            vm(14, 16, 128), vm(14, 16, 128), vm(14, 16, 128),
            vm(8, 16, 128), vm(32, 128), vm(2 * dims[0], 16, 128),
            vm(16, 128), vm(3, 2 * dims[0], 16, 128),
            vm(4 * dims[0] + 2, 32, 128), vm(3, 6, 16, 128), vm(10, 32, 128), vm(2, 10, 16, 128),
            vm(nx, ny, nz), vm(14, 16, 128), vm(2, 72 * dims[0], 128),
            vm(nx, ny, nz), vm(nx, ny, nz), vm(nx, ny, nz),
            vm(14, 16, 128), vm(14, 16, 128), vm(14, 16, 128),
            vm(ny, 128), vm(3, 2, ny + 8, 128),
        ]
        + halo1 + halo1
        + [
            vm(n, 8, 256), vm(n, 4, 128), vm(n, 4, 128), vm(4, 128), vm(4, 128),
            vm(2048, 128),
            pltpu.SemaphoreType.DMA((3,)), pltpu.SemaphoreType.DMA((1,)),
            pltpu.SemaphoreType.DMA((5,)), pltpu.SemaphoreType.DMA((3,)),
            pltpu.SemaphoreType.REGULAR((2,)),
        ],
        compiler_params=pltpu.CompilerParams(collective_id=0, has_side_effects=True),
        name="cycle",
    )(sources[0], stiffness, coarse_inverse)
    return result[None]


def solution(mesh):
    dims = tuple(mesh.shape[a] for a in ("gx", "gy", "gz"))

    def run(sources, stiffness, coarse_inverse):
        nx, ny, nz = stiffness.shape
        lanes = 128
        cells = coarse_inverse.shape[1]
        levels_fit = (
            sources.shape[0] == 1
            and nx == ny == 16
            and nz == lanes
            and dims[2] * nz == 4 * lanes
            and dims[1] * ny == 64
            and cells == 2 * lanes
            and dims[0] == 2
        )
        if levels_fit:
            return fused(dims, sources, stiffness, coarse_inverse)
        return per_device(sources, stiffness, coarse_inverse)

    in_specs = (P(None, "gx", "gy", "gz"), P("gx", "gy", "gz"), P(("gx", "gy", "gz"), None))
    out_specs = P(None, "gx", "gy", "gz")
    return jax.shard_map(
        run, mesh=mesh, in_specs=in_specs, out_specs=out_specs, check_vma=False
    )
```

```python
import functools
import jax
import jax.numpy as jnp
from jax import lax
from jax.experimental import pallas as pl
from jax.experimental.pallas import tpu as pltpu
from jax.sharding import PartitionSpec as P

damping = 0.8


def extended(cells, sides, width):
    for axis, dim in sides:
        count = lax.axis_size(axis)
        ends = count - 1
        head = lax.slice_in_dim(cells, 0, width, axis=dim)
        tail = lax.slice_in_dim(cells, cells.shape[dim] - width, cells.shape[dim], axis=dim)
        cells = jnp.concatenate(
            [
                lax.ppermute(tail, axis, [(i, (i + 1) % count) for i in range(ends)]),
                cells,
                lax.ppermute(head, axis, [((i + 1) % count, i) for i in range(ends)]),
            ],
            axis=dim,
        )
    return cells


def loop_sum(padded):
    total = padded[:, 2:, 1:-1, 1:-1] + padded[:, :-2, 1:-1, 1:-1]
    total = total + padded[:, 1:-1, 2:, 1:-1] + padded[:, 1:-1, :-2, 1:-1]
    total = total + padded[:, 1:-1, 1:-1, 2:] + padded[:, 1:-1, 1:-1, :-2]
    return total


def inner_part(values):
    return values[:, 1:-1, 1:-1, 1:-1]


def pre_smooth(source, weights):
    count = source.shape[0]
    stacked = jnp.concatenate([source, weights], axis=0)
    wide = extended(stacked, (("gx", 1), ("gy", 2), ("gz", 3)), 2)
    wide_source = wide[:count]
    wide_weights = wide[count:]
    safe_weights = jnp.where(wide_weights > 0.0, wide_weights, 1.0)
    first = damping * wide_source / (6.0 * safe_weights * safe_weights)
    first_scaled = wide_weights * first
    mid_weights = inner_part(wide_weights)
    mid_safe = inner_part(safe_weights)
    applied = mid_weights * (6.0 * inner_part(first_scaled) - loop_sum(first_scaled))
    second = inner_part(first) + damping * (inner_part(wide_source) - applied) / (
        6.0 * mid_safe * mid_safe
    )
    second_scaled = mid_weights * second
    answer = inner_part(second)
    resid = source - weights * (6.0 * inner_part(second_scaled) - loop_sum(second_scaled))
    return (answer, resid)


def post_smooth(answer, source, weights):
    scaled = weights * answer
    wide = extended(scaled, (("gx", 1), ("gy", 2), ("gz", 3)), 1)
    applied = weights * (6.0 * scaled - loop_sum(wide))
    return answer + damping * (source - applied) / (6.0 * weights * weights)


def coarsen(values):
    leading = values.shape[0]
    size_x, size_y, size_z = (values.shape[1], values.shape[2], values.shape[3])
    blocks = values.reshape((leading, size_x // 2, 2, size_y // 2, 2, size_z // 2, 2))
    return jnp.mean(blocks, axis=(2, 4, 6))


def refine(values):
    return jnp.repeat(jnp.repeat(jnp.repeat(values, 2, axis=1), 2, axis=2), 2, axis=3)


def per_device(sources, stiffness, coarse_inverse):
    weight_list = [stiffness[None]]
    for level in range(3):
        weight_list.append(0.5 * coarsen(weight_list[-1]))
    source_list = []
    answer_list = []
    current = sources
    for level in range(4):
        source_list.append(current)
        answer, resid = pre_smooth(current, weight_list[level])
        answer_list.append(answer)
        current = coarsen(resid)
    count = current.shape[0]
    flat_source = current.reshape((count, -1))
    solved = lax.dot_general(
        lax.all_gather(flat_source, ("gx", "gy", "gz"), axis=1, tiled=True),
        coarse_inverse,
        (((1,), (1,)), ((), ())),
        precision=lax.Precision.HIGHEST,
        preferred_element_type=jnp.float32,
    )
    correction = solved.reshape(current.shape)
    for level in range(3, -1, -1):
        correction = post_smooth(
            answer_list[level] + refine(correction), source_list[level], weight_list[level]
        )
    return correction


K = damping / 6.0
F32 = jnp.float32
BF = jnp.bfloat16


def iota(shape, dim):
    return lax.broadcasted_iota(jnp.int32, shape, dim)


def pick(condition):
    return jnp.where(condition, 1.0, 0.0).astype(BF)


def lanes_of(values, index):
    index = jnp.broadcast_to(index, values.shape)
    return jnp.take_along_axis(values, index, axis=1, mode="promise_in_bounds")


def exact_dot(values, chosen):
    total = None
    for _ in range(3):
        part = values.astype(BF)
        values = values - part.astype(F32)
        term = jnp.dot(part, chosen, preferred_element_type=F32)
        total = term if total is None else total + term
    return total


def around(c):
    rows, lanes = c.shape
    return (pltpu.roll(c, 1, 0) + pltpu.roll(c, rows - 1, 0)) + (
        pltpu.roll(c, 1, 1) + pltpu.roll(c, lanes - 1, 1)
    )


def side_sum(planes):
    rows = planes[0].shape[0]
    row = iota(planes[0].shape, 0)
    outs = []
    for p, c in enumerate(planes):
        s = jnp.where(row > 0, pltpu.roll(c, 1, 0), 0.0) + jnp.where(
            row < rows - 1, pltpu.roll(c, rows - 1, 0), 0.0
        )
        if p > 0:
            s = s + planes[p - 1]
        if p < len(planes) - 1:
            s = s + planes[p + 1]
        outs.append(s)
    return outs


def shifted(c, by):
    lane, lanes = iota(c.shape, 1), c.shape[1]
    inside = lane + by < lanes if by > 0 else lane + by >= 0
    return jnp.where(inside, pltpu.roll(c, -by % lanes, 1), 0.0)


def pair_sum(c, step):
    lanes = c.shape[1]
    even = (iota(c.shape, 1) // step) % 2 == 0
    return c + jnp.where(even, pltpu.roll(c, lanes - step, 1), pltpu.roll(c, step, 1))


def row_sum(c):
    for step in (4, 2, 1):
        c = c + pltpu.roll(c, step, 0)
    return c


def kernel(
    dims, b_hbm, w_hbm, m_hbm, f_ref,
    b_ref, w_ref, m_ref,
    V0, W0, U0, V1, W1, U1, TT, T2, T3, T4, P3, E2, P2, P1, P1s, IW, IW1, MP, W0m, W0p, F0, W1m, W1p, E10,
    SZ0, RZ0, S1v, SZv, RZv, R3v, RCv, S1w, SZw, RZw, R3w, RCw,
    GM, GW, GB, SW, SB,
    tally, load, sent, hr, gr, known,
):
    axes = ("gx", "gy", "gz")
    ix, iy, iz = (lax.axis_index(a) for a in axes)
    n = dims[0] * dims[1] * dims[2]
    me = (ix * dims[1] + iy) * dims[2] + iz

    def flip(i, bits):
        if bits == 1:
            return i + 1 - 2 * (i % 2)
        return {0: i, 2: (i + 2) % 4, 3: 3 - i}[bits]

    def mirrored(k):
        a, b, c = k
        y, z = dims[1] - 1 - iy, dims[2] - 1 - iz
        return ((ix + a) % dims[0], flip(y, b), flip(z, c))

    ends = (dims[1] - 1, dims[2] - 1)
    others = sorted(
        (c + (b + 1) // 2, a, b, c)
        for a in range(dims[0])
        for b in range(dims[1])
        for c in range(dims[2])
        if (a, b, c) != (0,) + ends
    )
    others = [k[1:] for k in others]

    barrier = pltpu.get_barrier_semaphore()

    def there(d):
        ok = None
        for i, s, c in zip((ix, iy, iz), dims, d):
            if c:
                t = (i + c < s) if c > 0 else (i + c >= 0)
                ok = t if ok is None else jnp.logical_and(ok, t)
        return ok

    def directions(most):
        found = []
        for dx in (-1, 0, 1):
            for dy in (-1, 0, 1):
                for dz in (-1, 0, 1):
                    if 0 < abs(dx) + abs(dy) + abs(dz) <= most:
                        found.append((dx, dy, dz))
        return sorted(found, key=lambda d: (-abs(d[1]), -abs(d[2]), abs(d[0])))

    def greet(sem):
        for d in directions(3):
            @pl.when(there(d))
            def _(d=d):
                pl.semaphore_signal(
                    sem, inc=1, device_id=(ix + d[0], iy + d[1], iz + d[2]),
                    device_id_type=pl.DeviceIdType.MESH,
                )

    loads = [
        pltpu.make_async_copy(src, dst, load.at[i])
        for i, (src, dst) in enumerate(((b_hbm, b_ref), (w_hbm, w_ref), (m_hbm, m_ref)))
    ]
    for copy in loads:
        copy.start()
    nx, ny = b_ref.shape[0], b_ref.shape[1]
    hx, hy = nx // 2, ny // 2

    def clear(ref, *where):
        part = ref.at[where] if where else ref
        part[...] = jnp.zeros(part.shape, F32)

    own = (pl.ds(0, ny), pl.ds(0, 128))
    clear(V0, pl.ds(0, 2), *own)
    clear(V0, pl.ds(nx + 2, 2), *own)
    clear(V0, pl.ds(1, nx + 2), pl.ds(ny, 8), pl.ds(0, 128))
    clear(W0, pl.ds(1, 1), *own)
    clear(W0, pl.ds(nx + 2, 1), *own)
    clear(W0, pl.ds(2, nx), pl.ds(ny, 8), pl.ds(0, 128))
    for D in (V1, W1):
        clear(D, pl.ds(0, 3))
        clear(D, pl.ds(hx + 3, 3))
        clear(D, pl.ds(3, hx), pl.ds(8, 8))
    for D in (RZ0, RZv, R3v, RCv, RZw, R3w, RCw):
        clear(D)
    greet(barrier)

    def span(i, s):
        return 1 + jnp.where(i > 0, 1, 0) + jnp.where(i < s - 1, 1, 0)

    greeted = span(ix, dims[0]) * span(iy, dims[1]) * span(iz, dims[2]) - 1

    def send(src, dst, d, sem):
        pltpu.make_async_remote_copy(
            src_ref=src, dst_ref=dst, send_sem=sent.at[0], recv_sem=sem,
            device_id=(ix + d[0], iy + d[1], iz + d[2]), device_id_type=pl.DeviceIdType.MESH,
        ).start()

    def send_all(found, pieces, sem):
        for d in found:
            @pl.when(there(d))
            def _(d=d):
                send(*pieces(d), d, sem)

    def span_x(c, size, pad, deep):
        if c == 0:
            return pl.ds(0, size), pl.ds(pad, size)
        if c > 0:
            return pl.ds(size - deep, deep), pl.ds(pad - deep, deep)
        return pl.ds(0, deep), pl.ds(pad + size, deep)

    def span_y(c, size, total, deep):
        if c == 0:
            return pl.ds(0, size), pl.ds(0, size)
        if c > 0:
            return pl.ds(size - deep, deep), pl.ds(total - deep, deep)
        return pl.ds(0, deep), pl.ds(size, deep)

    def flat(found):
        return [d for d in found if not d[2]]

    first = pl.ds(0, 128)

    def pieces0(d):
        dx, dy, dz = d
        if dz:
            a, b = span_y(dy, ny, ny + 8, 1)
            return SZ0.at[a], RZ0.at[1 - dx, (1 - dz) // 2, b]
        deep = 1 if dx and dy else 2
        a, b = span_x(dx, nx, 2, deep)
        e, f = span_y(dy, ny, ny + 8, deep)
        shifted = pl.ds(a.start + 2, a.size)
        return V0.at[shifted, e, first], V0.at[b, f, first]

    def faces0(d):
        a, b = span_x(d[0], nx, 2, 1)
        e, f = span_y(d[1], ny, ny + 8, 1)
        return W0.at[pl.ds(a.start + 2, a.size), e, first], W0.at[b, f, first]

    def pieces1(S1, D, SZ, RZ):
        def of(d):
            dx, dy, dz = d
            if dz:
                a, b = span_y(dy, 8, 16, 2)
                return SZ.at[a], RZ.at[1 - dx, (1 - dz) // 2, b]
            a, b = span_x(dx, hx, 3, 2 if dy else 3)
            e, f = span_y(dy, 8, 16, 2)
            return S1.at[a, e], D.at[b, f]
        return of

    def late1(S1, R3, SZ, RC):
        def of(d):
            dx, dy, dz = d
            if dz:
                row = pl.ds(7 if dy > 0 else 0, 1)
                return SZ.at[row], RC.at[(1 - dx) // 2, (1 - dz) // 2, row]
            row = pl.ds(5 if dy > 0 else 2, 1)
            return S1.at[:, row], R3.at[:, row]
        return of

    def matrix_rows(d):
        s, r = m_ref, GM.at[me]
        if d[2]:
            row = pl.ds(m_ref.shape[0] - 1 if d[2] > 0 else 0, 1)
            s, r = s.at[row], r.at[row]
        return s, r

    corners = [d for d in directions(3) if all(d)]
    lates = [(0, -1, 0), (0, 1, 0)] + corners

    def bytes_of(ref, sem):
        pltpu.make_async_copy(ref, ref, sem).wait()

    sides_y, sides_z = span(iy, dims[1]) - 1, span(iz, dims[2]) - 1

    def first_part(cy, cz):
        return 32 + 33 * cy + 32 * cz + cy * cz

    def face_part(cy, cz):
        return 16 + 16 * cy

    def second_part(cy, cz):
        return 24 + 20 * cy + 16 * cz + 2 * cy * cz

    def late_part(cy, cz):
        return 8 * cy + cy * cz

    def weight_part(cy, cz):
        return second_part(cy, cz) + late_part(cy, cz)

    def matrix_part(cy, cz):
        return 16 + 32 * cy + 4 * (1 + cy) * cz

    def everything(cy, cz):
        parts = (first_part, face_part, second_part, late_part, weight_part, matrix_part)
        return sum(part(cy, cz) for part in parts) + 8 * (n - 1)

    def take(part, sem):
        for cy in (1, 2):
            for cz in (1, 2):
                @pl.when(jnp.logical_and(sides_y == cy, sides_z == cz))
                def _(cy=cy, cz=cz):
                    bytes_of(tally.at[pl.ds(0, part(cy, cz))], sem)

    def spread(kind, src, dst, k):
        return pltpu.make_async_remote_copy(
            src_ref=src, dst_ref=dst.at[me], send_sem=sent.at[0], recv_sem=gr.at[kind],
            device_id=mirrored(k), device_id_type=pl.DeviceIdType.MESH,
        )

    def arrive(kind, dst):
        bytes_of(dst.at[pl.ds(0, n - 1)], gr.at[kind])


    for copy in loads[:2]:
        copy.wait()
    lane16 = iota((ny, 128), 1)
    packed = jnp.zeros((ny, 128), F32)
    for x in range(nx):
        w = w_ref[x]
        v = K * b_ref[x] / w
        V0[x + 2, 0:ny, 0:128] = v
        W0[x + 2, 0:ny, 0:128] = w
        for a, q in enumerate((v, w)):
            start = 8 * x + 4 * a
            moved = pltpu.roll(q, (start + 2) % 128, 1)
            packed = jnp.where((lane16 >= start) & (lane16 < start + 4), moved, packed)
    SZ0[...] = packed

    pl.semaphore_wait(barrier, greeted)
    send_all(directions(2), pieces0, hr.at[0])
    greet(known.at[0])
    send_all(flat(directions(1)), faces0, hr.at[3])

    lane_row = iota((1, 128), 1)
    low_half = jnp.minimum(2 * lane_row, 126)

    def coarsen0(planes):
        for i in range(hx):
            TT[i] = planes(2 * i) + planes(2 * i + 1)
        rows = [
            TT[i, pl.ds(0, hy, stride=2), :] + TT[i, pl.ds(1, hy, stride=2), :] for i in range(hx)
        ]
        rows = jnp.concatenate(rows, axis=0)
        return lanes_of(rows, low_half) + lanes_of(rows, low_half + 1)

    held_x = (lane_row // 32 + 4 - iz) % 4
    pairs = 2 * (lane_row % 32)

    def coarsen1(planes, SG):
        for i in range(hx // 2):
            T2[pl.ds(8 * i, 8), :] = planes(2 * i) + planes(2 * i + 1)
        pieces = [
            T2[pl.ds(8 * x, 4, stride=2), :] + T2[pl.ds(8 * x + 1, 4, stride=2), :]
            for x in range(4)
        ]
        rows = [jnp.concatenate(pieces[i : i + 2], axis=0) for i in (0, 2)]
        sums = [lanes_of(r, pairs) + lanes_of(r, pairs + 1) for r in rows]
        parts = [sums[x // 2][4 * (x % 2) : 4 * (x % 2) + 4] for x in range(4)]
        total = parts[0]
        for x in range(1, 4):
            total = jnp.where(held_x == x, parts[x], total)
        return total

    lane8 = iota((8, 128), 1)

    def pack1(S1, SZ, planes):
        out = jnp.zeros((8, 128), F32)
        for x in range(hx):
            q = planes[x]
            S1[x] = q
            s = 16 * x
            h = (s + 64) % 128
            out = jnp.where((lane8 >= h) & (lane8 < h + 3), pltpu.roll(q, (h - 61) % 128, 1), out)
            out = jnp.where(
                (lane8 >= s + 3) & (lane8 < s + 6), pltpu.roll(q, (s + 3) % 128, 1), out
            )
        SZ[...] = out

    w1 = 0.0625 * coarsen0(lambda x: w_ref[x])
    w1 = [w1[8 * x : 8 * x + 8, :] for x in range(hx)]
    pack1(S1w, SZw, w1)
    SW[...] = 0.0625 * coarsen1(lambda x: w1[x], SW)
    GW[me] = SW[...]
    loads[2].wait()
    GM[me] = m_ref[...]
    send_all(directions(2), pieces1(S1w, W1, SZw, RZw), hr.at[1])
    send_all(lates, late1(S1w, R3w, SZw, RCw), hr.at[1])
    send_all(directions(3), matrix_rows, gr.at[1])
    pl.semaphore_wait(known.at[0], greeted)
    greet(known.at[1])

    def coords(rows, lanes, cy, cz, by, bz):
        r, l = iota((rows, lanes), 0), iota((rows, lanes), 1)
        y = jnp.where(r < cy + (rows - cy) // 2, r, r - rows)
        z = jnp.where(l < cz + (lanes - cz) // 2, l, l - lanes)
        gy, gz = y + iy * cy, z + iz * cz
        ok = (gy >= 0) & (gy < dims[1] * cy) & (gz >= 0) & (gz < dims[2] * cz)
        near = (y >= -by) & (y < cy + by) & (z >= -bz) & (z < cz + bz)
        return jnp.where(ok & near, 1, 0)

    def plane_mask(base, x, cx):
        if 0 <= x < cx:
            return base > 0
        gx = x + ix * cx
        inside = jnp.where((gx >= 0) & (gx < dims[0] * cx), 1, 0)
        return base * inside > 0

    take(first_part, hr.at[0])
    mask0 = coords(24, 256, ny, 128, 1, 1) > 0
    row8 = iota((8, 128), 0)
    lane24 = iota((24, 128), 1)

    def z_ends(dx):
        return jnp.where(lane24 % 4 >= 2, RZ0[dx + 1, 1], RZ0[dx + 1, 0])

    for dx in (-1, 0, 1):
        ends = z_ends(dx)
        for x in {-1: (nx - 1,), 0: range(nx), 1: (0,)}[dx]:
            V0[x + 2 + dx * nx, :, 128:256] = pltpu.roll(ends, (126 - 8 * x) % 128, 1)

    def assemble_faces():
        ends = z_ends(0)
        for x in range(nx):
            p = x + 2
            W0[p, :, 128:256] = pltpu.roll(ends, (122 - 8 * x) % 128, 1)
            IW[x] = 1.0 / w_ref[x]
            W0m[x] = pltpu.roll(W0[p, 0:ny, :], 1, 1)[:, 0:128]
            W0p[x] = pltpu.roll(W0[p, 0:ny, :], 255, 1)[:, 0:128]
            F0[x] = 0.2 * U0[p, 0:ny, 0:128] + V0[p, 0:ny, 0:128] + K * own_sum(U0, p)

    def own_sum(ref, p):
        col, wide = ref[p, :, 0:128], ref[p, 0:ny, :]
        vert = pltpu.roll(col, 1, 0)[0:ny] + pltpu.roll(col, ny + 7, 0)[0:ny]
        flat_sum = pltpu.roll(wide, 1, 1)[:, 0:128] + pltpu.roll(wide, 255, 1)[:, 0:128]
        return (vert + flat_sum) + (ref[p - 1, 0:ny, 0:128] + ref[p + 1, 0:ny, 0:128])

    def exists(c):
        return (ix + c >= 0) & (ix + c < dims[0])

    for p, c in ((1, -1), (nx + 2, 1)):
        u = 1.2 * V0[p, 0:ny, 0:128] + K * own_sum(V0, p)
        U0[p, 0:ny, 0:128] = jnp.where(exists(c), u, 0.0)
    for p in range(2, nx + 2):
        c = V0[p]
        u = 1.2 * c + K * (around(c) + (V0[p - 1] + V0[p + 1]))
        U0[p] = jnp.where(mask0, u, 0.0)

    def resid0(x):
        p = x + 2
        return b_ref[x] - w_ref[x] * (6.0 * U0[p, 0:ny, 0:128] - own_sum(U0, p))

    b1 = 0.125 * coarsen0(resid0)
    b1 = [b1[8 * x : 8 * x + 8, :] for x in range(hx)]
    v1 = [jnp.where(lane8 < 64, K * b1[x] / jnp.where(lane8 < 64, w1[x], 1.0), 0.0) for x in range(hx)]
    pack1(S1v, SZv, v1)
    send_all(directions(2), pieces1(S1v, V1, SZv, RZv), hr.at[2])
    send_all(lates, late1(S1v, R3v, SZv, RCv), hr.at[4])
    pl.semaphore_wait(known.at[1], greeted)
    for k in others:
        spread(0, SW, GW, k).start()

    mask1 = coords(16, 128, 8, 64, 2, 2)
    mask_up = coords(16, 128, 8, 64, 1, 1)
    mask_own = coords(16, 128, 8, 64, 0, 0)
    lane1 = iota((16, 128), 1)

    def assemble1(S1, RZ, D):
        for dx in (-1, 0, 1):
            ends = jnp.where(lane1 % 16 < 3, RZ[dx + 1, 0], RZ[dx + 1, 1])
            for x in {-1: (hx - 2, hx - 1), 0: range(hx), 1: (0, 1)}[dx]:
                p = x + 3 + dx * hx
                moved = pltpu.roll(ends, (61 - 16 * x) % 128, 1)
                inner = S1[x] if dx == 0 else D[p, 0:8, :]
                D[p, 0:8, :] = jnp.where(lane8 < 64, inner, moved[0:8])
                D[p, 8:16, :] = jnp.where(lane8 < 64, D[p, 8:16, :], moved[8:16])

    def finish1(R3, RC, D):
        for x in range(hx):
            D[x + 3, 8:16, :] = jnp.where((row8 == 2) | (row8 == 5), R3[x], D[x + 3, 8:16, :])
        for slot, p, x in ((0, 2, hx - 1), (1, hx + 3, 0)):
            ends = jnp.where(lane8 % 16 < 3, RC[slot, 0], RC[slot, 1])
            moved = pltpu.roll(ends, (61 - 16 * x) % 128, 1)
            D[p, 8:16, :] = jnp.where(lane8 < 64, D[p, 8:16, :], moved)

    def smooth1(planes):
        for p in planes:
            c = V1[p]
            u = 1.2 * c + K * (around(c) + (V1[p - 1] + V1[p + 1]))
            U1[p] = jnp.where(plane_mask(mask1, p - 3, hx), u, 0.0)

    block = lane8 // 32

    def gathered(G):
        planes = []
        for gx in range(dims[0]):
            tiles = {}
            for t in range(dims[1] // 2):
                for z in range(dims[2]):
                    d0 = (gx * dims[1] + 2 * t) * dims[2] + z
                    tiles[t, z] = jnp.concatenate([G[d0], G[d0 + dims[2]]], axis=0)
            for x in range(4):
                parts = []
                for t in range(dims[1] // 2):
                    out = tiles[t, 0]
                    for z in range(1, dims[2]):
                        out = jnp.where(block == (x + z) % 4, tiles[t, z], out)
                    parts.append(out)
                planes.append(jnp.concatenate(parts, axis=0))
        return planes

    def turned(planes, by):
        return [
            pltpu.roll(c, (-32 * (X % 4) - by) % 128, 1) if X % 4 or by else c
            for X, c in enumerate(planes)
        ]

    def coarsen2(planes):
        c = len(planes) // 2
        for i in range(c):
            T3[i] = planes[2 * i] + planes[2 * i + 1]
        return [
            pair_sum(T3[i, pl.ds(0, 8, stride=2), :] + T3[i, pl.ds(1, 8, stride=2), :], 1)
            for i in range(c)
        ]

    take(second_part, hr.at[2])
    assemble1(S1v, RZv, V1)
    smooth1(range(2, hx + 4))

    def resid1(x):
        p = x + 3
        s = around(U1[p])[0:8, :] + (U1[p - 1, 0:8, :] + U1[p + 1, 0:8, :])
        return jnp.where(lane8 < 64, b1[x] - w1[x] * (6.0 * U1[p, 0:8, :] - s), 0.0)

    SB[...] = 0.125 * coarsen1(resid1, SB)
    GB[me] = SB[...]
    for k in others:
        spread(2, SB, GB, k).start()
    arrive(0, GW)
    turned_w2 = gathered(GW)
    scale2 = [K / q for q in turned_w2]
    w2 = turned(turned_w2, 0)
    w2m, w2p = [shifted(q, -1) for q in w2], [shifted(q, 1) for q in w2]
    unscale2 = [q * (1.0 / K) for q in w2]
    iw2 = [1.0 / q for q in w2]
    w3 = [0.0625 * q for q in coarsen2(w2)]
    around3 = {k: [shifted(q, 2 * k) if k else q for q in w3] for k in (-2, -1, 0, 1, 2)}
    iw3 = [1.0 / q for q in w3]
    inverse3 = {k: [shifted(q, 2 * k) if k else q for q in iw3] for k in (-1, 0, 1)}
    take(matrix_part, gr.at[1])
    take(face_part, hr.at[3])
    assemble_faces()
    take(weight_part, hr.at[1])
    assemble1(S1w, RZw, W1)
    finish1(R3w, RCw, W1)
    for p in range(2, hx + 4):
        inside = plane_mask(mask_up if 0 <= p - 3 < hx else mask_own, p - 3, hx)
        IW1[p] = jnp.where(inside, 1.0, 0.0) / jnp.where(inside, W1[p], 1.0)
        W1m[p] = pltpu.roll(W1[p], 1, 1)
        W1p[p] = pltpu.roll(W1[p], 127, 1)
    take(late_part, hr.at[4])
    finish1(R3v, RCv, V1)
    smooth1(range(1, hx + 5))
    for p in range(2, hx + 4):
        c = U1[p]
        E10[p] = 0.2 * c + V1[p] + K * (around(c) + (U1[p - 1] + U1[p + 1]))

    def near(i, c, size):
        return jnp.clip(i + c, 0, size - 1)

    steps = (-1, 0, 1)
    blocks = [(x, dy, dz) for x in range(dims[0]) for dy in steps for dz in steps]
    rows = jnp.concatenate(
        [
            GM[(x * dims[1] + near(iy, dy, dims[1])) * dims[2] + near(iz, dz, dims[2])]
            for x, dy, dz in blocks
        ],
        axis=0,
    )
    order = pick(
        iota((128, 128), 0) == (iota((128, 128), 1) % 4) * 32 + iota((128, 128), 1) // 4
    )
    for h in range(2):
        MP[h] = exact_dot(rows[:, 128 * h : 128 * h + 128], order)
    far = jnp.full((8, 128), -99)
    wanted = {-1: jnp.where(row8 == 7, -1, far), 0: row8, 1: jnp.where(row8 == 0, 8, far)}
    held = {}
    for k in (-2, -1, 0, 1, 2):
        cell = lane8 + 2 * k
        held[k] = jnp.where((cell >= 0) & (cell < 128), cell // 4 - 8 * iz, -50)
    moves = (0, 1, -1)
    double = [(lane_row + k + 256) // 2 % 128 for k in moves]
    depth = jnp.where(lane_row < 96, lane_row, lane_row - 128)
    here = [jnp.clip((depth + k + 256) // 2 - 128 + 32 * iz, 0, 127) for k in moves]
    even = lane8 % 2 == 0
    E2[...] = jnp.zeros_like(E2)
    arrive(2, GB)

    v_turned = [b * r for b, r in zip(gathered(GB), scale2)]
    v2 = turned(v_turned, 0)
    lane_wide = iota((16, 128), 1)
    before = [jnp.where(lane_wide > 0, q, 0.0) for q in turned(v_turned, -1)]
    after = [jnp.where(lane_wide < 127, q, 0.0) for q in turned(v_turned, 1)]
    u2 = [1.2 * v + K * (s + (a + b)) for v, s, a, b in zip(v2, side_sum(v2), before, after)]
    s2 = [s + (shifted(u, -1) + shifted(u, 1)) for s, u in zip(side_sum(u2), u2)]
    r2 = [v * k - w * (6.0 * u - s) for v, k, w, u, s in zip(v2, unscale2, w2, u2, s2)]
    base2 = [0.2 * u + v + K * s for u, v, s in zip(u2, v2, s2)]
    b3 = [0.125 * q for q in coarsen2(r2)]
    v3 = [K * b * r for b, r in zip(b3, iw3)]
    u3 = [
        1.2 * v + K * (s + (shifted(v, -2) + shifted(v, 2))) for v, s in zip(v3, side_sum(v3))
    ]
    s3 = [s + (shifted(u, -2) + shifted(u, 2)) for s, u in zip(side_sum(u3), u3)]
    r3 = [b - w * (6.0 * u - s) for b, w, u, s in zip(b3, w3, u3, s3)]
    base3 = [0.2 * u + v + K * s for u, v, s in zip(u3, v3, s3)]
    base3 = {k: [shifted(q, 2 * k) if k else q for q in base3] for k in (-1, 0, 1)}
    c4 = len(r3) // 2
    for i in range(c4):
        T4[pl.ds(8 * i, 8), :] = r3[2 * i] + r3[2 * i + 1]
    half = 4 * c4
    b4 = 0.125 * pair_sum(T4[pl.ds(0, half, stride=2), :] + T4[pl.ds(1, half, stride=2), :], 2)
    chosen = jnp.where(row8 % 4 == lane8 % 4, b4, 0.0)
    low = row_sum(jnp.where(row8 < 4, chosen, 0.0))
    high = row_sum(jnp.where(row8 >= 4, chosen, 0.0))
    solved = [
        jnp.sum(MP[0, 8 * k : 8 * k + 8, :] * low + MP[1, 8 * k : 8 * k + 8, :] * high,
                axis=1, keepdims=True)
        for k in range(len(blocks))
    ]
    q3 = {}
    for k in (-2, -1, 0, 1, 2):
        e4 = []
        for x in range(dims[0]):
            plane = jnp.zeros((8, 128), F32)
            for dy in steps:
                found = jnp.zeros((8, 128), F32)
                for dz in steps:
                    value = solved[blocks.index((x, dy, dz))]
                    found = jnp.where(held[k] == wanted[dz], value, found)
                plane = jnp.where(row8 // 2 == iy + dy, row_sum(found), plane)
            e4.append(plane)
        q3[k] = [w * e4[i // 2] for i, w in enumerate(around3[k])]
    e3 = {}
    for k in (-1, 0, 1):
        sides = side_sum(q3[k])
        e3[k] = [
            (base + 0.2 * q + K * (s + (a + b))) * r
            for base, q, s, a, b, r in zip(
                base3[k], q3[k], sides, q3[k - 1], q3[k + 1], inverse3[k]
            )
        ]
    for i in range(2 * dims[0]):
        middle = e3[0][i]
        views = (middle, jnp.where(even, middle, e3[1][i]), jnp.where(even, e3[-1][i], middle))
        for k, e in enumerate(views):
            P3[k, i, pl.ds(0, 8, stride=2), :] = e
            P3[k, i, pl.ds(1, 8, stride=2), :] = e
    q2 = [w * P3[0, i // 2] for i, w in enumerate(w2)]
    sides = side_sum(q2)
    for i, (base, q, s) in enumerate(zip(base2, q2, sides)):
        ends = w2p[i] * P3[1, i // 2] + w2m[i] * P3[2, i // 2]
        E2[i + 1, 8:24, :] = (base + 0.2 * q + K * (s + ends)) * iw2[i]

    seen = jnp.concatenate([E2[4 * ix + i, pl.ds(6 + 4 * iy, 8), :] for i in range(6)], axis=0)
    for k in range(3):
        wide2 = lanes_of(pltpu.roll(seen.reshape((6, 8, 128)), 6, 1).reshape((48, 128)), here[k])
        for i in range(6):
            q = wide2[8 * i : 8 * i + 8]
            P2[k, i, pl.ds(0, 8, stride=2), :] = q
            P2[k, i, pl.ds(1, 8, stride=2), :] = q
    q1 = {p: W1[p] * P2[0, (p - 3) // 2 + 1] for p in range(1, hx + 5)}
    e1 = []
    for p in range(2, hx + 4):
        q, i = q1[p], (p - 3) // 2 + 1
        ends = W1p[p] * P2[1, i] + W1m[p] * P2[2, i]
        s = (pltpu.roll(q, 1, 0) + pltpu.roll(q, 15, 0)) + ends + (q1[p - 1] + q1[p + 1])
        e1.append((E10[p] + 0.2 * q + K * s) * IW1[p])
    wide1 = lanes_of(jnp.concatenate(e1, axis=0), double[0])
    for i in range(hx + 2):
        q = wide1[16 * i : 16 * i + 16]
        P1[i, pl.ds(0, 16, stride=2), :] = q
        P1[i, pl.ds(1, 16, stride=2), :] = q
    for k in (1, 2):
        wide1 = lanes_of(jnp.concatenate([e[0:8] for e in e1[1:-1]], axis=0), double[k])
        for i in range(hx):
            q = wide1[8 * i : 8 * i + 8]
            P1s[k - 1, i + 1, pl.ds(0, 8, stride=2), :] = q
            P1s[k - 1, i + 1, pl.ds(1, 8, stride=2), :] = q

    def scaled(p):
        i = (p - 2) // 2 + 1
        if not 2 <= p < nx + 2:
            return W0[p, 0:ny, 0:128] * P1[i, 0:16, :]
        edge = jnp.where(row8 < 4, P1[i, 16:24, :], P1[i, 24:32, :])
        return W0[p, :, 0:128] * jnp.concatenate([P1[i, 0:16, :], edge], axis=0)

    q0 = {p: scaled(p) for p in range(1, nx + 3)}
    for x in range(nx):
        p, i = x + 2, x // 2 + 1
        q = q0[p]
        ends = W0p[x] * P1s[0, i] + W0m[x] * P1s[1, i]
        vert = pltpu.roll(q, 1, 0)[0:ny] + pltpu.roll(q, ny + 7, 0)[0:ny]
        s = vert + ends + (q0[p - 1][0:ny] + q0[p + 1][0:ny])
        f_ref[x] = (F0[x] + 0.2 * q[0:ny] + K * s) * IW[x]

    take(everything, sent.at[0])


def fused(dims, sources, stiffness, coarse_inverse):
    nx, ny, nz = stiffness.shape
    n = dims[0] * dims[1] * dims[2]
    vm = lambda *s: pltpu.VMEM(s, F32)
    halo1 = [vm(8, 8, 128), vm(8, 128), vm(3, 2, 16, 128), vm(8, 8, 128), vm(2, 2, 8, 128)]
    result = pl.pallas_call(
        functools.partial(kernel, dims),
        out_shape=pltpu.VMEM((nx, ny, nz), F32),
        in_specs=[pl.BlockSpec(memory_space=pl.ANY)] * 3,
        out_specs=pl.BlockSpec(memory_space=pltpu.VMEM),
        scratch_shapes=[
            vm(nx, ny, nz), vm(nx, ny, nz), vm(*coarse_inverse.shape),
            vm(nx + 4, 24, 256), vm(nx + 4, 24, 256), vm(nx + 4, 24, 256),
            vm(14, 16, 128), vm(14, 16, 128), vm(14, 16, 128),
            vm(8, 16, 128), vm(32, 128), vm(2 * dims[0], 16, 128),
            vm(16, 128), vm(3, 2 * dims[0], 16, 128),
            vm(4 * dims[0] + 2, 32, 128), vm(3, 6, 16, 128), vm(10, 32, 128), vm(2, 10, 16, 128),
            vm(nx, ny, nz), vm(14, 16, 128), vm(2, 72 * dims[0], 128),
            vm(nx, ny, nz), vm(nx, ny, nz), vm(nx, ny, nz),
            vm(14, 16, 128), vm(14, 16, 128), vm(14, 16, 128),
            vm(ny, 128), vm(3, 2, ny + 8, 128),
        ]
        + halo1 + halo1
        + [
            vm(n, 8, 256), vm(n, 4, 128), vm(n, 4, 128), vm(4, 128), vm(4, 128),
            vm(2048, 128),
            pltpu.SemaphoreType.DMA((3,)), pltpu.SemaphoreType.DMA((1,)),
            pltpu.SemaphoreType.DMA((5,)), pltpu.SemaphoreType.DMA((3,)),
            pltpu.SemaphoreType.REGULAR((2,)),
        ],
        compiler_params=pltpu.CompilerParams(collective_id=0, has_side_effects=True),
        name="cycle",
    )(sources[0], stiffness, coarse_inverse)
    return result[None]


def solution(mesh):
    dims = tuple(mesh.shape[a] for a in ("gx", "gy", "gz"))

    def run(sources, stiffness, coarse_inverse):
        nx, ny, nz = stiffness.shape
        lanes = 128
        cells = coarse_inverse.shape[1]
        levels_fit = (
            sources.shape[0] == 1
            and nx == ny == 16
            and nz == lanes
            and dims[2] * nz == 4 * lanes
            and dims[1] * ny == 64
            and cells == 2 * lanes
            and dims[0] == 2
        )
        if levels_fit:
            return fused(dims, sources, stiffness, coarse_inverse)
        return per_device(sources, stiffness, coarse_inverse)

    in_specs = (P(None, "gx", "gy", "gz"), P("gx", "gy", "gz"), P(("gx", "gy", "gz"), None))
    out_specs = P(None, "gx", "gy", "gz")
    return jax.shard_map(
        run, mesh=mesh, in_specs=in_specs, out_specs=out_specs, check_vma=False
    )
```

```python
import functools
import jax
import jax.numpy as jnp
from jax import lax
from jax.experimental import pallas as pl
from jax.experimental.pallas import tpu as pltpu
from jax.sharding import PartitionSpec as P

damping = 0.8


def extended(cells, sides, width):
    for axis, dim in sides:
        count = lax.axis_size(axis)
        ends = count - 1
        head = lax.slice_in_dim(cells, 0, width, axis=dim)
        tail = lax.slice_in_dim(cells, cells.shape[dim] - width, cells.shape[dim], axis=dim)
        cells = jnp.concatenate(
            [
                lax.ppermute(tail, axis, [(i, (i + 1) % count) for i in range(ends)]),
                cells,
                lax.ppermute(head, axis, [((i + 1) % count, i) for i in range(ends)]),
            ],
            axis=dim,
        )
    return cells


def loop_sum(padded):
    total = padded[:, 2:, 1:-1, 1:-1] + padded[:, :-2, 1:-1, 1:-1]
    total = total + padded[:, 1:-1, 2:, 1:-1] + padded[:, 1:-1, :-2, 1:-1]
    total = total + padded[:, 1:-1, 1:-1, 2:] + padded[:, 1:-1, 1:-1, :-2]
    return total


def inner_part(values):
    return values[:, 1:-1, 1:-1, 1:-1]


def pre_smooth(source, weights):
    count = source.shape[0]
    stacked = jnp.concatenate([source, weights], axis=0)
    wide = extended(stacked, (("gx", 1), ("gy", 2), ("gz", 3)), 2)
    wide_source = wide[:count]
    wide_weights = wide[count:]
    safe_weights = jnp.where(wide_weights > 0.0, wide_weights, 1.0)
    first = damping * wide_source / (6.0 * safe_weights * safe_weights)
    first_scaled = wide_weights * first
    mid_weights = inner_part(wide_weights)
    mid_safe = inner_part(safe_weights)
    applied = mid_weights * (6.0 * inner_part(first_scaled) - loop_sum(first_scaled))
    second = inner_part(first) + damping * (inner_part(wide_source) - applied) / (
        6.0 * mid_safe * mid_safe
    )
    second_scaled = mid_weights * second
    answer = inner_part(second)
    resid = source - weights * (6.0 * inner_part(second_scaled) - loop_sum(second_scaled))
    return (answer, resid)


def post_smooth(answer, source, weights):
    scaled = weights * answer
    wide = extended(scaled, (("gx", 1), ("gy", 2), ("gz", 3)), 1)
    applied = weights * (6.0 * scaled - loop_sum(wide))
    return answer + damping * (source - applied) / (6.0 * weights * weights)


def coarsen(values):
    leading = values.shape[0]
    size_x, size_y, size_z = (values.shape[1], values.shape[2], values.shape[3])
    blocks = values.reshape((leading, size_x // 2, 2, size_y // 2, 2, size_z // 2, 2))
    return jnp.mean(blocks, axis=(2, 4, 6))


def refine(values):
    return jnp.repeat(jnp.repeat(jnp.repeat(values, 2, axis=1), 2, axis=2), 2, axis=3)


def per_device(sources, stiffness, coarse_inverse):
    weight_list = [stiffness[None]]
    for level in range(3):
        weight_list.append(0.5 * coarsen(weight_list[-1]))
    source_list = []
    answer_list = []
    current = sources
    for level in range(4):
        source_list.append(current)
        answer, resid = pre_smooth(current, weight_list[level])
        answer_list.append(answer)
        current = coarsen(resid)
    count = current.shape[0]
    flat_source = current.reshape((count, -1))
    solved = lax.dot_general(
        lax.all_gather(flat_source, ("gx", "gy", "gz"), axis=1, tiled=True),
        coarse_inverse,
        (((1,), (1,)), ((), ())),
        precision=lax.Precision.HIGHEST,
        preferred_element_type=jnp.float32,
    )
    correction = solved.reshape(current.shape)
    for level in range(3, -1, -1):
        correction = post_smooth(
            answer_list[level] + refine(correction), source_list[level], weight_list[level]
        )
    return correction


K = damping / 6.0
F32 = jnp.float32
BF = jnp.bfloat16


def iota(shape, dim):
    return lax.broadcasted_iota(jnp.int32, shape, dim)


def pick(condition):
    return jnp.where(condition, 1.0, 0.0).astype(BF)


def lanes_of(values, index):
    index = jnp.broadcast_to(index, values.shape)
    return jnp.take_along_axis(values, index, axis=1, mode="promise_in_bounds")


def exact_dot(values, chosen):
    total = None
    for _ in range(3):
        part = values.astype(BF)
        values = values - part.astype(F32)
        term = jnp.dot(part, chosen, preferred_element_type=F32)
        total = term if total is None else total + term
    return total


def around(c):
    rows, lanes = c.shape
    return (pltpu.roll(c, 1, 0) + pltpu.roll(c, rows - 1, 0)) + (
        pltpu.roll(c, 1, 1) + pltpu.roll(c, lanes - 1, 1)
    )


def side_sum(planes):
    rows = planes[0].shape[0]
    row = iota(planes[0].shape, 0)
    outs = []
    for p, c in enumerate(planes):
        s = jnp.where(row > 0, pltpu.roll(c, 1, 0), 0.0) + jnp.where(
            row < rows - 1, pltpu.roll(c, rows - 1, 0), 0.0
        )
        if p > 0:
            s = s + planes[p - 1]
        if p < len(planes) - 1:
            s = s + planes[p + 1]
        outs.append(s)
    return outs


def shifted(c, by):
    lane, lanes = iota(c.shape, 1), c.shape[1]
    inside = lane + by < lanes if by > 0 else lane + by >= 0
    return jnp.where(inside, pltpu.roll(c, -by % lanes, 1), 0.0)


def pair_sum(c, step):
    lanes = c.shape[1]
    even = (iota(c.shape, 1) // step) % 2 == 0
    return c + jnp.where(even, pltpu.roll(c, lanes - step, 1), pltpu.roll(c, step, 1))


def row_sum(c):
    for step in (4, 2, 1):
        c = c + pltpu.roll(c, step, 0)
    return c


def kernel(
    dims, b_hbm, w_hbm, m_hbm, f_ref,
    b_ref, w_ref, m_ref,
    V0, W0, U0, V1, W1, U1, TT, T2, T3, T4, P3, E2, P2, P1, P1s, IW, IW1, MP, W0m, W0p, F0, R0, W1m, W1p, E10,
    SZ0, RZ0, S1v, SZv, RZv, R3v, RCv, S1w, SZw, RZw, R3w, RCw,
    GM, GW, GB, SW, SB,
    tally, load, sent, hr, gr, known,
):
    axes = ("gx", "gy", "gz")
    ix, iy, iz = (lax.axis_index(a) for a in axes)
    n = dims[0] * dims[1] * dims[2]
    me = (ix * dims[1] + iy) * dims[2] + iz

    def flip(i, bits):
        if bits == 1:
            return i + 1 - 2 * (i % 2)
        return {0: i, 2: (i + 2) % 4, 3: 3 - i}[bits]

    def mirrored(k):
        a, b, c = k
        y, z = dims[1] - 1 - iy, dims[2] - 1 - iz
        return ((ix + a) % dims[0], flip(y, b), flip(z, c))

    ends = (dims[1] - 1, dims[2] - 1)
    others = sorted(
        (c + (b + 1) // 2, a, b, c)
        for a in range(dims[0])
        for b in range(dims[1])
        for c in range(dims[2])
        if (a, b, c) != (0,) + ends
    )
    others = [k[1:] for k in others]

    barrier = pltpu.get_barrier_semaphore()

    def there(d):
        ok = None
        for i, s, c in zip((ix, iy, iz), dims, d):
            if c:
                t = (i + c < s) if c > 0 else (i + c >= 0)
                ok = t if ok is None else jnp.logical_and(ok, t)
        return ok

    def directions(most):
        found = []
        for dx in (-1, 0, 1):
            for dy in (-1, 0, 1):
                for dz in (-1, 0, 1):
                    if 0 < abs(dx) + abs(dy) + abs(dz) <= most:
                        found.append((dx, dy, dz))
        return sorted(found, key=lambda d: (-abs(d[1]), -abs(d[2]), abs(d[0])))

    def greet(sem):
        for d in directions(3):
            @pl.when(there(d))
            def _(d=d):
                pl.semaphore_signal(
                    sem, inc=1, device_id=(ix + d[0], iy + d[1], iz + d[2]),
                    device_id_type=pl.DeviceIdType.MESH,
                )

    loads = [
        pltpu.make_async_copy(src, dst, load.at[i])
        for i, (src, dst) in enumerate(((b_hbm, b_ref), (w_hbm, w_ref), (m_hbm, m_ref)))
    ]
    for copy in loads:
        copy.start()
    nx, ny = b_ref.shape[0], b_ref.shape[1]
    hx, hy = nx // 2, ny // 2

    def clear(ref, *where):
        part = ref.at[where] if where else ref
        part[...] = jnp.zeros(part.shape, F32)

    own = (pl.ds(0, ny), pl.ds(0, 128))
    clear(V0, pl.ds(0, 2), *own)
    clear(V0, pl.ds(nx + 2, 2), *own)
    clear(V0, pl.ds(1, nx + 2), pl.ds(ny, 8), pl.ds(0, 128))
    clear(W0, pl.ds(1, 1), *own)
    clear(W0, pl.ds(nx + 2, 1), *own)
    clear(W0, pl.ds(2, nx), pl.ds(ny, 8), pl.ds(0, 128))
    for D in (V1, W1):
        clear(D, pl.ds(0, 3))
        clear(D, pl.ds(hx + 3, 3))
        clear(D, pl.ds(3, hx), pl.ds(8, 8))
    for D in (RZ0, RZv, R3v, RCv, RZw, R3w, RCw):
        clear(D)
    greet(barrier)

    def span(i, s):
        return 1 + jnp.where(i > 0, 1, 0) + jnp.where(i < s - 1, 1, 0)

    greeted = span(ix, dims[0]) * span(iy, dims[1]) * span(iz, dims[2]) - 1

    def send(src, dst, d, sem):
        pltpu.make_async_remote_copy(
            src_ref=src, dst_ref=dst, send_sem=sent.at[0], recv_sem=sem,
            device_id=(ix + d[0], iy + d[1], iz + d[2]), device_id_type=pl.DeviceIdType.MESH,
        ).start()

    def send_all(found, pieces, sem):
        for d in found:
            @pl.when(there(d))
            def _(d=d):
                send(*pieces(d), d, sem)

    def span_x(c, size, pad, deep):
        if c == 0:
            return pl.ds(0, size), pl.ds(pad, size)
        if c > 0:
            return pl.ds(size - deep, deep), pl.ds(pad - deep, deep)
        return pl.ds(0, deep), pl.ds(pad + size, deep)

    def span_y(c, size, total, deep):
        if c == 0:
            return pl.ds(0, size), pl.ds(0, size)
        if c > 0:
            return pl.ds(size - deep, deep), pl.ds(total - deep, deep)
        return pl.ds(0, deep), pl.ds(size, deep)

    def flat(found):
        return [d for d in found if not d[2]]

    first = pl.ds(0, 128)

    def pieces0(d):
        dx, dy, dz = d
        if dz:
            a, b = span_y(dy, ny, ny + 8, 1)
            return SZ0.at[a], RZ0.at[1 - dx, (1 - dz) // 2, b]
        deep = 1 if dx and dy else 2
        a, b = span_x(dx, nx, 2, deep)
        e, f = span_y(dy, ny, ny + 8, deep)
        shifted = pl.ds(a.start + 2, a.size)
        return V0.at[shifted, e, first], V0.at[b, f, first]

    def faces0(d):
        a, b = span_x(d[0], nx, 2, 1)
        e, f = span_y(d[1], ny, ny + 8, 1)
        return W0.at[pl.ds(a.start + 2, a.size), e, first], W0.at[b, f, first]

    def pieces1(S1, D, SZ, RZ):
        def of(d):
            dx, dy, dz = d
            if dz:
                a, b = span_y(dy, 8, 16, 2)
                return SZ.at[a], RZ.at[1 - dx, (1 - dz) // 2, b]
            a, b = span_x(dx, hx, 3, 2 if dy else 3)
            e, f = span_y(dy, 8, 16, 2)
            return S1.at[a, e], D.at[b, f]
        return of

    def late1(S1, R3, SZ, RC):
        def of(d):
            dx, dy, dz = d
            if dz:
                row = pl.ds(7 if dy > 0 else 0, 1)
                return SZ.at[row], RC.at[(1 - dx) // 2, (1 - dz) // 2, row]
            row = pl.ds(5 if dy > 0 else 2, 1)
            return S1.at[:, row], R3.at[:, row]
        return of

    def matrix_rows(d):
        s, r = m_ref, GM.at[me]
        if d[2]:
            row = pl.ds(m_ref.shape[0] - 1 if d[2] > 0 else 0, 1)
            s, r = s.at[row], r.at[row]
        return s, r

    corners = [d for d in directions(3) if all(d)]
    lates = [(0, -1, 0), (0, 1, 0)] + corners

    def bytes_of(ref, sem):
        pltpu.make_async_copy(ref, ref, sem).wait()

    sides_y, sides_z = span(iy, dims[1]) - 1, span(iz, dims[2]) - 1

    def first_part(cy, cz):
        return 32 + 33 * cy + 32 * cz + cy * cz

    def face_part(cy, cz):
        return 16 + 16 * cy

    def second_part(cy, cz):
        return 24 + 20 * cy + 16 * cz + 2 * cy * cz

    def late_part(cy, cz):
        return 8 * cy + cy * cz

    def weight_part(cy, cz):
        return second_part(cy, cz) + late_part(cy, cz)

    def matrix_part(cy, cz):
        return 16 + 32 * cy + 4 * (1 + cy) * cz

    def everything(cy, cz):
        parts = (first_part, face_part, second_part, late_part, weight_part, matrix_part)
        return sum(part(cy, cz) for part in parts) + 8 * (n - 1)

    def take(part, sem):
        for cy in (1, 2):
            for cz in (1, 2):
                @pl.when(jnp.logical_and(sides_y == cy, sides_z == cz))
                def _(cy=cy, cz=cz):
                    bytes_of(tally.at[pl.ds(0, part(cy, cz))], sem)

    def spread(kind, src, dst, k):
        return pltpu.make_async_remote_copy(
            src_ref=src, dst_ref=dst.at[me], send_sem=sent.at[0], recv_sem=gr.at[kind],
            device_id=mirrored(k), device_id_type=pl.DeviceIdType.MESH,
        )

    def arrive(kind, dst):
        bytes_of(dst.at[pl.ds(0, n - 1)], gr.at[kind])


    for copy in loads[:2]:
        copy.wait()
    lane16 = iota((ny, 128), 1)
    packed = jnp.zeros((ny, 128), F32)
    for x in range(nx):
        w = w_ref[x]
        v = K * b_ref[x] / w
        V0[x + 2, 0:ny, 0:128] = v
        W0[x + 2, 0:ny, 0:128] = w
        for a, q in enumerate((v, w)):
            start = 8 * x + 4 * a
            moved = pltpu.roll(q, (start + 2) % 128, 1)
            packed = jnp.where((lane16 >= start) & (lane16 < start + 4), moved, packed)
    SZ0[...] = packed

    pl.semaphore_wait(barrier, greeted)
    send_all(directions(2), pieces0, hr.at[0])
    greet(known.at[0])
    send_all(flat(directions(1)), faces0, hr.at[3])

    lane_row = iota((1, 128), 1)
    low_half = jnp.minimum(2 * lane_row, 126)

    def coarsen0(planes):
        for i in range(hx):
            TT[i] = planes(2 * i) + planes(2 * i + 1)
        rows = [
            TT[i, pl.ds(0, hy, stride=2), :] + TT[i, pl.ds(1, hy, stride=2), :] for i in range(hx)
        ]
        rows = jnp.concatenate(rows, axis=0)
        return lanes_of(rows, low_half) + lanes_of(rows, low_half + 1)

    held_x = (lane_row // 32 + 4 - iz) % 4
    pairs = 2 * (lane_row % 32)

    def coarsen1(planes, SG):
        for i in range(hx // 2):
            T2[pl.ds(8 * i, 8), :] = planes(2 * i) + planes(2 * i + 1)
        pieces = [
            T2[pl.ds(8 * x, 4, stride=2), :] + T2[pl.ds(8 * x + 1, 4, stride=2), :]
            for x in range(4)
        ]
        rows = [jnp.concatenate(pieces[i : i + 2], axis=0) for i in (0, 2)]
        sums = [lanes_of(r, pairs) + lanes_of(r, pairs + 1) for r in rows]
        parts = [sums[x // 2][4 * (x % 2) : 4 * (x % 2) + 4] for x in range(4)]
        total = parts[0]
        for x in range(1, 4):
            total = jnp.where(held_x == x, parts[x], total)
        return total

    lane8 = iota((8, 128), 1)

    def pack1(S1, SZ, planes):
        out = jnp.zeros((8, 128), F32)
        for x in range(hx):
            q = planes[x]
            S1[x] = q
            s = 16 * x
            h = (s + 64) % 128
            out = jnp.where((lane8 >= h) & (lane8 < h + 3), pltpu.roll(q, (h - 61) % 128, 1), out)
            out = jnp.where(
                (lane8 >= s + 3) & (lane8 < s + 6), pltpu.roll(q, (s + 3) % 128, 1), out
            )
        SZ[...] = out

    w1 = 0.0625 * coarsen0(lambda x: w_ref[x])
    w1 = [w1[8 * x : 8 * x + 8, :] for x in range(hx)]
    pack1(S1w, SZw, w1)
    SW[...] = 0.0625 * coarsen1(lambda x: w1[x], SW)
    GW[me] = SW[...]
    loads[2].wait()
    GM[me] = m_ref[...]
    send_all(directions(2), pieces1(S1w, W1, SZw, RZw), hr.at[1])
    send_all(lates, late1(S1w, R3w, SZw, RCw), hr.at[1])
    send_all(directions(3), matrix_rows, gr.at[1])
    pl.semaphore_wait(known.at[0], greeted)
    greet(known.at[1])

    def coords(rows, lanes, cy, cz, by, bz):
        r, l = iota((rows, lanes), 0), iota((rows, lanes), 1)
        y = jnp.where(r < cy + (rows - cy) // 2, r, r - rows)
        z = jnp.where(l < cz + (lanes - cz) // 2, l, l - lanes)
        gy, gz = y + iy * cy, z + iz * cz
        ok = (gy >= 0) & (gy < dims[1] * cy) & (gz >= 0) & (gz < dims[2] * cz)
        near = (y >= -by) & (y < cy + by) & (z >= -bz) & (z < cz + bz)
        return jnp.where(ok & near, 1, 0)

    def plane_mask(base, x, cx):
        if 0 <= x < cx:
            return base > 0
        gx = x + ix * cx
        inside = jnp.where((gx >= 0) & (gx < dims[0] * cx), 1, 0)
        return base * inside > 0

    row8 = iota((8, 128), 0)
    row16, lane_own = iota((ny, 128), 0), iota((ny, 128), 1)

    def in_lanes(c):
        return shifted(c, -1) + shifted(c, 1)

    def in_rows(c):
        return jnp.where(row16 > 0, pltpu.roll(c, 1, 0), 0.0) + jnp.where(
            row16 < ny - 1, pltpu.roll(c, ny - 1, 0), 0.0
        )

    def beside(planes, x):
        found = [planes[i] for i in (x - 1, x + 1) if 0 <= i < nx]
        return found[0] + found[1] if len(found) > 1 else found[0]

    inner = [V0[x + 2, 0:ny, 0:128] for x in range(nx)]
    inner_u = [
        1.2 * c + K * (in_rows(c) + in_lanes(c) + beside(inner, x)) for x, c in enumerate(inner)
    ]
    for x, u in enumerate(inner_u):
        near_sum = in_rows(u) + in_lanes(u) + beside(inner_u, x)
        R0[x] = b_ref[x] - w_ref[x] * (6.0 * u - near_sum)
    kind = lane_own % 8
    packed = SZ0[...]
    own_ends = jnp.where(kind == 1, pltpu.roll(packed, 127, 1), pltpu.roll(packed, 1, 1))
    has_z = ((kind == 1) & (iz > 0)) | ((kind == 2) & (iz < dims[2] - 1))
    has_y = ((row8 == 7) & (iy > 0)) | ((row8 == 0) & (iy < dims[1] - 1))

    def exists(c):
        return (ix + c >= 0) & (ix + c < dims[0])

    take(first_part, hr.at[0])
    mask0 = coords(24, 256, ny, 128, 1, 1) > 0
    lane24 = iota((24, 128), 1)

    def z_ends(dx):
        return jnp.where(lane24 % 4 >= 2, RZ0[dx + 1, 1], RZ0[dx + 1, 0])

    ends = {dx: z_ends(dx) for dx in (-1, 0, 1)}

    def z_change():
        full, c = ends[0], ends[0][0:ny]
        above, below = pltpu.roll(full, 1, 1), pltpu.roll(full, 127, 1)
        left = pltpu.roll(jnp.where(lane_own >= 120, ends[-1][0:ny], c), 8, 1)
        right = pltpu.roll(jnp.where(lane_own < 8, ends[1][0:ny], c), 120, 1)
        outer = jnp.where(kind == 1, above[0:ny], below[0:ny])
        vert = (pltpu.roll(full, 1, 0) + pltpu.roll(full, ny + 7, 0))[0:ny]
        u = 1.2 * c + K * (outer + own_ends + vert + left + right)
        u = jnp.where(has_z, u, 0.0)
        across = jnp.where(lane_own >= 8, left, 0.0) + jnp.where(lane_own < 120, right, 0.0)
        d = K * (6.0 * c - in_rows(c) - across) - u
        low = jnp.where(kind == 1, d, -K * above[0:ny])
        high = jnp.where(kind == 2, d, -K * below[0:ny])
        swapped = jnp.where(lane8 % 8 == 1, below[ny:], above[ny:])
        return low, high, swapped

    low_end, high_end, edge_ends = z_change()
    side = [V0[p, ny : ny + 8, 0:128] for p in range(1, nx + 3)]

    def z_part(x):
        a = pltpu.roll(low_end, (-8 * x - 1) % 128, 1)
        b = pltpu.roll(high_end, (125 - 8 * x) % 128, 1)
        return jnp.where(lane_own < 2, a, jnp.where(lane_own >= 126, b, 0.0))

    def y_part(x):
        c = side[x + 1]
        ends_x = pltpu.roll(edge_ends, (126 - 8 * x) % 128, 1)
        flat_sum = in_lanes(c)
        edges = jnp.where((lane8 == 0) | (lane8 == 127), ends_x, 0.0)
        adjacent = jnp.where(
            row8 == 7, pltpu.roll(inner[x][0:8], 7, 0), pltpu.roll(inner[x][8:16], 1, 0)
        )
        outer = jnp.where(row8 == 7, pltpu.roll(c, 1, 0), pltpu.roll(c, 7, 0))
        u = 1.2 * c + K * (flat_sum + edges + adjacent + outer + side[x] + side[x + 2])
        u = jnp.where(has_y, u, 0.0)
        d = K * (6.0 * c - flat_sum - beside(side[1:-1], x)) - u
        first_rows = jnp.where(row8 == 1, -K * pltpu.roll(c, 2, 0), 0.0)
        first_rows = jnp.where(row8 == 0, pltpu.roll(d, 1, 0), first_rows)
        last_rows = jnp.where(row8 == 6, -K * pltpu.roll(c, 6, 0), 0.0)
        last_rows = jnp.where(row8 == 7, pltpu.roll(d, 7, 0), last_rows)
        return jnp.concatenate([first_rows, last_rows], axis=0)

    def x_part(p, c, x, edge):
        h, beyond = V0[p, 0:ny, 0:128], V0[p + c, 0:ny, 0:128]
        a = pltpu.roll(ends[c][0:ny], (-8 * x - 1) % 128, 1)
        b = pltpu.roll(ends[c][0:ny], (125 - 8 * x) % 128, 1)
        t = V0[p, ny : ny + 8, 0:128]
        rows = jnp.concatenate(
            [
                jnp.where(row8 == 0, pltpu.roll(t, 1, 0), 0.0),
                jnp.where(row8 == 7, pltpu.roll(t, 7, 0), 0.0),
            ],
            axis=0,
        )
        edges = jnp.where(lane_own == 0, a, jnp.where(lane_own == 127, b, 0.0)) + rows
        near_sum = in_lanes(h) + in_rows(h)
        u = 1.2 * h + K * (near_sum + edges + beyond + inner[edge])
        u = jnp.where(exists(c), u, 0.0)
        return K * (6.0 * h - near_sum) - u, -K * h

    x_parts = {}
    for p, c, x, edge in ((1, -1, nx - 1, 0), (nx + 2, 1, 0, nx - 1)):
        x_parts[edge], x_parts[edge - c] = x_part(p, c, x, edge)

    def resid0(x):
        change = z_part(x) + y_part(x)
        if x in x_parts:
            change = change + x_parts[x]
        return R0[x] - w_ref[x] * change

    def smooth0():
        for dx in (-1, 0, 1):
            for x in {-1: (nx - 1,), 0: range(nx), 1: (0,)}[dx]:
                moved = pltpu.roll(z_ends(dx), (126 - 8 * x) % 128, 1)
                V0[x + 2 + dx * nx, :, 128:256] = moved
        for p, c in ((1, -1), (nx + 2, 1)):
            u = 1.2 * V0[p, 0:ny, 0:128] + K * own_sum(V0, p)
            U0[p, 0:ny, 0:128] = jnp.where(exists(c), u, 0.0)
        for p in range(2, nx + 2):
            c = V0[p]
            u = 1.2 * c + K * (around(c) + (V0[p - 1] + V0[p + 1]))
            U0[p] = jnp.where(mask0, u, 0.0)

    def assemble_faces():
        moved = z_ends(0)
        for x in range(nx):
            p = x + 2
            W0[p, :, 128:256] = pltpu.roll(moved, (122 - 8 * x) % 128, 1)
            IW[x] = 1.0 / w_ref[x]
            W0m[x] = pltpu.roll(W0[p, 0:ny, :], 1, 1)[:, 0:128]
            W0p[x] = pltpu.roll(W0[p, 0:ny, :], 255, 1)[:, 0:128]
            F0[x] = 0.2 * U0[p, 0:ny, 0:128] + V0[p, 0:ny, 0:128] + K * own_sum(U0, p)

    def own_sum(ref, p):
        col, wide = ref[p, :, 0:128], ref[p, 0:ny, :]
        vert = pltpu.roll(col, 1, 0)[0:ny] + pltpu.roll(col, ny + 7, 0)[0:ny]
        flat_sum = pltpu.roll(wide, 1, 1)[:, 0:128] + pltpu.roll(wide, 255, 1)[:, 0:128]
        return (vert + flat_sum) + (ref[p - 1, 0:ny, 0:128] + ref[p + 1, 0:ny, 0:128])

    b1 = 0.125 * coarsen0(resid0)
    b1 = [b1[8 * x : 8 * x + 8, :] for x in range(hx)]
    v1 = [jnp.where(lane8 < 64, K * b1[x] / jnp.where(lane8 < 64, w1[x], 1.0), 0.0) for x in range(hx)]
    pack1(S1v, SZv, v1)
    send_all(directions(2), pieces1(S1v, V1, SZv, RZv), hr.at[2])
    send_all(lates, late1(S1v, R3v, SZv, RCv), hr.at[4])
    pl.semaphore_wait(known.at[1], greeted)
    for k in others:
        spread(0, SW, GW, k).start()

    mask1 = coords(16, 128, 8, 64, 2, 2)
    mask_up = coords(16, 128, 8, 64, 1, 1)
    mask_own = coords(16, 128, 8, 64, 0, 0)
    lane1 = iota((16, 128), 1)

    def assemble1(S1, RZ, D):
        for dx in (-1, 0, 1):
            ends = jnp.where(lane1 % 16 < 3, RZ[dx + 1, 0], RZ[dx + 1, 1])
            for x in {-1: (hx - 2, hx - 1), 0: range(hx), 1: (0, 1)}[dx]:
                p = x + 3 + dx * hx
                moved = pltpu.roll(ends, (61 - 16 * x) % 128, 1)
                inner = S1[x] if dx == 0 else D[p, 0:8, :]
                D[p, 0:8, :] = jnp.where(lane8 < 64, inner, moved[0:8])
                D[p, 8:16, :] = jnp.where(lane8 < 64, D[p, 8:16, :], moved[8:16])

    def finish1(R3, RC, D):
        for x in range(hx):
            D[x + 3, 8:16, :] = jnp.where((row8 == 2) | (row8 == 5), R3[x], D[x + 3, 8:16, :])
        for slot, p, x in ((0, 2, hx - 1), (1, hx + 3, 0)):
            ends = jnp.where(lane8 % 16 < 3, RC[slot, 0], RC[slot, 1])
            moved = pltpu.roll(ends, (61 - 16 * x) % 128, 1)
            D[p, 8:16, :] = jnp.where(lane8 < 64, D[p, 8:16, :], moved)

    def smooth1(planes):
        for p in planes:
            c = V1[p]
            u = 1.2 * c + K * (around(c) + (V1[p - 1] + V1[p + 1]))
            U1[p] = jnp.where(plane_mask(mask1, p - 3, hx), u, 0.0)

    block = lane8 // 32

    def gathered(G):
        planes = []
        for gx in range(dims[0]):
            tiles = {}
            for t in range(dims[1] // 2):
                for z in range(dims[2]):
                    d0 = (gx * dims[1] + 2 * t) * dims[2] + z
                    tiles[t, z] = jnp.concatenate([G[d0], G[d0 + dims[2]]], axis=0)
            for x in range(4):
                parts = []
                for t in range(dims[1] // 2):
                    out = tiles[t, 0]
                    for z in range(1, dims[2]):
                        out = jnp.where(block == (x + z) % 4, tiles[t, z], out)
                    parts.append(out)
                planes.append(jnp.concatenate(parts, axis=0))
        return planes

    def turned(planes, by):
        return [
            pltpu.roll(c, (-32 * (X % 4) - by) % 128, 1) if X % 4 or by else c
            for X, c in enumerate(planes)
        ]

    def coarsen2(planes):
        c = len(planes) // 2
        for i in range(c):
            T3[i] = planes[2 * i] + planes[2 * i + 1]
        return [
            pair_sum(T3[i, pl.ds(0, 8, stride=2), :] + T3[i, pl.ds(1, 8, stride=2), :], 1)
            for i in range(c)
        ]

    take(second_part, hr.at[2])
    assemble1(S1v, RZv, V1)
    smooth1(range(2, hx + 4))

    def resid1(x):
        p = x + 3
        s = around(U1[p])[0:8, :] + (U1[p - 1, 0:8, :] + U1[p + 1, 0:8, :])
        return jnp.where(lane8 < 64, b1[x] - w1[x] * (6.0 * U1[p, 0:8, :] - s), 0.0)

    SB[...] = 0.125 * coarsen1(resid1, SB)
    GB[me] = SB[...]
    for k in others:
        spread(2, SB, GB, k).start()
    arrive(0, GW)
    turned_w2 = gathered(GW)
    scale2 = [K / q for q in turned_w2]
    w2 = turned(turned_w2, 0)
    w2m, w2p = [shifted(q, -1) for q in w2], [shifted(q, 1) for q in w2]
    unscale2 = [q * (1.0 / K) for q in w2]
    iw2 = [1.0 / q for q in w2]
    w3 = [0.0625 * q for q in coarsen2(w2)]
    around3 = {k: [shifted(q, 2 * k) if k else q for q in w3] for k in (-2, -1, 0, 1, 2)}
    iw3 = [1.0 / q for q in w3]
    inverse3 = {k: [shifted(q, 2 * k) if k else q for q in iw3] for k in (-1, 0, 1)}
    take(matrix_part, gr.at[1])
    take(face_part, hr.at[3])
    smooth0()
    assemble_faces()
    take(weight_part, hr.at[1])
    assemble1(S1w, RZw, W1)
    finish1(R3w, RCw, W1)
    for p in range(2, hx + 4):
        inside = plane_mask(mask_up if 0 <= p - 3 < hx else mask_own, p - 3, hx)
        IW1[p] = jnp.where(inside, 1.0, 0.0) / jnp.where(inside, W1[p], 1.0)
        W1m[p] = pltpu.roll(W1[p], 1, 1)
        W1p[p] = pltpu.roll(W1[p], 127, 1)
    take(late_part, hr.at[4])
    finish1(R3v, RCv, V1)
    smooth1(range(1, hx + 5))
    for p in range(2, hx + 4):
        c = U1[p]
        E10[p] = 0.2 * c + V1[p] + K * (around(c) + (U1[p - 1] + U1[p + 1]))

    def near(i, c, size):
        return jnp.clip(i + c, 0, size - 1)

    steps = (-1, 0, 1)
    blocks = [(x, dy, dz) for x in range(dims[0]) for dy in steps for dz in steps]
    rows = jnp.concatenate(
        [
            GM[(x * dims[1] + near(iy, dy, dims[1])) * dims[2] + near(iz, dz, dims[2])]
            for x, dy, dz in blocks
        ],
        axis=0,
    )
    order = pick(
        iota((128, 128), 0) == (iota((128, 128), 1) % 4) * 32 + iota((128, 128), 1) // 4
    )
    for h in range(2):
        MP[h] = exact_dot(rows[:, 128 * h : 128 * h + 128], order)
    far = jnp.full((8, 128), -99)
    wanted = {-1: jnp.where(row8 == 7, -1, far), 0: row8, 1: jnp.where(row8 == 0, 8, far)}
    held = {}
    for k in (-2, -1, 0, 1, 2):
        cell = lane8 + 2 * k
        held[k] = jnp.where((cell >= 0) & (cell < 128), cell // 4 - 8 * iz, -50)
    moves = (0, 1, -1)
    double = [(lane_row + k + 256) // 2 % 128 for k in moves]
    depth = jnp.where(lane_row < 96, lane_row, lane_row - 128)
    here = [jnp.clip((depth + k + 256) // 2 - 128 + 32 * iz, 0, 127) for k in moves]
    even = lane8 % 2 == 0
    E2[...] = jnp.zeros_like(E2)
    arrive(2, GB)

    v_turned = [b * r for b, r in zip(gathered(GB), scale2)]
    v2 = turned(v_turned, 0)
    lane_wide = iota((16, 128), 1)
    before = [jnp.where(lane_wide > 0, q, 0.0) for q in turned(v_turned, -1)]
    after = [jnp.where(lane_wide < 127, q, 0.0) for q in turned(v_turned, 1)]
    u2 = [1.2 * v + K * (s + (a + b)) for v, s, a, b in zip(v2, side_sum(v2), before, after)]
    s2 = [s + (shifted(u, -1) + shifted(u, 1)) for s, u in zip(side_sum(u2), u2)]
    r2 = [v * k - w * (6.0 * u - s) for v, k, w, u, s in zip(v2, unscale2, w2, u2, s2)]
    base2 = [0.2 * u + v + K * s for u, v, s in zip(u2, v2, s2)]
    b3 = [0.125 * q for q in coarsen2(r2)]
    v3 = [K * b * r for b, r in zip(b3, iw3)]
    u3 = [
        1.2 * v + K * (s + (shifted(v, -2) + shifted(v, 2))) for v, s in zip(v3, side_sum(v3))
    ]
    s3 = [s + (shifted(u, -2) + shifted(u, 2)) for s, u in zip(side_sum(u3), u3)]
    r3 = [b - w * (6.0 * u - s) for b, w, u, s in zip(b3, w3, u3, s3)]
    base3 = [0.2 * u + v + K * s for u, v, s in zip(u3, v3, s3)]
    base3 = {k: [shifted(q, 2 * k) if k else q for q in base3] for k in (-1, 0, 1)}
    c4 = len(r3) // 2
    for i in range(c4):
        T4[pl.ds(8 * i, 8), :] = r3[2 * i] + r3[2 * i + 1]
    half = 4 * c4
    b4 = 0.125 * pair_sum(T4[pl.ds(0, half, stride=2), :] + T4[pl.ds(1, half, stride=2), :], 2)
    chosen = jnp.where(row8 % 4 == lane8 % 4, b4, 0.0)
    low = row_sum(jnp.where(row8 < 4, chosen, 0.0))
    high = row_sum(jnp.where(row8 >= 4, chosen, 0.0))
    solved = [
        jnp.sum(MP[0, 8 * k : 8 * k + 8, :] * low + MP[1, 8 * k : 8 * k + 8, :] * high,
                axis=1, keepdims=True)
        for k in range(len(blocks))
    ]
    q3 = {}
    for k in (-2, -1, 0, 1, 2):
        e4 = []
        for x in range(dims[0]):
            plane = jnp.zeros((8, 128), F32)
            for dy in steps:
                found = jnp.zeros((8, 128), F32)
                for dz in steps:
                    value = solved[blocks.index((x, dy, dz))]
                    found = jnp.where(held[k] == wanted[dz], value, found)
                plane = jnp.where(row8 // 2 == iy + dy, row_sum(found), plane)
            e4.append(plane)
        q3[k] = [w * e4[i // 2] for i, w in enumerate(around3[k])]
    e3 = {}
    for k in (-1, 0, 1):
        sides = side_sum(q3[k])
        e3[k] = [
            (base + 0.2 * q + K * (s + (a + b))) * r
            for base, q, s, a, b, r in zip(
                base3[k], q3[k], sides, q3[k - 1], q3[k + 1], inverse3[k]
            )
        ]
    for i in range(2 * dims[0]):
        middle = e3[0][i]
        views = (middle, jnp.where(even, middle, e3[1][i]), jnp.where(even, e3[-1][i], middle))
        for k, e in enumerate(views):
            P3[k, i, pl.ds(0, 8, stride=2), :] = e
            P3[k, i, pl.ds(1, 8, stride=2), :] = e
    q2 = [w * P3[0, i // 2] for i, w in enumerate(w2)]
    sides = side_sum(q2)
    for i, (base, q, s) in enumerate(zip(base2, q2, sides)):
        ends = w2p[i] * P3[1, i // 2] + w2m[i] * P3[2, i // 2]
        E2[i + 1, 8:24, :] = (base + 0.2 * q + K * (s + ends)) * iw2[i]

    seen = jnp.concatenate([E2[4 * ix + i, pl.ds(6 + 4 * iy, 8), :] for i in range(6)], axis=0)
    for k in range(3):
        wide2 = lanes_of(pltpu.roll(seen.reshape((6, 8, 128)), 6, 1).reshape((48, 128)), here[k])
        for i in range(6):
            q = wide2[8 * i : 8 * i + 8]
            P2[k, i, pl.ds(0, 8, stride=2), :] = q
            P2[k, i, pl.ds(1, 8, stride=2), :] = q
    q1 = {p: W1[p] * P2[0, (p - 3) // 2 + 1] for p in range(1, hx + 5)}
    e1 = []
    for p in range(2, hx + 4):
        q, i = q1[p], (p - 3) // 2 + 1
        ends = W1p[p] * P2[1, i] + W1m[p] * P2[2, i]
        s = (pltpu.roll(q, 1, 0) + pltpu.roll(q, 15, 0)) + ends + (q1[p - 1] + q1[p + 1])
        e1.append((E10[p] + 0.2 * q + K * s) * IW1[p])
    wide1 = lanes_of(jnp.concatenate(e1, axis=0), double[0])
    for i in range(hx + 2):
        q = wide1[16 * i : 16 * i + 16]
        P1[i, pl.ds(0, 16, stride=2), :] = q
        P1[i, pl.ds(1, 16, stride=2), :] = q
    for k in (1, 2):
        wide1 = lanes_of(jnp.concatenate([e[0:8] for e in e1[1:-1]], axis=0), double[k])
        for i in range(hx):
            q = wide1[8 * i : 8 * i + 8]
            P1s[k - 1, i + 1, pl.ds(0, 8, stride=2), :] = q
            P1s[k - 1, i + 1, pl.ds(1, 8, stride=2), :] = q

    def scaled(p):
        i = (p - 2) // 2 + 1
        if not 2 <= p < nx + 2:
            return W0[p, 0:ny, 0:128] * P1[i, 0:16, :]
        edge = jnp.where(row8 < 4, P1[i, 16:24, :], P1[i, 24:32, :])
        return W0[p, :, 0:128] * jnp.concatenate([P1[i, 0:16, :], edge], axis=0)

    q0 = {p: scaled(p) for p in range(1, nx + 3)}
    for x in range(nx):
        p, i = x + 2, x // 2 + 1
        q = q0[p]
        ends = W0p[x] * P1s[0, i] + W0m[x] * P1s[1, i]
        vert = pltpu.roll(q, 1, 0)[0:ny] + pltpu.roll(q, ny + 7, 0)[0:ny]
        s = vert + ends + (q0[p - 1][0:ny] + q0[p + 1][0:ny])
        f_ref[x] = (F0[x] + 0.2 * q[0:ny] + K * s) * IW[x]

    take(everything, sent.at[0])


def fused(dims, sources, stiffness, coarse_inverse):
    nx, ny, nz = stiffness.shape
    n = dims[0] * dims[1] * dims[2]
    vm = lambda *s: pltpu.VMEM(s, F32)
    halo1 = [vm(8, 8, 128), vm(8, 128), vm(3, 2, 16, 128), vm(8, 8, 128), vm(2, 2, 8, 128)]
    result = pl.pallas_call(
        functools.partial(kernel, dims),
        out_shape=pltpu.VMEM((nx, ny, nz), F32),
        in_specs=[pl.BlockSpec(memory_space=pl.ANY)] * 3,
        out_specs=pl.BlockSpec(memory_space=pltpu.VMEM),
        scratch_shapes=[
            vm(nx, ny, nz), vm(nx, ny, nz), vm(*coarse_inverse.shape),
            vm(nx + 4, 24, 256), vm(nx + 4, 24, 256), vm(nx + 4, 24, 256),
            vm(14, 16, 128), vm(14, 16, 128), vm(14, 16, 128),
            vm(8, 16, 128), vm(32, 128), vm(2 * dims[0], 16, 128),
            vm(16, 128), vm(3, 2 * dims[0], 16, 128),
            vm(4 * dims[0] + 2, 32, 128), vm(3, 6, 16, 128), vm(10, 32, 128), vm(2, 10, 16, 128),
            vm(nx, ny, nz), vm(14, 16, 128), vm(2, 72 * dims[0], 128),
            vm(nx, ny, nz), vm(nx, ny, nz), vm(nx, ny, nz), vm(nx, ny, nz),
            vm(14, 16, 128), vm(14, 16, 128), vm(14, 16, 128),
            vm(ny, 128), vm(3, 2, ny + 8, 128),
        ]
        + halo1 + halo1
        + [
            vm(n, 8, 256), vm(n, 4, 128), vm(n, 4, 128), vm(4, 128), vm(4, 128),
            vm(2048, 128),
            pltpu.SemaphoreType.DMA((3,)), pltpu.SemaphoreType.DMA((1,)),
            pltpu.SemaphoreType.DMA((5,)), pltpu.SemaphoreType.DMA((3,)),
            pltpu.SemaphoreType.REGULAR((2,)),
        ],
        compiler_params=pltpu.CompilerParams(collective_id=0, has_side_effects=True),
        name="cycle",
    )(sources[0], stiffness, coarse_inverse)
    return result[None]


def solution(mesh):
    dims = tuple(mesh.shape[a] for a in ("gx", "gy", "gz"))

    def run(sources, stiffness, coarse_inverse):
        nx, ny, nz = stiffness.shape
        lanes = 128
        cells = coarse_inverse.shape[1]
        levels_fit = (
            sources.shape[0] == 1
            and nx == ny == 16
            and nz == lanes
            and dims[2] * nz == 4 * lanes
            and dims[1] * ny == 64
            and cells == 2 * lanes
            and dims[0] == 2
        )
        if levels_fit:
            return fused(dims, sources, stiffness, coarse_inverse)
        return per_device(sources, stiffness, coarse_inverse)

    in_specs = (P(None, "gx", "gy", "gz"), P("gx", "gy", "gz"), P(("gx", "gy", "gz"), None))
    out_specs = P(None, "gx", "gy", "gz")
    return jax.shard_map(
        run, mesh=mesh, in_specs=in_specs, out_specs=out_specs, check_vma=False
    )
```

```python
import functools
import jax
import jax.numpy as jnp
from jax import lax
from jax.experimental import pallas as pl
from jax.experimental.pallas import tpu as pltpu
from jax.sharding import PartitionSpec as P

damping = 0.8


def extended(cells, sides, width):
    for axis, dim in sides:
        count = lax.axis_size(axis)
        ends = count - 1
        head = lax.slice_in_dim(cells, 0, width, axis=dim)
        tail = lax.slice_in_dim(cells, cells.shape[dim] - width, cells.shape[dim], axis=dim)
        cells = jnp.concatenate(
            [
                lax.ppermute(tail, axis, [(i, (i + 1) % count) for i in range(ends)]),
                cells,
                lax.ppermute(head, axis, [((i + 1) % count, i) for i in range(ends)]),
            ],
            axis=dim,
        )
    return cells


def loop_sum(padded):
    total = padded[:, 2:, 1:-1, 1:-1] + padded[:, :-2, 1:-1, 1:-1]
    total = total + padded[:, 1:-1, 2:, 1:-1] + padded[:, 1:-1, :-2, 1:-1]
    total = total + padded[:, 1:-1, 1:-1, 2:] + padded[:, 1:-1, 1:-1, :-2]
    return total


def inner_part(values):
    return values[:, 1:-1, 1:-1, 1:-1]


def pre_smooth(source, weights):
    count = source.shape[0]
    stacked = jnp.concatenate([source, weights], axis=0)
    wide = extended(stacked, (("gx", 1), ("gy", 2), ("gz", 3)), 2)
    wide_source = wide[:count]
    wide_weights = wide[count:]
    safe_weights = jnp.where(wide_weights > 0.0, wide_weights, 1.0)
    first = damping * wide_source / (6.0 * safe_weights * safe_weights)
    first_scaled = wide_weights * first
    mid_weights = inner_part(wide_weights)
    mid_safe = inner_part(safe_weights)
    applied = mid_weights * (6.0 * inner_part(first_scaled) - loop_sum(first_scaled))
    second = inner_part(first) + damping * (inner_part(wide_source) - applied) / (
        6.0 * mid_safe * mid_safe
    )
    second_scaled = mid_weights * second
    answer = inner_part(second)
    resid = source - weights * (6.0 * inner_part(second_scaled) - loop_sum(second_scaled))
    return (answer, resid)


def post_smooth(answer, source, weights):
    scaled = weights * answer
    wide = extended(scaled, (("gx", 1), ("gy", 2), ("gz", 3)), 1)
    applied = weights * (6.0 * scaled - loop_sum(wide))
    return answer + damping * (source - applied) / (6.0 * weights * weights)


def coarsen(values):
    leading = values.shape[0]
    size_x, size_y, size_z = (values.shape[1], values.shape[2], values.shape[3])
    blocks = values.reshape((leading, size_x // 2, 2, size_y // 2, 2, size_z // 2, 2))
    return jnp.mean(blocks, axis=(2, 4, 6))


def refine(values):
    return jnp.repeat(jnp.repeat(jnp.repeat(values, 2, axis=1), 2, axis=2), 2, axis=3)


def per_device(sources, stiffness, coarse_inverse):
    weight_list = [stiffness[None]]
    for level in range(3):
        weight_list.append(0.5 * coarsen(weight_list[-1]))
    source_list = []
    answer_list = []
    current = sources
    for level in range(4):
        source_list.append(current)
        answer, resid = pre_smooth(current, weight_list[level])
        answer_list.append(answer)
        current = coarsen(resid)
    count = current.shape[0]
    flat_source = current.reshape((count, -1))
    solved = lax.dot_general(
        lax.all_gather(flat_source, ("gx", "gy", "gz"), axis=1, tiled=True),
        coarse_inverse,
        (((1,), (1,)), ((), ())),
        precision=lax.Precision.HIGHEST,
        preferred_element_type=jnp.float32,
    )
    correction = solved.reshape(current.shape)
    for level in range(3, -1, -1):
        correction = post_smooth(
            answer_list[level] + refine(correction), source_list[level], weight_list[level]
        )
    return correction


K = damping / 6.0
F32 = jnp.float32
BF = jnp.bfloat16


def iota(shape, dim):
    return lax.broadcasted_iota(jnp.int32, shape, dim)


def pick(condition):
    return jnp.where(condition, 1.0, 0.0).astype(BF)


def lanes_of(values, index):
    index = jnp.broadcast_to(index, values.shape)
    return jnp.take_along_axis(values, index, axis=1, mode="promise_in_bounds")


def exact_dot(values, chosen):
    total = None
    for _ in range(3):
        part = values.astype(BF)
        values = values - part.astype(F32)
        term = jnp.dot(part, chosen, preferred_element_type=F32)
        total = term if total is None else total + term
    return total


def around(c):
    rows, lanes = c.shape
    return (pltpu.roll(c, 1, 0) + pltpu.roll(c, rows - 1, 0)) + (
        pltpu.roll(c, 1, 1) + pltpu.roll(c, lanes - 1, 1)
    )


def side_sum(planes):
    rows = planes[0].shape[0]
    row = iota(planes[0].shape, 0)
    outs = []
    for p, c in enumerate(planes):
        s = jnp.where(row > 0, pltpu.roll(c, 1, 0), 0.0) + jnp.where(
            row < rows - 1, pltpu.roll(c, rows - 1, 0), 0.0
        )
        if p > 0:
            s = s + planes[p - 1]
        if p < len(planes) - 1:
            s = s + planes[p + 1]
        outs.append(s)
    return outs


def shifted(c, by):
    lane, lanes = iota(c.shape, 1), c.shape[1]
    inside = lane + by < lanes if by > 0 else lane + by >= 0
    return jnp.where(inside, pltpu.roll(c, -by % lanes, 1), 0.0)


def pair_sum(c, step):
    lanes = c.shape[1]
    even = (iota(c.shape, 1) // step) % 2 == 0
    return c + jnp.where(even, pltpu.roll(c, lanes - step, 1), pltpu.roll(c, step, 1))


def row_sum(c):
    for step in (4, 2, 1):
        c = c + pltpu.roll(c, step, 0)
    return c


def kernel(
    dims, b_hbm, w_hbm, m_hbm, f_ref,
    b_ref, w_ref, m_ref,
    V0, W0, U0, V1, W1, U1, TT, T2, T3, T4, P3, E2, P2, P1, P1s, IW, IW1, MP, W0m, W0p, F0, R0, W1m, W1p, E10,
    SZ0, RZ0, S1v, SZv, RZv, R3v, RCv, S1w, SZw, RZw, R3w, RCw,
    GM, GW, GB, SW, SB,
    tally, load, sent, hr, known,
):
    axes = ("gx", "gy", "gz")
    ix, iy, iz = (lax.axis_index(a) for a in axes)
    n = dims[0] * dims[1] * dims[2]
    me = (ix * dims[1] + iy) * dims[2] + iz

    def flip(i, bits):
        if bits == 1:
            return i + 1 - 2 * (i % 2)
        return {0: i, 2: (i + 2) % 4, 3: 3 - i}[bits]

    def mirrored(k):
        a, b, c = k
        y, z = dims[1] - 1 - iy, dims[2] - 1 - iz
        return ((ix + a) % dims[0], flip(y, b), flip(z, c))

    ends = (dims[1] - 1, dims[2] - 1)
    others = sorted(
        (c + (b + 1) // 2, a, b, c)
        for a in range(dims[0])
        for b in range(dims[1])
        for c in range(dims[2])
        if (a, b, c) != (0,) + ends
    )
    others = [k[1:] for k in others]

    barrier = pltpu.get_barrier_semaphore()

    def there(d):
        ok = None
        for i, s, c in zip((ix, iy, iz), dims, d):
            if c:
                t = (i + c < s) if c > 0 else (i + c >= 0)
                ok = t if ok is None else jnp.logical_and(ok, t)
        return ok

    def directions(most):
        found = []
        for dx in (-1, 0, 1):
            for dy in (-1, 0, 1):
                for dz in (-1, 0, 1):
                    if 0 < abs(dx) + abs(dy) + abs(dz) <= most:
                        found.append((dx, dy, dz))
        return sorted(found, key=lambda d: (-abs(d[1]), -abs(d[2]), abs(d[0])))

    def greet(sem):
        for d in directions(3):
            @pl.when(there(d))
            def _(d=d):
                pl.semaphore_signal(
                    sem, inc=1, device_id=(ix + d[0], iy + d[1], iz + d[2]),
                    device_id_type=pl.DeviceIdType.MESH,
                )

    loads = [
        pltpu.make_async_copy(src, dst, load.at[i])
        for i, src, dst in ((0, b_hbm, b_ref), (0, w_hbm, w_ref), (1, m_hbm, m_ref))
    ]
    for copy in loads:
        copy.start()
    nx, ny = b_ref.shape[0], b_ref.shape[1]
    hx, hy = nx // 2, ny // 2

    def clear(ref, *where):
        part = ref.at[where] if where else ref
        part[...] = jnp.zeros(part.shape, F32)

    own = (pl.ds(0, ny), pl.ds(0, 128))
    clear(V0, pl.ds(0, 2), *own)
    clear(V0, pl.ds(nx + 2, 2), *own)
    clear(V0, pl.ds(1, nx + 2), pl.ds(ny, 8), pl.ds(0, 128))
    clear(W0, pl.ds(1, 1), *own)
    clear(W0, pl.ds(nx + 2, 1), *own)
    clear(W0, pl.ds(2, nx), pl.ds(ny, 8), pl.ds(0, 128))
    for D in (V1, W1):
        clear(D, pl.ds(0, 3))
        clear(D, pl.ds(hx + 3, 3))
        clear(D, pl.ds(3, hx), pl.ds(8, 8))
    for D in (RZ0, RZv, R3v, RCv, RZw, R3w, RCw):
        clear(D)
    greet(barrier)

    def span(i, s):
        return 1 + jnp.where(i > 0, 1, 0) + jnp.where(i < s - 1, 1, 0)

    greeted = span(ix, dims[0]) * span(iy, dims[1]) * span(iz, dims[2]) - 1

    def send(src, dst, d, sem):
        pltpu.make_async_remote_copy(
            src_ref=src, dst_ref=dst, send_sem=sent.at[0], recv_sem=sem,
            device_id=(ix + d[0], iy + d[1], iz + d[2]), device_id_type=pl.DeviceIdType.MESH,
        ).start()

    def send_all(found, pieces, sem):
        def start(group):
            for d in group:
                ok = there((d[0], 0, d[2]))
                if ok is None:
                    send(*pieces(d), d, sem)
                else:
                    @pl.when(ok)
                    def _(d=d):
                        send(*pieces(d), d, sem)

        low = iy < dims[1] // 2
        for c, inward in ((1, low), (-1, jnp.logical_not(low)), (1, jnp.logical_not(low)), (-1, low)):
            group = [d for d in found if d[1] == c]
            if group:
                @pl.when(jnp.logical_and(inward, there((0, c, 0))))
                def _(group=group):
                    start(group)
        start([d for d in found if d[1] == 0])

    def span_x(c, size, pad, deep):
        if c == 0:
            return pl.ds(0, size), pl.ds(pad, size)
        if c > 0:
            return pl.ds(size - deep, deep), pl.ds(pad - deep, deep)
        return pl.ds(0, deep), pl.ds(pad + size, deep)

    def span_y(c, size, total, deep):
        if c == 0:
            return pl.ds(0, size), pl.ds(0, size)
        if c > 0:
            return pl.ds(size - deep, deep), pl.ds(total - deep, deep)
        return pl.ds(0, deep), pl.ds(size, deep)

    def flat(found):
        return [d for d in found if not d[2]]

    first = pl.ds(0, 128)

    def pieces0(d):
        dx, dy, dz = d
        if dz:
            a, b = span_y(dy, ny, ny + 8, 1)
            return SZ0.at[a], RZ0.at[1 - dx, (1 - dz) // 2, b]
        deep = 1 if dx and dy else 2
        a, b = span_x(dx, nx, 2, deep)
        e, f = span_y(dy, ny, ny + 8, deep)
        shifted = pl.ds(a.start + 2, a.size)
        return V0.at[shifted, e, first], V0.at[b, f, first]

    def faces0(d):
        a, b = span_x(d[0], nx, 2, 1)
        e, f = span_y(d[1], ny, ny + 8, 1)
        return W0.at[pl.ds(a.start + 2, a.size), e, first], W0.at[b, f, first]

    def pieces1(S1, D, SZ, RZ):
        def of(d):
            dx, dy, dz = d
            if dz:
                a, b = span_y(dy, 8, 16, 2)
                return SZ.at[a], RZ.at[1 - dx, (1 - dz) // 2, b]
            a, b = span_x(dx, hx, 3, 2 if dy else 3)
            e, f = span_y(dy, 8, 16, 2)
            return S1.at[a, e], D.at[b, f]
        return of

    def late1(S1, R3, SZ, RC):
        def of(d):
            dx, dy, dz = d
            if dz:
                row = pl.ds(7 if dy > 0 else 0, 1)
                return SZ.at[row], RC.at[(1 - dx) // 2, (1 - dz) // 2, row]
            row = pl.ds(5 if dy > 0 else 2, 1)
            return S1.at[:, row], R3.at[:, row]
        return of

    def matrix_rows(d):
        s, r = m_ref, GM.at[me]
        if d[2]:
            row = pl.ds(m_ref.shape[0] - 1 if d[2] > 0 else 0, 1)
            s, r = s.at[row], r.at[row]
        return s, r

    corners = [d for d in directions(3) if all(d)]
    lates = [(0, -1, 0), (0, 1, 0)] + corners

    def bytes_of(ref, sem):
        pltpu.make_async_copy(ref, ref, sem).wait()

    sides_y, sides_z = span(iy, dims[1]) - 1, span(iz, dims[2]) - 1

    def first_part(cy, cz):
        return 32 + 33 * cy + 32 * cz + cy * cz

    def face_part(cy, cz):
        return 16 + 16 * cy

    def second_part(cy, cz):
        return 24 + 20 * cy + 16 * cz + 2 * cy * cz

    def late_part(cy, cz):
        return 8 * cy + cy * cz

    def weight_part(cy, cz):
        return second_part(cy, cz) + late_part(cy, cz)

    def matrix_part(cy, cz):
        return 16 + 32 * cy + 4 * (1 + cy) * cz

    def waiting_part(cy, cz):
        parts = (weight_part, late_part, face_part, matrix_part)
        return sum(part(cy, cz) for part in parts) + 4 * (n - 1)

    def everything(cy, cz):
        parts = (first_part, second_part, waiting_part)
        return sum(part(cy, cz) for part in parts) + 4 * (n - 1)

    def take(part, sem):
        for cy in (1, 2):
            for cz in (1, 2):
                @pl.when(jnp.logical_and(sides_y == cy, sides_z == cz))
                def _(cy=cy, cz=cz):
                    bytes_of(tally.at[pl.ds(0, part(cy, cz))], sem)

    def spread(kind, src, dst, k):
        return pltpu.make_async_remote_copy(
            src_ref=src, dst_ref=dst.at[me], send_sem=sent.at[0], recv_sem=hr.at[kind],
            device_id=mirrored(k), device_id_type=pl.DeviceIdType.MESH,
        )

    def arrive(kind, dst):
        bytes_of(dst.at[pl.ds(0, n - 1)], hr.at[kind])


    bytes_of(tally.at[pl.ds(0, 2 * nx * ny)], load.at[0])
    lane16 = iota((ny, 128), 1)
    packed = jnp.zeros((ny, 128), F32)
    for x in range(nx):
        w = w_ref[x]
        v = K * b_ref[x] / w
        V0[x + 2, 0:ny, 0:128] = v
        W0[x + 2, 0:ny, 0:128] = w
        for a, q in enumerate((v, w)):
            start = 8 * x + 4 * a
            moved = pltpu.roll(q, (start + 2) % 128, 1)
            packed = jnp.where((lane16 >= start) & (lane16 < start + 4), moved, packed)
    SZ0[...] = packed

    pl.semaphore_wait(barrier, greeted)
    send_all(directions(2), pieces0, hr.at[0])
    greet(known.at[0])
    send_all(flat(directions(1)), faces0, hr.at[1])

    lane_row = iota((1, 128), 1)
    low_half = jnp.minimum(2 * lane_row, 126)

    def coarsen0(planes):
        for i in range(hx):
            TT[i] = planes(2 * i) + planes(2 * i + 1)
        rows = [
            TT[i, pl.ds(0, hy, stride=2), :] + TT[i, pl.ds(1, hy, stride=2), :] for i in range(hx)
        ]
        rows = jnp.concatenate(rows, axis=0)
        return lanes_of(rows, low_half) + lanes_of(rows, low_half + 1)

    held_x = (lane_row // 32 + 4 - iz) % 4
    pairs = 2 * (lane_row % 32)

    def coarsen1(planes, SG):
        for i in range(hx // 2):
            T2[pl.ds(8 * i, 8), :] = planes(2 * i) + planes(2 * i + 1)
        pieces = [
            T2[pl.ds(8 * x, 4, stride=2), :] + T2[pl.ds(8 * x + 1, 4, stride=2), :]
            for x in range(4)
        ]
        rows = [jnp.concatenate(pieces[i : i + 2], axis=0) for i in (0, 2)]
        sums = [lanes_of(r, pairs) + lanes_of(r, pairs + 1) for r in rows]
        parts = [sums[x // 2][4 * (x % 2) : 4 * (x % 2) + 4] for x in range(4)]
        total = parts[0]
        for x in range(1, 4):
            total = jnp.where(held_x == x, parts[x], total)
        return total

    lane8 = iota((8, 128), 1)

    def pack1(S1, SZ, planes):
        out = jnp.zeros((8, 128), F32)
        for x in range(hx):
            q = planes[x]
            S1[x] = q
            s = 16 * x
            h = (s + 64) % 128
            out = jnp.where((lane8 >= h) & (lane8 < h + 3), pltpu.roll(q, (h - 61) % 128, 1), out)
            out = jnp.where(
                (lane8 >= s + 3) & (lane8 < s + 6), pltpu.roll(q, (s + 3) % 128, 1), out
            )
        SZ[...] = out

    w1 = 0.0625 * coarsen0(lambda x: w_ref[x])
    w1 = [w1[8 * x : 8 * x + 8, :] for x in range(hx)]
    pack1(S1w, SZw, w1)
    SW[...] = 0.0625 * coarsen1(lambda x: w1[x], SW)
    GW[me] = SW[...]
    loads[2].wait()
    GM[me] = m_ref[...]
    send_all(directions(2), pieces1(S1w, W1, SZw, RZw), hr.at[1])
    send_all(lates, late1(S1w, R3w, SZw, RCw), hr.at[1])
    send_all(directions(3), matrix_rows, hr.at[1])
    pl.semaphore_wait(known.at[0], greeted)
    greet(known.at[1])

    def coords(rows, lanes, cy, cz, by, bz):
        r, l = iota((rows, lanes), 0), iota((rows, lanes), 1)
        y = jnp.where(r < cy + (rows - cy) // 2, r, r - rows)
        z = jnp.where(l < cz + (lanes - cz) // 2, l, l - lanes)
        gy, gz = y + iy * cy, z + iz * cz
        ok = (gy >= 0) & (gy < dims[1] * cy) & (gz >= 0) & (gz < dims[2] * cz)
        near = (y >= -by) & (y < cy + by) & (z >= -bz) & (z < cz + bz)
        return jnp.where(ok & near, 1, 0)

    def plane_mask(base, x, cx):
        if 0 <= x < cx:
            return base > 0
        gx = x + ix * cx
        inside = jnp.where((gx >= 0) & (gx < dims[0] * cx), 1, 0)
        return base * inside > 0

    row8 = iota((8, 128), 0)
    row16, lane_own = iota((ny, 128), 0), iota((ny, 128), 1)

    def in_lanes(c):
        return shifted(c, -1) + shifted(c, 1)

    def in_rows(c):
        return jnp.where(row16 > 0, pltpu.roll(c, 1, 0), 0.0) + jnp.where(
            row16 < ny - 1, pltpu.roll(c, ny - 1, 0), 0.0
        )

    def beside(planes, x):
        found = [planes[i] for i in (x - 1, x + 1) if 0 <= i < nx]
        return found[0] + found[1] if len(found) > 1 else found[0]

    inner = [V0[x + 2, 0:ny, 0:128] for x in range(nx)]
    inner_u = [
        1.2 * c + K * (in_rows(c) + in_lanes(c) + beside(inner, x)) for x, c in enumerate(inner)
    ]
    for x, u in enumerate(inner_u):
        near_sum = in_rows(u) + in_lanes(u) + beside(inner_u, x)
        R0[x] = b_ref[x] - w_ref[x] * (6.0 * u - near_sum)
    kind = lane_own % 8
    packed = SZ0[...]
    own_ends = jnp.where(kind == 1, pltpu.roll(packed, 127, 1), pltpu.roll(packed, 1, 1))
    has_z = ((kind == 1) & (iz > 0)) | ((kind == 2) & (iz < dims[2] - 1))
    has_y = ((row8 == 7) & (iy > 0)) | ((row8 == 0) & (iy < dims[1] - 1))

    def exists(c):
        return (ix + c >= 0) & (ix + c < dims[0])

    take(first_part, hr.at[0])
    mask0 = coords(24, 256, ny, 128, 1, 1) > 0
    lane24 = iota((24, 128), 1)

    def z_ends(dx):
        return jnp.where(lane24 % 4 >= 2, RZ0[dx + 1, 1], RZ0[dx + 1, 0])

    ends = {dx: z_ends(dx) for dx in (-1, 0, 1)}

    def z_change():
        full, c = ends[0], ends[0][0:ny]
        above, below = pltpu.roll(full, 1, 1), pltpu.roll(full, 127, 1)
        left = pltpu.roll(jnp.where(lane_own >= 120, ends[-1][0:ny], c), 8, 1)
        right = pltpu.roll(jnp.where(lane_own < 8, ends[1][0:ny], c), 120, 1)
        outer = jnp.where(kind == 1, above[0:ny], below[0:ny])
        vert = (pltpu.roll(full, 1, 0) + pltpu.roll(full, ny + 7, 0))[0:ny]
        u = 1.2 * c + K * (outer + own_ends + vert + left + right)
        u = jnp.where(has_z, u, 0.0)
        across = jnp.where(lane_own >= 8, left, 0.0) + jnp.where(lane_own < 120, right, 0.0)
        d = K * (6.0 * c - in_rows(c) - across) - u
        low = jnp.where(kind == 1, d, -K * above[0:ny])
        high = jnp.where(kind == 2, d, -K * below[0:ny])
        swapped = jnp.where(lane8 % 8 == 1, below[ny:], above[ny:])
        return low, high, swapped

    low_end, high_end, edge_ends = z_change()
    side = [V0[p, ny : ny + 8, 0:128] for p in range(1, nx + 3)]

    def z_part(x):
        a = pltpu.roll(low_end, (-8 * x - 1) % 128, 1)
        b = pltpu.roll(high_end, (125 - 8 * x) % 128, 1)
        return jnp.where(lane_own < 2, a, jnp.where(lane_own >= 126, b, 0.0))

    def y_part(x):
        c = side[x + 1]
        ends_x = pltpu.roll(edge_ends, (126 - 8 * x) % 128, 1)
        flat_sum = in_lanes(c)
        edges = jnp.where((lane8 == 0) | (lane8 == 127), ends_x, 0.0)
        adjacent = jnp.where(
            row8 == 7, pltpu.roll(inner[x][0:8], 7, 0), pltpu.roll(inner[x][8:16], 1, 0)
        )
        outer = jnp.where(row8 == 7, pltpu.roll(c, 1, 0), pltpu.roll(c, 7, 0))
        u = 1.2 * c + K * (flat_sum + edges + adjacent + outer + side[x] + side[x + 2])
        u = jnp.where(has_y, u, 0.0)
        d = K * (6.0 * c - flat_sum - beside(side[1:-1], x)) - u
        first_rows = jnp.where(row8 == 1, -K * pltpu.roll(c, 2, 0), 0.0)
        first_rows = jnp.where(row8 == 0, pltpu.roll(d, 1, 0), first_rows)
        last_rows = jnp.where(row8 == 6, -K * pltpu.roll(c, 6, 0), 0.0)
        last_rows = jnp.where(row8 == 7, pltpu.roll(d, 7, 0), last_rows)
        return jnp.concatenate([first_rows, last_rows], axis=0)

    def x_part(p, c, x, edge):
        h, beyond = V0[p, 0:ny, 0:128], V0[p + c, 0:ny, 0:128]
        a = pltpu.roll(ends[c][0:ny], (-8 * x - 1) % 128, 1)
        b = pltpu.roll(ends[c][0:ny], (125 - 8 * x) % 128, 1)
        t = V0[p, ny : ny + 8, 0:128]
        rows = jnp.concatenate(
            [
                jnp.where(row8 == 0, pltpu.roll(t, 1, 0), 0.0),
                jnp.where(row8 == 7, pltpu.roll(t, 7, 0), 0.0),
            ],
            axis=0,
        )
        edges = jnp.where(lane_own == 0, a, jnp.where(lane_own == 127, b, 0.0)) + rows
        near_sum = in_lanes(h) + in_rows(h)
        u = 1.2 * h + K * (near_sum + edges + beyond + inner[edge])
        u = jnp.where(exists(c), u, 0.0)
        return K * (6.0 * h - near_sum) - u, -K * h

    x_parts = {}
    for p, c, x, edge in ((1, -1, nx - 1, 0), (nx + 2, 1, 0, nx - 1)):
        x_parts[edge], x_parts[edge - c] = x_part(p, c, x, edge)

    def resid0(x):
        change = z_part(x) + y_part(x)
        if x in x_parts:
            change = change + x_parts[x]
        return R0[x] - w_ref[x] * change

    def smooth0():
        for dx in (-1, 0, 1):
            for x in {-1: (nx - 1,), 0: range(nx), 1: (0,)}[dx]:
                moved = pltpu.roll(z_ends(dx), (126 - 8 * x) % 128, 1)
                V0[x + 2 + dx * nx, :, 128:256] = moved
        for p, c in ((1, -1), (nx + 2, 1)):
            u = 1.2 * V0[p, 0:ny, 0:128] + K * own_sum(V0, p)
            U0[p, 0:ny, 0:128] = jnp.where(exists(c), u, 0.0)
        for p in range(2, nx + 2):
            c = V0[p]
            u = 1.2 * c + K * (around(c) + (V0[p - 1] + V0[p + 1]))
            U0[p] = jnp.where(mask0, u, 0.0)

    def assemble_faces():
        moved = z_ends(0)
        for x in range(nx):
            p = x + 2
            W0[p, :, 128:256] = pltpu.roll(moved, (122 - 8 * x) % 128, 1)
            IW[x] = 1.0 / w_ref[x]
            W0m[x] = pltpu.roll(W0[p, 0:ny, :], 1, 1)[:, 0:128]
            W0p[x] = pltpu.roll(W0[p, 0:ny, :], 255, 1)[:, 0:128]
            F0[x] = 0.2 * U0[p, 0:ny, 0:128] + V0[p, 0:ny, 0:128] + K * own_sum(U0, p)

    def own_sum(ref, p):
        col, wide = ref[p, :, 0:128], ref[p, 0:ny, :]
        vert = pltpu.roll(col, 1, 0)[0:ny] + pltpu.roll(col, ny + 7, 0)[0:ny]
        flat_sum = pltpu.roll(wide, 1, 1)[:, 0:128] + pltpu.roll(wide, 255, 1)[:, 0:128]
        return (vert + flat_sum) + (ref[p - 1, 0:ny, 0:128] + ref[p + 1, 0:ny, 0:128])

    b1 = 0.125 * coarsen0(resid0)
    b1 = [b1[8 * x : 8 * x + 8, :] for x in range(hx)]
    v1 = [jnp.where(lane8 < 64, K * b1[x] / jnp.where(lane8 < 64, w1[x], 1.0), 0.0) for x in range(hx)]
    pack1(S1v, SZv, v1)
    send_all(directions(2), pieces1(S1v, V1, SZv, RZv), hr.at[2])
    send_all(lates, late1(S1v, R3v, SZv, RCv), hr.at[1])
    pl.semaphore_wait(known.at[1], greeted)
    for k in others:
        spread(1, SW, GW, k).start()

    mask1 = coords(16, 128, 8, 64, 2, 2)
    mask_up = coords(16, 128, 8, 64, 1, 1)
    mask_own = coords(16, 128, 8, 64, 0, 0)
    lane1 = iota((16, 128), 1)

    def assemble1(S1, RZ, D):
        for dx in (-1, 0, 1):
            ends = jnp.where(lane1 % 16 < 3, RZ[dx + 1, 0], RZ[dx + 1, 1])
            for x in {-1: (hx - 2, hx - 1), 0: range(hx), 1: (0, 1)}[dx]:
                p = x + 3 + dx * hx
                moved = pltpu.roll(ends, (61 - 16 * x) % 128, 1)
                inner = S1[x] if dx == 0 else D[p, 0:8, :]
                D[p, 0:8, :] = jnp.where(lane8 < 64, inner, moved[0:8])
                D[p, 8:16, :] = jnp.where(lane8 < 64, D[p, 8:16, :], moved[8:16])

    def finish1(R3, RC, D):
        for x in range(hx):
            D[x + 3, 8:16, :] = jnp.where((row8 == 2) | (row8 == 5), R3[x], D[x + 3, 8:16, :])
        for slot, p, x in ((0, 2, hx - 1), (1, hx + 3, 0)):
            ends = jnp.where(lane8 % 16 < 3, RC[slot, 0], RC[slot, 1])
            moved = pltpu.roll(ends, (61 - 16 * x) % 128, 1)
            D[p, 8:16, :] = jnp.where(lane8 < 64, D[p, 8:16, :], moved)

    def smooth1(planes):
        for p in planes:
            c = V1[p]
            u = 1.2 * c + K * (around(c) + (V1[p - 1] + V1[p + 1]))
            U1[p] = jnp.where(plane_mask(mask1, p - 3, hx), u, 0.0)

    block = lane8 // 32

    def gathered(G):
        planes = []
        for gx in range(dims[0]):
            tiles = {}
            for t in range(dims[1] // 2):
                for z in range(dims[2]):
                    d0 = (gx * dims[1] + 2 * t) * dims[2] + z
                    tiles[t, z] = jnp.concatenate([G[d0], G[d0 + dims[2]]], axis=0)
            for x in range(4):
                parts = []
                for t in range(dims[1] // 2):
                    out = tiles[t, 0]
                    for z in range(1, dims[2]):
                        out = jnp.where(block == (x + z) % 4, tiles[t, z], out)
                    parts.append(out)
                planes.append(jnp.concatenate(parts, axis=0))
        return planes

    def turned(planes, by):
        return [
            pltpu.roll(c, (-32 * (X % 4) - by) % 128, 1) if X % 4 or by else c
            for X, c in enumerate(planes)
        ]

    def coarsen2(planes):
        c = len(planes) // 2
        for i in range(c):
            T3[i] = planes[2 * i] + planes[2 * i + 1]
        return [
            pair_sum(T3[i, pl.ds(0, 8, stride=2), :] + T3[i, pl.ds(1, 8, stride=2), :], 1)
            for i in range(c)
        ]

    take(second_part, hr.at[2])
    assemble1(S1v, RZv, V1)
    smooth1(range(2, hx + 4))

    def resid1(x):
        p = x + 3
        s = around(U1[p])[0:8, :] + (U1[p - 1, 0:8, :] + U1[p + 1, 0:8, :])
        return jnp.where(lane8 < 64, b1[x] - w1[x] * (6.0 * U1[p, 0:8, :] - s), 0.0)

    SB[...] = 0.125 * coarsen1(resid1, SB)
    GB[me] = SB[...]
    for k in others:
        spread(3, SB, GB, k).start()
    take(waiting_part, hr.at[1])
    turned_w2 = gathered(GW)
    scale2 = [K / q for q in turned_w2]
    w2 = turned(turned_w2, 0)
    w2m, w2p = [shifted(q, -1) for q in w2], [shifted(q, 1) for q in w2]
    unscale2 = [q * (1.0 / K) for q in w2]
    iw2 = [1.0 / q for q in w2]
    w3 = [0.0625 * q for q in coarsen2(w2)]
    around3 = {k: [shifted(q, 2 * k) if k else q for q in w3] for k in (-2, -1, 0, 1, 2)}
    iw3 = [1.0 / q for q in w3]
    inverse3 = {k: [shifted(q, 2 * k) if k else q for q in iw3] for k in (-1, 0, 1)}
    smooth0()
    assemble_faces()
    assemble1(S1w, RZw, W1)
    finish1(R3w, RCw, W1)
    for p in range(2, hx + 4):
        inside = plane_mask(mask_up if 0 <= p - 3 < hx else mask_own, p - 3, hx)
        IW1[p] = jnp.where(inside, 1.0, 0.0) / jnp.where(inside, W1[p], 1.0)
        W1m[p] = pltpu.roll(W1[p], 1, 1)
        W1p[p] = pltpu.roll(W1[p], 127, 1)
    finish1(R3v, RCv, V1)
    smooth1(range(1, hx + 5))
    for p in range(2, hx + 4):
        c = U1[p]
        E10[p] = 0.2 * c + V1[p] + K * (around(c) + (U1[p - 1] + U1[p + 1]))

    def near(i, c, size):
        return jnp.clip(i + c, 0, size - 1)

    steps = (-1, 0, 1)
    blocks = [(x, dy, dz) for x in range(dims[0]) for dy in steps for dz in steps]
    rows = jnp.concatenate(
        [
            GM[(x * dims[1] + near(iy, dy, dims[1])) * dims[2] + near(iz, dz, dims[2])]
            for x, dy, dz in blocks
        ],
        axis=0,
    )
    order = pick(
        iota((128, 128), 0) == (iota((128, 128), 1) % 4) * 32 + iota((128, 128), 1) // 4
    )
    for h in range(2):
        MP[h] = exact_dot(rows[:, 128 * h : 128 * h + 128], order)
    far = jnp.full((8, 128), -99)
    wanted = {-1: jnp.where(row8 == 7, -1, far), 0: row8, 1: jnp.where(row8 == 0, 8, far)}
    held = {}
    for k in (-2, -1, 0, 1, 2):
        cell = lane8 + 2 * k
        held[k] = jnp.where((cell >= 0) & (cell < 128), cell // 4 - 8 * iz, -50)
    moves = (0, 1, -1)
    double = [(lane_row + k + 256) // 2 % 128 for k in moves]
    depth = jnp.where(lane_row < 96, lane_row, lane_row - 128)
    here = [jnp.clip((depth + k + 256) // 2 - 128 + 32 * iz, 0, 127) for k in moves]
    even = lane8 % 2 == 0
    E2[...] = jnp.zeros_like(E2)
    arrive(3, GB)

    v_turned = [b * r for b, r in zip(gathered(GB), scale2)]
    v2 = turned(v_turned, 0)
    lane_wide = iota((16, 128), 1)
    before = [jnp.where(lane_wide > 0, q, 0.0) for q in turned(v_turned, -1)]
    after = [jnp.where(lane_wide < 127, q, 0.0) for q in turned(v_turned, 1)]
    u2 = [1.2 * v + K * (s + (a + b)) for v, s, a, b in zip(v2, side_sum(v2), before, after)]
    s2 = [s + (shifted(u, -1) + shifted(u, 1)) for s, u in zip(side_sum(u2), u2)]
    r2 = [v * k - w * (6.0 * u - s) for v, k, w, u, s in zip(v2, unscale2, w2, u2, s2)]
    base2 = [0.2 * u + v + K * s for u, v, s in zip(u2, v2, s2)]
    b3 = [0.125 * q for q in coarsen2(r2)]
    v3 = [K * b * r for b, r in zip(b3, iw3)]
    u3 = [
        1.2 * v + K * (s + (shifted(v, -2) + shifted(v, 2))) for v, s in zip(v3, side_sum(v3))
    ]
    s3 = [s + (shifted(u, -2) + shifted(u, 2)) for s, u in zip(side_sum(u3), u3)]
    r3 = [b - w * (6.0 * u - s) for b, w, u, s in zip(b3, w3, u3, s3)]
    base3 = [0.2 * u + v + K * s for u, v, s in zip(u3, v3, s3)]
    base3 = {k: [shifted(q, 2 * k) if k else q for q in base3] for k in (-1, 0, 1)}
    c4 = len(r3) // 2
    for i in range(c4):
        T4[pl.ds(8 * i, 8), :] = r3[2 * i] + r3[2 * i + 1]
    half = 4 * c4
    b4 = 0.125 * pair_sum(T4[pl.ds(0, half, stride=2), :] + T4[pl.ds(1, half, stride=2), :], 2)
    chosen = jnp.where(row8 % 4 == lane8 % 4, b4, 0.0)
    low = row_sum(jnp.where(row8 < 4, chosen, 0.0))
    high = row_sum(jnp.where(row8 >= 4, chosen, 0.0))
    solved = [
        jnp.sum(MP[0, 8 * k : 8 * k + 8, :] * low + MP[1, 8 * k : 8 * k + 8, :] * high,
                axis=1, keepdims=True)
        for k in range(len(blocks))
    ]
    q3 = {}
    for k in (-2, -1, 0, 1, 2):
        e4 = []
        for x in range(dims[0]):
            plane = jnp.zeros((8, 128), F32)
            for dy in steps:
                found = jnp.zeros((8, 128), F32)
                for dz in steps:
                    value = solved[blocks.index((x, dy, dz))]
                    found = jnp.where(held[k] == wanted[dz], value, found)
                plane = jnp.where(row8 // 2 == iy + dy, row_sum(found), plane)
            e4.append(plane)
        q3[k] = [w * e4[i // 2] for i, w in enumerate(around3[k])]
    e3 = {}
    for k in (-1, 0, 1):
        sides = side_sum(q3[k])
        e3[k] = [
            (base + 0.2 * q + K * (s + (a + b))) * r
            for base, q, s, a, b, r in zip(
                base3[k], q3[k], sides, q3[k - 1], q3[k + 1], inverse3[k]
            )
        ]
    for i in range(2 * dims[0]):
        middle = e3[0][i]
        views = (middle, jnp.where(even, middle, e3[1][i]), jnp.where(even, e3[-1][i], middle))
        for k, e in enumerate(views):
            P3[k, i, pl.ds(0, 8, stride=2), :] = e
            P3[k, i, pl.ds(1, 8, stride=2), :] = e
    q2 = [w * P3[0, i // 2] for i, w in enumerate(w2)]
    sides = side_sum(q2)
    for i, (base, q, s) in enumerate(zip(base2, q2, sides)):
        ends = w2p[i] * P3[1, i // 2] + w2m[i] * P3[2, i // 2]
        E2[i + 1, 8:24, :] = (base + 0.2 * q + K * (s + ends)) * iw2[i]

    seen = jnp.concatenate([E2[4 * ix + i, pl.ds(6 + 4 * iy, 8), :] for i in range(6)], axis=0)
    for k in range(3):
        wide2 = lanes_of(pltpu.roll(seen.reshape((6, 8, 128)), 6, 1).reshape((48, 128)), here[k])
        for i in range(6):
            q = wide2[8 * i : 8 * i + 8]
            P2[k, i, pl.ds(0, 8, stride=2), :] = q
            P2[k, i, pl.ds(1, 8, stride=2), :] = q
    q1 = {p: W1[p] * P2[0, (p - 3) // 2 + 1] for p in range(1, hx + 5)}
    e1 = []
    for p in range(2, hx + 4):
        q, i = q1[p], (p - 3) // 2 + 1
        ends = W1p[p] * P2[1, i] + W1m[p] * P2[2, i]
        s = (pltpu.roll(q, 1, 0) + pltpu.roll(q, 15, 0)) + ends + (q1[p - 1] + q1[p + 1])
        e1.append((E10[p] + 0.2 * q + K * s) * IW1[p])
    wide1 = lanes_of(jnp.concatenate(e1, axis=0), double[0])
    for i in range(hx + 2):
        q = wide1[16 * i : 16 * i + 16]
        P1[i, pl.ds(0, 16, stride=2), :] = q
        P1[i, pl.ds(1, 16, stride=2), :] = q
    for k in (1, 2):
        wide1 = lanes_of(jnp.concatenate([e[0:8] for e in e1[1:-1]], axis=0), double[k])
        for i in range(hx):
            q = wide1[8 * i : 8 * i + 8]
            P1s[k - 1, i + 1, pl.ds(0, 8, stride=2), :] = q
            P1s[k - 1, i + 1, pl.ds(1, 8, stride=2), :] = q

    def scaled(p):
        i = (p - 2) // 2 + 1
        if not 2 <= p < nx + 2:
            return W0[p, 0:ny, 0:128] * P1[i, 0:16, :]
        edge = jnp.where(row8 < 4, P1[i, 16:24, :], P1[i, 24:32, :])
        return W0[p, :, 0:128] * jnp.concatenate([P1[i, 0:16, :], edge], axis=0)

    q0 = {p: scaled(p) for p in range(1, nx + 3)}
    for x in range(nx):
        p, i = x + 2, x // 2 + 1
        q = q0[p]
        ends = W0p[x] * P1s[0, i] + W0m[x] * P1s[1, i]
        vert = pltpu.roll(q, 1, 0)[0:ny] + pltpu.roll(q, ny + 7, 0)[0:ny]
        s = vert + ends + (q0[p - 1][0:ny] + q0[p + 1][0:ny])
        f_ref[x] = (F0[x] + 0.2 * q[0:ny] + K * s) * IW[x]

    take(everything, sent.at[0])


def fused(dims, sources, stiffness, coarse_inverse):
    nx, ny, nz = stiffness.shape
    n = dims[0] * dims[1] * dims[2]
    vm = lambda *s: pltpu.VMEM(s, F32)
    halo1 = [vm(8, 8, 128), vm(8, 128), vm(3, 2, 16, 128), vm(8, 8, 128), vm(2, 2, 8, 128)]
    result = pl.pallas_call(
        functools.partial(kernel, dims),
        out_shape=pltpu.VMEM((nx, ny, nz), F32),
        in_specs=[pl.BlockSpec(memory_space=pl.ANY)] * 3,
        out_specs=pl.BlockSpec(memory_space=pltpu.VMEM),
        scratch_shapes=[
            vm(nx, ny, nz), vm(nx, ny, nz), vm(*coarse_inverse.shape),
            vm(nx + 4, 24, 256), vm(nx + 4, 24, 256), vm(nx + 4, 24, 256),
            vm(14, 16, 128), vm(14, 16, 128), vm(14, 16, 128),
            vm(8, 16, 128), vm(32, 128), vm(2 * dims[0], 16, 128),
            vm(16, 128), vm(3, 2 * dims[0], 16, 128),
            vm(4 * dims[0] + 2, 32, 128), vm(3, 6, 16, 128), vm(10, 32, 128), vm(2, 10, 16, 128),
            vm(nx, ny, nz), vm(14, 16, 128), vm(2, 72 * dims[0], 128),
            vm(nx, ny, nz), vm(nx, ny, nz), vm(nx, ny, nz), vm(nx, ny, nz),
            vm(14, 16, 128), vm(14, 16, 128), vm(14, 16, 128),
            vm(ny, 128), vm(3, 2, ny + 8, 128),
        ]
        + halo1 + halo1
        + [
            vm(n, 8, 256), vm(n, 4, 128), vm(n, 4, 128), vm(4, 128), vm(4, 128),
            vm(2048, 128),
            pltpu.SemaphoreType.DMA((2,)), pltpu.SemaphoreType.DMA((1,)),
            pltpu.SemaphoreType.DMA((4,)),
            pltpu.SemaphoreType.REGULAR((2,)),
        ],
        compiler_params=pltpu.CompilerParams(collective_id=0, has_side_effects=True),
        name="cycle",
    )(sources[0], stiffness, coarse_inverse)
    return result[None]


def solution(mesh):
    dims = tuple(mesh.shape[a] for a in ("gx", "gy", "gz"))

    def run(sources, stiffness, coarse_inverse):
        nx, ny, nz = stiffness.shape
        lanes = 128
        cells = coarse_inverse.shape[1]
        levels_fit = (
            sources.shape[0] == 1
            and nx == ny == 16
            and nz == lanes
            and dims[2] * nz == 4 * lanes
            and dims[1] * ny == 64
            and cells == 2 * lanes
            and dims[0] == 2
        )
        if levels_fit:
            return fused(dims, sources, stiffness, coarse_inverse)
        return per_device(sources, stiffness, coarse_inverse)

    in_specs = (P(None, "gx", "gy", "gz"), P("gx", "gy", "gz"), P(("gx", "gy", "gz"), None))
    out_specs = P(None, "gx", "gy", "gz")
    return jax.shard_map(
        run, mesh=mesh, in_specs=in_specs, out_specs=out_specs, check_vma=False
    )
```

```python
import functools
import jax
import jax.numpy as jnp
from jax import lax
from jax.experimental import pallas as pl
from jax.experimental.pallas import tpu as pltpu
from jax.sharding import PartitionSpec as P

damping = 0.8


def extended(cells, sides, width):
    for axis, dim in sides:
        count = lax.axis_size(axis)
        ends = count - 1
        head = lax.slice_in_dim(cells, 0, width, axis=dim)
        tail = lax.slice_in_dim(cells, cells.shape[dim] - width, cells.shape[dim], axis=dim)
        cells = jnp.concatenate(
            [
                lax.ppermute(tail, axis, [(i, (i + 1) % count) for i in range(ends)]),
                cells,
                lax.ppermute(head, axis, [((i + 1) % count, i) for i in range(ends)]),
            ],
            axis=dim,
        )
    return cells


def loop_sum(padded):
    total = padded[:, 2:, 1:-1, 1:-1] + padded[:, :-2, 1:-1, 1:-1]
    total = total + padded[:, 1:-1, 2:, 1:-1] + padded[:, 1:-1, :-2, 1:-1]
    total = total + padded[:, 1:-1, 1:-1, 2:] + padded[:, 1:-1, 1:-1, :-2]
    return total


def inner_part(values):
    return values[:, 1:-1, 1:-1, 1:-1]


def pre_smooth(source, weights):
    count = source.shape[0]
    stacked = jnp.concatenate([source, weights], axis=0)
    wide = extended(stacked, (("gx", 1), ("gy", 2), ("gz", 3)), 2)
    wide_source = wide[:count]
    wide_weights = wide[count:]
    safe_weights = jnp.where(wide_weights > 0.0, wide_weights, 1.0)
    first = damping * wide_source / (6.0 * safe_weights * safe_weights)
    first_scaled = wide_weights * first
    mid_weights = inner_part(wide_weights)
    mid_safe = inner_part(safe_weights)
    applied = mid_weights * (6.0 * inner_part(first_scaled) - loop_sum(first_scaled))
    second = inner_part(first) + damping * (inner_part(wide_source) - applied) / (
        6.0 * mid_safe * mid_safe
    )
    second_scaled = mid_weights * second
    answer = inner_part(second)
    resid = source - weights * (6.0 * inner_part(second_scaled) - loop_sum(second_scaled))
    return (answer, resid)


def post_smooth(answer, source, weights):
    scaled = weights * answer
    wide = extended(scaled, (("gx", 1), ("gy", 2), ("gz", 3)), 1)
    applied = weights * (6.0 * scaled - loop_sum(wide))
    return answer + damping * (source - applied) / (6.0 * weights * weights)


def coarsen(values):
    leading = values.shape[0]
    size_x, size_y, size_z = (values.shape[1], values.shape[2], values.shape[3])
    blocks = values.reshape((leading, size_x // 2, 2, size_y // 2, 2, size_z // 2, 2))
    return jnp.mean(blocks, axis=(2, 4, 6))


def refine(values):
    return jnp.repeat(jnp.repeat(jnp.repeat(values, 2, axis=1), 2, axis=2), 2, axis=3)


def per_device(sources, stiffness, coarse_inverse):
    weight_list = [stiffness[None]]
    for level in range(3):
        weight_list.append(0.5 * coarsen(weight_list[-1]))
    source_list = []
    answer_list = []
    current = sources
    for level in range(4):
        source_list.append(current)
        answer, resid = pre_smooth(current, weight_list[level])
        answer_list.append(answer)
        current = coarsen(resid)
    count = current.shape[0]
    flat_source = current.reshape((count, -1))
    solved = lax.dot_general(
        lax.all_gather(flat_source, ("gx", "gy", "gz"), axis=1, tiled=True),
        coarse_inverse,
        (((1,), (1,)), ((), ())),
        precision=lax.Precision.HIGHEST,
        preferred_element_type=jnp.float32,
    )
    correction = solved.reshape(current.shape)
    for level in range(3, -1, -1):
        correction = post_smooth(
            answer_list[level] + refine(correction), source_list[level], weight_list[level]
        )
    return correction


K = damping / 6.0
F32 = jnp.float32
BF = jnp.bfloat16


def iota(shape, dim):
    return lax.broadcasted_iota(jnp.int32, shape, dim)


def pick(condition):
    return jnp.where(condition, 1.0, 0.0).astype(BF)


def lanes_of(values, index):
    index = jnp.broadcast_to(index, values.shape)
    return jnp.take_along_axis(values, index, axis=1, mode="promise_in_bounds")


def exact_dot(values, chosen):
    total = None
    for _ in range(3):
        part = values.astype(BF)
        values = values - part.astype(F32)
        term = jnp.dot(part, chosen, preferred_element_type=F32)
        total = term if total is None else total + term
    return total


def around(c):
    rows, lanes = c.shape
    return (pltpu.roll(c, 1, 0) + pltpu.roll(c, rows - 1, 0)) + (
        pltpu.roll(c, 1, 1) + pltpu.roll(c, lanes - 1, 1)
    )


def side_sum(planes):
    rows = planes[0].shape[0]
    row = iota(planes[0].shape, 0)
    outs = []
    for p, c in enumerate(planes):
        s = jnp.where(row > 0, pltpu.roll(c, 1, 0), 0.0) + jnp.where(
            row < rows - 1, pltpu.roll(c, rows - 1, 0), 0.0
        )
        if p > 0:
            s = s + planes[p - 1]
        if p < len(planes) - 1:
            s = s + planes[p + 1]
        outs.append(s)
    return outs


def shifted(c, by):
    lane, lanes = iota(c.shape, 1), c.shape[1]
    inside = lane + by < lanes if by > 0 else lane + by >= 0
    return jnp.where(inside, pltpu.roll(c, -by % lanes, 1), 0.0)


def pair_sum(c, step):
    lanes = c.shape[1]
    even = (iota(c.shape, 1) // step) % 2 == 0
    return c + jnp.where(even, pltpu.roll(c, lanes - step, 1), pltpu.roll(c, step, 1))


def row_sum(c):
    for step in (4, 2, 1):
        c = c + pltpu.roll(c, step, 0)
    return c


def kernel(
    dims, b_hbm, w_hbm, m_hbm, f_ref,
    b_ref, w_ref, m_ref,
    V0, W0, U0, V1, W1, U1, TT, T2, T3, T4, P3, E2, P2, P1, P1s, IW, IW1, MP, W0m, W0p, F0, R0, W1m, W1p, E10,
    SZ0, RZ0, S1v, SZv, RZv, R3v, RCv, S1w, SZw, RZw, R3w, RCw,
    GM, GW, GB, SW, SB,
    tally, load, sent, hr, known,
):
    axes = ("gx", "gy", "gz")
    ix, iy, iz = (lax.axis_index(a) for a in axes)
    n = dims[0] * dims[1] * dims[2]
    me = (ix * dims[1] + iy) * dims[2] + iz

    def flip(i, bits):
        if bits == 1:
            return i + 1 - 2 * (i % 2)
        return {0: i, 2: (i + 2) % 4, 3: 3 - i}[bits]

    def mirrored(k):
        a, b, c = k
        y, z = dims[1] - 1 - iy, dims[2] - 1 - iz
        return ((ix + a) % dims[0], flip(y, b), flip(z, c))

    ends = (dims[1] - 1, dims[2] - 1)
    others = sorted(
        (c + (b + 1) // 2, a, b, c)
        for a in range(dims[0])
        for b in range(dims[1])
        for c in range(dims[2])
        if (a, b, c) != (0,) + ends
    )
    others = [k[1:] for k in others]

    barrier = pltpu.get_barrier_semaphore()

    def there(d):
        ok = None
        for i, s, c in zip((ix, iy, iz), dims, d):
            if c:
                t = (i + c < s) if c > 0 else (i + c >= 0)
                ok = t if ok is None else jnp.logical_and(ok, t)
        return ok

    def directions(most):
        found = []
        for dx in (-1, 0, 1):
            for dy in (-1, 0, 1):
                for dz in (-1, 0, 1):
                    if 0 < abs(dx) + abs(dy) + abs(dz) <= most:
                        found.append((dx, dy, dz))
        return sorted(found, key=lambda d: (-abs(d[1]), -abs(d[2]), abs(d[0])))

    def greet(sem):
        for d in directions(3):
            @pl.when(there(d))
            def _(d=d):
                pl.semaphore_signal(
                    sem, inc=1, device_id=(ix + d[0], iy + d[1], iz + d[2]),
                    device_id_type=pl.DeviceIdType.MESH,
                )

    loads = [
        pltpu.make_async_copy(src, dst, load.at[i])
        for i, src, dst in ((0, b_hbm, b_ref), (0, w_hbm, w_ref), (1, m_hbm, m_ref))
    ]
    for copy in loads:
        copy.start()
    nx, ny = b_ref.shape[0], b_ref.shape[1]
    hx, hy = nx // 2, ny // 2

    def clear(ref, *where):
        part = ref.at[where] if where else ref
        part[...] = jnp.zeros(part.shape, F32)

    own = (pl.ds(0, ny), pl.ds(0, 128))
    clear(V0, pl.ds(0, 2), *own)
    clear(V0, pl.ds(nx + 2, 2), *own)
    clear(V0, pl.ds(1, nx + 2), pl.ds(ny, 8), pl.ds(0, 128))
    clear(W0, pl.ds(1, 1), *own)
    clear(W0, pl.ds(nx + 2, 1), *own)
    clear(W0, pl.ds(2, nx), pl.ds(ny, 8), pl.ds(0, 128))
    for D in (V1, W1):
        clear(D, pl.ds(0, 3))
        clear(D, pl.ds(hx + 3, 3))
        clear(D, pl.ds(3, hx), pl.ds(8, 8))
    for D in (RZ0, RZv, R3v, RCv, RZw, R3w, RCw):
        clear(D)
    greet(barrier)

    def span(i, s):
        return 1 + jnp.where(i > 0, 1, 0) + jnp.where(i < s - 1, 1, 0)

    greeted = span(ix, dims[0]) * span(iy, dims[1]) * span(iz, dims[2]) - 1

    def send(src, dst, d, sem):
        pltpu.make_async_remote_copy(
            src_ref=src, dst_ref=dst, send_sem=sent.at[0], recv_sem=sem,
            device_id=(ix + d[0], iy + d[1], iz + d[2]), device_id_type=pl.DeviceIdType.MESH,
        ).start()

    def send_all(found, pieces, sem):
        def start(group):
            for d in group:
                ok = there((d[0], 0, d[2]))
                if ok is None:
                    send(*pieces(d), d, sem)
                else:
                    @pl.when(ok)
                    def _(d=d):
                        send(*pieces(d), d, sem)

        low = iy < dims[1] // 2
        for c, inward in ((1, low), (-1, jnp.logical_not(low)), (1, jnp.logical_not(low)), (-1, low)):
            group = [d for d in found if d[1] == c]
            if group:
                @pl.when(jnp.logical_and(inward, there((0, c, 0))))
                def _(group=group):
                    start(group)
        start([d for d in found if d[1] == 0])

    def span_x(c, size, pad, deep):
        if c == 0:
            return pl.ds(0, size), pl.ds(pad, size)
        if c > 0:
            return pl.ds(size - deep, deep), pl.ds(pad - deep, deep)
        return pl.ds(0, deep), pl.ds(pad + size, deep)

    def span_y(c, size, total, deep):
        if c == 0:
            return pl.ds(0, size), pl.ds(0, size)
        if c > 0:
            return pl.ds(size - deep, deep), pl.ds(total - deep, deep)
        return pl.ds(0, deep), pl.ds(size, deep)

    def flat(found):
        return [d for d in found if not d[2]]

    first = pl.ds(0, 128)

    def pieces0(d):
        dx, dy, dz = d
        if dz:
            a, b = span_y(dy, ny, ny + 8, 1)
            return SZ0.at[a], RZ0.at[1 - dx, (1 - dz) // 2, b]
        deep = 1 if dx and dy else 2
        a, b = span_x(dx, nx, 2, deep)
        e, f = span_y(dy, ny, ny + 8, deep)
        shifted = pl.ds(a.start + 2, a.size)
        return V0.at[shifted, e, first], V0.at[b, f, first]

    def faces0(d):
        a, b = span_x(d[0], nx, 2, 1)
        e, f = span_y(d[1], ny, ny + 8, 1)
        return W0.at[pl.ds(a.start + 2, a.size), e, first], W0.at[b, f, first]

    def pieces1(S1, D, SZ, RZ):
        def of(d):
            dx, dy, dz = d
            if dz:
                a, b = span_y(dy, 8, 16, 2)
                return SZ.at[a], RZ.at[1 - dx, (1 - dz) // 2, b]
            a, b = span_x(dx, hx, 3, 2 if dy else 3)
            e, f = span_y(dy, 8, 16, 2)
            return S1.at[a, e], D.at[b, f]
        return of

    def late1(S1, R3, SZ, RC):
        def of(d):
            dx, dy, dz = d
            if dz:
                row = pl.ds(7 if dy > 0 else 0, 1)
                return SZ.at[row], RC.at[(1 - dx) // 2, (1 - dz) // 2, row]
            row = pl.ds(5 if dy > 0 else 2, 1)
            return S1.at[:, row], R3.at[:, row]
        return of

    def matrix_rows(d):
        s, r = m_ref, GM.at[me]
        if d[2]:
            row = pl.ds(m_ref.shape[0] - 1 if d[2] > 0 else 0, 1)
            s, r = s.at[row], r.at[row]
        return s, r

    corners = [d for d in directions(3) if all(d)]
    lates = [(0, -1, 0), (0, 1, 0)] + corners

    def bytes_of(ref, sem):
        pltpu.make_async_copy(ref, ref, sem).wait()

    sides_y, sides_z = span(iy, dims[1]) - 1, span(iz, dims[2]) - 1

    def first_part(cy, cz):
        return 32 + 33 * cy + 32 * cz + cy * cz

    def face_part(cy, cz):
        return 16 + 16 * cy

    def second_part(cy, cz):
        return 24 + 20 * cy + 16 * cz + 2 * cy * cz

    def late_part(cy, cz):
        return 8 * cy + cy * cz

    def weight_part(cy, cz):
        return second_part(cy, cz) + late_part(cy, cz)

    def matrix_part(cy, cz):
        return 16 + 32 * cy + 4 * (1 + cy) * cz

    def waiting_part(cy, cz):
        parts = (weight_part, late_part, face_part, matrix_part)
        return sum(part(cy, cz) for part in parts) + 4 * (n - 1)

    def everything(cy, cz):
        parts = (first_part, second_part, waiting_part)
        return sum(part(cy, cz) for part in parts) + 4 * (n - 1)

    def take(part, sem):
        for cy in (1, 2):
            for cz in (1, 2):
                @pl.when(jnp.logical_and(sides_y == cy, sides_z == cz))
                def _(cy=cy, cz=cz):
                    bytes_of(tally.at[pl.ds(0, part(cy, cz))], sem)

    def spread(kind, src, dst, k):
        return pltpu.make_async_remote_copy(
            src_ref=src, dst_ref=dst.at[me], send_sem=sent.at[0], recv_sem=hr.at[kind],
            device_id=mirrored(k), device_id_type=pl.DeviceIdType.MESH,
        )

    def arrive(kind, dst):
        bytes_of(dst.at[pl.ds(0, n - 1)], hr.at[kind])


    bytes_of(tally.at[pl.ds(0, 2 * nx * ny)], load.at[0])
    lane16 = iota((ny, 128), 1)
    packed = jnp.zeros((ny, 128), F32)
    for x in range(nx):
        w = w_ref[x]
        v = K * b_ref[x] / w
        V0[x + 2, 0:ny, 0:128] = v
        W0[x + 2, 0:ny, 0:128] = w
        for a, q in enumerate((v, w)):
            start = 8 * x + 4 * a
            moved = pltpu.roll(q, (start + 2) % 128, 1)
            packed = jnp.where((lane16 >= start) & (lane16 < start + 4), moved, packed)
    SZ0[...] = packed

    pl.semaphore_wait(barrier, greeted)
    send_all(directions(2), pieces0, hr.at[0])
    greet(known.at[0])
    send_all(flat(directions(1)), faces0, hr.at[1])

    lane_row = iota((1, 128), 1)
    low_half = jnp.minimum(2 * lane_row, 126)

    def coarsen0(planes):
        for i in range(hx):
            TT[i] = planes(2 * i) + planes(2 * i + 1)
        rows = [
            TT[i, pl.ds(0, hy, stride=2), :] + TT[i, pl.ds(1, hy, stride=2), :] for i in range(hx)
        ]
        rows = jnp.concatenate(rows, axis=0)
        return lanes_of(rows, low_half) + lanes_of(rows, low_half + 1)

    held_x = (lane_row // 32 + 4 - iz) % 4
    pairs = 2 * (lane_row % 32)

    def coarsen1(planes, SG):
        for i in range(hx // 2):
            T2[pl.ds(8 * i, 8), :] = planes(2 * i) + planes(2 * i + 1)
        pieces = [
            T2[pl.ds(8 * x, 4, stride=2), :] + T2[pl.ds(8 * x + 1, 4, stride=2), :]
            for x in range(4)
        ]
        rows = [jnp.concatenate(pieces[i : i + 2], axis=0) for i in (0, 2)]
        sums = [lanes_of(r, pairs) + lanes_of(r, pairs + 1) for r in rows]
        parts = [sums[x // 2][4 * (x % 2) : 4 * (x % 2) + 4] for x in range(4)]
        total = parts[0]
        for x in range(1, 4):
            total = jnp.where(held_x == x, parts[x], total)
        return total

    lane8 = iota((8, 128), 1)

    def pack1(S1, SZ, planes):
        out = jnp.zeros((8, 128), F32)
        for x in range(hx):
            q = planes[x]
            S1[x] = q
            s = 16 * x
            h = (s + 64) % 128
            out = jnp.where((lane8 >= h) & (lane8 < h + 3), pltpu.roll(q, (h - 61) % 128, 1), out)
            out = jnp.where(
                (lane8 >= s + 3) & (lane8 < s + 6), pltpu.roll(q, (s + 3) % 128, 1), out
            )
        SZ[...] = out

    w1 = 0.0625 * coarsen0(lambda x: w_ref[x])
    w1 = [w1[8 * x : 8 * x + 8, :] for x in range(hx)]
    pack1(S1w, SZw, w1)
    SW[...] = 0.0625 * coarsen1(lambda x: w1[x], SW)
    GW[me] = SW[...]
    loads[2].wait()
    GM[me] = m_ref[...]
    send_all(directions(2), pieces1(S1w, W1, SZw, RZw), hr.at[1])
    send_all(lates, late1(S1w, R3w, SZw, RCw), hr.at[1])
    send_all(directions(3), matrix_rows, hr.at[1])
    pl.semaphore_wait(known.at[0], greeted)
    greet(known.at[1])

    def coords(rows, lanes, cy, cz, by, bz):
        r, l = iota((rows, lanes), 0), iota((rows, lanes), 1)
        y = jnp.where(r < cy + (rows - cy) // 2, r, r - rows)
        z = jnp.where(l < cz + (lanes - cz) // 2, l, l - lanes)
        gy, gz = y + iy * cy, z + iz * cz
        ok = (gy >= 0) & (gy < dims[1] * cy) & (gz >= 0) & (gz < dims[2] * cz)
        near = (y >= -by) & (y < cy + by) & (z >= -bz) & (z < cz + bz)
        return jnp.where(ok & near, 1, 0)

    def plane_mask(base, x, cx):
        if 0 <= x < cx:
            return base > 0
        gx = x + ix * cx
        inside = jnp.where((gx >= 0) & (gx < dims[0] * cx), 1, 0)
        return base * inside > 0

    row8 = iota((8, 128), 0)
    row16, lane_own = iota((ny, 128), 0), iota((ny, 128), 1)

    def in_lanes(c):
        return shifted(c, -1) + shifted(c, 1)

    def in_rows(c):
        return jnp.where(row16 > 0, pltpu.roll(c, 1, 0), 0.0) + jnp.where(
            row16 < ny - 1, pltpu.roll(c, ny - 1, 0), 0.0
        )

    def beside(planes, x):
        found = [planes[i] for i in (x - 1, x + 1) if 0 <= i < nx]
        return found[0] + found[1] if len(found) > 1 else found[0]

    inner = [V0[x + 2, 0:ny, 0:128] for x in range(nx)]
    inner_u = [
        1.2 * c + K * (in_rows(c) + in_lanes(c) + beside(inner, x)) for x, c in enumerate(inner)
    ]
    for x, u in enumerate(inner_u):
        near_sum = in_rows(u) + in_lanes(u) + beside(inner_u, x)
        R0[x] = b_ref[x] - w_ref[x] * (6.0 * u - near_sum)
    kind = lane_own % 8
    packed = SZ0[...]
    own_ends = jnp.where(kind == 1, pltpu.roll(packed, 127, 1), pltpu.roll(packed, 1, 1))
    has_z = ((kind == 1) & (iz > 0)) | ((kind == 2) & (iz < dims[2] - 1))
    has_y = ((row8 == 7) & (iy > 0)) | ((row8 == 0) & (iy < dims[1] - 1))

    def exists(c):
        return (ix + c >= 0) & (ix + c < dims[0])

    take(first_part, hr.at[0])
    mask0 = coords(24, 256, ny, 128, 1, 1) > 0
    lane24 = iota((24, 128), 1)

    def z_ends(dx):
        return jnp.where(lane24 % 4 >= 2, RZ0[dx + 1, 1], RZ0[dx + 1, 0])

    ends = {dx: z_ends(dx) for dx in (-1, 0, 1)}

    def z_change():
        full, c = ends[0], ends[0][0:ny]
        above, below = pltpu.roll(full, 1, 1), pltpu.roll(full, 127, 1)
        left = pltpu.roll(jnp.where(lane_own >= 120, ends[-1][0:ny], c), 8, 1)
        right = pltpu.roll(jnp.where(lane_own < 8, ends[1][0:ny], c), 120, 1)
        outer = jnp.where(kind == 1, above[0:ny], below[0:ny])
        vert = (pltpu.roll(full, 1, 0) + pltpu.roll(full, ny + 7, 0))[0:ny]
        u = 1.2 * c + K * (outer + own_ends + vert + left + right)
        u = jnp.where(has_z, u, 0.0)
        across = jnp.where(lane_own >= 8, left, 0.0) + jnp.where(lane_own < 120, right, 0.0)
        d = K * (6.0 * c - in_rows(c) - across) - u
        low = jnp.where(kind == 1, d, -K * above[0:ny])
        high = jnp.where(kind == 2, d, -K * below[0:ny])
        swapped = jnp.where(lane8 % 8 == 1, below[ny:], above[ny:])
        return low, high, swapped

    low_end, high_end, edge_ends = z_change()
    side = [V0[p, ny : ny + 8, 0:128] for p in range(1, nx + 3)]

    def z_part(x):
        a = pltpu.roll(low_end, (-8 * x - 1) % 128, 1)
        b = pltpu.roll(high_end, (125 - 8 * x) % 128, 1)
        return jnp.where(lane_own < 2, a, jnp.where(lane_own >= 126, b, 0.0))

    def y_part(x):
        c = side[x + 1]
        ends_x = pltpu.roll(edge_ends, (126 - 8 * x) % 128, 1)
        flat_sum = in_lanes(c)
        edges = jnp.where((lane8 == 0) | (lane8 == 127), ends_x, 0.0)
        adjacent = jnp.where(
            row8 == 7, pltpu.roll(inner[x][0:8], 7, 0), pltpu.roll(inner[x][8:16], 1, 0)
        )
        outer = jnp.where(row8 == 7, pltpu.roll(c, 1, 0), pltpu.roll(c, 7, 0))
        u = 1.2 * c + K * (flat_sum + edges + adjacent + outer + side[x] + side[x + 2])
        u = jnp.where(has_y, u, 0.0)
        d = K * (6.0 * c - flat_sum - beside(side[1:-1], x)) - u
        first_rows = jnp.where(row8 == 1, -K * pltpu.roll(c, 2, 0), 0.0)
        first_rows = jnp.where(row8 == 0, pltpu.roll(d, 1, 0), first_rows)
        last_rows = jnp.where(row8 == 6, -K * pltpu.roll(c, 6, 0), 0.0)
        last_rows = jnp.where(row8 == 7, pltpu.roll(d, 7, 0), last_rows)
        return jnp.concatenate([first_rows, last_rows], axis=0)

    def x_part(p, c, x, edge):
        h, beyond = V0[p, 0:ny, 0:128], V0[p + c, 0:ny, 0:128]
        a = pltpu.roll(ends[c][0:ny], (-8 * x - 1) % 128, 1)
        b = pltpu.roll(ends[c][0:ny], (125 - 8 * x) % 128, 1)
        t = V0[p, ny : ny + 8, 0:128]
        rows = jnp.concatenate(
            [
                jnp.where(row8 == 0, pltpu.roll(t, 1, 0), 0.0),
                jnp.where(row8 == 7, pltpu.roll(t, 7, 0), 0.0),
            ],
            axis=0,
        )
        edges = jnp.where(lane_own == 0, a, jnp.where(lane_own == 127, b, 0.0)) + rows
        near_sum = in_lanes(h) + in_rows(h)
        u = 1.2 * h + K * (near_sum + edges + beyond + inner[edge])
        u = jnp.where(exists(c), u, 0.0)
        return K * (6.0 * h - near_sum) - u, -K * h

    x_parts = {}
    for p, c, x, edge in ((1, -1, nx - 1, 0), (nx + 2, 1, 0, nx - 1)):
        x_parts[edge], x_parts[edge - c] = x_part(p, c, x, edge)

    def resid0(x):
        change = z_part(x) + y_part(x)
        if x in x_parts:
            change = change + x_parts[x]
        return R0[x] - w_ref[x] * change

    def smooth0():
        for dx in (-1, 0, 1):
            for x in {-1: (nx - 1,), 0: range(nx), 1: (0,)}[dx]:
                moved = pltpu.roll(z_ends(dx), (126 - 8 * x) % 128, 1)
                V0[x + 2 + dx * nx, :, 128:256] = moved
        for p, c in ((1, -1), (nx + 2, 1)):
            u = 1.2 * V0[p, 0:ny, 0:128] + K * own_sum(V0, p)
            U0[p, 0:ny, 0:128] = jnp.where(exists(c), u, 0.0)
        for p in range(2, nx + 2):
            c = V0[p]
            u = 1.2 * c + K * (around(c) + (V0[p - 1] + V0[p + 1]))
            U0[p] = jnp.where(mask0, u, 0.0)

    def assemble_faces():
        moved = z_ends(0)
        for x in range(nx):
            p = x + 2
            W0[p, :, 128:256] = pltpu.roll(moved, (122 - 8 * x) % 128, 1)
            IW[x] = 1.0 / w_ref[x]
            W0m[x] = pltpu.roll(W0[p, 0:ny, :], 1, 1)[:, 0:128]
            W0p[x] = pltpu.roll(W0[p, 0:ny, :], 255, 1)[:, 0:128]
            F0[x] = 0.2 * U0[p, 0:ny, 0:128] + V0[p, 0:ny, 0:128] + K * own_sum(U0, p)

    def own_sum(ref, p):
        col, wide = ref[p, :, 0:128], ref[p, 0:ny, :]
        vert = pltpu.roll(col, 1, 0)[0:ny] + pltpu.roll(col, ny + 7, 0)[0:ny]
        flat_sum = pltpu.roll(wide, 1, 1)[:, 0:128] + pltpu.roll(wide, 255, 1)[:, 0:128]
        return (vert + flat_sum) + (ref[p - 1, 0:ny, 0:128] + ref[p + 1, 0:ny, 0:128])

    b1 = 0.125 * coarsen0(resid0)
    b1 = [b1[8 * x : 8 * x + 8, :] for x in range(hx)]
    v1 = [jnp.where(lane8 < 64, K * b1[x] / jnp.where(lane8 < 64, w1[x], 1.0), 0.0) for x in range(hx)]
    pack1(S1v, SZv, v1)
    send_all(directions(2), pieces1(S1v, V1, SZv, RZv), hr.at[2])
    send_all(lates, late1(S1v, R3v, SZv, RCv), hr.at[1])
    pl.semaphore_wait(known.at[1], greeted)
    for k in others:
        spread(1, SW, GW, k).start()

    mask1 = coords(16, 128, 8, 64, 2, 2)
    mask_up = coords(16, 128, 8, 64, 1, 1)
    mask_own = coords(16, 128, 8, 64, 0, 0)
    lane1 = iota((16, 128), 1)

    def assemble1(S1, RZ, D):
        for dx in (-1, 0, 1):
            ends = jnp.where(lane1 % 16 < 3, RZ[dx + 1, 0], RZ[dx + 1, 1])
            for x in {-1: (hx - 2, hx - 1), 0: range(hx), 1: (0, 1)}[dx]:
                p = x + 3 + dx * hx
                moved = pltpu.roll(ends, (61 - 16 * x) % 128, 1)
                inner = S1[x] if dx == 0 else D[p, 0:8, :]
                D[p, 0:8, :] = jnp.where(lane8 < 64, inner, moved[0:8])
                D[p, 8:16, :] = jnp.where(lane8 < 64, D[p, 8:16, :], moved[8:16])

    def finish1(R3, RC, D):
        for x in range(hx):
            D[x + 3, 8:16, :] = jnp.where((row8 == 2) | (row8 == 5), R3[x], D[x + 3, 8:16, :])
        for slot, p, x in ((0, 2, hx - 1), (1, hx + 3, 0)):
            ends = jnp.where(lane8 % 16 < 3, RC[slot, 0], RC[slot, 1])
            moved = pltpu.roll(ends, (61 - 16 * x) % 128, 1)
            D[p, 8:16, :] = jnp.where(lane8 < 64, D[p, 8:16, :], moved)

    def smooth1(planes):
        for p in planes:
            c = V1[p]
            u = 1.2 * c + K * (around(c) + (V1[p - 1] + V1[p + 1]))
            U1[p] = jnp.where(plane_mask(mask1, p - 3, hx), u, 0.0)

    block = lane8 // 32

    def gathered(G):
        planes = []
        for gx in range(dims[0]):
            tiles = {}
            for t in range(dims[1] // 2):
                for z in range(dims[2]):
                    d0 = (gx * dims[1] + 2 * t) * dims[2] + z
                    tiles[t, z] = jnp.concatenate([G[d0], G[d0 + dims[2]]], axis=0)
            for x in range(4):
                parts = []
                for t in range(dims[1] // 2):
                    out = tiles[t, 0]
                    for z in range(1, dims[2]):
                        out = jnp.where(block == (x + z) % 4, tiles[t, z], out)
                    parts.append(out)
                planes.append(jnp.concatenate(parts, axis=0))
        return planes

    def turned(planes, by):
        return [
            pltpu.roll(c, (-32 * (X % 4) - by) % 128, 1) if X % 4 or by else c
            for X, c in enumerate(planes)
        ]

    def coarsen2(planes):
        c = len(planes) // 2
        for i in range(c):
            T3[i] = planes[2 * i] + planes[2 * i + 1]
        return [
            pair_sum(T3[i, pl.ds(0, 8, stride=2), :] + T3[i, pl.ds(1, 8, stride=2), :], 1)
            for i in range(c)
        ]

    take(second_part, hr.at[2])
    assemble1(S1v, RZv, V1)
    smooth1(range(2, hx + 4))

    def resid1(x):
        p = x + 3
        s = around(U1[p])[0:8, :] + (U1[p - 1, 0:8, :] + U1[p + 1, 0:8, :])
        return jnp.where(lane8 < 64, b1[x] - w1[x] * (6.0 * U1[p, 0:8, :] - s), 0.0)

    SB[...] = 0.125 * coarsen1(resid1, SB)
    GB[me] = SB[...]
    for k in others:
        spread(3, SB, GB, k).start()
    take(waiting_part, hr.at[1])
    turned_w2 = gathered(GW)
    scale2 = [K / q for q in turned_w2]
    w2 = turned(turned_w2, 0)
    w2m, w2p = [shifted(q, -1) for q in w2], [shifted(q, 1) for q in w2]
    unscale2 = [q * (1.0 / K) for q in w2]
    iw2 = [1.0 / q for q in w2]
    w3 = [0.0625 * q for q in coarsen2(w2)]
    around3 = {k: [shifted(q, 2 * k) if k else q for q in w3] for k in (-2, -1, 0, 1, 2)}
    iw3 = [1.0 / q for q in w3]
    inverse3 = {k: [shifted(q, 2 * k) if k else q for q in iw3] for k in (-1, 0, 1)}
    smooth0()
    assemble_faces()
    assemble1(S1w, RZw, W1)
    finish1(R3w, RCw, W1)
    for p in range(2, hx + 4):
        inside = plane_mask(mask_up if 0 <= p - 3 < hx else mask_own, p - 3, hx)
        IW1[p] = jnp.where(inside, 1.0, 0.0) / jnp.where(inside, W1[p], 1.0)
        W1m[p] = pltpu.roll(W1[p], 1, 1)
        W1p[p] = pltpu.roll(W1[p], 127, 1)
    finish1(R3v, RCv, V1)
    smooth1(range(1, hx + 5))
    for p in range(2, hx + 4):
        c = U1[p]
        E10[p] = 0.2 * c + V1[p] + K * (around(c) + (U1[p - 1] + U1[p + 1]))

    def near(i, c, size):
        return jnp.clip(i + c, 0, size - 1)

    steps = (-1, 0, 1)
    blocks = [(x, dy, dz) for x in range(dims[0]) for dy in steps for dz in steps]
    rows = jnp.concatenate(
        [
            GM[(x * dims[1] + near(iy, dy, dims[1])) * dims[2] + near(iz, dz, dims[2])]
            for x, dy, dz in blocks
        ],
        axis=0,
    )
    order = pick(
        iota((128, 128), 0) == (iota((128, 128), 1) % 4) * 32 + iota((128, 128), 1) // 4
    )
    for h in range(2):
        MP[h] = exact_dot(rows[:, 128 * h : 128 * h + 128], order)
    other_w = [jnp.where(lane8 // 2 % 2 == 0, a, b) for a, b in zip(around3[1], around3[-1])]
    other_c = [q * (1.0 / K) for q in other_w]
    far = jnp.full((8, 128), -99)
    wanted = {-1: jnp.where(row8 == 7, -1, far), 0: row8, 1: jnp.where(row8 == 0, 8, far)}
    held = {}
    for k in (-2, -1, 0, 1, 2):
        cell = lane8 + 2 * k
        held[k] = jnp.where((cell >= 0) & (cell < 128), cell // 4 - 8 * iz, -50)
    moves = (0, 1, -1)
    double = [(lane_row + k + 256) // 2 % 128 for k in moves]
    depth = jnp.where(lane_row < 96, lane_row, lane_row - 128)
    here = [jnp.clip((depth + k + 256) // 2 - 128 + 32 * iz, 0, 127) for k in moves]
    even = lane8 % 2 == 0
    E2[...] = jnp.zeros_like(E2)
    arrive(3, GB)

    v_turned = [b * r for b, r in zip(gathered(GB), scale2)]
    v2 = turned(v_turned, 0)
    lane_wide = iota((16, 128), 1)
    before = [jnp.where(lane_wide > 0, q, 0.0) for q in turned(v_turned, -1)]
    after = [jnp.where(lane_wide < 127, q, 0.0) for q in turned(v_turned, 1)]
    u2 = [1.2 * v + K * (s + (a + b)) for v, s, a, b in zip(v2, side_sum(v2), before, after)]
    s2 = [s + (shifted(u, -1) + shifted(u, 1)) for s, u in zip(side_sum(u2), u2)]
    r2 = [v * k - w * (6.0 * u - s) for v, k, w, u, s in zip(v2, unscale2, w2, u2, s2)]
    base2 = [0.2 * u + v + K * s for u, v, s in zip(u2, v2, s2)]
    b3 = [0.125 * q for q in coarsen2(r2)]
    v3 = {0: [K * b * r for b, r in zip(b3, iw3)]}
    for k in (-3, -2, -1, 1, 2, 3):
        v3[k] = [shifted(v, 2 * k) for v in v3[0]]
    u3 = {}
    for k in (-2, -1, 0, 1, 2):
        u3[k] = [
            1.2 * v + K * (s + (a + b))
            for v, s, a, b in zip(v3[k], side_sum(v3[k]), v3[k - 1], v3[k + 1])
        ]
        if k:
            cell = lane8 + 2 * k
            u3[k] = [jnp.where((cell >= 0) & (cell < 128), u, 0.0) for u in u3[k]]
    even3 = lane8 // 2 % 2 == 0

    def partner(q, k):
        return [jnp.where(even3, a, b) for a, b in zip(q[k], q[-k])]

    s3 = [s + (a + b) for s, a, b in zip(side_sum(u3[0]), u3[-1], u3[1])]
    r3 = [b - w * (6.0 * u - s) for b, w, u, s in zip(b3, w3, u3[0], s3)]
    base3 = [0.2 * u + v + K * s for u, v, s in zip(u3[0], v3[0], s3)]
    base3 = {k: [shifted(q, 2 * k) if k else q for q in base3] for k in (-1, 0, 1)}
    other_u, other_v = partner(u3, 1), partner(v3, 1)
    sides = side_sum(other_u)
    r3 = [
        r + v * c - w * (6.0 * u - (s + a + b))
        for r, v, c, w, u, s, a, b in zip(
            r3, other_v, other_c, other_w, other_u, sides, u3[0], partner(u3, 2)
        )
    ]
    c4 = len(r3) // 2
    for i in range(c4):
        T4[pl.ds(8 * i, 8), :] = r3[2 * i] + r3[2 * i + 1]
    half = 4 * c4
    b4 = 0.125 * (T4[pl.ds(0, half, stride=2), :] + T4[pl.ds(1, half, stride=2), :])
    chosen = jnp.where(row8 % 4 == lane8 % 4, b4, 0.0)
    low = row_sum(jnp.where(row8 < 4, chosen, 0.0))
    high = row_sum(jnp.where(row8 >= 4, chosen, 0.0))
    solved = [
        jnp.sum(MP[0, 8 * k : 8 * k + 8, :] * low + MP[1, 8 * k : 8 * k + 8, :] * high,
                axis=1, keepdims=True)
        for k in range(len(blocks))
    ]
    q3 = {}
    for k in (-2, -1, 0, 1, 2):
        e4 = []
        for x in range(dims[0]):
            plane = jnp.zeros((8, 128), F32)
            for dy in steps:
                found = jnp.zeros((8, 128), F32)
                for dz in steps:
                    value = solved[blocks.index((x, dy, dz))]
                    found = jnp.where(held[k] == wanted[dz], value, found)
                plane = jnp.where(row8 // 2 == iy + dy, row_sum(found), plane)
            e4.append(plane)
        q3[k] = [w * e4[i // 2] for i, w in enumerate(around3[k])]
    e3 = {}
    for k in (-1, 0, 1):
        sides = side_sum(q3[k])
        e3[k] = [
            (base + 0.2 * q + K * (s + (a + b))) * r
            for base, q, s, a, b, r in zip(
                base3[k], q3[k], sides, q3[k - 1], q3[k + 1], inverse3[k]
            )
        ]
    for i in range(2 * dims[0]):
        middle = e3[0][i]
        views = (middle, jnp.where(even, middle, e3[1][i]), jnp.where(even, e3[-1][i], middle))
        for k, e in enumerate(views):
            P3[k, i, pl.ds(0, 8, stride=2), :] = e
            P3[k, i, pl.ds(1, 8, stride=2), :] = e
    q2 = [w * P3[0, i // 2] for i, w in enumerate(w2)]
    sides = side_sum(q2)
    for i, (base, q, s) in enumerate(zip(base2, q2, sides)):
        ends = w2p[i] * P3[1, i // 2] + w2m[i] * P3[2, i // 2]
        E2[i + 1, 8:24, :] = (base + 0.2 * q + K * (s + ends)) * iw2[i]

    seen = jnp.concatenate([E2[4 * ix + i, pl.ds(6 + 4 * iy, 8), :] for i in range(6)], axis=0)
    for k in range(3):
        wide2 = lanes_of(pltpu.roll(seen.reshape((6, 8, 128)), 6, 1).reshape((48, 128)), here[k])
        for i in range(6):
            q = wide2[8 * i : 8 * i + 8]
            P2[k, i, pl.ds(0, 8, stride=2), :] = q
            P2[k, i, pl.ds(1, 8, stride=2), :] = q
    q1 = {p: W1[p] * P2[0, (p - 3) // 2 + 1] for p in range(1, hx + 5)}
    e1 = []
    for p in range(2, hx + 4):
        q, i = q1[p], (p - 3) // 2 + 1
        ends = W1p[p] * P2[1, i] + W1m[p] * P2[2, i]
        s = (pltpu.roll(q, 1, 0) + pltpu.roll(q, 15, 0)) + ends + (q1[p - 1] + q1[p + 1])
        e1.append((E10[p] + 0.2 * q + K * s) * IW1[p])
    wide1 = lanes_of(jnp.concatenate(e1, axis=0), double[0])
    for i in range(hx + 2):
        q = wide1[16 * i : 16 * i + 16]
        P1[i, pl.ds(0, 16, stride=2), :] = q
        P1[i, pl.ds(1, 16, stride=2), :] = q
    for k in (1, 2):
        wide1 = lanes_of(jnp.concatenate([e[0:8] for e in e1[1:-1]], axis=0), double[k])
        for i in range(hx):
            q = wide1[8 * i : 8 * i + 8]
            P1s[k - 1, i + 1, pl.ds(0, 8, stride=2), :] = q
            P1s[k - 1, i + 1, pl.ds(1, 8, stride=2), :] = q

    def scaled(p):
        i = (p - 2) // 2 + 1
        if not 2 <= p < nx + 2:
            return W0[p, 0:ny, 0:128] * P1[i, 0:16, :]
        edge = jnp.where(row8 < 4, P1[i, 16:24, :], P1[i, 24:32, :])
        return W0[p, :, 0:128] * jnp.concatenate([P1[i, 0:16, :], edge], axis=0)

    q0 = {p: scaled(p) for p in range(1, nx + 3)}
    for x in range(nx):
        p, i = x + 2, x // 2 + 1
        q = q0[p]
        ends = W0p[x] * P1s[0, i] + W0m[x] * P1s[1, i]
        vert = pltpu.roll(q, 1, 0)[0:ny] + pltpu.roll(q, ny + 7, 0)[0:ny]
        s = vert + ends + (q0[p - 1][0:ny] + q0[p + 1][0:ny])
        f_ref[x] = (F0[x] + 0.2 * q[0:ny] + K * s) * IW[x]

    take(everything, sent.at[0])


def fused(dims, sources, stiffness, coarse_inverse):
    nx, ny, nz = stiffness.shape
    n = dims[0] * dims[1] * dims[2]
    vm = lambda *s: pltpu.VMEM(s, F32)
    halo1 = [vm(8, 8, 128), vm(8, 128), vm(3, 2, 16, 128), vm(8, 8, 128), vm(2, 2, 8, 128)]
    result = pl.pallas_call(
        functools.partial(kernel, dims),
        out_shape=pltpu.VMEM((nx, ny, nz), F32),
        in_specs=[pl.BlockSpec(memory_space=pl.ANY)] * 3,
        out_specs=pl.BlockSpec(memory_space=pltpu.VMEM),
        scratch_shapes=[
            vm(nx, ny, nz), vm(nx, ny, nz), vm(*coarse_inverse.shape),
            vm(nx + 4, 24, 256), vm(nx + 4, 24, 256), vm(nx + 4, 24, 256),
            vm(14, 16, 128), vm(14, 16, 128), vm(14, 16, 128),
            vm(8, 16, 128), vm(32, 128), vm(2 * dims[0], 16, 128),
            vm(16, 128), vm(3, 2 * dims[0], 16, 128),
            vm(4 * dims[0] + 2, 32, 128), vm(3, 6, 16, 128), vm(10, 32, 128), vm(2, 10, 16, 128),
            vm(nx, ny, nz), vm(14, 16, 128), vm(2, 72 * dims[0], 128),
            vm(nx, ny, nz), vm(nx, ny, nz), vm(nx, ny, nz), vm(nx, ny, nz),
            vm(14, 16, 128), vm(14, 16, 128), vm(14, 16, 128),
            vm(ny, 128), vm(3, 2, ny + 8, 128),
        ]
        + halo1 + halo1
        + [
            vm(n, 8, 256), vm(n, 4, 128), vm(n, 4, 128), vm(4, 128), vm(4, 128),
            vm(2048, 128),
            pltpu.SemaphoreType.DMA((2,)), pltpu.SemaphoreType.DMA((1,)),
            pltpu.SemaphoreType.DMA((4,)),
            pltpu.SemaphoreType.REGULAR((2,)),
        ],
        compiler_params=pltpu.CompilerParams(collective_id=0, has_side_effects=True),
        name="cycle",
    )(sources[0], stiffness, coarse_inverse)
    return result[None]


def solution(mesh):
    dims = tuple(mesh.shape[a] for a in ("gx", "gy", "gz"))

    def run(sources, stiffness, coarse_inverse):
        nx, ny, nz = stiffness.shape
        lanes = 128
        cells = coarse_inverse.shape[1]
        levels_fit = (
            sources.shape[0] == 1
            and nx == ny == 16
            and nz == lanes
            and dims[2] * nz == 4 * lanes
            and dims[1] * ny == 64
            and cells == 2 * lanes
            and dims[0] == 2
        )
        if levels_fit:
            return fused(dims, sources, stiffness, coarse_inverse)
        return per_device(sources, stiffness, coarse_inverse)

    in_specs = (P(None, "gx", "gy", "gz"), P("gx", "gy", "gz"), P(("gx", "gy", "gz"), None))
    out_specs = P(None, "gx", "gy", "gz")
    return jax.shard_map(
        run, mesh=mesh, in_specs=in_specs, out_specs=out_specs, check_vma=False
    )
```

```python
import functools
import jax
import jax.numpy as jnp
from jax import lax
from jax.experimental import pallas as pl
from jax.experimental.pallas import tpu as pltpu
from jax.sharding import PartitionSpec as P

damping = 0.8


def extended(cells, sides, width):
    for axis, dim in sides:
        count = lax.axis_size(axis)
        ends = count - 1
        head = lax.slice_in_dim(cells, 0, width, axis=dim)
        tail = lax.slice_in_dim(cells, cells.shape[dim] - width, cells.shape[dim], axis=dim)
        cells = jnp.concatenate(
            [
                lax.ppermute(tail, axis, [(i, (i + 1) % count) for i in range(ends)]),
                cells,
                lax.ppermute(head, axis, [((i + 1) % count, i) for i in range(ends)]),
            ],
            axis=dim,
        )
    return cells


def loop_sum(padded):
    total = padded[:, 2:, 1:-1, 1:-1] + padded[:, :-2, 1:-1, 1:-1]
    total = total + padded[:, 1:-1, 2:, 1:-1] + padded[:, 1:-1, :-2, 1:-1]
    total = total + padded[:, 1:-1, 1:-1, 2:] + padded[:, 1:-1, 1:-1, :-2]
    return total


def inner_part(values):
    return values[:, 1:-1, 1:-1, 1:-1]


def pre_smooth(source, weights):
    count = source.shape[0]
    stacked = jnp.concatenate([source, weights], axis=0)
    wide = extended(stacked, (("gx", 1), ("gy", 2), ("gz", 3)), 2)
    wide_source = wide[:count]
    wide_weights = wide[count:]
    safe_weights = jnp.where(wide_weights > 0.0, wide_weights, 1.0)
    first = damping * wide_source / (6.0 * safe_weights * safe_weights)
    first_scaled = wide_weights * first
    mid_weights = inner_part(wide_weights)
    mid_safe = inner_part(safe_weights)
    applied = mid_weights * (6.0 * inner_part(first_scaled) - loop_sum(first_scaled))
    second = inner_part(first) + damping * (inner_part(wide_source) - applied) / (
        6.0 * mid_safe * mid_safe
    )
    second_scaled = mid_weights * second
    answer = inner_part(second)
    resid = source - weights * (6.0 * inner_part(second_scaled) - loop_sum(second_scaled))
    return (answer, resid)


def post_smooth(answer, source, weights):
    scaled = weights * answer
    wide = extended(scaled, (("gx", 1), ("gy", 2), ("gz", 3)), 1)
    applied = weights * (6.0 * scaled - loop_sum(wide))
    return answer + damping * (source - applied) / (6.0 * weights * weights)


def coarsen(values):
    leading = values.shape[0]
    size_x, size_y, size_z = (values.shape[1], values.shape[2], values.shape[3])
    blocks = values.reshape((leading, size_x // 2, 2, size_y // 2, 2, size_z // 2, 2))
    return jnp.mean(blocks, axis=(2, 4, 6))


def refine(values):
    return jnp.repeat(jnp.repeat(jnp.repeat(values, 2, axis=1), 2, axis=2), 2, axis=3)


def per_device(sources, stiffness, coarse_inverse):
    weight_list = [stiffness[None]]
    for level in range(3):
        weight_list.append(0.5 * coarsen(weight_list[-1]))
    source_list = []
    answer_list = []
    current = sources
    for level in range(4):
        source_list.append(current)
        answer, resid = pre_smooth(current, weight_list[level])
        answer_list.append(answer)
        current = coarsen(resid)
    count = current.shape[0]
    flat_source = current.reshape((count, -1))
    solved = lax.dot_general(
        lax.all_gather(flat_source, ("gx", "gy", "gz"), axis=1, tiled=True),
        coarse_inverse,
        (((1,), (1,)), ((), ())),
        precision=lax.Precision.HIGHEST,
        preferred_element_type=jnp.float32,
    )
    correction = solved.reshape(current.shape)
    for level in range(3, -1, -1):
        correction = post_smooth(
            answer_list[level] + refine(correction), source_list[level], weight_list[level]
        )
    return correction


K = damping / 6.0
F32 = jnp.float32
BF = jnp.bfloat16


def iota(shape, dim):
    return lax.broadcasted_iota(jnp.int32, shape, dim)


def pick(condition):
    return jnp.where(condition, 1.0, 0.0).astype(BF)


def lanes_of(values, index):
    index = jnp.broadcast_to(index, values.shape)
    return jnp.take_along_axis(values, index, axis=1, mode="promise_in_bounds")


def exact_dot(values, chosen):
    total = None
    for _ in range(3):
        part = values.astype(BF)
        values = values - part.astype(F32)
        term = jnp.dot(part, chosen, preferred_element_type=F32)
        total = term if total is None else total + term
    return total


def around(c):
    rows, lanes = c.shape
    return (pltpu.roll(c, 1, 0) + pltpu.roll(c, rows - 1, 0)) + (
        pltpu.roll(c, 1, 1) + pltpu.roll(c, lanes - 1, 1)
    )


def side_sum(planes):
    rows = planes[0].shape[0]
    row = iota(planes[0].shape, 0)
    outs = []
    for p, c in enumerate(planes):
        s = jnp.where(row > 0, pltpu.roll(c, 1, 0), 0.0) + jnp.where(
            row < rows - 1, pltpu.roll(c, rows - 1, 0), 0.0
        )
        if p > 0:
            s = s + planes[p - 1]
        if p < len(planes) - 1:
            s = s + planes[p + 1]
        outs.append(s)
    return outs


def shifted(c, by):
    lane, lanes = iota(c.shape, 1), c.shape[1]
    inside = lane + by < lanes if by > 0 else lane + by >= 0
    return jnp.where(inside, pltpu.roll(c, -by % lanes, 1), 0.0)


def pair_sum(c, step):
    lanes = c.shape[1]
    even = (iota(c.shape, 1) // step) % 2 == 0
    return c + jnp.where(even, pltpu.roll(c, lanes - step, 1), pltpu.roll(c, step, 1))


def row_sum(c):
    for step in (4, 2, 1):
        c = c + pltpu.roll(c, step, 0)
    return c


def kernel(
    dims, b_hbm, w_hbm, m_hbm, f_ref,
    b_ref, w_ref, m_ref,
    V0, W0, U0, V1, W1, U1, TT, T2, T3, T4, P3, E2, P2, P1, P1s, IW, IW1, MP, W0m, W0p, F0, R0, W1m, W1p, E10,
    SZ0, RZ0, S1v, SZv, RZv, R3v, RCv, S1w, SZw, RZw, R3w, RCw,
    GM, GW, GB, SW, SB,
    tally, load, sent, hr, known,
):
    axes = ("gx", "gy", "gz")
    ix, iy, iz = (lax.axis_index(a) for a in axes)
    n = dims[0] * dims[1] * dims[2]
    me = (ix * dims[1] + iy) * dims[2] + iz

    def flip(i, bits):
        if bits == 1:
            return i + 1 - 2 * (i % 2)
        return {0: i, 2: (i + 2) % 4, 3: 3 - i}[bits]

    def mirrored(k):
        a, b, c = k
        y, z = dims[1] - 1 - iy, dims[2] - 1 - iz
        return ((ix + a) % dims[0], flip(y, b), flip(z, c))

    ends = (dims[1] - 1, dims[2] - 1)
    others = sorted(
        (c + (b + 1) // 2, a, b, c)
        for a in range(dims[0])
        for b in range(dims[1])
        for c in range(dims[2])
        if (a, b, c) != (0,) + ends
    )
    others = [k[1:] for k in others]

    barrier = pltpu.get_barrier_semaphore()

    def there(d):
        ok = None
        for i, s, c in zip((ix, iy, iz), dims, d):
            if c:
                t = (i + c < s) if c > 0 else (i + c >= 0)
                ok = t if ok is None else jnp.logical_and(ok, t)
        return ok

    def directions(most):
        found = []
        for dx in (-1, 0, 1):
            for dy in (-1, 0, 1):
                for dz in (-1, 0, 1):
                    if 0 < abs(dx) + abs(dy) + abs(dz) <= most:
                        found.append((dx, dy, dz))
        return sorted(found, key=lambda d: (-abs(d[1]), -abs(d[2]), abs(d[0])))

    def greet(sem, levels=(1, -1, 0)):
        for dz in levels:
            for dy in (1, -1, 0):
                for dx in range(dims[0]):
                    if not (dx or dy or dz):
                        continue

                    def signal(dx=dx, dy=dy, dz=dz):
                        pl.semaphore_signal(
                            sem, inc=1, device_id=((ix + dx) % dims[0], iy + dy, iz + dz),
                            device_id_type=pl.DeviceIdType.MESH,
                        )

                    ok = there((0, dy, dz))
                    if ok is None:
                        signal()
                    else:
                        pl.when(ok)(signal)

    loads = [
        pltpu.make_async_copy(src, dst, load.at[i])
        for i, src, dst in ((0, b_hbm, b_ref), (0, w_hbm, w_ref), (1, m_hbm, m_ref))
    ]
    for copy in loads:
        copy.start()
    nx, ny = b_ref.shape[0], b_ref.shape[1]
    hx, hy = nx // 2, ny // 2

    def clear(ref, *where):
        part = ref.at[where] if where else ref
        part[...] = jnp.zeros(part.shape, F32)

    own = (pl.ds(0, ny), pl.ds(0, 128))
    clear(V0, pl.ds(0, 2), *own)
    clear(V0, pl.ds(nx + 2, 2), *own)
    clear(V0, pl.ds(1, nx + 2), pl.ds(ny, 8), pl.ds(0, 128))
    clear(W0, pl.ds(1, 1), *own)
    clear(W0, pl.ds(nx + 2, 1), *own)
    clear(W0, pl.ds(2, nx), pl.ds(ny, 8), pl.ds(0, 128))
    for D in (V1, W1):
        clear(D, pl.ds(0, 3))
        clear(D, pl.ds(hx + 3, 3))
        clear(D, pl.ds(3, hx), pl.ds(8, 8))
    for D in (RZ0, RZv, R3v, RCv, RZw, R3w, RCw):
        clear(D)
    greet(barrier, (1, 0))

    def span(i, s):
        return 1 + jnp.where(i > 0, 1, 0) + jnp.where(i < s - 1, 1, 0)

    plane = dims[0] * span(iy, dims[1])
    greeted = span(ix, dims[0]) * span(iy, dims[1]) * span(iz, dims[2]) - 1

    def send(src, dst, d, sem):
        pltpu.make_async_remote_copy(
            src_ref=src, dst_ref=dst, send_sem=sent.at[0], recv_sem=sem,
            device_id=(ix + d[0], iy + d[1], iz + d[2]), device_id_type=pl.DeviceIdType.MESH,
        ).start()

    def send_all(found, pieces, sem):
        def start(group):
            for d in group:
                ok = there((d[0], 0, d[2]))
                if ok is None:
                    send(*pieces(d), d, sem)
                else:
                    @pl.when(ok)
                    def _(d=d):
                        send(*pieces(d), d, sem)

        low = iy < dims[1] // 2
        for c, inward in ((1, low), (-1, jnp.logical_not(low)), (1, jnp.logical_not(low)), (-1, low)):
            group = [d for d in found if d[1] == c]
            if group:
                @pl.when(jnp.logical_and(inward, there((0, c, 0))))
                def _(group=group):
                    start(group)
        start([d for d in found if d[1] == 0])

    def span_x(c, size, pad, deep):
        if c == 0:
            return pl.ds(0, size), pl.ds(pad, size)
        if c > 0:
            return pl.ds(size - deep, deep), pl.ds(pad - deep, deep)
        return pl.ds(0, deep), pl.ds(pad + size, deep)

    def span_y(c, size, total, deep):
        if c == 0:
            return pl.ds(0, size), pl.ds(0, size)
        if c > 0:
            return pl.ds(size - deep, deep), pl.ds(total - deep, deep)
        return pl.ds(0, deep), pl.ds(size, deep)

    def flat(found):
        return [d for d in found if not d[2]]

    first = pl.ds(0, 128)

    def pieces0(d):
        dx, dy, dz = d
        if dz:
            a, b = span_y(dy, ny, ny + 8, 1)
            return SZ0.at[a], RZ0.at[1 - dx, (1 - dz) // 2, b]
        deep = 1 if dx and dy else 2
        a, b = span_x(dx, nx, 2, deep)
        e, f = span_y(dy, ny, ny + 8, deep)
        shifted = pl.ds(a.start + 2, a.size)
        return V0.at[shifted, e, first], V0.at[b, f, first]

    def faces0(d):
        a, b = span_x(d[0], nx, 2, 1)
        e, f = span_y(d[1], ny, ny + 8, 1)
        return W0.at[pl.ds(a.start + 2, a.size), e, first], W0.at[b, f, first]

    def pieces1(S1, D, SZ, RZ):
        def of(d):
            dx, dy, dz = d
            if dz:
                a, b = span_y(dy, 8, 16, 2)
                return SZ.at[a], RZ.at[1 - dx, (1 - dz) // 2, b]
            a, b = span_x(dx, hx, 3, 2 if dy else 3)
            e, f = span_y(dy, 8, 16, 2)
            return S1.at[a, e], D.at[b, f]
        return of

    def late1(S1, R3, SZ, RC):
        def of(d):
            dx, dy, dz = d
            if dz:
                row = pl.ds(7 if dy > 0 else 0, 1)
                return SZ.at[row], RC.at[(1 - dx) // 2, (1 - dz) // 2, row]
            row = pl.ds(5 if dy > 0 else 2, 1)
            return S1.at[:, row], R3.at[:, row]
        return of

    def matrix_rows(d):
        s, r = m_ref, GM.at[me]
        if d[2]:
            row = pl.ds(m_ref.shape[0] - 1 if d[2] > 0 else 0, 1)
            s, r = s.at[row], r.at[row]
        return s, r

    corners = [d for d in directions(3) if all(d)]
    lates = [(0, -1, 0), (0, 1, 0)] + corners

    def bytes_of(ref, sem):
        pltpu.make_async_copy(ref, ref, sem).wait()

    sides_y, sides_z = span(iy, dims[1]) - 1, span(iz, dims[2]) - 1

    def first_part(cy, cz):
        return 32 + 33 * cy + 32 * cz + cy * cz

    def face_part(cy, cz):
        return 16 + 16 * cy

    def second_part(cy, cz):
        return 24 + 20 * cy + 16 * cz + 2 * cy * cz

    def late_part(cy, cz):
        return 8 * cy + cy * cz

    def weight_part(cy, cz):
        return second_part(cy, cz) + late_part(cy, cz)

    def matrix_part(cy, cz):
        return 16 + 32 * cy + 4 * (1 + cy) * cz

    def waiting_part(cy, cz):
        parts = (weight_part, late_part, face_part, matrix_part)
        return sum(part(cy, cz) for part in parts) + 4 * (n - 1)

    def everything(cy, cz):
        parts = (first_part, second_part, waiting_part)
        return sum(part(cy, cz) for part in parts) + 4 * (n - 1)

    def take(part, sem):
        for cy in (1, 2):
            for cz in (1, 2):
                @pl.when(jnp.logical_and(sides_y == cy, sides_z == cz))
                def _(cy=cy, cz=cz):
                    bytes_of(tally.at[pl.ds(0, part(cy, cz))], sem)

    def spread(kind, src, dst, k):
        return pltpu.make_async_remote_copy(
            src_ref=src, dst_ref=dst.at[me], send_sem=sent.at[0], recv_sem=hr.at[kind],
            device_id=mirrored(k), device_id_type=pl.DeviceIdType.MESH,
        )

    def arrive(kind, dst):
        bytes_of(dst.at[pl.ds(0, n - 1)], hr.at[kind])


    has_lower, has_upper = iz > 0, iz < dims[2] - 1
    pl.semaphore_wait(barrier, plane * jnp.where(has_lower, 2, 1) - 1)
    greet(known.at[2], (-1,))
    bytes_of(tally.at[pl.ds(0, 2 * nx * ny)], load.at[0])
    lane16 = iota((ny, 128), 1)
    packed = jnp.zeros((ny, 128), F32)
    for x in range(nx):
        w = w_ref[x]
        v = K * b_ref[x] / w
        V0[x + 2, 0:ny, 0:128] = v
        W0[x + 2, 0:ny, 0:128] = w
        for a, q in enumerate((v, w)):
            start = 8 * x + 4 * a
            moved = pltpu.roll(q, (start + 2) % 128, 1)
            packed = jnp.where((lane16 >= start) & (lane16 < start + 4), moved, packed)
    SZ0[...] = packed

    send_all([d for d in directions(2) if d[2] <= 0], pieces0, hr.at[0])

    @pl.when(has_upper)
    def _():
        pl.semaphore_wait(known.at[2], plane)

    send_all([d for d in directions(2) if d[2] > 0], pieces0, hr.at[0])
    greet(known.at[0])
    send_all(flat(directions(1)), faces0, hr.at[1])

    lane_row = iota((1, 128), 1)
    low_half = jnp.minimum(2 * lane_row, 126)

    def coarsen0(planes):
        for i in range(hx):
            TT[i] = planes(2 * i) + planes(2 * i + 1)
        rows = [
            TT[i, pl.ds(0, hy, stride=2), :] + TT[i, pl.ds(1, hy, stride=2), :] for i in range(hx)
        ]
        rows = jnp.concatenate(rows, axis=0)
        return lanes_of(rows, low_half) + lanes_of(rows, low_half + 1)

    held_x = (lane_row // 32 + 4 - iz) % 4
    pairs = 2 * (lane_row % 32)

    def coarsen1(planes, SG):
        for i in range(hx // 2):
            T2[pl.ds(8 * i, 8), :] = planes(2 * i) + planes(2 * i + 1)
        pieces = [
            T2[pl.ds(8 * x, 4, stride=2), :] + T2[pl.ds(8 * x + 1, 4, stride=2), :]
            for x in range(4)
        ]
        rows = [jnp.concatenate(pieces[i : i + 2], axis=0) for i in (0, 2)]
        sums = [lanes_of(r, pairs) + lanes_of(r, pairs + 1) for r in rows]
        parts = [sums[x // 2][4 * (x % 2) : 4 * (x % 2) + 4] for x in range(4)]
        total = parts[0]
        for x in range(1, 4):
            total = jnp.where(held_x == x, parts[x], total)
        return total

    lane8 = iota((8, 128), 1)

    def pack1(S1, SZ, planes):
        out = jnp.zeros((8, 128), F32)
        for x in range(hx):
            q = planes[x]
            S1[x] = q
            s = 16 * x
            h = (s + 64) % 128
            out = jnp.where((lane8 >= h) & (lane8 < h + 3), pltpu.roll(q, (h - 61) % 128, 1), out)
            out = jnp.where(
                (lane8 >= s + 3) & (lane8 < s + 6), pltpu.roll(q, (s + 3) % 128, 1), out
            )
        SZ[...] = out

    w1 = 0.0625 * coarsen0(lambda x: w_ref[x])
    w1 = [w1[8 * x : 8 * x + 8, :] for x in range(hx)]
    pack1(S1w, SZw, w1)
    SW[...] = 0.0625 * coarsen1(lambda x: w1[x], SW)
    GW[me] = SW[...]
    loads[2].wait()
    GM[me] = m_ref[...]
    send_all(directions(2), pieces1(S1w, W1, SZw, RZw), hr.at[1])
    send_all(lates, late1(S1w, R3w, SZw, RCw), hr.at[1])
    send_all(directions(3), matrix_rows, hr.at[1])
    pl.semaphore_wait(known.at[0], greeted)
    greet(known.at[1])

    def coords(rows, lanes, cy, cz, by, bz):
        r, l = iota((rows, lanes), 0), iota((rows, lanes), 1)
        y = jnp.where(r < cy + (rows - cy) // 2, r, r - rows)
        z = jnp.where(l < cz + (lanes - cz) // 2, l, l - lanes)
        gy, gz = y + iy * cy, z + iz * cz
        ok = (gy >= 0) & (gy < dims[1] * cy) & (gz >= 0) & (gz < dims[2] * cz)
        near = (y >= -by) & (y < cy + by) & (z >= -bz) & (z < cz + bz)
        return jnp.where(ok & near, 1, 0)

    def plane_mask(base, x, cx):
        if 0 <= x < cx:
            return base > 0
        gx = x + ix * cx
        inside = jnp.where((gx >= 0) & (gx < dims[0] * cx), 1, 0)
        return base * inside > 0

    row8 = iota((8, 128), 0)
    row16, lane_own = iota((ny, 128), 0), iota((ny, 128), 1)

    def in_lanes(c):
        return shifted(c, -1) + shifted(c, 1)

    def in_rows(c):
        return jnp.where(row16 > 0, pltpu.roll(c, 1, 0), 0.0) + jnp.where(
            row16 < ny - 1, pltpu.roll(c, ny - 1, 0), 0.0
        )

    def beside(planes, x):
        found = [planes[i] for i in (x - 1, x + 1) if 0 <= i < nx]
        return found[0] + found[1] if len(found) > 1 else found[0]

    inner = [V0[x + 2, 0:ny, 0:128] for x in range(nx)]
    inner_u = [
        1.2 * c + K * (in_rows(c) + in_lanes(c) + beside(inner, x)) for x, c in enumerate(inner)
    ]
    for x, u in enumerate(inner_u):
        near_sum = in_rows(u) + in_lanes(u) + beside(inner_u, x)
        R0[x] = b_ref[x] - w_ref[x] * (6.0 * u - near_sum)
    kind = lane_own % 8
    packed = SZ0[...]
    own_ends = jnp.where(kind == 1, pltpu.roll(packed, 127, 1), pltpu.roll(packed, 1, 1))
    has_z = ((kind == 1) & (iz > 0)) | ((kind == 2) & (iz < dims[2] - 1))
    has_y = ((row8 == 7) & (iy > 0)) | ((row8 == 0) & (iy < dims[1] - 1))

    def exists(c):
        return (ix + c >= 0) & (ix + c < dims[0])

    take(first_part, hr.at[0])
    mask0 = coords(24, 256, ny, 128, 1, 1) > 0
    lane24 = iota((24, 128), 1)

    def z_ends(dx):
        return jnp.where(lane24 % 4 >= 2, RZ0[dx + 1, 1], RZ0[dx + 1, 0])

    ends = {dx: z_ends(dx) for dx in (-1, 0, 1)}

    def z_change():
        full, c = ends[0], ends[0][0:ny]
        above, below = pltpu.roll(full, 1, 1), pltpu.roll(full, 127, 1)
        left = pltpu.roll(jnp.where(lane_own >= 120, ends[-1][0:ny], c), 8, 1)
        right = pltpu.roll(jnp.where(lane_own < 8, ends[1][0:ny], c), 120, 1)
        outer = jnp.where(kind == 1, above[0:ny], below[0:ny])
        vert = (pltpu.roll(full, 1, 0) + pltpu.roll(full, ny + 7, 0))[0:ny]
        u = 1.2 * c + K * (outer + own_ends + vert + left + right)
        u = jnp.where(has_z, u, 0.0)
        across = jnp.where(lane_own >= 8, left, 0.0) + jnp.where(lane_own < 120, right, 0.0)
        d = K * (6.0 * c - in_rows(c) - across) - u
        low = jnp.where(kind == 1, d, -K * above[0:ny])
        high = jnp.where(kind == 2, d, -K * below[0:ny])
        swapped = jnp.where(lane8 % 8 == 1, below[ny:], above[ny:])
        return low, high, swapped

    low_end, high_end, edge_ends = z_change()
    side = [V0[p, ny : ny + 8, 0:128] for p in range(1, nx + 3)]

    def z_part(x):
        a = pltpu.roll(low_end, (-8 * x - 1) % 128, 1)
        b = pltpu.roll(high_end, (125 - 8 * x) % 128, 1)
        return jnp.where(lane_own < 2, a, jnp.where(lane_own >= 126, b, 0.0))

    def y_part(x):
        c = side[x + 1]
        ends_x = pltpu.roll(edge_ends, (126 - 8 * x) % 128, 1)
        flat_sum = in_lanes(c)
        edges = jnp.where((lane8 == 0) | (lane8 == 127), ends_x, 0.0)
        adjacent = jnp.where(
            row8 == 7, pltpu.roll(inner[x][0:8], 7, 0), pltpu.roll(inner[x][8:16], 1, 0)
        )
        outer = jnp.where(row8 == 7, pltpu.roll(c, 1, 0), pltpu.roll(c, 7, 0))
        u = 1.2 * c + K * (flat_sum + edges + adjacent + outer + side[x] + side[x + 2])
        u = jnp.where(has_y, u, 0.0)
        d = K * (6.0 * c - flat_sum - beside(side[1:-1], x)) - u
        first_rows = jnp.where(row8 == 1, -K * pltpu.roll(c, 2, 0), 0.0)
        first_rows = jnp.where(row8 == 0, pltpu.roll(d, 1, 0), first_rows)
        last_rows = jnp.where(row8 == 6, -K * pltpu.roll(c, 6, 0), 0.0)
        last_rows = jnp.where(row8 == 7, pltpu.roll(d, 7, 0), last_rows)
        return jnp.concatenate([first_rows, last_rows], axis=0)

    def x_part(p, c, x, edge):
        h, beyond = V0[p, 0:ny, 0:128], V0[p + c, 0:ny, 0:128]
        a = pltpu.roll(ends[c][0:ny], (-8 * x - 1) % 128, 1)
        b = pltpu.roll(ends[c][0:ny], (125 - 8 * x) % 128, 1)
        t = V0[p, ny : ny + 8, 0:128]
        rows = jnp.concatenate(
            [
                jnp.where(row8 == 0, pltpu.roll(t, 1, 0), 0.0),
                jnp.where(row8 == 7, pltpu.roll(t, 7, 0), 0.0),
            ],
            axis=0,
        )
        edges = jnp.where(lane_own == 0, a, jnp.where(lane_own == 127, b, 0.0)) + rows
        near_sum = in_lanes(h) + in_rows(h)
        u = 1.2 * h + K * (near_sum + edges + beyond + inner[edge])
        u = jnp.where(exists(c), u, 0.0)
        return K * (6.0 * h - near_sum) - u, -K * h

    x_parts = {}
    for p, c, x, edge in ((1, -1, nx - 1, 0), (nx + 2, 1, 0, nx - 1)):
        x_parts[edge], x_parts[edge - c] = x_part(p, c, x, edge)

    def resid0(x):
        change = z_part(x) + y_part(x)
        if x in x_parts:
            change = change + x_parts[x]
        return R0[x] - w_ref[x] * change

    def smooth0():
        for dx in (-1, 0, 1):
            for x in {-1: (nx - 1,), 0: range(nx), 1: (0,)}[dx]:
                moved = pltpu.roll(z_ends(dx), (126 - 8 * x) % 128, 1)
                V0[x + 2 + dx * nx, :, 128:256] = moved
        for p, c in ((1, -1), (nx + 2, 1)):
            u = 1.2 * V0[p, 0:ny, 0:128] + K * own_sum(V0, p)
            U0[p, 0:ny, 0:128] = jnp.where(exists(c), u, 0.0)
        for p in range(2, nx + 2):
            c = V0[p]
            u = 1.2 * c + K * (around(c) + (V0[p - 1] + V0[p + 1]))
            U0[p] = jnp.where(mask0, u, 0.0)

    def assemble_faces():
        moved = z_ends(0)
        for x in range(nx):
            p = x + 2
            W0[p, :, 128:256] = pltpu.roll(moved, (122 - 8 * x) % 128, 1)
            IW[x] = 1.0 / w_ref[x]
            W0m[x] = pltpu.roll(W0[p, 0:ny, :], 1, 1)[:, 0:128]
            W0p[x] = pltpu.roll(W0[p, 0:ny, :], 255, 1)[:, 0:128]
            F0[x] = 0.2 * U0[p, 0:ny, 0:128] + V0[p, 0:ny, 0:128] + K * own_sum(U0, p)

    def own_sum(ref, p):
        col, wide = ref[p, :, 0:128], ref[p, 0:ny, :]
        vert = pltpu.roll(col, 1, 0)[0:ny] + pltpu.roll(col, ny + 7, 0)[0:ny]
        flat_sum = pltpu.roll(wide, 1, 1)[:, 0:128] + pltpu.roll(wide, 255, 1)[:, 0:128]
        return (vert + flat_sum) + (ref[p - 1, 0:ny, 0:128] + ref[p + 1, 0:ny, 0:128])

    b1 = 0.125 * coarsen0(resid0)
    b1 = [b1[8 * x : 8 * x + 8, :] for x in range(hx)]
    v1 = [jnp.where(lane8 < 64, K * b1[x] / jnp.where(lane8 < 64, w1[x], 1.0), 0.0) for x in range(hx)]
    pack1(S1v, SZv, v1)
    send_all(directions(2), pieces1(S1v, V1, SZv, RZv), hr.at[2])
    send_all(lates, late1(S1v, R3v, SZv, RCv), hr.at[1])
    pl.semaphore_wait(known.at[1], greeted)
    for k in others:
        spread(1, SW, GW, k).start()

    mask1 = coords(16, 128, 8, 64, 2, 2)
    mask_up = coords(16, 128, 8, 64, 1, 1)
    mask_own = coords(16, 128, 8, 64, 0, 0)
    lane1 = iota((16, 128), 1)

    def assemble1(S1, RZ, D):
        for dx in (-1, 0, 1):
            ends = jnp.where(lane1 % 16 < 3, RZ[dx + 1, 0], RZ[dx + 1, 1])
            for x in {-1: (hx - 2, hx - 1), 0: range(hx), 1: (0, 1)}[dx]:
                p = x + 3 + dx * hx
                moved = pltpu.roll(ends, (61 - 16 * x) % 128, 1)
                inner = S1[x] if dx == 0 else D[p, 0:8, :]
                D[p, 0:8, :] = jnp.where(lane8 < 64, inner, moved[0:8])
                D[p, 8:16, :] = jnp.where(lane8 < 64, D[p, 8:16, :], moved[8:16])

    def finish1(R3, RC, D):
        for x in range(hx):
            D[x + 3, 8:16, :] = jnp.where((row8 == 2) | (row8 == 5), R3[x], D[x + 3, 8:16, :])
        for slot, p, x in ((0, 2, hx - 1), (1, hx + 3, 0)):
            ends = jnp.where(lane8 % 16 < 3, RC[slot, 0], RC[slot, 1])
            moved = pltpu.roll(ends, (61 - 16 * x) % 128, 1)
            D[p, 8:16, :] = jnp.where(lane8 < 64, D[p, 8:16, :], moved)

    def smooth1(planes):
        for p in planes:
            c = V1[p]
            u = 1.2 * c + K * (around(c) + (V1[p - 1] + V1[p + 1]))
            U1[p] = jnp.where(plane_mask(mask1, p - 3, hx), u, 0.0)

    block = lane8 // 32

    def gathered(G):
        planes = []
        for gx in range(dims[0]):
            tiles = {}
            for t in range(dims[1] // 2):
                for z in range(dims[2]):
                    d0 = (gx * dims[1] + 2 * t) * dims[2] + z
                    tiles[t, z] = jnp.concatenate([G[d0], G[d0 + dims[2]]], axis=0)
            for x in range(4):
                parts = []
                for t in range(dims[1] // 2):
                    out = tiles[t, 0]
                    for z in range(1, dims[2]):
                        out = jnp.where(block == (x + z) % 4, tiles[t, z], out)
                    parts.append(out)
                planes.append(jnp.concatenate(parts, axis=0))
        return planes

    def turned(planes, by):
        return [
            pltpu.roll(c, (-32 * (X % 4) - by) % 128, 1) if X % 4 or by else c
            for X, c in enumerate(planes)
        ]

    def coarsen2(planes):
        c = len(planes) // 2
        for i in range(c):
            T3[i] = planes[2 * i] + planes[2 * i + 1]
        return [
            pair_sum(T3[i, pl.ds(0, 8, stride=2), :] + T3[i, pl.ds(1, 8, stride=2), :], 1)
            for i in range(c)
        ]

    take(second_part, hr.at[2])
    assemble1(S1v, RZv, V1)
    smooth1(range(2, hx + 4))

    def resid1(x):
        p = x + 3
        s = around(U1[p])[0:8, :] + (U1[p - 1, 0:8, :] + U1[p + 1, 0:8, :])
        return jnp.where(lane8 < 64, b1[x] - w1[x] * (6.0 * U1[p, 0:8, :] - s), 0.0)

    SB[...] = 0.125 * coarsen1(resid1, SB)
    GB[me] = SB[...]
    for k in others:
        spread(3, SB, GB, k).start()
    take(waiting_part, hr.at[1])
    turned_w2 = gathered(GW)
    scale2 = [K / q for q in turned_w2]
    w2 = turned(turned_w2, 0)
    w2m, w2p = [shifted(q, -1) for q in w2], [shifted(q, 1) for q in w2]
    unscale2 = [q * (1.0 / K) for q in w2]
    iw2 = [1.0 / q for q in w2]
    w3 = [0.0625 * q for q in coarsen2(w2)]
    around3 = {k: [shifted(q, 2 * k) if k else q for q in w3] for k in (-2, -1, 0, 1, 2)}
    iw3 = [1.0 / q for q in w3]
    inverse3 = {k: [shifted(q, 2 * k) if k else q for q in iw3] for k in (-1, 0, 1)}
    smooth0()
    assemble_faces()
    assemble1(S1w, RZw, W1)
    finish1(R3w, RCw, W1)
    for p in range(2, hx + 4):
        inside = plane_mask(mask_up if 0 <= p - 3 < hx else mask_own, p - 3, hx)
        IW1[p] = jnp.where(inside, 1.0, 0.0) / jnp.where(inside, W1[p], 1.0)
        W1m[p] = pltpu.roll(W1[p], 1, 1)
        W1p[p] = pltpu.roll(W1[p], 127, 1)
    finish1(R3v, RCv, V1)
    smooth1(range(1, hx + 5))
    for p in range(2, hx + 4):
        c = U1[p]
        E10[p] = 0.2 * c + V1[p] + K * (around(c) + (U1[p - 1] + U1[p + 1]))

    def near(i, c, size):
        return jnp.clip(i + c, 0, size - 1)

    steps = (-1, 0, 1)
    blocks = [(x, dy, dz) for x in range(dims[0]) for dy in steps for dz in steps]
    rows = jnp.concatenate(
        [
            GM[(x * dims[1] + near(iy, dy, dims[1])) * dims[2] + near(iz, dz, dims[2])]
            for x, dy, dz in blocks
        ],
        axis=0,
    )
    order = pick(
        iota((128, 128), 0) == (iota((128, 128), 1) % 4) * 32 + iota((128, 128), 1) // 4
    )
    for h in range(2):
        MP[h] = exact_dot(rows[:, 128 * h : 128 * h + 128], order)
    other_w = [jnp.where(lane8 // 2 % 2 == 0, a, b) for a, b in zip(around3[1], around3[-1])]
    other_c = [q * (1.0 / K) for q in other_w]
    far = jnp.full((8, 128), -99)
    wanted = {-1: jnp.where(row8 == 7, -1, far), 0: row8, 1: jnp.where(row8 == 0, 8, far)}
    held = {}
    for k in (-2, -1, 0, 1, 2):
        cell = lane8 + 2 * k
        held[k] = jnp.where((cell >= 0) & (cell < 128), cell // 4 - 8 * iz, -50)
    moves = (0, 1, -1)
    double = [(lane_row + k + 256) // 2 % 128 for k in moves]
    depth = jnp.where(lane_row < 96, lane_row, lane_row - 128)
    here = [jnp.clip((depth + k + 256) // 2 - 128 + 32 * iz, 0, 127) for k in moves]
    even = lane8 % 2 == 0
    E2[...] = jnp.zeros_like(E2)
    arrive(3, GB)

    v_turned = [b * r for b, r in zip(gathered(GB), scale2)]
    v2 = turned(v_turned, 0)
    lane_wide = iota((16, 128), 1)
    before = [jnp.where(lane_wide > 0, q, 0.0) for q in turned(v_turned, -1)]
    after = [jnp.where(lane_wide < 127, q, 0.0) for q in turned(v_turned, 1)]
    u2 = [1.2 * v + K * (s + (a + b)) for v, s, a, b in zip(v2, side_sum(v2), before, after)]
    s2 = [s + (shifted(u, -1) + shifted(u, 1)) for s, u in zip(side_sum(u2), u2)]
    r2 = [v * k - w * (6.0 * u - s) for v, k, w, u, s in zip(v2, unscale2, w2, u2, s2)]
    base2 = [0.2 * u + v + K * s for u, v, s in zip(u2, v2, s2)]
    b3 = [0.125 * q for q in coarsen2(r2)]
    v3 = {0: [K * b * r for b, r in zip(b3, iw3)]}
    for k in (-3, -2, -1, 1, 2, 3):
        v3[k] = [shifted(v, 2 * k) for v in v3[0]]
    u3 = {}
    for k in (-2, -1, 0, 1, 2):
        u3[k] = [
            1.2 * v + K * (s + (a + b))
            for v, s, a, b in zip(v3[k], side_sum(v3[k]), v3[k - 1], v3[k + 1])
        ]
        if k:
            cell = lane8 + 2 * k
            u3[k] = [jnp.where((cell >= 0) & (cell < 128), u, 0.0) for u in u3[k]]
    even3 = lane8 // 2 % 2 == 0

    def partner(q, k):
        return [jnp.where(even3, a, b) for a, b in zip(q[k], q[-k])]

    s3 = [s + (a + b) for s, a, b in zip(side_sum(u3[0]), u3[-1], u3[1])]
    r3 = [b - w * (6.0 * u - s) for b, w, u, s in zip(b3, w3, u3[0], s3)]
    base3 = [0.2 * u + v + K * s for u, v, s in zip(u3[0], v3[0], s3)]
    base3 = {k: [shifted(q, 2 * k) if k else q for q in base3] for k in (-1, 0, 1)}
    other_u, other_v = partner(u3, 1), partner(v3, 1)
    sides = side_sum(other_u)
    r3 = [
        r + v * c - w * (6.0 * u - (s + a + b))
        for r, v, c, w, u, s, a, b in zip(
            r3, other_v, other_c, other_w, other_u, sides, u3[0], partner(u3, 2)
        )
    ]
    c4 = len(r3) // 2
    for i in range(c4):
        T4[pl.ds(8 * i, 8), :] = r3[2 * i] + r3[2 * i + 1]
    half = 4 * c4
    b4 = 0.125 * (T4[pl.ds(0, half, stride=2), :] + T4[pl.ds(1, half, stride=2), :])
    chosen = jnp.where(row8 % 4 == lane8 % 4, b4, 0.0)
    low = row_sum(jnp.where(row8 < 4, chosen, 0.0))
    high = row_sum(jnp.where(row8 >= 4, chosen, 0.0))
    solved = [
        jnp.sum(MP[0, 8 * k : 8 * k + 8, :] * low + MP[1, 8 * k : 8 * k + 8, :] * high,
                axis=1, keepdims=True)
        for k in range(len(blocks))
    ]
    q3 = {}
    for k in (-2, -1, 0, 1, 2):
        e4 = []
        for x in range(dims[0]):
            plane = jnp.zeros((8, 128), F32)
            for dy in steps:
                found = jnp.zeros((8, 128), F32)
                for dz in steps:
                    value = solved[blocks.index((x, dy, dz))]
                    found = jnp.where(held[k] == wanted[dz], value, found)
                plane = jnp.where(row8 // 2 == iy + dy, row_sum(found), plane)
            e4.append(plane)
        q3[k] = [w * e4[i // 2] for i, w in enumerate(around3[k])]
    e3 = {}
    for k in (-1, 0, 1):
        sides = side_sum(q3[k])
        e3[k] = [
            (base + 0.2 * q + K * (s + (a + b))) * r
            for base, q, s, a, b, r in zip(
                base3[k], q3[k], sides, q3[k - 1], q3[k + 1], inverse3[k]
            )
        ]
    for i in range(2 * dims[0]):
        middle = e3[0][i]
        views = (middle, jnp.where(even, middle, e3[1][i]), jnp.where(even, e3[-1][i], middle))
        for k, e in enumerate(views):
            P3[k, i, pl.ds(0, 8, stride=2), :] = e
            P3[k, i, pl.ds(1, 8, stride=2), :] = e
    q2 = [w * P3[0, i // 2] for i, w in enumerate(w2)]
    sides = side_sum(q2)
    for i, (base, q, s) in enumerate(zip(base2, q2, sides)):
        ends = w2p[i] * P3[1, i // 2] + w2m[i] * P3[2, i // 2]
        E2[i + 1, 8:24, :] = (base + 0.2 * q + K * (s + ends)) * iw2[i]

    seen = jnp.concatenate([E2[4 * ix + i, pl.ds(6 + 4 * iy, 8), :] for i in range(6)], axis=0)
    for k in range(3):
        wide2 = lanes_of(pltpu.roll(seen.reshape((6, 8, 128)), 6, 1).reshape((48, 128)), here[k])
        for i in range(6):
            q = wide2[8 * i : 8 * i + 8]
            P2[k, i, pl.ds(0, 8, stride=2), :] = q
            P2[k, i, pl.ds(1, 8, stride=2), :] = q
    q1 = {p: W1[p] * P2[0, (p - 3) // 2 + 1] for p in range(1, hx + 5)}
    e1 = []
    for p in range(2, hx + 4):
        q, i = q1[p], (p - 3) // 2 + 1
        ends = W1p[p] * P2[1, i] + W1m[p] * P2[2, i]
        s = (pltpu.roll(q, 1, 0) + pltpu.roll(q, 15, 0)) + ends + (q1[p - 1] + q1[p + 1])
        e1.append((E10[p] + 0.2 * q + K * s) * IW1[p])
    wide1 = lanes_of(jnp.concatenate(e1, axis=0), double[0])
    for i in range(hx + 2):
        q = wide1[16 * i : 16 * i + 16]
        P1[i, pl.ds(0, 16, stride=2), :] = q
        P1[i, pl.ds(1, 16, stride=2), :] = q
    for k in (1, 2):
        wide1 = lanes_of(jnp.concatenate([e[0:8] for e in e1[1:-1]], axis=0), double[k])
        for i in range(hx):
            q = wide1[8 * i : 8 * i + 8]
            P1s[k - 1, i + 1, pl.ds(0, 8, stride=2), :] = q
            P1s[k - 1, i + 1, pl.ds(1, 8, stride=2), :] = q

    def scaled(p):
        i = (p - 2) // 2 + 1
        if not 2 <= p < nx + 2:
            return W0[p, 0:ny, 0:128] * P1[i, 0:16, :]
        edge = jnp.where(row8 < 4, P1[i, 16:24, :], P1[i, 24:32, :])
        return W0[p, :, 0:128] * jnp.concatenate([P1[i, 0:16, :], edge], axis=0)

    q0 = {p: scaled(p) for p in range(1, nx + 3)}
    for x in range(nx):
        p, i = x + 2, x // 2 + 1
        q = q0[p]
        ends = W0p[x] * P1s[0, i] + W0m[x] * P1s[1, i]
        vert = pltpu.roll(q, 1, 0)[0:ny] + pltpu.roll(q, ny + 7, 0)[0:ny]
        s = vert + ends + (q0[p - 1][0:ny] + q0[p + 1][0:ny])
        f_ref[x] = (F0[x] + 0.2 * q[0:ny] + K * s) * IW[x]

    take(everything, sent.at[0])


def fused(dims, sources, stiffness, coarse_inverse):
    nx, ny, nz = stiffness.shape
    n = dims[0] * dims[1] * dims[2]
    vm = lambda *s: pltpu.VMEM(s, F32)
    halo1 = [vm(8, 8, 128), vm(8, 128), vm(3, 2, 16, 128), vm(8, 8, 128), vm(2, 2, 8, 128)]
    result = pl.pallas_call(
        functools.partial(kernel, dims),
        out_shape=pltpu.VMEM((nx, ny, nz), F32),
        in_specs=[pl.BlockSpec(memory_space=pl.ANY)] * 3,
        out_specs=pl.BlockSpec(memory_space=pltpu.VMEM),
        scratch_shapes=[
            vm(nx, ny, nz), vm(nx, ny, nz), vm(*coarse_inverse.shape),
            vm(nx + 4, 24, 256), vm(nx + 4, 24, 256), vm(nx + 4, 24, 256),
            vm(14, 16, 128), vm(14, 16, 128), vm(14, 16, 128),
            vm(8, 16, 128), vm(32, 128), vm(2 * dims[0], 16, 128),
            vm(16, 128), vm(3, 2 * dims[0], 16, 128),
            vm(4 * dims[0] + 2, 32, 128), vm(3, 6, 16, 128), vm(10, 32, 128), vm(2, 10, 16, 128),
            vm(nx, ny, nz), vm(14, 16, 128), vm(2, 72 * dims[0], 128),
            vm(nx, ny, nz), vm(nx, ny, nz), vm(nx, ny, nz), vm(nx, ny, nz),
            vm(14, 16, 128), vm(14, 16, 128), vm(14, 16, 128),
            vm(ny, 128), vm(3, 2, ny + 8, 128),
        ]
        + halo1 + halo1
        + [
            vm(n, 8, 256), vm(n, 4, 128), vm(n, 4, 128), vm(4, 128), vm(4, 128),
            vm(2048, 128),
            pltpu.SemaphoreType.DMA((2,)), pltpu.SemaphoreType.DMA((1,)),
            pltpu.SemaphoreType.DMA((4,)),
            pltpu.SemaphoreType.REGULAR((3,)),
        ],
        compiler_params=pltpu.CompilerParams(collective_id=0, has_side_effects=True),
        name="cycle",
    )(sources[0], stiffness, coarse_inverse)
    return result[None]


def solution(mesh):
    dims = tuple(mesh.shape[a] for a in ("gx", "gy", "gz"))

    def run(sources, stiffness, coarse_inverse):
        nx, ny, nz = stiffness.shape
        lanes = 128
        cells = coarse_inverse.shape[1]
        levels_fit = (
            sources.shape[0] == 1
            and nx == ny == 16
            and nz == lanes
            and dims[2] * nz == 4 * lanes
            and dims[1] * ny == 64
            and cells == 2 * lanes
            and dims[0] == 2
        )
        if levels_fit:
            return fused(dims, sources, stiffness, coarse_inverse)
        return per_device(sources, stiffness, coarse_inverse)

    in_specs = (P(None, "gx", "gy", "gz"), P("gx", "gy", "gz"), P(("gx", "gy", "gz"), None))
    out_specs = P(None, "gx", "gy", "gz")
    return jax.shard_map(
        run, mesh=mesh, in_specs=in_specs, out_specs=out_specs, check_vma=False
    )
```

```python
import functools
import jax
import jax.numpy as jnp
from jax import lax
from jax.experimental import pallas as pl
from jax.experimental.pallas import tpu as pltpu
from jax.sharding import PartitionSpec as P

damping = 0.8


def extended(cells, sides, width):
    for axis, dim in sides:
        count = lax.axis_size(axis)
        ends = count - 1
        head = lax.slice_in_dim(cells, 0, width, axis=dim)
        tail = lax.slice_in_dim(cells, cells.shape[dim] - width, cells.shape[dim], axis=dim)
        cells = jnp.concatenate(
            [
                lax.ppermute(tail, axis, [(i, (i + 1) % count) for i in range(ends)]),
                cells,
                lax.ppermute(head, axis, [((i + 1) % count, i) for i in range(ends)]),
            ],
            axis=dim,
        )
    return cells


def loop_sum(padded):
    total = padded[:, 2:, 1:-1, 1:-1] + padded[:, :-2, 1:-1, 1:-1]
    total = total + padded[:, 1:-1, 2:, 1:-1] + padded[:, 1:-1, :-2, 1:-1]
    total = total + padded[:, 1:-1, 1:-1, 2:] + padded[:, 1:-1, 1:-1, :-2]
    return total


def inner_part(values):
    return values[:, 1:-1, 1:-1, 1:-1]


def pre_smooth(source, weights):
    count = source.shape[0]
    stacked = jnp.concatenate([source, weights], axis=0)
    wide = extended(stacked, (("gx", 1), ("gy", 2), ("gz", 3)), 2)
    wide_source = wide[:count]
    wide_weights = wide[count:]
    safe_weights = jnp.where(wide_weights > 0.0, wide_weights, 1.0)
    first = damping * wide_source / (6.0 * safe_weights * safe_weights)
    first_scaled = wide_weights * first
    mid_weights = inner_part(wide_weights)
    mid_safe = inner_part(safe_weights)
    applied = mid_weights * (6.0 * inner_part(first_scaled) - loop_sum(first_scaled))
    second = inner_part(first) + damping * (inner_part(wide_source) - applied) / (
        6.0 * mid_safe * mid_safe
    )
    second_scaled = mid_weights * second
    answer = inner_part(second)
    resid = source - weights * (6.0 * inner_part(second_scaled) - loop_sum(second_scaled))
    return (answer, resid)


def post_smooth(answer, source, weights):
    scaled = weights * answer
    wide = extended(scaled, (("gx", 1), ("gy", 2), ("gz", 3)), 1)
    applied = weights * (6.0 * scaled - loop_sum(wide))
    return answer + damping * (source - applied) / (6.0 * weights * weights)


def coarsen(values):
    leading = values.shape[0]
    size_x, size_y, size_z = (values.shape[1], values.shape[2], values.shape[3])
    blocks = values.reshape((leading, size_x // 2, 2, size_y // 2, 2, size_z // 2, 2))
    return jnp.mean(blocks, axis=(2, 4, 6))


def refine(values):
    return jnp.repeat(jnp.repeat(jnp.repeat(values, 2, axis=1), 2, axis=2), 2, axis=3)


def per_device(sources, stiffness, coarse_inverse):
    weight_list = [stiffness[None]]
    for level in range(3):
        weight_list.append(0.5 * coarsen(weight_list[-1]))
    source_list = []
    answer_list = []
    current = sources
    for level in range(4):
        source_list.append(current)
        answer, resid = pre_smooth(current, weight_list[level])
        answer_list.append(answer)
        current = coarsen(resid)
    count = current.shape[0]
    flat_source = current.reshape((count, -1))
    solved = lax.dot_general(
        lax.all_gather(flat_source, ("gx", "gy", "gz"), axis=1, tiled=True),
        coarse_inverse,
        (((1,), (1,)), ((), ())),
        precision=lax.Precision.HIGHEST,
        preferred_element_type=jnp.float32,
    )
    correction = solved.reshape(current.shape)
    for level in range(3, -1, -1):
        correction = post_smooth(
            answer_list[level] + refine(correction), source_list[level], weight_list[level]
        )
    return correction


K = damping / 6.0
F32 = jnp.float32
BF = jnp.bfloat16


def iota(shape, dim):
    return lax.broadcasted_iota(jnp.int32, shape, dim)


def pick(condition):
    return jnp.where(condition, 1.0, 0.0).astype(BF)


def lanes_of(values, index):
    index = jnp.broadcast_to(index, values.shape)
    return jnp.take_along_axis(values, index, axis=1, mode="promise_in_bounds")


def exact_dot(values, chosen):
    total = None
    for _ in range(3):
        part = values.astype(BF)
        values = values - part.astype(F32)
        term = jnp.dot(part, chosen, preferred_element_type=F32)
        total = term if total is None else total + term
    return total


def around(c):
    rows, lanes = c.shape
    return (pltpu.roll(c, 1, 0) + pltpu.roll(c, rows - 1, 0)) + (
        pltpu.roll(c, 1, 1) + pltpu.roll(c, lanes - 1, 1)
    )


def side_sum(planes):
    rows = planes[0].shape[0]
    row = iota(planes[0].shape, 0)
    outs = []
    for p, c in enumerate(planes):
        s = jnp.where(row > 0, pltpu.roll(c, 1, 0), 0.0) + jnp.where(
            row < rows - 1, pltpu.roll(c, rows - 1, 0), 0.0
        )
        if p > 0:
            s = s + planes[p - 1]
        if p < len(planes) - 1:
            s = s + planes[p + 1]
        outs.append(s)
    return outs


def shifted(c, by):
    lane, lanes = iota(c.shape, 1), c.shape[1]
    inside = lane + by < lanes if by > 0 else lane + by >= 0
    return jnp.where(inside, pltpu.roll(c, -by % lanes, 1), 0.0)


def pair_sum(c, step):
    lanes = c.shape[1]
    even = (iota(c.shape, 1) // step) % 2 == 0
    return c + jnp.where(even, pltpu.roll(c, lanes - step, 1), pltpu.roll(c, step, 1))


def row_sum(c):
    for step in (4, 2, 1):
        c = c + pltpu.roll(c, step, 0)
    return c


def kernel(
    dims, b_hbm, w_hbm, m_hbm, f_ref,
    b_ref, w_ref, m_ref,
    V0, W0, U0, V1, W1, U1, TT, T2, T3, T4, P3, E2, P2, P1, P1s, IW, IW1, MP, W0m, W0p, F0, R0, W1m, W1p, E10,
    SZ0, RZ0, S1v, SZv, RZv, R3v, RCv, S1w, SZw, RZw, R3w, RCw,
    GM, GW, GB, SW, SB,
    tally, load, sent, hr, known,
):
    axes = ("gx", "gy", "gz")
    ix, iy, iz = (lax.axis_index(a) for a in axes)
    n = dims[0] * dims[1] * dims[2]
    me = (ix * dims[1] + iy) * dims[2] + iz

    def flip(i, bits):
        if bits == 1:
            return i + 1 - 2 * (i % 2)
        return {0: i, 2: (i + 2) % 4, 3: 3 - i}[bits]

    def mirrored(k):
        a, b, c = k
        y, z = dims[1] - 1 - iy, dims[2] - 1 - iz
        return ((ix + a) % dims[0], flip(y, b), flip(z, c))

    ends = (dims[1] - 1, dims[2] - 1)
    others = sorted(
        (c + (b + 1) // 2, a, b, c)
        for a in range(dims[0])
        for b in range(dims[1])
        for c in range(dims[2])
        if (a, b, c) != (0,) + ends
    )
    others = [k[1:] for k in others]

    barrier = pltpu.get_barrier_semaphore()

    def there(d):
        ok = None
        for i, s, c in zip((ix, iy, iz), dims, d):
            if c:
                t = (i + c < s) if c > 0 else (i + c >= 0)
                ok = t if ok is None else jnp.logical_and(ok, t)
        return ok

    def directions(most):
        found = []
        for dx in (-1, 0, 1):
            for dy in (-1, 0, 1):
                for dz in (-1, 0, 1):
                    if 0 < abs(dx) + abs(dy) + abs(dz) <= most:
                        found.append((dx, dy, dz))
        return sorted(found, key=lambda d: (-abs(d[1]), -abs(d[2]), abs(d[0])))

    def greet(sem):
        for dy, dz in ((1, 1), (1, -1), (-1, 1), (-1, -1), (1, 0), (-1, 0), (0, 1), (0, -1), (0, 0)):
            for dx in range(dims[0]):
                if not (dx or dy or dz):
                    continue

                def signal(dx=dx, dy=dy, dz=dz):
                    pl.semaphore_signal(
                        sem, inc=1, device_id=((ix + dx) % dims[0], iy + dy, iz + dz),
                        device_id_type=pl.DeviceIdType.MESH,
                    )

                ok = there((0, dy, dz))
                if ok is None:
                    signal()
                else:
                    pl.when(ok)(signal)

    loads = [
        pltpu.make_async_copy(src, dst, load.at[i])
        for i, src, dst in ((0, b_hbm, b_ref), (0, w_hbm, w_ref), (1, m_hbm, m_ref))
    ]
    for copy in loads:
        copy.start()
    nx, ny = b_ref.shape[0], b_ref.shape[1]
    hx, hy = nx // 2, ny // 2

    def clear(ref, *where):
        part = ref.at[where] if where else ref
        part[...] = jnp.zeros(part.shape, F32)

    own = (pl.ds(0, ny), pl.ds(0, 128))
    clear(V0, pl.ds(0, 2), *own)
    clear(V0, pl.ds(nx + 2, 2), *own)
    clear(V0, pl.ds(1, nx + 2), pl.ds(ny, 8), pl.ds(0, 128))
    clear(W0, pl.ds(1, 1), *own)
    clear(W0, pl.ds(nx + 2, 1), *own)
    clear(W0, pl.ds(2, nx), pl.ds(ny, 8), pl.ds(0, 128))
    for D in (V1, W1):
        clear(D, pl.ds(0, 3))
        clear(D, pl.ds(hx + 3, 3))
        clear(D, pl.ds(3, hx), pl.ds(8, 8))
    for D in (RZ0, RZv, R3v, RCv, RZw, R3w, RCw):
        clear(D)
    greet(barrier)

    def span(i, s):
        return 1 + jnp.where(i > 0, 1, 0) + jnp.where(i < s - 1, 1, 0)

    greeted = span(ix, dims[0]) * span(iy, dims[1]) * span(iz, dims[2]) - 1

    def send(src, dst, d, sem):
        pltpu.make_async_remote_copy(
            src_ref=src, dst_ref=dst, send_sem=sent.at[0], recv_sem=sem,
            device_id=(ix + d[0], iy + d[1], iz + d[2]), device_id_type=pl.DeviceIdType.MESH,
        ).start()

    def send_all(found, pieces, sem):
        def start(group):
            for d in group:
                ok = there((d[0], 0, d[2]))
                if ok is None:
                    send(*pieces(d), d, sem)
                else:
                    @pl.when(ok)
                    def _(d=d):
                        send(*pieces(d), d, sem)

        low = iy < dims[1] // 2
        for c, inward in ((1, low), (-1, jnp.logical_not(low)), (1, jnp.logical_not(low)), (-1, low)):
            group = [d for d in found if d[1] == c]
            if group:
                @pl.when(jnp.logical_and(inward, there((0, c, 0))))
                def _(group=group):
                    start(group)
        start([d for d in found if d[1] == 0])

    def span_x(c, size, pad, deep):
        if c == 0:
            return pl.ds(0, size), pl.ds(pad, size)
        if c > 0:
            return pl.ds(size - deep, deep), pl.ds(pad - deep, deep)
        return pl.ds(0, deep), pl.ds(pad + size, deep)

    def span_y(c, size, total, deep):
        if c == 0:
            return pl.ds(0, size), pl.ds(0, size)
        if c > 0:
            return pl.ds(size - deep, deep), pl.ds(total - deep, deep)
        return pl.ds(0, deep), pl.ds(size, deep)

    def flat(found):
        return [d for d in found if not d[2]]

    first = pl.ds(0, 128)

    def pieces0(d):
        dx, dy, dz = d
        if dz:
            a, b = span_y(dy, ny, ny + 8, 1)
            return SZ0.at[a], RZ0.at[1 - dx, (1 - dz) // 2, b]
        deep = 1 if dx and dy else 2
        a, b = span_x(dx, nx, 2, deep)
        e, f = span_y(dy, ny, ny + 8, deep)
        shifted = pl.ds(a.start + 2, a.size)
        return V0.at[shifted, e, first], V0.at[b, f, first]

    def faces0(d):
        a, b = span_x(d[0], nx, 2, 1)
        e, f = span_y(d[1], ny, ny + 8, 1)
        return W0.at[pl.ds(a.start + 2, a.size), e, first], W0.at[b, f, first]

    def pieces1(S1, D, SZ, RZ):
        def of(d):
            dx, dy, dz = d
            if dz:
                a, b = span_y(dy, 8, 16, 2)
                return SZ.at[a], RZ.at[1 - dx, (1 - dz) // 2, b]
            a, b = span_x(dx, hx, 3, 2 if dy else 3)
            e, f = span_y(dy, 8, 16, 2)
            return S1.at[a, e], D.at[b, f]
        return of

    def late1(S1, R3, SZ, RC):
        def of(d):
            dx, dy, dz = d
            if dz:
                row = pl.ds(7 if dy > 0 else 0, 1)
                return SZ.at[row], RC.at[(1 - dx) // 2, (1 - dz) // 2, row]
            row = pl.ds(5 if dy > 0 else 2, 1)
            return S1.at[:, row], R3.at[:, row]
        return of

    def matrix_rows(d):
        s, r = m_ref, GM.at[me]
        if d[2]:
            row = pl.ds(m_ref.shape[0] - 1 if d[2] > 0 else 0, 1)
            s, r = s.at[row], r.at[row]
        return s, r

    corners = [d for d in directions(3) if all(d)]
    lates = [(0, -1, 0), (0, 1, 0)] + corners

    def bytes_of(ref, sem):
        pltpu.make_async_copy(ref, ref, sem).wait()

    sides_y, sides_z = span(iy, dims[1]) - 1, span(iz, dims[2]) - 1

    def first_part(cy, cz):
        return 32 + 33 * cy + 32 * cz + cy * cz

    def face_part(cy, cz):
        return 16 + 16 * cy

    def second_part(cy, cz):
        return 24 + 20 * cy + 16 * cz + 2 * cy * cz

    def late_part(cy, cz):
        return 8 * cy + cy * cz

    def weight_part(cy, cz):
        return second_part(cy, cz) + late_part(cy, cz)

    def matrix_part(cy, cz):
        return 16 + 32 * cy + 4 * (1 + cy) * cz

    def waiting_part(cy, cz):
        parts = (weight_part, late_part, face_part, matrix_part)
        return sum(part(cy, cz) for part in parts) + 4 * (n - 1)

    def everything(cy, cz):
        parts = (first_part, second_part, waiting_part)
        return sum(part(cy, cz) for part in parts) + 4 * (n - 1)

    def take(part, sem):
        for cy in (1, 2):
            for cz in (1, 2):
                @pl.when(jnp.logical_and(sides_y == cy, sides_z == cz))
                def _(cy=cy, cz=cz):
                    bytes_of(tally.at[pl.ds(0, part(cy, cz))], sem)

    def spread(kind, src, dst, k):
        return pltpu.make_async_remote_copy(
            src_ref=src, dst_ref=dst.at[me], send_sem=sent.at[0], recv_sem=hr.at[kind],
            device_id=mirrored(k), device_id_type=pl.DeviceIdType.MESH,
        )

    def arrive(kind, dst):
        bytes_of(dst.at[pl.ds(0, n - 1)], hr.at[kind])


    bytes_of(tally.at[pl.ds(0, 2 * nx * ny)], load.at[0])
    lane16 = iota((ny, 128), 1)
    packed = jnp.zeros((ny, 128), F32)
    for x in range(nx):
        w = w_ref[x]
        v = K * b_ref[x] / w
        V0[x + 2, 0:ny, 0:128] = v
        W0[x + 2, 0:ny, 0:128] = w
        for a, q in enumerate((v, w)):
            start = 8 * x + 4 * a
            moved = pltpu.roll(q, (start + 2) % 128, 1)
            packed = jnp.where((lane16 >= start) & (lane16 < start + 4), moved, packed)
    SZ0[...] = packed

    pl.semaphore_wait(barrier, greeted)
    send_all(directions(2), pieces0, hr.at[0])
    greet(known.at[0])
    send_all(flat(directions(1)), faces0, hr.at[1])

    lane_row = iota((1, 128), 1)
    low_half = jnp.minimum(2 * lane_row, 126)
    within, tile = lane_row % 16, lane_row // 16
    side_at = 2 * jnp.where(within < 3, within + 61, jnp.where(within < 6, within - 3, 0))
    owner = jnp.where(within < 3, (tile + 4) % 8, tile)

    def coarsen0(planes):
        for i in range(hx):
            TT[i] = planes(2 * i) + planes(2 * i + 1)
        rows = [
            TT[i, pl.ds(0, hy, stride=2), :] + TT[i, pl.ds(1, hy, stride=2), :] for i in range(hx)
        ]
        rows = jnp.concatenate(rows, axis=0)
        fine = lanes_of(rows, low_half) + lanes_of(rows, low_half + 1)
        sides = lanes_of(rows, side_at) + lanes_of(rows, side_at + 1)
        packed = sides[0:8]
        for x in range(1, hx):
            packed = jnp.where(owner == x, sides[8 * x : 8 * x + 8], packed)
        return fine, packed

    held_x = (lane_row // 32 + 4 - iz) % 4
    pairs = 2 * (lane_row % 32)

    def coarsen1(planes, SG):
        for i in range(hx // 2):
            T2[pl.ds(8 * i, 8), :] = planes(2 * i) + planes(2 * i + 1)
        pieces = [
            T2[pl.ds(8 * x, 4, stride=2), :] + T2[pl.ds(8 * x + 1, 4, stride=2), :]
            for x in range(4)
        ]
        rows = [jnp.concatenate(pieces[i : i + 2], axis=0) for i in (0, 2)]
        sums = [lanes_of(r, pairs) + lanes_of(r, pairs + 1) for r in rows]
        parts = [sums[x // 2][4 * (x % 2) : 4 * (x % 2) + 4] for x in range(4)]
        total = parts[0]
        for x in range(1, 4):
            total = jnp.where(held_x == x, parts[x], total)
        return total

    lane8 = iota((8, 128), 1)

    fine, packed = coarsen0(lambda x: w_ref[x])
    SZw[...] = 0.0625 * packed
    w1 = [0.0625 * fine[8 * x : 8 * x + 8, :] for x in range(hx)]
    for x in range(hx):
        S1w[x] = w1[x]
    SW[...] = 0.0625 * coarsen1(lambda x: w1[x], SW)
    GW[me] = SW[...]
    loads[2].wait()
    GM[me] = m_ref[...]
    send_all(directions(2), pieces1(S1w, W1, SZw, RZw), hr.at[1])
    send_all(lates, late1(S1w, R3w, SZw, RCw), hr.at[1])
    send_all(directions(3), matrix_rows, hr.at[1])
    pl.semaphore_wait(known.at[0], greeted)
    greet(known.at[1])

    def coords(rows, lanes, cy, cz, by, bz):
        r, l = iota((rows, lanes), 0), iota((rows, lanes), 1)
        y = jnp.where(r < cy + (rows - cy) // 2, r, r - rows)
        z = jnp.where(l < cz + (lanes - cz) // 2, l, l - lanes)
        gy, gz = y + iy * cy, z + iz * cz
        ok = (gy >= 0) & (gy < dims[1] * cy) & (gz >= 0) & (gz < dims[2] * cz)
        near = (y >= -by) & (y < cy + by) & (z >= -bz) & (z < cz + bz)
        return jnp.where(ok & near, 1, 0)

    def plane_mask(base, x, cx):
        if 0 <= x < cx:
            return base > 0
        gx = x + ix * cx
        inside = jnp.where((gx >= 0) & (gx < dims[0] * cx), 1, 0)
        return base * inside > 0

    row8 = iota((8, 128), 0)
    row16, lane_own = iota((ny, 128), 0), iota((ny, 128), 1)

    def in_lanes(c):
        return shifted(c, -1) + shifted(c, 1)

    def in_rows(c):
        return jnp.where(row16 > 0, pltpu.roll(c, 1, 0), 0.0) + jnp.where(
            row16 < ny - 1, pltpu.roll(c, ny - 1, 0), 0.0
        )

    def beside(planes, x):
        found = [planes[i] for i in (x - 1, x + 1) if 0 <= i < nx]
        return found[0] + found[1] if len(found) > 1 else found[0]

    inner = [V0[x + 2, 0:ny, 0:128] for x in range(nx)]
    inner_u = [
        1.2 * c + K * (in_rows(c) + in_lanes(c) + beside(inner, x)) for x, c in enumerate(inner)
    ]
    for x, u in enumerate(inner_u):
        near_sum = in_rows(u) + in_lanes(u) + beside(inner_u, x)
        R0[x] = b_ref[x] - w_ref[x] * (6.0 * u - near_sum)
    kind = lane_own % 8
    packed = SZ0[...]
    own_ends = jnp.where(kind == 1, pltpu.roll(packed, 127, 1), pltpu.roll(packed, 1, 1))
    has_z = ((kind == 1) & (iz > 0)) | ((kind == 2) & (iz < dims[2] - 1))
    has_y = ((row8 == 7) & (iy > 0)) | ((row8 == 0) & (iy < dims[1] - 1))

    def exists(c):
        return (ix + c >= 0) & (ix + c < dims[0])

    scale1 = [jnp.where(lane8 < 64, (0.125 * K) / jnp.where(lane8 < 64, w, 1.0), 0.0) for w in w1]
    side_scale = (0.125 * K) / SZw[...]
    take(first_part, hr.at[0])
    mask0 = coords(24, 256, ny, 128, 1, 1) > 0
    lane24 = iota((24, 128), 1)

    def z_ends(dx):
        return jnp.where(lane24 % 4 >= 2, RZ0[dx + 1, 1], RZ0[dx + 1, 0])

    ends = {dx: z_ends(dx) for dx in (-1, 0, 1)}

    def z_change():
        full, c = ends[0], ends[0][0:ny]
        above, below = pltpu.roll(full, 1, 1), pltpu.roll(full, 127, 1)
        left = pltpu.roll(jnp.where(lane_own >= 120, ends[-1][0:ny], c), 8, 1)
        right = pltpu.roll(jnp.where(lane_own < 8, ends[1][0:ny], c), 120, 1)
        outer = jnp.where(kind == 1, above[0:ny], below[0:ny])
        vert = (pltpu.roll(full, 1, 0) + pltpu.roll(full, ny + 7, 0))[0:ny]
        u = 1.2 * c + K * (outer + own_ends + vert + left + right)
        u = jnp.where(has_z, u, 0.0)
        across = jnp.where(lane_own >= 8, left, 0.0) + jnp.where(lane_own < 120, right, 0.0)
        d = K * (6.0 * c - in_rows(c) - across) - u
        low = jnp.where(kind == 1, d, -K * above[0:ny])
        high = jnp.where(kind == 2, d, -K * below[0:ny])
        swapped = jnp.where(lane8 % 8 == 1, below[ny:], above[ny:])
        return low, high, swapped

    low_end, high_end, edge_ends = z_change()
    side = [V0[p, ny : ny + 8, 0:128] for p in range(1, nx + 3)]

    def z_part(x):
        a = pltpu.roll(low_end, (-8 * x - 1) % 128, 1)
        b = pltpu.roll(high_end, (125 - 8 * x) % 128, 1)
        return jnp.where(lane_own < 2, a, jnp.where(lane_own >= 126, b, 0.0))

    def y_part(x):
        c = side[x + 1]
        ends_x = pltpu.roll(edge_ends, (126 - 8 * x) % 128, 1)
        flat_sum = in_lanes(c)
        edges = jnp.where((lane8 == 0) | (lane8 == 127), ends_x, 0.0)
        adjacent = jnp.where(
            row8 == 7, pltpu.roll(inner[x][0:8], 7, 0), pltpu.roll(inner[x][8:16], 1, 0)
        )
        outer = jnp.where(row8 == 7, pltpu.roll(c, 1, 0), pltpu.roll(c, 7, 0))
        u = 1.2 * c + K * (flat_sum + edges + adjacent + outer + side[x] + side[x + 2])
        u = jnp.where(has_y, u, 0.0)
        d = K * (6.0 * c - flat_sum - beside(side[1:-1], x)) - u
        first_rows = jnp.where(row8 == 1, -K * pltpu.roll(c, 2, 0), 0.0)
        first_rows = jnp.where(row8 == 0, pltpu.roll(d, 1, 0), first_rows)
        last_rows = jnp.where(row8 == 6, -K * pltpu.roll(c, 6, 0), 0.0)
        last_rows = jnp.where(row8 == 7, pltpu.roll(d, 7, 0), last_rows)
        return jnp.concatenate([first_rows, last_rows], axis=0)

    def x_part(p, c, x, edge):
        h, beyond = V0[p, 0:ny, 0:128], V0[p + c, 0:ny, 0:128]
        a = pltpu.roll(ends[c][0:ny], (-8 * x - 1) % 128, 1)
        b = pltpu.roll(ends[c][0:ny], (125 - 8 * x) % 128, 1)
        t = V0[p, ny : ny + 8, 0:128]
        rows = jnp.concatenate(
            [
                jnp.where(row8 == 0, pltpu.roll(t, 1, 0), 0.0),
                jnp.where(row8 == 7, pltpu.roll(t, 7, 0), 0.0),
            ],
            axis=0,
        )
        edges = jnp.where(lane_own == 0, a, jnp.where(lane_own == 127, b, 0.0)) + rows
        near_sum = in_lanes(h) + in_rows(h)
        u = 1.2 * h + K * (near_sum + edges + beyond + inner[edge])
        u = jnp.where(exists(c), u, 0.0)
        return K * (6.0 * h - near_sum) - u, -K * h

    x_parts = {}
    for p, c, x, edge in ((1, -1, nx - 1, 0), (nx + 2, 1, 0, nx - 1)):
        x_parts[edge], x_parts[edge - c] = x_part(p, c, x, edge)

    def resid0(x):
        change = z_part(x) + y_part(x)
        if x in x_parts:
            change = change + x_parts[x]
        return R0[x] - w_ref[x] * change

    def smooth0():
        for dx in (-1, 0, 1):
            for x in {-1: (nx - 1,), 0: range(nx), 1: (0,)}[dx]:
                moved = pltpu.roll(z_ends(dx), (126 - 8 * x) % 128, 1)
                V0[x + 2 + dx * nx, :, 128:256] = moved
        for p, c in ((1, -1), (nx + 2, 1)):
            u = 1.2 * V0[p, 0:ny, 0:128] + K * own_sum(V0, p)
            U0[p, 0:ny, 0:128] = jnp.where(exists(c), u, 0.0)
        for p in range(2, nx + 2):
            c = V0[p]
            u = 1.2 * c + K * (around(c) + (V0[p - 1] + V0[p + 1]))
            U0[p] = jnp.where(mask0, u, 0.0)

    def assemble_faces():
        moved = z_ends(0)
        for x in range(nx):
            p = x + 2
            W0[p, :, 128:256] = pltpu.roll(moved, (122 - 8 * x) % 128, 1)
            IW[x] = 1.0 / w_ref[x]
            W0m[x] = pltpu.roll(W0[p, 0:ny, :], 1, 1)[:, 0:128]
            W0p[x] = pltpu.roll(W0[p, 0:ny, :], 255, 1)[:, 0:128]
            F0[x] = 0.2 * U0[p, 0:ny, 0:128] + V0[p, 0:ny, 0:128] + K * own_sum(U0, p)

    def own_sum(ref, p):
        col, wide = ref[p, :, 0:128], ref[p, 0:ny, :]
        vert = pltpu.roll(col, 1, 0)[0:ny] + pltpu.roll(col, ny + 7, 0)[0:ny]
        flat_sum = pltpu.roll(wide, 1, 1)[:, 0:128] + pltpu.roll(wide, 255, 1)[:, 0:128]
        return (vert + flat_sum) + (ref[p - 1, 0:ny, 0:128] + ref[p + 1, 0:ny, 0:128])

    fine, packed = coarsen0(resid0)
    SZv[...] = packed * side_scale
    for x in range(hx):
        S1v[x] = fine[8 * x : 8 * x + 8, :] * scale1[x]
    b1 = [0.125 * fine[8 * x : 8 * x + 8, :] for x in range(hx)]
    send_all(directions(2), pieces1(S1v, V1, SZv, RZv), hr.at[2])
    send_all(lates, late1(S1v, R3v, SZv, RCv), hr.at[1])
    pl.semaphore_wait(known.at[1], greeted)
    for k in others:
        spread(1, SW, GW, k).start()

    mask1 = coords(16, 128, 8, 64, 2, 2)
    mask_up = coords(16, 128, 8, 64, 1, 1)
    mask_own = coords(16, 128, 8, 64, 0, 0)
    lane1 = iota((16, 128), 1)

    def assemble1(S1, RZ, D):
        for dx in (-1, 0, 1):
            ends = jnp.where(lane1 % 16 < 3, RZ[dx + 1, 0], RZ[dx + 1, 1])
            for x in {-1: (hx - 2, hx - 1), 0: range(hx), 1: (0, 1)}[dx]:
                p = x + 3 + dx * hx
                moved = pltpu.roll(ends, (61 - 16 * x) % 128, 1)
                inner = S1[x] if dx == 0 else D[p, 0:8, :]
                D[p, 0:8, :] = jnp.where(lane8 < 64, inner, moved[0:8])
                D[p, 8:16, :] = jnp.where(lane8 < 64, D[p, 8:16, :], moved[8:16])

    def finish1(R3, RC, D):
        for x in range(hx):
            D[x + 3, 8:16, :] = jnp.where((row8 == 2) | (row8 == 5), R3[x], D[x + 3, 8:16, :])
        for slot, p, x in ((0, 2, hx - 1), (1, hx + 3, 0)):
            ends = jnp.where(lane8 % 16 < 3, RC[slot, 0], RC[slot, 1])
            moved = pltpu.roll(ends, (61 - 16 * x) % 128, 1)
            D[p, 8:16, :] = jnp.where(lane8 < 64, D[p, 8:16, :], moved)

    def smooth1(planes):
        for p in planes:
            c = V1[p]
            u = 1.2 * c + K * (around(c) + (V1[p - 1] + V1[p + 1]))
            U1[p] = jnp.where(plane_mask(mask1, p - 3, hx), u, 0.0)

    block = lane8 // 32

    def gathered(G):
        planes = []
        for gx in range(dims[0]):
            tiles = {}
            for t in range(dims[1] // 2):
                for z in range(dims[2]):
                    d0 = (gx * dims[1] + 2 * t) * dims[2] + z
                    tiles[t, z] = jnp.concatenate([G[d0], G[d0 + dims[2]]], axis=0)
            for x in range(4):
                parts = []
                for t in range(dims[1] // 2):
                    out = tiles[t, 0]
                    for z in range(1, dims[2]):
                        out = jnp.where(block == (x + z) % 4, tiles[t, z], out)
                    parts.append(out)
                planes.append(jnp.concatenate(parts, axis=0))
        return planes

    def turned(planes, by):
        return [
            pltpu.roll(c, (-32 * (X % 4) - by) % 128, 1) if X % 4 or by else c
            for X, c in enumerate(planes)
        ]

    def row_pairs(planes):
        c = len(planes) // 2
        for i in range(c):
            T3[i] = planes[2 * i] + planes[2 * i + 1]
        return [
            T3[i, pl.ds(0, 8, stride=2), :] + T3[i, pl.ds(1, 8, stride=2), :] for i in range(c)
        ]

    take(second_part, hr.at[2])
    assemble1(S1v, RZv, V1)
    smooth1(range(2, hx + 4))

    def resid1(x):
        p = x + 3
        s = around(U1[p])[0:8, :] + (U1[p - 1, 0:8, :] + U1[p + 1, 0:8, :])
        return jnp.where(lane8 < 64, b1[x] - w1[x] * (6.0 * U1[p, 0:8, :] - s), 0.0)

    SB[...] = 0.125 * coarsen1(resid1, SB)
    GB[me] = SB[...]
    for k in others:
        spread(3, SB, GB, k).start()
    take(waiting_part, hr.at[1])
    turned_w2 = gathered(GW)
    scale2 = [K / q for q in turned_w2]
    w2 = turned(turned_w2, 0)
    w2m, w2p = [shifted(q, -1) for q in w2], [shifted(q, 1) for q in w2]
    unscale2 = [q * (1.0 / K) for q in w2]
    iw2 = [1.0 / q for q in w2]
    w3 = [0.0625 * pair_sum(q, 1) for q in row_pairs(w2)]
    around3 = {k: [shifted(q, 2 * k) if k else q for q in w3] for k in (-2, -1, 0, 1, 2)}
    iw3 = [1.0 / q for q in w3]
    scale3 = {
        k: [(0.125 * K) * (shifted(q, 2 * k) if k else q) for q in iw3] for k in range(-3, 4)
    }
    inverse3 = {k: [shifted(q, 2 * k) if k else q for q in iw3] for k in (-1, 0, 1)}
    smooth0()
    assemble_faces()
    assemble1(S1w, RZw, W1)
    finish1(R3w, RCw, W1)
    for p in range(2, hx + 4):
        inside = plane_mask(mask_up if 0 <= p - 3 < hx else mask_own, p - 3, hx)
        IW1[p] = jnp.where(inside, 1.0, 0.0) / jnp.where(inside, W1[p], 1.0)
        W1m[p] = pltpu.roll(W1[p], 1, 1)
        W1p[p] = pltpu.roll(W1[p], 127, 1)
    finish1(R3v, RCv, V1)
    smooth1(range(1, hx + 5))
    for p in range(2, hx + 4):
        c = U1[p]
        E10[p] = 0.2 * c + V1[p] + K * (around(c) + (U1[p - 1] + U1[p + 1]))

    def near(i, c, size):
        return jnp.clip(i + c, 0, size - 1)

    steps = (-1, 0, 1)
    blocks = [(x, dy, dz) for x in range(dims[0]) for dy in steps for dz in steps]
    rows = jnp.concatenate(
        [
            GM[(x * dims[1] + near(iy, dy, dims[1])) * dims[2] + near(iz, dz, dims[2])]
            for x, dy, dz in blocks
        ],
        axis=0,
    )
    order = pick(
        iota((128, 128), 0) == (iota((128, 128), 1) % 4) * 32 + iota((128, 128), 1) // 4
    )
    for h in range(2):
        MP[h] = exact_dot(rows[:, 128 * h : 128 * h + 128], order)
    other_w = [jnp.where(lane8 // 2 % 2 == 0, a, b) for a, b in zip(around3[1], around3[-1])]
    other_c = [q * (1.0 / K) for q in other_w]
    far = jnp.full((8, 128), -99)
    wanted = {-1: jnp.where(row8 == 7, -1, far), 0: row8, 1: jnp.where(row8 == 0, 8, far)}
    held = {}
    for k in (-2, -1, 0, 1, 2):
        cell = lane8 + 2 * k
        held[k] = jnp.where((cell >= 0) & (cell < 128), cell // 4 - 8 * iz, -50)
    moves = (0, 1, -1)
    double = [(lane_row + k + 256) // 2 % 128 for k in moves]
    depth = jnp.where(lane_row < 96, lane_row, lane_row - 128)
    here = [jnp.clip((depth + k + 256) // 2 - 128 + 32 * iz, 0, 127) for k in moves]
    even = lane8 % 2 == 0
    E2[...] = jnp.zeros_like(E2)
    arrive(3, GB)

    v_turned = [b * r for b, r in zip(gathered(GB), scale2)]
    v2 = turned(v_turned, 0)
    lane_wide = iota((16, 128), 1)
    before = [jnp.where(lane_wide > 0, q, 0.0) for q in turned(v_turned, -1)]
    after = [jnp.where(lane_wide < 127, q, 0.0) for q in turned(v_turned, 1)]
    u2 = [1.2 * v + K * (s + (a + b)) for v, s, a, b in zip(v2, side_sum(v2), before, after)]
    s2 = [s + (shifted(u, -1) + shifted(u, 1)) for s, u in zip(side_sum(u2), u2)]
    r2 = [v * k - w * (6.0 * u - s) for v, k, w, u, s in zip(v2, unscale2, w2, u2, s2)]
    base2 = [0.2 * u + v + K * s for u, v, s in zip(u2, v2, s2)]
    summed = row_pairs(r2)
    turns = {
        m: [pltpu.roll(q, -m % 128, 1) if m else q for q in summed] for m in range(-7, 8)
    }
    v3 = {}
    for k in (-3, -2, -1, 0, 1, 2, 3):
        pairs = [
            q + jnp.where(even, a, b)
            for q, a, b in zip(turns[2 * k], turns[2 * k + 1], turns[2 * k - 1])
        ]
        v3[k] = [q * r for q, r in zip(pairs, scale3[k])]
        if not k:
            b3 = [0.125 * q for q in pairs]
    u3 = {}
    for k in (-2, -1, 0, 1, 2):
        u3[k] = [
            1.2 * v + K * (s + (a + b))
            for v, s, a, b in zip(v3[k], side_sum(v3[k]), v3[k - 1], v3[k + 1])
        ]
        if k:
            cell = lane8 + 2 * k
            u3[k] = [jnp.where((cell >= 0) & (cell < 128), u, 0.0) for u in u3[k]]
    even3 = lane8 // 2 % 2 == 0

    def partner(q, k):
        return [jnp.where(even3, a, b) for a, b in zip(q[k], q[-k])]

    s3 = [s + (a + b) for s, a, b in zip(side_sum(u3[0]), u3[-1], u3[1])]
    r3 = [b - w * (6.0 * u - s) for b, w, u, s in zip(b3, w3, u3[0], s3)]
    base3 = [0.2 * u + v + K * s for u, v, s in zip(u3[0], v3[0], s3)]
    base3 = {k: [shifted(q, 2 * k) if k else q for q in base3] for k in (-1, 0, 1)}
    other_u, other_v = partner(u3, 1), partner(v3, 1)
    sides = side_sum(other_u)
    r3 = [
        r + v * c - w * (6.0 * u - (s + a + b))
        for r, v, c, w, u, s, a, b in zip(
            r3, other_v, other_c, other_w, other_u, sides, u3[0], partner(u3, 2)
        )
    ]
    c4 = len(r3) // 2
    for i in range(c4):
        T4[pl.ds(8 * i, 8), :] = r3[2 * i] + r3[2 * i + 1]
    half = 4 * c4
    b4 = 0.125 * (T4[pl.ds(0, half, stride=2), :] + T4[pl.ds(1, half, stride=2), :])
    chosen = jnp.where(row8 % 4 == lane8 % 4, b4, 0.0)
    low = row_sum(jnp.where(row8 < 4, chosen, 0.0))
    high = row_sum(jnp.where(row8 >= 4, chosen, 0.0))
    solved = [
        jnp.sum(MP[0, 8 * k : 8 * k + 8, :] * low + MP[1, 8 * k : 8 * k + 8, :] * high,
                axis=1, keepdims=True)
        for k in range(len(blocks))
    ]
    q3 = {}
    for k in (-2, -1, 0, 1, 2):
        e4 = []
        for x in range(dims[0]):
            plane = jnp.zeros((8, 128), F32)
            for dy in steps:
                found = jnp.zeros((8, 128), F32)
                for dz in steps:
                    value = solved[blocks.index((x, dy, dz))]
                    found = jnp.where(held[k] == wanted[dz], value, found)
                plane = jnp.where(row8 // 2 == iy + dy, row_sum(found), plane)
            e4.append(plane)
        q3[k] = [w * e4[i // 2] for i, w in enumerate(around3[k])]
    e3 = {}
    for k in (-1, 0, 1):
        sides = side_sum(q3[k])
        e3[k] = [
            (base + 0.2 * q + K * (s + (a + b))) * r
            for base, q, s, a, b, r in zip(
                base3[k], q3[k], sides, q3[k - 1], q3[k + 1], inverse3[k]
            )
        ]
    for i in range(2 * dims[0]):
        middle = e3[0][i]
        views = (middle, jnp.where(even, middle, e3[1][i]), jnp.where(even, e3[-1][i], middle))
        for k, e in enumerate(views):
            P3[k, i, pl.ds(0, 8, stride=2), :] = e
            P3[k, i, pl.ds(1, 8, stride=2), :] = e
    q2 = [w * P3[0, i // 2] for i, w in enumerate(w2)]
    sides = side_sum(q2)
    for i, (base, q, s) in enumerate(zip(base2, q2, sides)):
        ends = w2p[i] * P3[1, i // 2] + w2m[i] * P3[2, i // 2]
        E2[i + 1, 8:24, :] = (base + 0.2 * q + K * (s + ends)) * iw2[i]

    seen = jnp.concatenate([E2[4 * ix + i, pl.ds(6 + 4 * iy, 8), :] for i in range(6)], axis=0)
    for k in range(3):
        wide2 = lanes_of(pltpu.roll(seen.reshape((6, 8, 128)), 6, 1).reshape((48, 128)), here[k])
        for i in range(6):
            q = wide2[8 * i : 8 * i + 8]
            P2[k, i, pl.ds(0, 8, stride=2), :] = q
            P2[k, i, pl.ds(1, 8, stride=2), :] = q
    q1 = {p: W1[p] * P2[0, (p - 3) // 2 + 1] for p in range(1, hx + 5)}
    e1 = []
    for p in range(2, hx + 4):
        q, i = q1[p], (p - 3) // 2 + 1
        ends = W1p[p] * P2[1, i] + W1m[p] * P2[2, i]
        s = (pltpu.roll(q, 1, 0) + pltpu.roll(q, 15, 0)) + ends + (q1[p - 1] + q1[p + 1])
        e1.append((E10[p] + 0.2 * q + K * s) * IW1[p])
    wide1 = lanes_of(jnp.concatenate(e1, axis=0), double[0])
    for i in range(hx + 2):
        q = wide1[16 * i : 16 * i + 16]
        P1[i, pl.ds(0, 16, stride=2), :] = q
        P1[i, pl.ds(1, 16, stride=2), :] = q
    for k in (1, 2):
        wide1 = lanes_of(jnp.concatenate([e[0:8] for e in e1[1:-1]], axis=0), double[k])
        for i in range(hx):
            q = wide1[8 * i : 8 * i + 8]
            P1s[k - 1, i + 1, pl.ds(0, 8, stride=2), :] = q
            P1s[k - 1, i + 1, pl.ds(1, 8, stride=2), :] = q

    def scaled(p):
        i = (p - 2) // 2 + 1
        if not 2 <= p < nx + 2:
            return W0[p, 0:ny, 0:128] * P1[i, 0:16, :]
        edge = jnp.where(row8 < 4, P1[i, 16:24, :], P1[i, 24:32, :])
        return W0[p, :, 0:128] * jnp.concatenate([P1[i, 0:16, :], edge], axis=0)

    q0 = {p: scaled(p) for p in range(1, nx + 3)}
    for x in range(nx):
        p, i = x + 2, x // 2 + 1
        q = q0[p]
        ends = W0p[x] * P1s[0, i] + W0m[x] * P1s[1, i]
        vert = pltpu.roll(q, 1, 0)[0:ny] + pltpu.roll(q, ny + 7, 0)[0:ny]
        s = vert + ends + (q0[p - 1][0:ny] + q0[p + 1][0:ny])
        f_ref[x] = (F0[x] + 0.2 * q[0:ny] + K * s) * IW[x]

    take(everything, sent.at[0])


def fused(dims, sources, stiffness, coarse_inverse):
    nx, ny, nz = stiffness.shape
    n = dims[0] * dims[1] * dims[2]
    vm = lambda *s: pltpu.VMEM(s, F32)
    halo1 = [vm(8, 8, 128), vm(8, 128), vm(3, 2, 16, 128), vm(8, 8, 128), vm(2, 2, 8, 128)]
    result = pl.pallas_call(
        functools.partial(kernel, dims),
        out_shape=pltpu.VMEM((nx, ny, nz), F32),
        in_specs=[pl.BlockSpec(memory_space=pl.ANY)] * 3,
        out_specs=pl.BlockSpec(memory_space=pltpu.VMEM),
        scratch_shapes=[
            vm(nx, ny, nz), vm(nx, ny, nz), vm(*coarse_inverse.shape),
            vm(nx + 4, 24, 256), vm(nx + 4, 24, 256), vm(nx + 4, 24, 256),
            vm(14, 16, 128), vm(14, 16, 128), vm(14, 16, 128),
            vm(8, 16, 128), vm(32, 128), vm(2 * dims[0], 16, 128),
            vm(16, 128), vm(3, 2 * dims[0], 16, 128),
            vm(4 * dims[0] + 2, 32, 128), vm(3, 6, 16, 128), vm(10, 32, 128), vm(2, 10, 16, 128),
            vm(nx, ny, nz), vm(14, 16, 128), vm(2, 72 * dims[0], 128),
            vm(nx, ny, nz), vm(nx, ny, nz), vm(nx, ny, nz), vm(nx, ny, nz),
            vm(14, 16, 128), vm(14, 16, 128), vm(14, 16, 128),
            vm(ny, 128), vm(3, 2, ny + 8, 128),
        ]
        + halo1 + halo1
        + [
            vm(n, 8, 256), vm(n, 4, 128), vm(n, 4, 128), vm(4, 128), vm(4, 128),
            vm(2048, 128),
            pltpu.SemaphoreType.DMA((2,)), pltpu.SemaphoreType.DMA((1,)),
            pltpu.SemaphoreType.DMA((4,)),
            pltpu.SemaphoreType.REGULAR((2,)),
        ],
        compiler_params=pltpu.CompilerParams(collective_id=0, has_side_effects=True),
        name="cycle",
    )(sources[0], stiffness, coarse_inverse)
    return result[None]


def solution(mesh):
    dims = tuple(mesh.shape[a] for a in ("gx", "gy", "gz"))

    def run(sources, stiffness, coarse_inverse):
        nx, ny, nz = stiffness.shape
        lanes = 128
        cells = coarse_inverse.shape[1]
        levels_fit = (
            sources.shape[0] == 1
            and nx == ny == 16
            and nz == lanes
            and dims[2] * nz == 4 * lanes
            and dims[1] * ny == 64
            and cells == 2 * lanes
            and dims[0] == 2
        )
        if levels_fit:
            return fused(dims, sources, stiffness, coarse_inverse)
        return per_device(sources, stiffness, coarse_inverse)

    in_specs = (P(None, "gx", "gy", "gz"), P("gx", "gy", "gz"), P(("gx", "gy", "gz"), None))
    out_specs = P(None, "gx", "gy", "gz")
    return jax.shard_map(
        run, mesh=mesh, in_specs=in_specs, out_specs=out_specs, check_vma=False
    )
```

```python
import functools
import jax
import jax.numpy as jnp
from jax import lax
from jax.experimental import pallas as pl
from jax.experimental.pallas import tpu as pltpu
from jax.sharding import PartitionSpec as P

damping = 0.8


def extended(cells, sides, width):
    for axis, dim in sides:
        count = lax.axis_size(axis)
        ends = count - 1
        head = lax.slice_in_dim(cells, 0, width, axis=dim)
        tail = lax.slice_in_dim(cells, cells.shape[dim] - width, cells.shape[dim], axis=dim)
        cells = jnp.concatenate(
            [
                lax.ppermute(tail, axis, [(i, (i + 1) % count) for i in range(ends)]),
                cells,
                lax.ppermute(head, axis, [((i + 1) % count, i) for i in range(ends)]),
            ],
            axis=dim,
        )
    return cells


def loop_sum(padded):
    total = padded[:, 2:, 1:-1, 1:-1] + padded[:, :-2, 1:-1, 1:-1]
    total = total + padded[:, 1:-1, 2:, 1:-1] + padded[:, 1:-1, :-2, 1:-1]
    total = total + padded[:, 1:-1, 1:-1, 2:] + padded[:, 1:-1, 1:-1, :-2]
    return total


def inner_part(values):
    return values[:, 1:-1, 1:-1, 1:-1]


def pre_smooth(source, weights):
    count = source.shape[0]
    stacked = jnp.concatenate([source, weights], axis=0)
    wide = extended(stacked, (("gx", 1), ("gy", 2), ("gz", 3)), 2)
    wide_source = wide[:count]
    wide_weights = wide[count:]
    safe_weights = jnp.where(wide_weights > 0.0, wide_weights, 1.0)
    first = damping * wide_source / (6.0 * safe_weights * safe_weights)
    first_scaled = wide_weights * first
    mid_weights = inner_part(wide_weights)
    mid_safe = inner_part(safe_weights)
    applied = mid_weights * (6.0 * inner_part(first_scaled) - loop_sum(first_scaled))
    second = inner_part(first) + damping * (inner_part(wide_source) - applied) / (
        6.0 * mid_safe * mid_safe
    )
    second_scaled = mid_weights * second
    answer = inner_part(second)
    resid = source - weights * (6.0 * inner_part(second_scaled) - loop_sum(second_scaled))
    return (answer, resid)


def post_smooth(answer, source, weights):
    scaled = weights * answer
    wide = extended(scaled, (("gx", 1), ("gy", 2), ("gz", 3)), 1)
    applied = weights * (6.0 * scaled - loop_sum(wide))
    return answer + damping * (source - applied) / (6.0 * weights * weights)


def coarsen(values):
    leading = values.shape[0]
    size_x, size_y, size_z = (values.shape[1], values.shape[2], values.shape[3])
    blocks = values.reshape((leading, size_x // 2, 2, size_y // 2, 2, size_z // 2, 2))
    return jnp.mean(blocks, axis=(2, 4, 6))


def refine(values):
    return jnp.repeat(jnp.repeat(jnp.repeat(values, 2, axis=1), 2, axis=2), 2, axis=3)


def per_device(sources, stiffness, coarse_inverse):
    weight_list = [stiffness[None]]
    for level in range(3):
        weight_list.append(0.5 * coarsen(weight_list[-1]))
    source_list = []
    answer_list = []
    current = sources
    for level in range(4):
        source_list.append(current)
        answer, resid = pre_smooth(current, weight_list[level])
        answer_list.append(answer)
        current = coarsen(resid)
    count = current.shape[0]
    flat_source = current.reshape((count, -1))
    solved = lax.dot_general(
        lax.all_gather(flat_source, ("gx", "gy", "gz"), axis=1, tiled=True),
        coarse_inverse,
        (((1,), (1,)), ((), ())),
        precision=lax.Precision.HIGHEST,
        preferred_element_type=jnp.float32,
    )
    correction = solved.reshape(current.shape)
    for level in range(3, -1, -1):
        correction = post_smooth(
            answer_list[level] + refine(correction), source_list[level], weight_list[level]
        )
    return correction


K = damping / 6.0
F32 = jnp.float32
BF = jnp.bfloat16


def iota(shape, dim):
    return lax.broadcasted_iota(jnp.int32, shape, dim)


def pick(condition):
    return jnp.where(condition, 1.0, 0.0).astype(BF)


def lanes_of(values, index):
    index = jnp.broadcast_to(index, values.shape)
    return jnp.take_along_axis(values, index, axis=1, mode="promise_in_bounds")


def exact_dot(values, chosen):
    total = None
    for _ in range(3):
        part = values.astype(BF)
        values = values - part.astype(F32)
        term = jnp.dot(part, chosen, preferred_element_type=F32)
        total = term if total is None else total + term
    return total


def around(c):
    rows, lanes = c.shape
    return (pltpu.roll(c, 1, 0) + pltpu.roll(c, rows - 1, 0)) + (
        pltpu.roll(c, 1, 1) + pltpu.roll(c, lanes - 1, 1)
    )


def side_sum(planes):
    rows = planes[0].shape[0]
    row = iota(planes[0].shape, 0)
    outs = []
    for p, c in enumerate(planes):
        s = jnp.where(row > 0, pltpu.roll(c, 1, 0), 0.0) + jnp.where(
            row < rows - 1, pltpu.roll(c, rows - 1, 0), 0.0
        )
        if p > 0:
            s = s + planes[p - 1]
        if p < len(planes) - 1:
            s = s + planes[p + 1]
        outs.append(s)
    return outs


def shifted(c, by):
    lane, lanes = iota(c.shape, 1), c.shape[1]
    inside = lane + by < lanes if by > 0 else lane + by >= 0
    return jnp.where(inside, pltpu.roll(c, -by % lanes, 1), 0.0)


def pair_sum(c, step):
    lanes = c.shape[1]
    even = (iota(c.shape, 1) // step) % 2 == 0
    return c + jnp.where(even, pltpu.roll(c, lanes - step, 1), pltpu.roll(c, step, 1))


def row_sum(c):
    for step in (4, 2, 1):
        c = c + pltpu.roll(c, step, 0)
    return c


def kernel(
    dims, b_hbm, w_hbm, m_hbm, f_ref,
    b_ref, w_ref, m_ref,
    V0, W0, U0, V1, W1, U1, TT, T2, T3, T4, P3, E2, P2, P1, P1s, IW, IW1, MP, W0m, W0p, F0, R0, W1m, W1p, E10,
    SZ0, RZ0, S1v, SZv, RZv, R3v, RCv, S1w, SZw, RZw, R3w, RCw,
    GM, GW, GB, SW, SB,
    tally, load, sent, hr, known,
):
    axes = ("gx", "gy", "gz")
    ix, iy, iz = (lax.axis_index(a) for a in axes)
    n = dims[0] * dims[1] * dims[2]
    me = (ix * dims[1] + iy) * dims[2] + iz

    def flip(i, bits):
        if bits == 1:
            return i + 1 - 2 * (i % 2)
        return {0: i, 2: (i + 2) % 4, 3: 3 - i}[bits]

    def mirrored(k):
        a, b, c = k
        y, z = dims[1] - 1 - iy, dims[2] - 1 - iz
        return ((ix + a) % dims[0], flip(y, b), flip(z, c))

    ends = (dims[1] - 1, dims[2] - 1)
    others = sorted(
        (c + (b + 1) // 2, a, b, c)
        for a in range(dims[0])
        for b in range(dims[1])
        for c in range(dims[2])
        if (a, b, c) != (0,) + ends
    )
    others = [k[1:] for k in others]

    barrier = pltpu.get_barrier_semaphore()

    def there(d):
        ok = None
        for i, s, c in zip((ix, iy, iz), dims, d):
            if c:
                t = (i + c < s) if c > 0 else (i + c >= 0)
                ok = t if ok is None else jnp.logical_and(ok, t)
        return ok

    def directions(most):
        found = []
        for dx in (-1, 0, 1):
            for dy in (-1, 0, 1):
                for dz in (-1, 0, 1):
                    if 0 < abs(dx) + abs(dy) + abs(dz) <= most:
                        found.append((dx, dy, dz))
        return sorted(found, key=lambda d: (-abs(d[1]), -abs(d[2]), abs(d[0])))

    def greet(sem):
        for dy, dz in ((1, 1), (1, -1), (-1, 1), (-1, -1), (1, 0), (-1, 0), (0, 1), (0, -1), (0, 0)):
            for dx in range(dims[0]):
                if not (dx or dy or dz):
                    continue

                def signal(dx=dx, dy=dy, dz=dz):
                    pl.semaphore_signal(
                        sem, inc=1, device_id=((ix + dx) % dims[0], iy + dy, iz + dz),
                        device_id_type=pl.DeviceIdType.MESH,
                    )

                ok = there((0, dy, dz))
                if ok is None:
                    signal()
                else:
                    pl.when(ok)(signal)

    loads = [
        pltpu.make_async_copy(src, dst, load.at[i])
        for i, src, dst in ((0, b_hbm, b_ref), (0, w_hbm, w_ref), (1, m_hbm, m_ref))
    ]
    for copy in loads:
        copy.start()
    nx, ny = b_ref.shape[0], b_ref.shape[1]
    hx, hy = nx // 2, ny // 2

    def clear(ref, *where):
        part = ref.at[where] if where else ref
        part[...] = jnp.zeros(part.shape, F32)

    own = (pl.ds(0, ny), pl.ds(0, 128))
    clear(V0, pl.ds(0, 2), *own)
    clear(V0, pl.ds(nx + 2, 2), *own)
    clear(V0, pl.ds(1, nx + 2), pl.ds(ny, 8), pl.ds(0, 128))
    clear(W0, pl.ds(1, 1), *own)
    clear(W0, pl.ds(nx + 2, 1), *own)
    clear(W0, pl.ds(2, nx), pl.ds(ny, 8), pl.ds(0, 128))
    for D in (V1, W1):
        clear(D, pl.ds(0, 3))
        clear(D, pl.ds(hx + 3, 3))
        clear(D, pl.ds(3, hx), pl.ds(8, 8))
    for D in (RZ0, RZv, R3v, RCv, RZw, R3w, RCw):
        clear(D)
    greet(barrier)

    def span(i, s):
        return 1 + jnp.where(i > 0, 1, 0) + jnp.where(i < s - 1, 1, 0)

    greeted = span(ix, dims[0]) * span(iy, dims[1]) * span(iz, dims[2]) - 1

    def send(src, dst, d, sem):
        pltpu.make_async_remote_copy(
            src_ref=src, dst_ref=dst, send_sem=sent.at[0], recv_sem=sem,
            device_id=(ix + d[0], iy + d[1], iz + d[2]), device_id_type=pl.DeviceIdType.MESH,
        ).start()

    def send_all(found, pieces, sem):
        def start(group):
            for d in group:
                ok = there((d[0], 0, d[2]))
                if ok is None:
                    send(*pieces(d), d, sem)
                else:
                    @pl.when(ok)
                    def _(d=d):
                        send(*pieces(d), d, sem)

        low = iy < dims[1] // 2
        for c, inward in ((1, low), (-1, jnp.logical_not(low)), (1, jnp.logical_not(low)), (-1, low)):
            group = [d for d in found if d[1] == c]
            if group:
                @pl.when(jnp.logical_and(inward, there((0, c, 0))))
                def _(group=group):
                    start(group)
        start([d for d in found if d[1] == 0])

    def span_x(c, size, pad, deep):
        if c == 0:
            return pl.ds(0, size), pl.ds(pad, size)
        if c > 0:
            return pl.ds(size - deep, deep), pl.ds(pad - deep, deep)
        return pl.ds(0, deep), pl.ds(pad + size, deep)

    def span_y(c, size, total, deep):
        if c == 0:
            return pl.ds(0, size), pl.ds(0, size)
        if c > 0:
            return pl.ds(size - deep, deep), pl.ds(total - deep, deep)
        return pl.ds(0, deep), pl.ds(size, deep)

    def flat(found):
        return [d for d in found if not d[2]]

    first = pl.ds(0, 128)

    def pieces0(d):
        dx, dy, dz = d
        if dz:
            a, b = span_y(dy, ny, ny + 8, 1)
            return SZ0.at[a], RZ0.at[1 - dx, (1 - dz) // 2, b]
        deep = 1 if dx and dy else 2
        a, b = span_x(dx, nx, 2, deep)
        e, f = span_y(dy, ny, ny + 8, deep)
        shifted = pl.ds(a.start + 2, a.size)
        return V0.at[shifted, e, first], V0.at[b, f, first]

    def faces0(d):
        a, b = span_x(d[0], nx, 2, 1)
        e, f = span_y(d[1], ny, ny + 8, 1)
        return W0.at[pl.ds(a.start + 2, a.size), e, first], W0.at[b, f, first]

    def pieces1(S1, D, SZ, RZ):
        def of(d):
            dx, dy, dz = d
            if dz:
                a, b = span_y(dy, 8, 16, 2)
                return SZ.at[a], RZ.at[1 - dx, (1 - dz) // 2, b]
            a, b = span_x(dx, hx, 3, 2 if dy else 3)
            e, f = span_y(dy, 8, 16, 2)
            return S1.at[a, e], D.at[b, f]
        return of

    def late1(S1, R3, SZ, RC):
        def of(d):
            dx, dy, dz = d
            if dz:
                row = pl.ds(7 if dy > 0 else 0, 1)
                return SZ.at[row], RC.at[(1 - dx) // 2, (1 - dz) // 2, row]
            row = pl.ds(5 if dy > 0 else 2, 1)
            return S1.at[:, row], R3.at[:, row]
        return of

    def matrix_rows(d):
        s, r = m_ref, GM.at[me]
        if d[2]:
            row = pl.ds(m_ref.shape[0] - 1 if d[2] > 0 else 0, 1)
            s, r = s.at[row], r.at[row]
        return s, r

    corners = [d for d in directions(3) if all(d)]
    lates = [(0, -1, 0), (0, 1, 0)] + corners

    def bytes_of(ref, sem):
        pltpu.make_async_copy(ref, ref, sem).wait()

    sides_y, sides_z = span(iy, dims[1]) - 1, span(iz, dims[2]) - 1

    def first_part(cy, cz):
        return 32 + 33 * cy + 32 * cz + cy * cz

    def face_part(cy, cz):
        return 16 + 16 * cy

    def second_part(cy, cz):
        return 24 + 20 * cy + 16 * cz + 2 * cy * cz

    def late_part(cy, cz):
        return 8 * cy + cy * cz

    def weight_part(cy, cz):
        return second_part(cy, cz) + late_part(cy, cz)

    def matrix_part(cy, cz):
        return 16 + 32 * cy + 4 * (1 + cy) * cz

    def waiting_part(cy, cz):
        parts = (weight_part, late_part, face_part, matrix_part)
        return sum(part(cy, cz) for part in parts) + 4 * (n - 1)

    def everything(cy, cz):
        parts = (first_part, second_part, waiting_part)
        return sum(part(cy, cz) for part in parts) + 4 * (n - 1)

    def take(part, sem):
        for cy in (1, 2):
            for cz in (1, 2):
                @pl.when(jnp.logical_and(sides_y == cy, sides_z == cz))
                def _(cy=cy, cz=cz):
                    bytes_of(tally.at[pl.ds(0, part(cy, cz))], sem)

    def spread(kind, src, dst, k):
        return pltpu.make_async_remote_copy(
            src_ref=src, dst_ref=dst.at[me], send_sem=sent.at[0], recv_sem=hr.at[kind],
            device_id=mirrored(k), device_id_type=pl.DeviceIdType.MESH,
        )

    def arrive(kind, dst):
        bytes_of(dst.at[pl.ds(0, n - 1)], hr.at[kind])


    bytes_of(tally.at[pl.ds(0, 2 * nx * ny)], load.at[0])
    lane16 = iota((ny, 128), 1)
    packed = jnp.zeros((ny, 128), F32)
    for x in range(nx):
        w = w_ref[x]
        v = K * b_ref[x] / w
        V0[x + 2, 0:ny, 0:128] = v
        W0[x + 2, 0:ny, 0:128] = w
        for a, q in enumerate((v, w)):
            start = 8 * x + 4 * a
            moved = pltpu.roll(q, (start + 2) % 128, 1)
            packed = jnp.where((lane16 >= start) & (lane16 < start + 4), moved, packed)
    SZ0[...] = packed

    pl.semaphore_wait(barrier, greeted)
    send_all(directions(2), pieces0, hr.at[0])
    greet(known.at[0])
    send_all(flat(directions(1)), faces0, hr.at[1])

    lane_row = iota((1, 128), 1)
    low_half = jnp.minimum(2 * lane_row, 126)
    within, tile = lane_row % 16, lane_row // 16
    side_at = 2 * jnp.where(within < 3, within + 61, jnp.where(within < 6, within - 3, 0))
    owner = jnp.where(within < 3, (tile + 4) % 8, tile)

    def coarsen0(planes):
        for i in range(hx):
            TT[i] = planes(2 * i) + planes(2 * i + 1)
        rows = [
            TT[i, pl.ds(0, hy, stride=2), :] + TT[i, pl.ds(1, hy, stride=2), :] for i in range(hx)
        ]
        rows = jnp.concatenate(rows, axis=0)
        fine = lanes_of(rows, low_half) + lanes_of(rows, low_half + 1)
        sides = lanes_of(rows, side_at) + lanes_of(rows, side_at + 1)
        packed = sides[0:8]
        for x in range(1, hx):
            packed = jnp.where(owner == x, sides[8 * x : 8 * x + 8], packed)
        return fine, packed

    held_x = (lane_row // 32 + 4 - iz) % 4
    pairs = 2 * (lane_row % 32)

    def coarsen1(planes, SG):
        for i in range(hx // 2):
            T2[pl.ds(8 * i, 8), :] = planes(2 * i) + planes(2 * i + 1)
        pieces = [
            T2[pl.ds(8 * x, 4, stride=2), :] + T2[pl.ds(8 * x + 1, 4, stride=2), :]
            for x in range(4)
        ]
        rows = [jnp.concatenate(pieces[i : i + 2], axis=0) for i in (0, 2)]
        sums = [lanes_of(r, pairs) + lanes_of(r, pairs + 1) for r in rows]
        parts = [sums[x // 2][4 * (x % 2) : 4 * (x % 2) + 4] for x in range(4)]
        total = parts[0]
        for x in range(1, 4):
            total = jnp.where(held_x == x, parts[x], total)
        return total

    lane8 = iota((8, 128), 1)

    fine, packed = coarsen0(lambda x: w_ref[x])
    SZw[...] = 0.0625 * packed
    w1 = [0.0625 * fine[8 * x : 8 * x + 8, :] for x in range(hx)]
    for x in range(hx):
        S1w[x] = w1[x]
    SW[...] = 0.0625 * coarsen1(lambda x: w1[x], SW)
    GW[me] = SW[...]
    loads[2].wait()
    GM[me] = m_ref[...]
    send_all(directions(2), pieces1(S1w, W1, SZw, RZw), hr.at[1])
    send_all(lates, late1(S1w, R3w, SZw, RCw), hr.at[1])
    send_all(directions(3), matrix_rows, hr.at[1])
    pl.semaphore_wait(known.at[0], greeted)
    greet(known.at[1])

    def coords(rows, lanes, cy, cz, by, bz):
        r, l = iota((rows, lanes), 0), iota((rows, lanes), 1)
        y = jnp.where(r < cy + (rows - cy) // 2, r, r - rows)
        z = jnp.where(l < cz + (lanes - cz) // 2, l, l - lanes)
        gy, gz = y + iy * cy, z + iz * cz
        ok = (gy >= 0) & (gy < dims[1] * cy) & (gz >= 0) & (gz < dims[2] * cz)
        near = (y >= -by) & (y < cy + by) & (z >= -bz) & (z < cz + bz)
        return jnp.where(ok & near, 1, 0)

    def plane_mask(base, x, cx):
        if 0 <= x < cx:
            return base > 0
        gx = x + ix * cx
        inside = jnp.where((gx >= 0) & (gx < dims[0] * cx), 1, 0)
        return base * inside > 0

    row8 = iota((8, 128), 0)
    row16, lane_own = iota((ny, 128), 0), iota((ny, 128), 1)

    def in_lanes(c):
        return shifted(c, -1) + shifted(c, 1)

    def in_rows(c):
        return jnp.where(row16 > 0, pltpu.roll(c, 1, 0), 0.0) + jnp.where(
            row16 < ny - 1, pltpu.roll(c, ny - 1, 0), 0.0
        )

    def beside(planes, x):
        found = [planes[i] for i in (x - 1, x + 1) if 0 <= i < nx]
        return found[0] + found[1] if len(found) > 1 else found[0]

    inner = [V0[x + 2, 0:ny, 0:128] for x in range(nx)]
    inner_u = [
        1.2 * c + K * (in_rows(c) + in_lanes(c) + beside(inner, x)) for x, c in enumerate(inner)
    ]
    for x, u in enumerate(inner_u):
        near_sum = in_rows(u) + in_lanes(u) + beside(inner_u, x)
        R0[x] = b_ref[x] - w_ref[x] * (6.0 * u - near_sum)
    kind = lane_own % 8
    packed = SZ0[...]
    own_ends = jnp.where(kind == 1, pltpu.roll(packed, 127, 1), pltpu.roll(packed, 1, 1))
    has_z = ((kind == 1) & (iz > 0)) | ((kind == 2) & (iz < dims[2] - 1))
    has_y = ((row8 == 7) & (iy > 0)) | ((row8 == 0) & (iy < dims[1] - 1))

    def exists(c):
        return (ix + c >= 0) & (ix + c < dims[0])

    scale1 = [jnp.where(lane8 < 64, (0.125 * K) / jnp.where(lane8 < 64, w, 1.0), 0.0) for w in w1]
    side_scale = (0.125 * K) / SZw[...]
    take(first_part, hr.at[0])
    mask0 = coords(24, 256, ny, 128, 1, 1) > 0
    lane24 = iota((24, 128), 1)

    def z_ends(dx):
        return jnp.where(lane24 % 4 >= 2, RZ0[dx + 1, 1], RZ0[dx + 1, 0])

    ends = {dx: z_ends(dx) for dx in (-1, 0, 1)}

    def z_change():
        full, c = ends[0], ends[0][0:ny]
        above, below = pltpu.roll(full, 1, 1), pltpu.roll(full, 127, 1)
        left = pltpu.roll(jnp.where(lane_own >= 120, ends[-1][0:ny], c), 8, 1)
        right = pltpu.roll(jnp.where(lane_own < 8, ends[1][0:ny], c), 120, 1)
        outer = jnp.where(kind == 1, above[0:ny], below[0:ny])
        vert = (pltpu.roll(full, 1, 0) + pltpu.roll(full, ny + 7, 0))[0:ny]
        u = 1.2 * c + K * (outer + own_ends + vert + left + right)
        u = jnp.where(has_z, u, 0.0)
        across = jnp.where(lane_own >= 8, left, 0.0) + jnp.where(lane_own < 120, right, 0.0)
        d = K * (6.0 * c - in_rows(c) - across) - u
        low = jnp.where(kind == 1, d, -K * above[0:ny])
        high = jnp.where(kind == 2, d, -K * below[0:ny])
        swapped = jnp.where(lane8 % 8 == 1, below[ny:], above[ny:])
        return low, high, swapped

    low_end, high_end, edge_ends = z_change()
    side = [V0[p, ny : ny + 8, 0:128] for p in range(1, nx + 3)]

    def z_part(x):
        a = pltpu.roll(low_end, (-8 * x - 1) % 128, 1)
        b = pltpu.roll(high_end, (125 - 8 * x) % 128, 1)
        return jnp.where(lane_own < 2, a, jnp.where(lane_own >= 126, b, 0.0))

    def y_part(x):
        c = side[x + 1]
        ends_x = pltpu.roll(edge_ends, (126 - 8 * x) % 128, 1)
        flat_sum = in_lanes(c)
        edges = jnp.where((lane8 == 0) | (lane8 == 127), ends_x, 0.0)
        adjacent = jnp.where(
            row8 == 7, pltpu.roll(inner[x][0:8], 7, 0), pltpu.roll(inner[x][8:16], 1, 0)
        )
        outer = jnp.where(row8 == 7, pltpu.roll(c, 1, 0), pltpu.roll(c, 7, 0))
        u = 1.2 * c + K * (flat_sum + edges + adjacent + outer + side[x] + side[x + 2])
        u = jnp.where(has_y, u, 0.0)
        d = K * (6.0 * c - flat_sum - beside(side[1:-1], x)) - u
        first_rows = jnp.where(row8 == 1, -K * pltpu.roll(c, 2, 0), 0.0)
        first_rows = jnp.where(row8 == 0, pltpu.roll(d, 1, 0), first_rows)
        last_rows = jnp.where(row8 == 6, -K * pltpu.roll(c, 6, 0), 0.0)
        last_rows = jnp.where(row8 == 7, pltpu.roll(d, 7, 0), last_rows)
        return jnp.concatenate([first_rows, last_rows], axis=0)

    def x_part(p, c, x, edge):
        h, beyond = V0[p, 0:ny, 0:128], V0[p + c, 0:ny, 0:128]
        a = pltpu.roll(ends[c][0:ny], (-8 * x - 1) % 128, 1)
        b = pltpu.roll(ends[c][0:ny], (125 - 8 * x) % 128, 1)
        t = V0[p, ny : ny + 8, 0:128]
        rows = jnp.concatenate(
            [
                jnp.where(row8 == 0, pltpu.roll(t, 1, 0), 0.0),
                jnp.where(row8 == 7, pltpu.roll(t, 7, 0), 0.0),
            ],
            axis=0,
        )
        edges = jnp.where(lane_own == 0, a, jnp.where(lane_own == 127, b, 0.0)) + rows
        near_sum = in_lanes(h) + in_rows(h)
        u = 1.2 * h + K * (near_sum + edges + beyond + inner[edge])
        u = jnp.where(exists(c), u, 0.0)
        return K * (6.0 * h - near_sum) - u, -K * h

    x_parts = {}
    for p, c, x, edge in ((1, -1, nx - 1, 0), (nx + 2, 1, 0, nx - 1)):
        x_parts[edge], x_parts[edge - c] = x_part(p, c, x, edge)

    def resid0(x):
        change = z_part(x) + y_part(x)
        if x in x_parts:
            change = change + x_parts[x]
        return R0[x] - w_ref[x] * change

    def smooth0():
        for dx in (-1, 0, 1):
            for x in {-1: (nx - 1,), 0: range(nx), 1: (0,)}[dx]:
                moved = pltpu.roll(z_ends(dx), (126 - 8 * x) % 128, 1)
                V0[x + 2 + dx * nx, :, 128:256] = moved
        for p, c in ((1, -1), (nx + 2, 1)):
            u = 1.2 * V0[p, 0:ny, 0:128] + K * own_sum(V0, p)
            U0[p, 0:ny, 0:128] = jnp.where(exists(c), u, 0.0)
        for p in range(2, nx + 2):
            c = V0[p]
            u = 1.2 * c + K * (around(c) + (V0[p - 1] + V0[p + 1]))
            U0[p] = jnp.where(mask0, u, 0.0)

    def assemble_faces():
        moved = z_ends(0)
        for x in range(nx):
            p = x + 2
            W0[p, :, 128:256] = pltpu.roll(moved, (122 - 8 * x) % 128, 1)
            IW[x] = 1.0 / w_ref[x]
            W0m[x] = pltpu.roll(W0[p, 0:ny, :], 1, 1)[:, 0:128]
            W0p[x] = pltpu.roll(W0[p, 0:ny, :], 255, 1)[:, 0:128]
            F0[x] = 0.2 * U0[p, 0:ny, 0:128] + V0[p, 0:ny, 0:128] + K * own_sum(U0, p)

    def own_sum(ref, p):
        col, wide = ref[p, :, 0:128], ref[p, 0:ny, :]
        vert = pltpu.roll(col, 1, 0)[0:ny] + pltpu.roll(col, ny + 7, 0)[0:ny]
        flat_sum = pltpu.roll(wide, 1, 1)[:, 0:128] + pltpu.roll(wide, 255, 1)[:, 0:128]
        return (vert + flat_sum) + (ref[p - 1, 0:ny, 0:128] + ref[p + 1, 0:ny, 0:128])

    fine, packed = coarsen0(resid0)
    SZv[...] = packed * side_scale
    for x in range(hx):
        S1v[x] = fine[8 * x : 8 * x + 8, :] * scale1[x]
    b1 = [0.125 * fine[8 * x : 8 * x + 8, :] for x in range(hx)]
    send_all(directions(2), pieces1(S1v, V1, SZv, RZv), hr.at[2])
    send_all(lates, late1(S1v, R3v, SZv, RCv), hr.at[1])
    pl.semaphore_wait(known.at[1], greeted)
    for k in others:
        spread(1, SW, GW, k).start()

    mask1 = coords(16, 128, 8, 64, 2, 2)
    mask_up = coords(16, 128, 8, 64, 1, 1)
    mask_own = coords(16, 128, 8, 64, 0, 0)
    lane1 = iota((16, 128), 1)

    def assemble1(S1, RZ, D):
        for dx in (-1, 0, 1):
            ends = jnp.where(lane1 % 16 < 3, RZ[dx + 1, 0], RZ[dx + 1, 1])
            for x in {-1: (hx - 2, hx - 1), 0: range(hx), 1: (0, 1)}[dx]:
                p = x + 3 + dx * hx
                moved = pltpu.roll(ends, (61 - 16 * x) % 128, 1)
                inner = S1[x] if dx == 0 else D[p, 0:8, :]
                D[p, 0:8, :] = jnp.where(lane8 < 64, inner, moved[0:8])
                D[p, 8:16, :] = jnp.where(lane8 < 64, D[p, 8:16, :], moved[8:16])

    def finish1(R3, RC, D):
        for x in range(hx):
            D[x + 3, 8:16, :] = jnp.where((row8 == 2) | (row8 == 5), R3[x], D[x + 3, 8:16, :])
        for slot, p, x in ((0, 2, hx - 1), (1, hx + 3, 0)):
            ends = jnp.where(lane8 % 16 < 3, RC[slot, 0], RC[slot, 1])
            moved = pltpu.roll(ends, (61 - 16 * x) % 128, 1)
            D[p, 8:16, :] = jnp.where(lane8 < 64, D[p, 8:16, :], moved)

    def smooth1(planes):
        for p in planes:
            c = V1[p]
            u = 1.2 * c + K * (around(c) + (V1[p - 1] + V1[p + 1]))
            U1[p] = jnp.where(plane_mask(mask1, p - 3, hx), u, 0.0)

    block = lane8 // 32

    def gathered(G):
        planes = []
        for gx in range(dims[0]):
            tiles = {}
            for t in range(dims[1] // 2):
                for z in range(dims[2]):
                    d0 = (gx * dims[1] + 2 * t) * dims[2] + z
                    tiles[t, z] = jnp.concatenate([G[d0], G[d0 + dims[2]]], axis=0)
            for x in range(4):
                parts = []
                for t in range(dims[1] // 2):
                    out = tiles[t, 0]
                    for z in range(1, dims[2]):
                        out = jnp.where(block == (x + z) % 4, tiles[t, z], out)
                    parts.append(out)
                planes.append(jnp.concatenate(parts, axis=0))
        return planes

    def turned(planes, by):
        return [
            pltpu.roll(c, (-32 * (X % 4) - by) % 128, 1) if X % 4 or by else c
            for X, c in enumerate(planes)
        ]

    def row_pairs(planes):
        c = len(planes) // 2
        for i in range(c):
            T3[i] = planes[2 * i] + planes[2 * i + 1]
        return [
            T3[i, pl.ds(0, 8, stride=2), :] + T3[i, pl.ds(1, 8, stride=2), :] for i in range(c)
        ]

    take(second_part, hr.at[2])
    assemble1(S1v, RZv, V1)
    smooth1(range(2, hx + 4))

    def resid1(x):
        p = x + 3
        s = around(U1[p])[0:8, :] + (U1[p - 1, 0:8, :] + U1[p + 1, 0:8, :])
        return jnp.where(lane8 < 64, b1[x] - w1[x] * (6.0 * U1[p, 0:8, :] - s), 0.0)

    SB[...] = 0.125 * coarsen1(resid1, SB)
    GB[me] = SB[...]
    for k in others:
        spread(3, SB, GB, k).start()
    take(waiting_part, hr.at[1])
    turned_w2 = gathered(GW)
    scale2 = [K / q for q in turned_w2]
    w2 = turned(turned_w2, 0)
    w2m, w2p = [shifted(q, -1) for q in w2], [shifted(q, 1) for q in w2]
    unscale2 = [q * (1.0 / K) for q in w2]
    iw2 = [1.0 / q for q in w2]
    w3 = [0.0625 * pair_sum(q, 1) for q in row_pairs(w2)]
    around3 = {k: [shifted(q, 2 * k) if k else q for q in w3] for k in (-2, -1, 0, 1, 2)}
    iw3 = [1.0 / q for q in w3]
    scale3 = {
        k: [(0.125 * K) * (shifted(q, 2 * k) if k else q) for q in iw3] for k in range(-3, 4)
    }
    inverse3 = {k: [shifted(q, 2 * k) if k else q for q in iw3] for k in (-1, 0, 1)}
    smooth0()
    assemble_faces()
    assemble1(S1w, RZw, W1)
    finish1(R3w, RCw, W1)
    for p in range(2, hx + 4):
        inside = plane_mask(mask_up if 0 <= p - 3 < hx else mask_own, p - 3, hx)
        IW1[p] = jnp.where(inside, 1.0, 0.0) / jnp.where(inside, W1[p], 1.0)
        W1m[p] = pltpu.roll(W1[p], 1, 1)
        W1p[p] = pltpu.roll(W1[p], 127, 1)
    finish1(R3v, RCv, V1)
    smooth1(range(1, hx + 5))
    for p in range(2, hx + 4):
        c = U1[p]
        E10[p] = 0.2 * c + V1[p] + K * (around(c) + (U1[p - 1] + U1[p + 1]))

    def near(i, c, size):
        return jnp.clip(i + c, 0, size - 1)

    steps = (-1, 0, 1)
    blocks = [(x, dy, dz) for x in range(dims[0]) for dy in steps for dz in steps]
    rows = jnp.concatenate(
        [
            GM[(x * dims[1] + near(iy, dy, dims[1])) * dims[2] + near(iz, dz, dims[2])]
            for x, dy, dz in blocks
        ],
        axis=0,
    )
    order = pick(
        iota((128, 128), 0) == (iota((128, 128), 1) % 4) * 32 + iota((128, 128), 1) // 4
    )
    for h in range(2):
        MP[h] = exact_dot(rows[:, 128 * h : 128 * h + 128], order)
    other_w = [jnp.where(lane8 // 2 % 2 == 0, a, b) for a, b in zip(around3[1], around3[-1])]
    other_c = [q * (1.0 / K) for q in other_w]
    far = jnp.full((8, 128), -99)
    wanted = {-1: jnp.where(row8 == 7, -1, far), 0: row8, 1: jnp.where(row8 == 0, 8, far)}
    held = {}
    for k in (-1, 0, 1):
        cell = lane8 + 4 * k
        held[k] = jnp.where((cell >= 0) & (cell < 128), cell // 4 - 8 * iz, -50)
    moves = (0, 1, -1)
    double = [(lane_row + k + 256) // 2 % 128 for k in moves]
    depth = jnp.where(lane_row < 96, lane_row, lane_row - 128)
    here = [jnp.clip((depth + k + 256) // 2 - 128 + 32 * iz, 0, 127) for k in moves]
    even = lane8 % 2 == 0
    E2[...] = jnp.zeros_like(E2)
    arrive(3, GB)

    v_turned = [b * r for b, r in zip(gathered(GB), scale2)]
    v2 = turned(v_turned, 0)
    lane_wide = iota((16, 128), 1)
    before = [jnp.where(lane_wide > 0, q, 0.0) for q in turned(v_turned, -1)]
    after = [jnp.where(lane_wide < 127, q, 0.0) for q in turned(v_turned, 1)]
    u2 = [1.2 * v + K * (s + (a + b)) for v, s, a, b in zip(v2, side_sum(v2), before, after)]
    s2 = [s + (shifted(u, -1) + shifted(u, 1)) for s, u in zip(side_sum(u2), u2)]
    r2 = [v * k - w * (6.0 * u - s) for v, k, w, u, s in zip(v2, unscale2, w2, u2, s2)]
    base2 = [0.2 * u + v + K * s for u, v, s in zip(u2, v2, s2)]
    summed = row_pairs(r2)
    turns = {
        m: [pltpu.roll(q, -m % 128, 1) if m else q for q in summed] for m in range(-7, 8)
    }
    v3 = {}
    for k in (-3, -2, -1, 0, 1, 2, 3):
        pairs = [
            q + jnp.where(even, a, b)
            for q, a, b in zip(turns[2 * k], turns[2 * k + 1], turns[2 * k - 1])
        ]
        v3[k] = [q * r for q, r in zip(pairs, scale3[k])]
        if not k:
            b3 = [0.125 * q for q in pairs]
    u3 = {}
    for k in (-2, -1, 0, 1, 2):
        u3[k] = [
            1.2 * v + K * (s + (a + b))
            for v, s, a, b in zip(v3[k], side_sum(v3[k]), v3[k - 1], v3[k + 1])
        ]
        if k:
            cell = lane8 + 2 * k
            u3[k] = [jnp.where((cell >= 0) & (cell < 128), u, 0.0) for u in u3[k]]
    even3 = lane8 // 2 % 2 == 0

    def partner(q, k):
        return [jnp.where(even3, a, b) for a, b in zip(q[k], q[-k])]

    s3 = [s + (a + b) for s, a, b in zip(side_sum(u3[0]), u3[-1], u3[1])]
    r3 = [b - w * (6.0 * u - s) for b, w, u, s in zip(b3, w3, u3[0], s3)]
    base3 = [0.2 * u + v + K * s for u, v, s in zip(u3[0], v3[0], s3)]
    base3 = {k: [shifted(q, 2 * k) if k else q for q in base3] for k in (-1, 0, 1)}
    other_u, other_v = partner(u3, 1), partner(v3, 1)
    sides = side_sum(other_u)
    r3 = [
        r + v * c - w * (6.0 * u - (s + a + b))
        for r, v, c, w, u, s, a, b in zip(
            r3, other_v, other_c, other_w, other_u, sides, u3[0], partner(u3, 2)
        )
    ]
    c4 = len(r3) // 2
    for i in range(c4):
        T4[pl.ds(8 * i, 8), :] = r3[2 * i] + r3[2 * i + 1]
    half = 4 * c4
    b4 = 0.125 * (T4[pl.ds(0, half, stride=2), :] + T4[pl.ds(1, half, stride=2), :])
    chosen = jnp.where(row8 % 4 == lane8 % 4, b4, 0.0)
    low = row_sum(jnp.where(row8 < 4, chosen, 0.0))
    high = row_sum(jnp.where(row8 >= 4, chosen, 0.0))
    solved = [
        jnp.sum(MP[0, 8 * k : 8 * k + 8, :] * low + MP[1, 8 * k : 8 * k + 8, :] * high,
                axis=1, keepdims=True)
        for k in range(len(blocks))
    ]
    e4 = {}
    for k in (-1, 0, 1):
        e4[k] = []
        for x in range(dims[0]):
            plane = jnp.zeros((8, 128), F32)
            for dy in steps:
                found = jnp.zeros((8, 128), F32)
                for dz in steps:
                    value = solved[blocks.index((x, dy, dz))]
                    found = jnp.where(held[k] == wanted[dz], value, found)
                plane = jnp.where(row8 // 2 == iy + dy, row_sum(found), plane)
            e4[k].append(plane)
    e4 = {
        -2: e4[-1],
        -1: [jnp.where(even3, a, b) for a, b in zip(e4[-1], e4[0])],
        0: e4[0],
        1: [jnp.where(even3, a, b) for a, b in zip(e4[0], e4[1])],
        2: e4[1],
    }
    q3 = {k: [w * e4[k][i // 2] for i, w in enumerate(around3[k])] for k in e4}
    e3 = {}
    for k in (-1, 0, 1):
        sides = side_sum(q3[k])
        e3[k] = [
            (base + 0.2 * q + K * (s + (a + b))) * r
            for base, q, s, a, b, r in zip(
                base3[k], q3[k], sides, q3[k - 1], q3[k + 1], inverse3[k]
            )
        ]
    for i in range(2 * dims[0]):
        middle = e3[0][i]
        views = (middle, jnp.where(even, middle, e3[1][i]), jnp.where(even, e3[-1][i], middle))
        for k, e in enumerate(views):
            P3[k, i, pl.ds(0, 8, stride=2), :] = e
            P3[k, i, pl.ds(1, 8, stride=2), :] = e
    q2 = [w * P3[0, i // 2] for i, w in enumerate(w2)]
    sides = side_sum(q2)
    for i, (base, q, s) in enumerate(zip(base2, q2, sides)):
        ends = w2p[i] * P3[1, i // 2] + w2m[i] * P3[2, i // 2]
        E2[i + 1, 8:24, :] = (base + 0.2 * q + K * (s + ends)) * iw2[i]

    seen = jnp.concatenate([E2[4 * ix + i, pl.ds(6 + 4 * iy, 8), :] for i in range(6)], axis=0)
    for k in range(3):
        wide2 = lanes_of(pltpu.roll(seen.reshape((6, 8, 128)), 6, 1).reshape((48, 128)), here[k])
        for i in range(6):
            q = wide2[8 * i : 8 * i + 8]
            P2[k, i, pl.ds(0, 8, stride=2), :] = q
            P2[k, i, pl.ds(1, 8, stride=2), :] = q
    q1 = {p: W1[p] * P2[0, (p - 3) // 2 + 1] for p in range(1, hx + 5)}
    e1 = []
    for p in range(2, hx + 4):
        q, i = q1[p], (p - 3) // 2 + 1
        ends = W1p[p] * P2[1, i] + W1m[p] * P2[2, i]
        s = (pltpu.roll(q, 1, 0) + pltpu.roll(q, 15, 0)) + ends + (q1[p - 1] + q1[p + 1])
        e1.append((E10[p] + 0.2 * q + K * s) * IW1[p])
    wide1 = lanes_of(jnp.concatenate(e1, axis=0), double[0])
    for i in range(hx + 2):
        q = wide1[16 * i : 16 * i + 16]
        P1[i, pl.ds(0, 16, stride=2), :] = q
        P1[i, pl.ds(1, 16, stride=2), :] = q
    for k in (1, 2):
        wide1 = lanes_of(jnp.concatenate([e[0:8] for e in e1[1:-1]], axis=0), double[k])
        for i in range(hx):
            q = wide1[8 * i : 8 * i + 8]
            P1s[k - 1, i + 1, pl.ds(0, 8, stride=2), :] = q
            P1s[k - 1, i + 1, pl.ds(1, 8, stride=2), :] = q

    def scaled(p):
        i = (p - 2) // 2 + 1
        if not 2 <= p < nx + 2:
            return W0[p, 0:ny, 0:128] * P1[i, 0:16, :]
        edge = jnp.where(row8 < 4, P1[i, 16:24, :], P1[i, 24:32, :])
        return W0[p, :, 0:128] * jnp.concatenate([P1[i, 0:16, :], edge], axis=0)

    q0 = {p: scaled(p) for p in range(1, nx + 3)}
    for x in range(nx):
        p, i = x + 2, x // 2 + 1
        q = q0[p]
        ends = W0p[x] * P1s[0, i] + W0m[x] * P1s[1, i]
        vert = pltpu.roll(q, 1, 0)[0:ny] + pltpu.roll(q, ny + 7, 0)[0:ny]
        s = vert + ends + (q0[p - 1][0:ny] + q0[p + 1][0:ny])
        f_ref[x] = (F0[x] + 0.2 * q[0:ny] + K * s) * IW[x]

    take(everything, sent.at[0])


def fused(dims, sources, stiffness, coarse_inverse):
    nx, ny, nz = stiffness.shape
    n = dims[0] * dims[1] * dims[2]
    vm = lambda *s: pltpu.VMEM(s, F32)
    halo1 = [vm(8, 8, 128), vm(8, 128), vm(3, 2, 16, 128), vm(8, 8, 128), vm(2, 2, 8, 128)]
    result = pl.pallas_call(
        functools.partial(kernel, dims),
        out_shape=pltpu.VMEM((nx, ny, nz), F32),
        in_specs=[pl.BlockSpec(memory_space=pl.ANY)] * 3,
        out_specs=pl.BlockSpec(memory_space=pltpu.VMEM),
        scratch_shapes=[
            vm(nx, ny, nz), vm(nx, ny, nz), vm(*coarse_inverse.shape),
            vm(nx + 4, 24, 256), vm(nx + 4, 24, 256), vm(nx + 4, 24, 256),
            vm(14, 16, 128), vm(14, 16, 128), vm(14, 16, 128),
            vm(8, 16, 128), vm(32, 128), vm(2 * dims[0], 16, 128),
            vm(16, 128), vm(3, 2 * dims[0], 16, 128),
            vm(4 * dims[0] + 2, 32, 128), vm(3, 6, 16, 128), vm(10, 32, 128), vm(2, 10, 16, 128),
            vm(nx, ny, nz), vm(14, 16, 128), vm(2, 72 * dims[0], 128),
            vm(nx, ny, nz), vm(nx, ny, nz), vm(nx, ny, nz), vm(nx, ny, nz),
            vm(14, 16, 128), vm(14, 16, 128), vm(14, 16, 128),
            vm(ny, 128), vm(3, 2, ny + 8, 128),
        ]
        + halo1 + halo1
        + [
            vm(n, 8, 256), vm(n, 4, 128), vm(n, 4, 128), vm(4, 128), vm(4, 128),
            vm(2048, 128),
            pltpu.SemaphoreType.DMA((2,)), pltpu.SemaphoreType.DMA((1,)),
            pltpu.SemaphoreType.DMA((4,)),
            pltpu.SemaphoreType.REGULAR((2,)),
        ],
        compiler_params=pltpu.CompilerParams(collective_id=0, has_side_effects=True),
        name="cycle",
    )(sources[0], stiffness, coarse_inverse)
    return result[None]


def solution(mesh):
    dims = tuple(mesh.shape[a] for a in ("gx", "gy", "gz"))

    def run(sources, stiffness, coarse_inverse):
        nx, ny, nz = stiffness.shape
        lanes = 128
        cells = coarse_inverse.shape[1]
        levels_fit = (
            sources.shape[0] == 1
            and nx == ny == 16
            and nz == lanes
            and dims[2] * nz == 4 * lanes
            and dims[1] * ny == 64
            and cells == 2 * lanes
            and dims[0] == 2
        )
        if levels_fit:
            return fused(dims, sources, stiffness, coarse_inverse)
        return per_device(sources, stiffness, coarse_inverse)

    in_specs = (P(None, "gx", "gy", "gz"), P("gx", "gy", "gz"), P(("gx", "gy", "gz"), None))
    out_specs = P(None, "gx", "gy", "gz")
    return jax.shard_map(
        run, mesh=mesh, in_specs=in_specs, out_specs=out_specs, check_vma=False
    )
```

```python
import functools
import jax
import jax.numpy as jnp
from jax import lax
from jax.experimental import pallas as pl
from jax.experimental.pallas import tpu as pltpu
from jax.sharding import PartitionSpec as P

damping = 0.8


def extended(cells, sides, width):
    for axis, dim in sides:
        count = lax.axis_size(axis)
        ends = count - 1
        head = lax.slice_in_dim(cells, 0, width, axis=dim)
        tail = lax.slice_in_dim(cells, cells.shape[dim] - width, cells.shape[dim], axis=dim)
        cells = jnp.concatenate(
            [
                lax.ppermute(tail, axis, [(i, (i + 1) % count) for i in range(ends)]),
                cells,
                lax.ppermute(head, axis, [((i + 1) % count, i) for i in range(ends)]),
            ],
            axis=dim,
        )
    return cells


def loop_sum(padded):
    total = padded[:, 2:, 1:-1, 1:-1] + padded[:, :-2, 1:-1, 1:-1]
    total = total + padded[:, 1:-1, 2:, 1:-1] + padded[:, 1:-1, :-2, 1:-1]
    total = total + padded[:, 1:-1, 1:-1, 2:] + padded[:, 1:-1, 1:-1, :-2]
    return total


def inner_part(values):
    return values[:, 1:-1, 1:-1, 1:-1]


def pre_smooth(source, weights):
    count = source.shape[0]
    stacked = jnp.concatenate([source, weights], axis=0)
    wide = extended(stacked, (("gx", 1), ("gy", 2), ("gz", 3)), 2)
    wide_source = wide[:count]
    wide_weights = wide[count:]
    safe_weights = jnp.where(wide_weights > 0.0, wide_weights, 1.0)
    first = damping * wide_source / (6.0 * safe_weights * safe_weights)
    first_scaled = wide_weights * first
    mid_weights = inner_part(wide_weights)
    mid_safe = inner_part(safe_weights)
    applied = mid_weights * (6.0 * inner_part(first_scaled) - loop_sum(first_scaled))
    second = inner_part(first) + damping * (inner_part(wide_source) - applied) / (
        6.0 * mid_safe * mid_safe
    )
    second_scaled = mid_weights * second
    answer = inner_part(second)
    resid = source - weights * (6.0 * inner_part(second_scaled) - loop_sum(second_scaled))
    return (answer, resid)


def post_smooth(answer, source, weights):
    scaled = weights * answer
    wide = extended(scaled, (("gx", 1), ("gy", 2), ("gz", 3)), 1)
    applied = weights * (6.0 * scaled - loop_sum(wide))
    return answer + damping * (source - applied) / (6.0 * weights * weights)


def coarsen(values):
    leading = values.shape[0]
    size_x, size_y, size_z = (values.shape[1], values.shape[2], values.shape[3])
    blocks = values.reshape((leading, size_x // 2, 2, size_y // 2, 2, size_z // 2, 2))
    return jnp.mean(blocks, axis=(2, 4, 6))


def refine(values):
    return jnp.repeat(jnp.repeat(jnp.repeat(values, 2, axis=1), 2, axis=2), 2, axis=3)


def per_device(sources, stiffness, coarse_inverse):
    weight_list = [stiffness[None]]
    for level in range(3):
        weight_list.append(0.5 * coarsen(weight_list[-1]))
    source_list = []
    answer_list = []
    current = sources
    for level in range(4):
        source_list.append(current)
        answer, resid = pre_smooth(current, weight_list[level])
        answer_list.append(answer)
        current = coarsen(resid)
    count = current.shape[0]
    flat_source = current.reshape((count, -1))
    solved = lax.dot_general(
        lax.all_gather(flat_source, ("gx", "gy", "gz"), axis=1, tiled=True),
        coarse_inverse,
        (((1,), (1,)), ((), ())),
        precision=lax.Precision.HIGHEST,
        preferred_element_type=jnp.float32,
    )
    correction = solved.reshape(current.shape)
    for level in range(3, -1, -1):
        correction = post_smooth(
            answer_list[level] + refine(correction), source_list[level], weight_list[level]
        )
    return correction


K = damping / 6.0
F32 = jnp.float32
BF = jnp.bfloat16


def iota(shape, dim):
    return lax.broadcasted_iota(jnp.int32, shape, dim)


def pick(condition):
    return jnp.where(condition, 1.0, 0.0).astype(BF)


def lanes_of(values, index):
    index = jnp.broadcast_to(index, values.shape)
    return jnp.take_along_axis(values, index, axis=1, mode="promise_in_bounds")


def exact_dot(values, chosen):
    total = None
    for _ in range(3):
        part = values.astype(BF)
        values = values - part.astype(F32)
        term = jnp.dot(part, chosen, preferred_element_type=F32)
        total = term if total is None else total + term
    return total


def around(c):
    rows, lanes = c.shape
    return (pltpu.roll(c, 1, 0) + pltpu.roll(c, rows - 1, 0)) + (
        pltpu.roll(c, 1, 1) + pltpu.roll(c, lanes - 1, 1)
    )


def side_sum(planes):
    rows = planes[0].shape[0]
    row = iota(planes[0].shape, 0)
    outs = []
    for p, c in enumerate(planes):
        s = jnp.where(row > 0, pltpu.roll(c, 1, 0), 0.0) + jnp.where(
            row < rows - 1, pltpu.roll(c, rows - 1, 0), 0.0
        )
        if p > 0:
            s = s + planes[p - 1]
        if p < len(planes) - 1:
            s = s + planes[p + 1]
        outs.append(s)
    return outs


def shifted(c, by):
    lane, lanes = iota(c.shape, 1), c.shape[1]
    inside = lane + by < lanes if by > 0 else lane + by >= 0
    return jnp.where(inside, pltpu.roll(c, -by % lanes, 1), 0.0)


def pair_sum(c, step):
    lanes = c.shape[1]
    even = (iota(c.shape, 1) // step) % 2 == 0
    return c + jnp.where(even, pltpu.roll(c, lanes - step, 1), pltpu.roll(c, step, 1))


def row_sum(c):
    for step in (4, 2, 1):
        c = c + pltpu.roll(c, step, 0)
    return c


def kernel(
    dims, b_hbm, w_hbm, m_hbm, f_ref,
    b_ref, w_ref, m_ref,
    V0, W0, U0, V1, W1, U1, TT, T2, T3, T4, P3, E2, P2, P1, P1s, IW, IW1, MP, W0m, W0p, F0, R0, W1m, W1p, E10,
    SZ0, RZ0, S1v, SZv, RZv, R3v, RCv, S1w, SZw, RZw, R3w, RCw,
    GM, GW, GB, SW, SB,
    tally, load, sent, hr, known,
):
    axes = ("gx", "gy", "gz")
    ix, iy, iz = (lax.axis_index(a) for a in axes)
    n = dims[0] * dims[1] * dims[2]
    me = (ix * dims[1] + iy) * dims[2] + iz

    def flip(i, bits):
        if bits == 1:
            return i + 1 - 2 * (i % 2)
        return {0: i, 2: (i + 2) % 4, 3: 3 - i}[bits]

    def mirrored(k):
        a, b, c = k
        y, z = dims[1] - 1 - iy, dims[2] - 1 - iz
        return ((ix + a) % dims[0], flip(y, b), flip(z, c))

    ends = (dims[1] - 1, dims[2] - 1)
    others = sorted(
        (c, (b + 1) // 2, a, b, c)
        for a in range(dims[0])
        for b in range(dims[1])
        for c in range(dims[2])
        if (a, b, c) != (0,) + ends
    )
    others = [k[2:] for k in others]

    barrier = pltpu.get_barrier_semaphore()

    def there(d):
        ok = None
        for i, s, c in zip((ix, iy, iz), dims, d):
            if c:
                t = (i + c < s) if c > 0 else (i + c >= 0)
                ok = t if ok is None else jnp.logical_and(ok, t)
        return ok

    def directions(most):
        found = []
        for dx in (-1, 0, 1):
            for dy in (-1, 0, 1):
                for dz in (-1, 0, 1):
                    if 0 < abs(dx) + abs(dy) + abs(dz) <= most:
                        found.append((dx, dy, dz))
        return sorted(found, key=lambda d: (-abs(d[1]), -abs(d[2]), abs(d[0])))

    def greet(sem):
        for dy, dz in ((1, 1), (1, -1), (-1, 1), (-1, -1), (1, 0), (-1, 0), (0, 1), (0, -1), (0, 0)):
            for dx in range(dims[0]):
                if not (dx or dy or dz):
                    continue

                def signal(dx=dx, dy=dy, dz=dz):
                    pl.semaphore_signal(
                        sem, inc=1, device_id=((ix + dx) % dims[0], iy + dy, iz + dz),
                        device_id_type=pl.DeviceIdType.MESH,
                    )

                ok = there((0, dy, dz))
                if ok is None:
                    signal()
                else:
                    pl.when(ok)(signal)

    loads = [
        pltpu.make_async_copy(src, dst, load.at[i])
        for i, src, dst in ((0, b_hbm, b_ref), (0, w_hbm, w_ref), (1, m_hbm, m_ref))
    ]
    for copy in loads:
        copy.start()
    nx, ny = b_ref.shape[0], b_ref.shape[1]
    hx, hy = nx // 2, ny // 2

    def clear(ref, *where):
        part = ref.at[where] if where else ref
        part[...] = jnp.zeros(part.shape, F32)

    own = (pl.ds(0, ny), pl.ds(0, 128))
    clear(V0, pl.ds(0, 2), *own)
    clear(V0, pl.ds(nx + 2, 2), *own)
    clear(V0, pl.ds(1, nx + 2), pl.ds(ny, 8), pl.ds(0, 128))
    clear(W0, pl.ds(1, 1), *own)
    clear(W0, pl.ds(nx + 2, 1), *own)
    clear(W0, pl.ds(2, nx), pl.ds(ny, 8), pl.ds(0, 128))
    for D in (V1, W1):
        clear(D, pl.ds(0, 3))
        clear(D, pl.ds(hx + 3, 3))
        clear(D, pl.ds(3, hx), pl.ds(8, 8))
    for D in (RZ0, RZv, R3v, RCv, RZw, R3w, RCw):
        clear(D)
    greet(barrier)

    def span(i, s):
        return 1 + jnp.where(i > 0, 1, 0) + jnp.where(i < s - 1, 1, 0)

    greeted = span(ix, dims[0]) * span(iy, dims[1]) * span(iz, dims[2]) - 1

    def send(src, dst, d, sem):
        pltpu.make_async_remote_copy(
            src_ref=src, dst_ref=dst, send_sem=sent.at[0], recv_sem=sem,
            device_id=(ix + d[0], iy + d[1], iz + d[2]), device_id_type=pl.DeviceIdType.MESH,
        ).start()

    def send_all(found, pieces, sem):
        def start(group):
            for d in group:
                ok = there((d[0], 0, d[2]))
                if ok is None:
                    send(*pieces(d), d, sem)
                else:
                    @pl.when(ok)
                    def _(d=d):
                        send(*pieces(d), d, sem)

        low = iy < dims[1] // 2
        for c, inward in ((1, low), (-1, jnp.logical_not(low)), (1, jnp.logical_not(low)), (-1, low)):
            group = [d for d in found if d[1] == c]
            if group:
                @pl.when(jnp.logical_and(inward, there((0, c, 0))))
                def _(group=group):
                    start(group)
        start([d for d in found if d[1] == 0])

    def span_x(c, size, pad, deep):
        if c == 0:
            return pl.ds(0, size), pl.ds(pad, size)
        if c > 0:
            return pl.ds(size - deep, deep), pl.ds(pad - deep, deep)
        return pl.ds(0, deep), pl.ds(pad + size, deep)

    def span_y(c, size, total, deep):
        if c == 0:
            return pl.ds(0, size), pl.ds(0, size)
        if c > 0:
            return pl.ds(size - deep, deep), pl.ds(total - deep, deep)
        return pl.ds(0, deep), pl.ds(size, deep)

    def flat(found):
        return [d for d in found if not d[2]]

    first = pl.ds(0, 128)

    def pieces0(d):
        dx, dy, dz = d
        if dz:
            a, b = span_y(dy, ny, ny + 8, 1)
            return SZ0.at[a], RZ0.at[1 - dx, (1 - dz) // 2, b]
        deep = 1 if dx and dy else 2
        a, b = span_x(dx, nx, 2, deep)
        e, f = span_y(dy, ny, ny + 8, deep)
        shifted = pl.ds(a.start + 2, a.size)
        return V0.at[shifted, e, first], V0.at[b, f, first]

    def faces0(d):
        a, b = span_x(d[0], nx, 2, 1)
        e, f = span_y(d[1], ny, ny + 8, 1)
        return W0.at[pl.ds(a.start + 2, a.size), e, first], W0.at[b, f, first]

    def pieces1(S1, D, SZ, RZ):
        def of(d):
            dx, dy, dz = d
            if dz:
                a, b = span_y(dy, 8, 16, 2)
                return SZ.at[a], RZ.at[1 - dx, (1 - dz) // 2, b]
            a, b = span_x(dx, hx, 3, 2 if dy else 3)
            e, f = span_y(dy, 8, 16, 2)
            return S1.at[a, e], D.at[b, f]
        return of

    def late1(S1, R3, SZ, RC):
        def of(d):
            dx, dy, dz = d
            if dz:
                row = pl.ds(7 if dy > 0 else 0, 1)
                return SZ.at[row], RC.at[(1 - dx) // 2, (1 - dz) // 2, row]
            row = pl.ds(5 if dy > 0 else 2, 1)
            return S1.at[:, row], R3.at[:, row]
        return of

    def matrix_rows(d):
        s, r = m_ref, GM.at[me]
        if d[2]:
            row = pl.ds(m_ref.shape[0] - 1 if d[2] > 0 else 0, 1)
            s, r = s.at[row], r.at[row]
        return s, r

    corners = [d for d in directions(3) if all(d)]
    lates = [(0, -1, 0), (0, 1, 0)] + corners

    def bytes_of(ref, sem):
        pltpu.make_async_copy(ref, ref, sem).wait()

    sides_y, sides_z = span(iy, dims[1]) - 1, span(iz, dims[2]) - 1

    def first_part(cy, cz):
        return 32 + 33 * cy + 32 * cz + cy * cz

    def face_part(cy, cz):
        return 16 + 16 * cy

    def second_part(cy, cz):
        return 24 + 20 * cy + 16 * cz + 2 * cy * cz

    def late_part(cy, cz):
        return 8 * cy + cy * cz

    def weight_part(cy, cz):
        return second_part(cy, cz) + late_part(cy, cz)

    def matrix_part(cy, cz):
        return 16 + 32 * cy + 4 * (1 + cy) * cz

    def waiting_part(cy, cz):
        parts = (weight_part, late_part, face_part, matrix_part)
        return sum(part(cy, cz) for part in parts) + 4 * (n - 1)

    def everything(cy, cz):
        parts = (first_part, second_part, waiting_part)
        return sum(part(cy, cz) for part in parts) + 4 * (n - 1)

    def take(part, sem):
        for cy in (1, 2):
            for cz in (1, 2):
                @pl.when(jnp.logical_and(sides_y == cy, sides_z == cz))
                def _(cy=cy, cz=cz):
                    bytes_of(tally.at[pl.ds(0, part(cy, cz))], sem)

    def spread(kind, src, dst, k):
        return pltpu.make_async_remote_copy(
            src_ref=src, dst_ref=dst.at[me], send_sem=sent.at[0], recv_sem=hr.at[kind],
            device_id=mirrored(k), device_id_type=pl.DeviceIdType.MESH,
        )

    def arrive(kind, dst):
        bytes_of(dst.at[pl.ds(0, n - 1)], hr.at[kind])


    bytes_of(tally.at[pl.ds(0, 2 * nx * ny)], load.at[0])
    lane16 = iota((ny, 128), 1)
    packed = jnp.zeros((ny, 128), F32)
    for x in range(nx):
        w = w_ref[x]
        v = K * b_ref[x] / w
        V0[x + 2, 0:ny, 0:128] = v
        W0[x + 2, 0:ny, 0:128] = w
        for a, q in enumerate((v, w)):
            start = 8 * x + 4 * a
            moved = pltpu.roll(q, (start + 2) % 128, 1)
            packed = jnp.where((lane16 >= start) & (lane16 < start + 4), moved, packed)
    SZ0[...] = packed

    pl.semaphore_wait(barrier, greeted)
    send_all(directions(2), pieces0, hr.at[0])
    greet(known.at[0])
    send_all(flat(directions(1)), faces0, hr.at[1])

    lane_row = iota((1, 128), 1)
    low_half = jnp.minimum(2 * lane_row, 126)
    within, tile = lane_row % 16, lane_row // 16
    side_at = 2 * jnp.where(within < 3, within + 61, jnp.where(within < 6, within - 3, 0))
    owner = jnp.where(within < 3, (tile + 4) % 8, tile)

    def coarsen0(planes):
        for i in range(hx):
            TT[i] = planes(2 * i) + planes(2 * i + 1)
        rows = [
            TT[i, pl.ds(0, hy, stride=2), :] + TT[i, pl.ds(1, hy, stride=2), :] for i in range(hx)
        ]
        rows = jnp.concatenate(rows, axis=0)
        fine = lanes_of(rows, low_half) + lanes_of(rows, low_half + 1)
        sides = lanes_of(rows, side_at) + lanes_of(rows, side_at + 1)
        packed = sides[0:8]
        for x in range(1, hx):
            packed = jnp.where(owner == x, sides[8 * x : 8 * x + 8], packed)
        return fine, packed

    held_x = (lane_row // 32 + 4 - iz) % 4
    pairs = 2 * (lane_row % 32)

    def coarsen1(planes, SG):
        for i in range(hx // 2):
            T2[pl.ds(8 * i, 8), :] = planes(2 * i) + planes(2 * i + 1)
        pieces = [
            T2[pl.ds(8 * x, 4, stride=2), :] + T2[pl.ds(8 * x + 1, 4, stride=2), :]
            for x in range(4)
        ]
        rows = [jnp.concatenate(pieces[i : i + 2], axis=0) for i in (0, 2)]
        sums = [lanes_of(r, pairs) + lanes_of(r, pairs + 1) for r in rows]
        parts = [sums[x // 2][4 * (x % 2) : 4 * (x % 2) + 4] for x in range(4)]
        total = parts[0]
        for x in range(1, 4):
            total = jnp.where(held_x == x, parts[x], total)
        return total

    lane8 = iota((8, 128), 1)

    fine, packed = coarsen0(lambda x: w_ref[x])
    SZw[...] = 0.0625 * packed
    w1 = [0.0625 * fine[8 * x : 8 * x + 8, :] for x in range(hx)]
    for x in range(hx):
        S1w[x] = w1[x]
    SW[...] = 0.0625 * coarsen1(lambda x: w1[x], SW)
    GW[me] = SW[...]
    loads[2].wait()
    GM[me] = m_ref[...]
    send_all(directions(2), pieces1(S1w, W1, SZw, RZw), hr.at[1])
    send_all(lates, late1(S1w, R3w, SZw, RCw), hr.at[1])
    send_all(directions(3), matrix_rows, hr.at[1])
    pl.semaphore_wait(known.at[0], greeted)
    greet(known.at[1])

    def coords(rows, lanes, cy, cz, by, bz):
        r, l = iota((rows, lanes), 0), iota((rows, lanes), 1)
        y = jnp.where(r < cy + (rows - cy) // 2, r, r - rows)
        z = jnp.where(l < cz + (lanes - cz) // 2, l, l - lanes)
        gy, gz = y + iy * cy, z + iz * cz
        ok = (gy >= 0) & (gy < dims[1] * cy) & (gz >= 0) & (gz < dims[2] * cz)
        near = (y >= -by) & (y < cy + by) & (z >= -bz) & (z < cz + bz)
        return jnp.where(ok & near, 1, 0)

    def plane_mask(base, x, cx):
        if 0 <= x < cx:
            return base > 0
        gx = x + ix * cx
        inside = jnp.where((gx >= 0) & (gx < dims[0] * cx), 1, 0)
        return base * inside > 0

    row8 = iota((8, 128), 0)
    row16, lane_own = iota((ny, 128), 0), iota((ny, 128), 1)

    def in_lanes(c):
        return shifted(c, -1) + shifted(c, 1)

    def in_rows(c):
        return jnp.where(row16 > 0, pltpu.roll(c, 1, 0), 0.0) + jnp.where(
            row16 < ny - 1, pltpu.roll(c, ny - 1, 0), 0.0
        )

    def beside(planes, x):
        found = [planes[i] for i in (x - 1, x + 1) if 0 <= i < nx]
        return found[0] + found[1] if len(found) > 1 else found[0]

    inner = [V0[x + 2, 0:ny, 0:128] for x in range(nx)]
    inner_u = [
        1.2 * c + K * (in_rows(c) + in_lanes(c) + beside(inner, x)) for x, c in enumerate(inner)
    ]
    for x, u in enumerate(inner_u):
        near_sum = in_rows(u) + in_lanes(u) + beside(inner_u, x)
        R0[x] = b_ref[x] - w_ref[x] * (6.0 * u - near_sum)
    kind = lane_own % 8
    packed = SZ0[...]
    own_ends = jnp.where(kind == 1, pltpu.roll(packed, 127, 1), pltpu.roll(packed, 1, 1))
    has_z = ((kind == 1) & (iz > 0)) | ((kind == 2) & (iz < dims[2] - 1))
    has_y = ((row8 == 7) & (iy > 0)) | ((row8 == 0) & (iy < dims[1] - 1))

    def exists(c):
        return (ix + c >= 0) & (ix + c < dims[0])

    scale1 = [jnp.where(lane8 < 64, (0.125 * K) / jnp.where(lane8 < 64, w, 1.0), 0.0) for w in w1]
    side_scale = (0.125 * K) / SZw[...]
    take(first_part, hr.at[0])
    mask0 = coords(24, 256, ny, 128, 1, 1) > 0
    lane24 = iota((24, 128), 1)

    def z_ends(dx):
        return jnp.where(lane24 % 4 >= 2, RZ0[dx + 1, 1], RZ0[dx + 1, 0])

    ends = {dx: z_ends(dx) for dx in (-1, 0, 1)}

    def z_change():
        full, c = ends[0], ends[0][0:ny]
        above, below = pltpu.roll(full, 1, 1), pltpu.roll(full, 127, 1)
        left = pltpu.roll(jnp.where(lane_own >= 120, ends[-1][0:ny], c), 8, 1)
        right = pltpu.roll(jnp.where(lane_own < 8, ends[1][0:ny], c), 120, 1)
        outer = jnp.where(kind == 1, above[0:ny], below[0:ny])
        vert = (pltpu.roll(full, 1, 0) + pltpu.roll(full, ny + 7, 0))[0:ny]
        u = 1.2 * c + K * (outer + own_ends + vert + left + right)
        u = jnp.where(has_z, u, 0.0)
        across = jnp.where(lane_own >= 8, left, 0.0) + jnp.where(lane_own < 120, right, 0.0)
        d = K * (6.0 * c - in_rows(c) - across) - u
        low = jnp.where(kind == 1, d, -K * above[0:ny])
        high = jnp.where(kind == 2, d, -K * below[0:ny])
        swapped = jnp.where(lane8 % 8 == 1, below[ny:], above[ny:])
        return low, high, swapped

    low_end, high_end, edge_ends = z_change()
    side = [V0[p, ny : ny + 8, 0:128] for p in range(1, nx + 3)]

    def z_part(x):
        a = pltpu.roll(low_end, (-8 * x - 1) % 128, 1)
        b = pltpu.roll(high_end, (125 - 8 * x) % 128, 1)
        return jnp.where(lane_own < 2, a, jnp.where(lane_own >= 126, b, 0.0))

    def y_part(x):
        c = side[x + 1]
        ends_x = pltpu.roll(edge_ends, (126 - 8 * x) % 128, 1)
        flat_sum = in_lanes(c)
        edges = jnp.where((lane8 == 0) | (lane8 == 127), ends_x, 0.0)
        adjacent = jnp.where(
            row8 == 7, pltpu.roll(inner[x][0:8], 7, 0), pltpu.roll(inner[x][8:16], 1, 0)
        )
        outer = jnp.where(row8 == 7, pltpu.roll(c, 1, 0), pltpu.roll(c, 7, 0))
        u = 1.2 * c + K * (flat_sum + edges + adjacent + outer + side[x] + side[x + 2])
        u = jnp.where(has_y, u, 0.0)
        d = K * (6.0 * c - flat_sum - beside(side[1:-1], x)) - u
        first_rows = jnp.where(row8 == 1, -K * pltpu.roll(c, 2, 0), 0.0)
        first_rows = jnp.where(row8 == 0, pltpu.roll(d, 1, 0), first_rows)
        last_rows = jnp.where(row8 == 6, -K * pltpu.roll(c, 6, 0), 0.0)
        last_rows = jnp.where(row8 == 7, pltpu.roll(d, 7, 0), last_rows)
        return jnp.concatenate([first_rows, last_rows], axis=0)

    def x_part(p, c, x, edge):
        h, beyond = V0[p, 0:ny, 0:128], V0[p + c, 0:ny, 0:128]
        a = pltpu.roll(ends[c][0:ny], (-8 * x - 1) % 128, 1)
        b = pltpu.roll(ends[c][0:ny], (125 - 8 * x) % 128, 1)
        t = V0[p, ny : ny + 8, 0:128]
        rows = jnp.concatenate(
            [
                jnp.where(row8 == 0, pltpu.roll(t, 1, 0), 0.0),
                jnp.where(row8 == 7, pltpu.roll(t, 7, 0), 0.0),
            ],
            axis=0,
        )
        edges = jnp.where(lane_own == 0, a, jnp.where(lane_own == 127, b, 0.0)) + rows
        near_sum = in_lanes(h) + in_rows(h)
        u = 1.2 * h + K * (near_sum + edges + beyond + inner[edge])
        u = jnp.where(exists(c), u, 0.0)
        return K * (6.0 * h - near_sum) - u, -K * h

    x_parts = {}
    for p, c, x, edge in ((1, -1, nx - 1, 0), (nx + 2, 1, 0, nx - 1)):
        x_parts[edge], x_parts[edge - c] = x_part(p, c, x, edge)

    def resid0(x):
        change = z_part(x) + y_part(x)
        if x in x_parts:
            change = change + x_parts[x]
        return R0[x] - w_ref[x] * change

    def smooth0():
        for dx in (-1, 0, 1):
            for x in {-1: (nx - 1,), 0: range(nx), 1: (0,)}[dx]:
                moved = pltpu.roll(z_ends(dx), (126 - 8 * x) % 128, 1)
                V0[x + 2 + dx * nx, :, 128:256] = moved
        for p, c in ((1, -1), (nx + 2, 1)):
            u = 1.2 * V0[p, 0:ny, 0:128] + K * own_sum(V0, p)
            U0[p, 0:ny, 0:128] = jnp.where(exists(c), u, 0.0)
        for p in range(2, nx + 2):
            c = V0[p]
            u = 1.2 * c + K * (around(c) + (V0[p - 1] + V0[p + 1]))
            U0[p] = jnp.where(mask0, u, 0.0)

    def assemble_faces():
        moved = z_ends(0)
        for x in range(nx):
            p = x + 2
            W0[p, :, 128:256] = pltpu.roll(moved, (122 - 8 * x) % 128, 1)
            IW[x] = 1.0 / w_ref[x]
            W0m[x] = pltpu.roll(W0[p, 0:ny, :], 1, 1)[:, 0:128]
            W0p[x] = pltpu.roll(W0[p, 0:ny, :], 255, 1)[:, 0:128]
            F0[x] = 0.2 * U0[p, 0:ny, 0:128] + V0[p, 0:ny, 0:128] + K * own_sum(U0, p)

    def own_sum(ref, p):
        col, wide = ref[p, :, 0:128], ref[p, 0:ny, :]
        vert = pltpu.roll(col, 1, 0)[0:ny] + pltpu.roll(col, ny + 7, 0)[0:ny]
        flat_sum = pltpu.roll(wide, 1, 1)[:, 0:128] + pltpu.roll(wide, 255, 1)[:, 0:128]
        return (vert + flat_sum) + (ref[p - 1, 0:ny, 0:128] + ref[p + 1, 0:ny, 0:128])

    fine, packed = coarsen0(resid0)
    SZv[...] = packed * side_scale
    for x in range(hx):
        S1v[x] = fine[8 * x : 8 * x + 8, :] * scale1[x]
    b1 = [0.125 * fine[8 * x : 8 * x + 8, :] for x in range(hx)]
    send_all(directions(2), pieces1(S1v, V1, SZv, RZv), hr.at[2])
    pl.semaphore_wait(known.at[1], greeted)
    for k in others:
        spread(1, SW, GW, k).start()
    send_all(lates, late1(S1v, R3v, SZv, RCv), hr.at[1])

    mask1 = coords(16, 128, 8, 64, 2, 2)
    mask_up = coords(16, 128, 8, 64, 1, 1)
    mask_own = coords(16, 128, 8, 64, 0, 0)
    lane1 = iota((16, 128), 1)

    def assemble1(S1, RZ, D):
        for dx in (-1, 0, 1):
            ends = jnp.where(lane1 % 16 < 3, RZ[dx + 1, 0], RZ[dx + 1, 1])
            for x in {-1: (hx - 2, hx - 1), 0: range(hx), 1: (0, 1)}[dx]:
                p = x + 3 + dx * hx
                moved = pltpu.roll(ends, (61 - 16 * x) % 128, 1)
                inner = S1[x] if dx == 0 else D[p, 0:8, :]
                D[p, 0:8, :] = jnp.where(lane8 < 64, inner, moved[0:8])
                D[p, 8:16, :] = jnp.where(lane8 < 64, D[p, 8:16, :], moved[8:16])

    def finish1(R3, RC, D):
        for x in range(hx):
            D[x + 3, 8:16, :] = jnp.where((row8 == 2) | (row8 == 5), R3[x], D[x + 3, 8:16, :])
        for slot, p, x in ((0, 2, hx - 1), (1, hx + 3, 0)):
            ends = jnp.where(lane8 % 16 < 3, RC[slot, 0], RC[slot, 1])
            moved = pltpu.roll(ends, (61 - 16 * x) % 128, 1)
            D[p, 8:16, :] = jnp.where(lane8 < 64, D[p, 8:16, :], moved)

    def smooth1(planes):
        for p in planes:
            c = V1[p]
            u = 1.2 * c + K * (around(c) + (V1[p - 1] + V1[p + 1]))
            U1[p] = jnp.where(plane_mask(mask1, p - 3, hx), u, 0.0)

    block = lane8 // 32

    def gathered(G):
        planes = []
        for gx in range(dims[0]):
            tiles = {}
            for t in range(dims[1] // 2):
                for z in range(dims[2]):
                    d0 = (gx * dims[1] + 2 * t) * dims[2] + z
                    tiles[t, z] = jnp.concatenate([G[d0], G[d0 + dims[2]]], axis=0)
            for x in range(4):
                parts = []
                for t in range(dims[1] // 2):
                    out = tiles[t, 0]
                    for z in range(1, dims[2]):
                        out = jnp.where(block == (x + z) % 4, tiles[t, z], out)
                    parts.append(out)
                planes.append(jnp.concatenate(parts, axis=0))
        return planes

    def turned(planes, by):
        return [
            pltpu.roll(c, (-32 * (X % 4) - by) % 128, 1) if X % 4 or by else c
            for X, c in enumerate(planes)
        ]

    def row_pairs(planes):
        c = len(planes) // 2
        for i in range(c):
            T3[i] = planes[2 * i] + planes[2 * i + 1]
        return [
            T3[i, pl.ds(0, 8, stride=2), :] + T3[i, pl.ds(1, 8, stride=2), :] for i in range(c)
        ]

    take(second_part, hr.at[2])
    assemble1(S1v, RZv, V1)
    smooth1(range(2, hx + 4))

    def resid1(x):
        p = x + 3
        s = around(U1[p])[0:8, :] + (U1[p - 1, 0:8, :] + U1[p + 1, 0:8, :])
        return jnp.where(lane8 < 64, b1[x] - w1[x] * (6.0 * U1[p, 0:8, :] - s), 0.0)

    SB[...] = 0.125 * coarsen1(resid1, SB)
    GB[me] = SB[...]
    for k in others:
        spread(3, SB, GB, k).start()
    take(waiting_part, hr.at[1])
    turned_w2 = gathered(GW)
    scale2 = [K / q for q in turned_w2]
    w2 = turned(turned_w2, 0)
    w2m, w2p = [shifted(q, -1) for q in w2], [shifted(q, 1) for q in w2]
    unscale2 = [q * (1.0 / K) for q in w2]
    iw2 = [1.0 / q for q in w2]
    w3 = [0.0625 * pair_sum(q, 1) for q in row_pairs(w2)]
    around3 = {k: [shifted(q, 2 * k) if k else q for q in w3] for k in (-2, -1, 0, 1, 2)}
    iw3 = [1.0 / q for q in w3]
    scale3 = {
        k: [(0.125 * K) * (shifted(q, 2 * k) if k else q) for q in iw3] for k in range(-3, 4)
    }
    inverse3 = {k: [shifted(q, 2 * k) if k else q for q in iw3] for k in (-1, 0, 1)}
    smooth0()
    assemble_faces()
    assemble1(S1w, RZw, W1)
    finish1(R3w, RCw, W1)
    for p in range(2, hx + 4):
        inside = plane_mask(mask_up if 0 <= p - 3 < hx else mask_own, p - 3, hx)
        IW1[p] = jnp.where(inside, 1.0, 0.0) / jnp.where(inside, W1[p], 1.0)
        W1m[p] = pltpu.roll(W1[p], 1, 1)
        W1p[p] = pltpu.roll(W1[p], 127, 1)
    finish1(R3v, RCv, V1)
    smooth1(range(1, hx + 5))
    for p in range(2, hx + 4):
        c = U1[p]
        E10[p] = 0.2 * c + V1[p] + K * (around(c) + (U1[p - 1] + U1[p + 1]))

    def near(i, c, size):
        return jnp.clip(i + c, 0, size - 1)

    steps = (-1, 0, 1)
    blocks = [(x, dy, dz) for x in range(dims[0]) for dy in steps for dz in steps]
    rows = jnp.concatenate(
        [
            GM[(x * dims[1] + near(iy, dy, dims[1])) * dims[2] + near(iz, dz, dims[2])]
            for x, dy, dz in blocks
        ],
        axis=0,
    )
    order = pick(
        iota((128, 128), 0) == (iota((128, 128), 1) % 4) * 32 + iota((128, 128), 1) // 4
    )
    for h in range(2):
        MP[h] = exact_dot(rows[:, 128 * h : 128 * h + 128], order)
    other_w = [jnp.where(lane8 // 2 % 2 == 0, a, b) for a, b in zip(around3[1], around3[-1])]
    other_c = [q * (1.0 / K) for q in other_w]
    far = jnp.full((8, 128), -99)
    wanted = {-1: jnp.where(row8 == 7, -1, far), 0: row8, 1: jnp.where(row8 == 0, 8, far)}
    held = {}
    for k in (-1, 0, 1):
        cell = lane8 + 4 * k
        held[k] = jnp.where((cell >= 0) & (cell < 128), cell // 4 - 8 * iz, -50)
    moves = (0, 1, -1)
    double = [(lane_row + k + 256) // 2 % 128 for k in moves]
    depth = jnp.where(lane_row < 96, lane_row, lane_row - 128)
    here = [jnp.clip((depth + k + 256) // 2 - 128 + 32 * iz, 0, 127) for k in moves]
    even = lane8 % 2 == 0
    E2[...] = jnp.zeros_like(E2)
    arrive(3, GB)

    v_turned = [b * r for b, r in zip(gathered(GB), scale2)]
    v2 = turned(v_turned, 0)
    lane_wide = iota((16, 128), 1)
    before = [jnp.where(lane_wide > 0, q, 0.0) for q in turned(v_turned, -1)]
    after = [jnp.where(lane_wide < 127, q, 0.0) for q in turned(v_turned, 1)]
    u2 = [1.2 * v + K * (s + (a + b)) for v, s, a, b in zip(v2, side_sum(v2), before, after)]
    s2 = [s + (shifted(u, -1) + shifted(u, 1)) for s, u in zip(side_sum(u2), u2)]
    r2 = [v * k - w * (6.0 * u - s) for v, k, w, u, s in zip(v2, unscale2, w2, u2, s2)]
    base2 = [0.2 * u + v + K * s for u, v, s in zip(u2, v2, s2)]
    summed = row_pairs(r2)
    turns = {
        m: [pltpu.roll(q, -m % 128, 1) if m else q for q in summed] for m in range(-7, 8)
    }
    v3 = {}
    for k in (-3, -2, -1, 0, 1, 2, 3):
        pairs = [
            q + jnp.where(even, a, b)
            for q, a, b in zip(turns[2 * k], turns[2 * k + 1], turns[2 * k - 1])
        ]
        v3[k] = [q * r for q, r in zip(pairs, scale3[k])]
        if not k:
            b3 = [0.125 * q for q in pairs]
    u3 = {}
    for k in (-2, -1, 0, 1, 2):
        u3[k] = [
            1.2 * v + K * (s + (a + b))
            for v, s, a, b in zip(v3[k], side_sum(v3[k]), v3[k - 1], v3[k + 1])
        ]
        if k:
            cell = lane8 + 2 * k
            u3[k] = [jnp.where((cell >= 0) & (cell < 128), u, 0.0) for u in u3[k]]
    even3 = lane8 // 2 % 2 == 0

    def partner(q, k):
        return [jnp.where(even3, a, b) for a, b in zip(q[k], q[-k])]

    s3 = [s + (a + b) for s, a, b in zip(side_sum(u3[0]), u3[-1], u3[1])]
    r3 = [b - w * (6.0 * u - s) for b, w, u, s in zip(b3, w3, u3[0], s3)]
    base3 = [0.2 * u + v + K * s for u, v, s in zip(u3[0], v3[0], s3)]
    base3 = {k: [shifted(q, 2 * k) if k else q for q in base3] for k in (-1, 0, 1)}
    other_u, other_v = partner(u3, 1), partner(v3, 1)
    sides = side_sum(other_u)
    r3 = [
        r + v * c - w * (6.0 * u - (s + a + b))
        for r, v, c, w, u, s, a, b in zip(
            r3, other_v, other_c, other_w, other_u, sides, u3[0], partner(u3, 2)
        )
    ]
    c4 = len(r3) // 2
    for i in range(c4):
        T4[pl.ds(8 * i, 8), :] = r3[2 * i] + r3[2 * i + 1]
    half = 4 * c4
    b4 = 0.125 * (T4[pl.ds(0, half, stride=2), :] + T4[pl.ds(1, half, stride=2), :])
    chosen = jnp.where(row8 % 4 == lane8 % 4, b4, 0.0)
    low = row_sum(jnp.where(row8 < 4, chosen, 0.0))
    high = row_sum(jnp.where(row8 >= 4, chosen, 0.0))
    solved = [
        jnp.sum(MP[0, 8 * k : 8 * k + 8, :] * low + MP[1, 8 * k : 8 * k + 8, :] * high,
                axis=1, keepdims=True)
        for k in range(len(blocks))
    ]
    e4 = {}
    for k in (-1, 0, 1):
        e4[k] = []
        for x in range(dims[0]):
            plane = jnp.zeros((8, 128), F32)
            for dy in steps:
                found = jnp.zeros((8, 128), F32)
                for dz in steps:
                    value = solved[blocks.index((x, dy, dz))]
                    found = jnp.where(held[k] == wanted[dz], value, found)
                plane = jnp.where(row8 // 2 == iy + dy, row_sum(found), plane)
            e4[k].append(plane)
    e4 = {
        -2: e4[-1],
        -1: [jnp.where(even3, a, b) for a, b in zip(e4[-1], e4[0])],
        0: e4[0],
        1: [jnp.where(even3, a, b) for a, b in zip(e4[0], e4[1])],
        2: e4[1],
    }
    q3 = {k: [w * e4[k][i // 2] for i, w in enumerate(around3[k])] for k in e4}
    e3 = {}
    for k in (-1, 0, 1):
        sides = side_sum(q3[k])
        e3[k] = [
            (base + 0.2 * q + K * (s + (a + b))) * r
            for base, q, s, a, b, r in zip(
                base3[k], q3[k], sides, q3[k - 1], q3[k + 1], inverse3[k]
            )
        ]
    for i in range(2 * dims[0]):
        middle = e3[0][i]
        views = (middle, jnp.where(even, middle, e3[1][i]), jnp.where(even, e3[-1][i], middle))
        for k, e in enumerate(views):
            P3[k, i, pl.ds(0, 8, stride=2), :] = e
            P3[k, i, pl.ds(1, 8, stride=2), :] = e
    q2 = [w * P3[0, i // 2] for i, w in enumerate(w2)]
    sides = side_sum(q2)
    for i, (base, q, s) in enumerate(zip(base2, q2, sides)):
        ends = w2p[i] * P3[1, i // 2] + w2m[i] * P3[2, i // 2]
        E2[i + 1, 8:24, :] = (base + 0.2 * q + K * (s + ends)) * iw2[i]

    seen = jnp.concatenate([E2[4 * ix + i, pl.ds(6 + 4 * iy, 8), :] for i in range(6)], axis=0)
    for k in range(3):
        wide2 = lanes_of(pltpu.roll(seen.reshape((6, 8, 128)), 6, 1).reshape((48, 128)), here[k])
        for i in range(6):
            q = wide2[8 * i : 8 * i + 8]
            P2[k, i, pl.ds(0, 8, stride=2), :] = q
            P2[k, i, pl.ds(1, 8, stride=2), :] = q
    q1 = {p: W1[p] * P2[0, (p - 3) // 2 + 1] for p in range(1, hx + 5)}
    e1 = []
    for p in range(2, hx + 4):
        q, i = q1[p], (p - 3) // 2 + 1
        ends = W1p[p] * P2[1, i] + W1m[p] * P2[2, i]
        s = (pltpu.roll(q, 1, 0) + pltpu.roll(q, 15, 0)) + ends + (q1[p - 1] + q1[p + 1])
        e1.append((E10[p] + 0.2 * q + K * s) * IW1[p])
    wide1 = lanes_of(jnp.concatenate(e1, axis=0), double[0])
    for i in range(hx + 2):
        q = wide1[16 * i : 16 * i + 16]
        P1[i, pl.ds(0, 16, stride=2), :] = q
        P1[i, pl.ds(1, 16, stride=2), :] = q
    for k in (1, 2):
        wide1 = lanes_of(jnp.concatenate([e[0:8] for e in e1[1:-1]], axis=0), double[k])
        for i in range(hx):
            q = wide1[8 * i : 8 * i + 8]
            P1s[k - 1, i + 1, pl.ds(0, 8, stride=2), :] = q
            P1s[k - 1, i + 1, pl.ds(1, 8, stride=2), :] = q

    def scaled(p):
        i = (p - 2) // 2 + 1
        if not 2 <= p < nx + 2:
            return W0[p, 0:ny, 0:128] * P1[i, 0:16, :]
        edge = jnp.where(row8 < 4, P1[i, 16:24, :], P1[i, 24:32, :])
        return W0[p, :, 0:128] * jnp.concatenate([P1[i, 0:16, :], edge], axis=0)

    q0 = {p: scaled(p) for p in range(1, nx + 3)}
    for x in range(nx):
        p, i = x + 2, x // 2 + 1
        q = q0[p]
        ends = W0p[x] * P1s[0, i] + W0m[x] * P1s[1, i]
        vert = pltpu.roll(q, 1, 0)[0:ny] + pltpu.roll(q, ny + 7, 0)[0:ny]
        s = vert + ends + (q0[p - 1][0:ny] + q0[p + 1][0:ny])
        f_ref[x] = (F0[x] + 0.2 * q[0:ny] + K * s) * IW[x]

    take(everything, sent.at[0])


def fused(dims, sources, stiffness, coarse_inverse):
    nx, ny, nz = stiffness.shape
    n = dims[0] * dims[1] * dims[2]
    vm = lambda *s: pltpu.VMEM(s, F32)
    halo1 = [vm(8, 8, 128), vm(8, 128), vm(3, 2, 16, 128), vm(8, 8, 128), vm(2, 2, 8, 128)]
    result = pl.pallas_call(
        functools.partial(kernel, dims),
        out_shape=pltpu.VMEM((nx, ny, nz), F32),
        in_specs=[pl.BlockSpec(memory_space=pl.ANY)] * 3,
        out_specs=pl.BlockSpec(memory_space=pltpu.VMEM),
        scratch_shapes=[
            vm(nx, ny, nz), vm(nx, ny, nz), vm(*coarse_inverse.shape),
            vm(nx + 4, 24, 256), vm(nx + 4, 24, 256), vm(nx + 4, 24, 256),
            vm(14, 16, 128), vm(14, 16, 128), vm(14, 16, 128),
            vm(8, 16, 128), vm(32, 128), vm(2 * dims[0], 16, 128),
            vm(16, 128), vm(3, 2 * dims[0], 16, 128),
            vm(4 * dims[0] + 2, 32, 128), vm(3, 6, 16, 128), vm(10, 32, 128), vm(2, 10, 16, 128),
            vm(nx, ny, nz), vm(14, 16, 128), vm(2, 72 * dims[0], 128),
            vm(nx, ny, nz), vm(nx, ny, nz), vm(nx, ny, nz), vm(nx, ny, nz),
            vm(14, 16, 128), vm(14, 16, 128), vm(14, 16, 128),
            vm(ny, 128), vm(3, 2, ny + 8, 128),
        ]
        + halo1 + halo1
        + [
            vm(n, 8, 256), vm(n, 4, 128), vm(n, 4, 128), vm(4, 128), vm(4, 128),
            vm(2048, 128),
            pltpu.SemaphoreType.DMA((2,)), pltpu.SemaphoreType.DMA((1,)),
            pltpu.SemaphoreType.DMA((4,)),
            pltpu.SemaphoreType.REGULAR((2,)),
        ],
        compiler_params=pltpu.CompilerParams(collective_id=0, has_side_effects=True),
        name="cycle",
    )(sources[0], stiffness, coarse_inverse)
    return result[None]


def solution(mesh):
    dims = tuple(mesh.shape[a] for a in ("gx", "gy", "gz"))

    def run(sources, stiffness, coarse_inverse):
        nx, ny, nz = stiffness.shape
        lanes = 128
        cells = coarse_inverse.shape[1]
        levels_fit = (
            sources.shape[0] == 1
            and nx == ny == 16
            and nz == lanes
            and dims[2] * nz == 4 * lanes
            and dims[1] * ny == 64
            and cells == 2 * lanes
            and dims[0] == 2
        )
        if levels_fit:
            return fused(dims, sources, stiffness, coarse_inverse)
        return per_device(sources, stiffness, coarse_inverse)

    in_specs = (P(None, "gx", "gy", "gz"), P("gx", "gy", "gz"), P(("gx", "gy", "gz"), None))
    out_specs = P(None, "gx", "gy", "gz")
    return jax.shard_map(
        run, mesh=mesh, in_specs=in_specs, out_specs=out_specs, check_vma=False
    )
```
